32 devices in a mesh: fsdp: 32 (over z, y, x, core).
Axes of the slice: x: 2, y: 2, z: 4, core: 2. Of those that a mesh axis runs over, the one named last changes fastest.
Arguments:
- tokens: bfloat16 [32768, 768], P('fsdp'), may hold values from -80 to 80
- segment_ids: int32 [32768], P('fsdp'), may hold values from 0 to 20, as said below
- pad_mask: int32 [32768], P('fsdp'), may hold values from 0 to 1, as said below
- w_qkv: bfloat16 [768, 2304], P('fsdp'), may hold values from -0.25 to 0.25
- bias_query: bfloat16 [768], P('fsdp'), may hold values from -3 to 3
- bias_value: bfloat16 [768], P('fsdp'), may hold values from -3 to 3
- w_out: bfloat16 [768, 768], P('fsdp'), may hold values from -1.25 to 1.25
- bias_out: bfloat16 [768], P('fsdp'), may hold values from -3 to 3
- gain_one: bfloat16 [768], P('fsdp'), may hold values from 0.25 to 1.75
- shift_one: bfloat16 [768], P('fsdp'), may hold values from -3 to 3
- w_up: bfloat16 [768, 3072], P('fsdp'), may hold values from -0.21875 to 0.21875
- bias_up: bfloat16 [3072], P('fsdp'), may hold values from -3 to 3
- w_down: bfloat16 [3072, 768], P('fsdp'), may hold values from -0.109375 to 0.109375
- bias_down: bfloat16 [768], P('fsdp'), may hold values from -3 to 3
- gain_two: bfloat16 [768], P('fsdp'), may hold values from 0.25 to 1.75
- shift_two: bfloat16 [768], P('fsdp'), may hold values from -3 to 3
- cotangent: bfloat16 [32768, 768], P('fsdp'), may hold values from -6 to 6
Outputs:
- layer_out: bfloat16 [32768, 768], P('fsdp')
- grad_tokens: float32 [32768, 768], P('fsdp')
- grad_w_qkv: float32 [768, 2304], P('fsdp')
- grad_bias_query: float32 [768], P('fsdp')
- grad_bias_value: float32 [768], P('fsdp')
- grad_w_out: float32 [768, 768], P('fsdp')
- grad_bias_out: float32 [768], P('fsdp')
- grad_gain_one: float32 [768], P('fsdp')
- grad_shift_one: float32 [768], P('fsdp')
- grad_w_up: float32 [768, 3072], P('fsdp')
- grad_bias_up: float32 [3072], P('fsdp')
- grad_w_down: float32 [3072, 768], P('fsdp')
- grad_bias_down: float32 [768], P('fsdp')
- grad_gain_two: float32 [768], P('fsdp')
- grad_shift_two: float32 [768], P('fsdp')
The draws below stay inside these ranges and needn't reach their ends.
Inputs may be any that keep to these rules, and one draw needn't show every extreme that they name: `segment_ids`: sequence numbers of the packed tokens, starting at 0 and never falling; there are exactly 21 sequences, each of 1024 to 2048 tokens, and one holds exactly 2048. `pad_mask`: the first token of every sequence is 1.
All inputs are finite; a program needn't handle non-finite values.
Results may differ from the reference program's by a relative error of at most 0.015.
The reference program's roundings to bfloat16 on the way (of `context` and `hidden`) count: a program that leaves them out, or rounds other values in their place, can miss the bound.
Values may be sent and summed in bfloat16 or wider, within the bound.
A program may use at most 320 MiB of HBM per device.

```python
import jax
import jax.numpy as jnp
from jax import lax

D = 768
HEADS = 12
HEAD_DIM = 64
FF = 3072
TOK_DEV = 1024
LEN_MAX = 2048
TOKENS = 32768
N_FSDP = 32


def make_segments(key):
    base_key = jax.random.fold_in(key, 11)
    count = 4 * TOKENS // (3 * LEN_MAX)
    others = count - 1
    half_len = LEN_MAX // 2
    extra_total = TOKENS - LEN_MAX - others * half_len
    weights = jax.random.randint(base_key, (others,), 4, 6).astype(jnp.int32)
    weight_sum = jnp.sum(weights)
    extras = extra_total * weights // weight_sum
    remainder = extra_total - jnp.sum(extras)
    slot = jnp.arange(others, dtype=jnp.int32)
    extras = extras + (slot < remainder).astype(jnp.int32)
    other_lengths = half_len + extras
    longest_at = jax.random.randint(jax.random.fold_in(base_key, 3), (), 0, 4).astype(jnp.int32)
    place = jnp.arange(count, dtype=jnp.int32)
    from_low = other_lengths[jnp.clip(place, 0, others - 1)]
    from_high = other_lengths[jnp.clip(place - 1, 0, others - 1)]
    lengths = jnp.where(place < longest_at, from_low, jnp.where(place == longest_at, LEN_MAX, from_high)).astype(jnp.int32)
    seq_ends = jnp.cumsum(lengths)
    position = jnp.arange(TOKENS, dtype=jnp.int32)
    return jnp.sum((position[:, None] >= seq_ends[None, :]).astype(jnp.int32), axis=1).astype(jnp.int32)


def draw_segment_ids(key, part):
    return make_segments(key)


def draw_pad_mask(key, part):
    segments = make_segments(key)
    before = jnp.concatenate([jnp.full((1,), -1, jnp.int32), segments[:-1]])
    starts = segments != before
    draws = jax.random.randint(jax.random.fold_in(key, 13), (TOKENS,), 0, 8)
    return jnp.where(starts | (draws > 0), 1, 0).astype(jnp.int32)


def draw_tokens(key, part):
    base = jax.random.normal(key, (TOKENS, D), jnp.float32)
    return jnp.clip(base, -80.0, 80.0).astype(jnp.bfloat16)


def draw_w_qkv(key, part):
    base = jax.random.normal(key, (D, 3 * D), jnp.float32) * (1.0 / D ** 0.5)
    return jnp.clip(base, -0.25, 0.25).astype(jnp.bfloat16)


def steps_of(stream_key, dims, cuts, smallest, largest):
    loudness = 1.0
    for dim, shards_of in cuts:
        steps = jax.random.uniform(jax.random.fold_in(jax.random.fold_in(stream_key, 6), dim), (shards_of,), jnp.float32, smallest / len(cuts), largest / len(cuts))
        loudness = loudness * jnp.repeat(jnp.exp(steps), dims[dim] // shards_of).reshape((-1,) + (1,) * (len(dims) - 1 - dim))
    return loudness


def normal_values(own_key, dims, deviation, most, split=(), kind=jnp.bfloat16):
    gain = steps_of(own_key, dims, split, -0.22, 0.18) if split else 1.0
    entries = jax.random.normal(own_key, dims, jnp.float32) * deviation * gain
    return jnp.minimum(jnp.maximum(entries, -most), most).astype(kind)


def setup_inputs(seed: int = 0) -> dict:
    keys = jax.random.split(jax.random.key(seed), 18)
    return {
        "tokens": draw_tokens(jax.random.fold_in(keys[17], 71), 0),
        "segment_ids": draw_segment_ids(jax.random.fold_in(keys[17], 71), 0),
        "pad_mask": draw_pad_mask(jax.random.fold_in(keys[17], 71), 0),
        "w_qkv": draw_w_qkv(jax.random.fold_in(keys[17], 71), 0),
        "bias_query": normal_values(keys[4], (D,), 0.5, 3.0, ((0, 32),)),
        "bias_value": normal_values(keys[5], (D,), 0.5, 3.0, ((0, 32),)),
        "w_out": normal_values(keys[6], (D, D), (D // 32) ** -0.5, 1.25, ((0, 32),)),
        "bias_out": normal_values(keys[7], (D,), 0.5, 3.0, ((0, 32),)),
        "gain_one": jnp.clip(1.0 + 0.15 * jax.random.normal(keys[8], (D,), jnp.float32), 0.25, 1.75).astype(jnp.bfloat16),
        "shift_one": normal_values(keys[9], (D,), 0.5, 3.0, ((0, 32),)),
        "w_up": normal_values(keys[10], (D, FF), D ** -0.5, 0.21875, ((0, 32),)),
        "bias_up": normal_values(keys[11], (FF,), 0.5, 3.0, ((0, 32),)),
        "w_down": normal_values(keys[12], (FF, D), FF ** -0.5, 0.109375, ((0, 32),)),
        "bias_down": normal_values(keys[13], (D,), 0.5, 3.0, ((0, 32),)),
        "gain_two": jnp.clip(1.0 + 0.15 * jax.random.normal(keys[14], (D,), jnp.float32), 0.25, 1.75).astype(jnp.bfloat16),
        "shift_two": normal_values(keys[15], (D,), 0.5, 3.0, ((0, 32),)),
        "cotangent": normal_values(keys[16], (TOKENS, D), 1.0, 6.0, ((0, 32),)),
    }


@jax.custom_vjp
def low(v):
    return lax.optimization_barrier(v.astype(jnp.bfloat16)).astype(jnp.float32)

@jax.custom_vjp
def low_back(v):
    return v

def low_keep(v):
    return (low(v), None)

def low_pass(kept, grad):
    return (grad,)

def back_keep(v):
    return (v, None)

def back_low(kept, grad):
    return (low(grad),)
low.defvjp(low_keep, low_pass)
low_back.defvjp(back_keep, back_low)
highest = lax.Precision.HIGHEST

def round_both(value_in):
    return low(low_back(value_in))

def norm_rows(hidden, gain_row, shift_row):
    centre = hidden - lax.optimization_barrier(jnp.mean(hidden, axis=-1, keepdims=True))
    spread = lax.optimization_barrier(jnp.mean(centre * centre, axis=-1, keepdims=True))
    return centre * lax.rsqrt(spread + 1e-12) * gain_row + shift_row

def gelu_exact(pre_act):
    return 0.5 * pre_act * (1.0 + jax.scipy.special.erf(pre_act * 0.7071067811865476))

def attention(queries, key_rows, values, segment_ids, pad_mask):
    row_count = TOK_DEV
    device_reach = (LEN_MAX - 2) // row_count + 1
    window_rows = (2 * device_reach + 1) * row_count
    margin_rows = device_reach * row_count
    key_tag = jnp.pad(jnp.where(pad_mask == 1, segment_ids + 1, 0), (margin_rows, margin_rows)).astype(jnp.int32)
    query_tag = (segment_ids + 1).astype(jnp.int32)
    key_pad = jnp.pad(key_rows, ((margin_rows, margin_rows), (0, 0)))
    value_pad = jnp.pad(values, ((margin_rows, margin_rows), (0, 0)))

    def block(block_index):
        first_row = (block_index * row_count).astype(jnp.int32)
        q_block = lax.dynamic_slice_in_dim(queries, first_row, row_count, 0).reshape(row_count, HEADS, HEAD_DIM)
        k_block = lax.dynamic_slice_in_dim(key_pad, first_row, window_rows, 0).reshape(window_rows, HEADS, HEAD_DIM)
        v_block = lax.dynamic_slice_in_dim(value_pad, first_row, window_rows, 0).reshape(window_rows, HEADS, HEAD_DIM)
        q_tags = lax.dynamic_slice_in_dim(query_tag, first_row, row_count, 0)
        k_tags = lax.dynamic_slice_in_dim(key_tag, first_row, window_rows, 0)
        allowed = q_tags[:, None] == k_tags[None, :]
        raw_scores = jnp.einsum('qhd,khd->hqk', q_block, k_block, precision=highest)
        scores = jnp.where(allowed[None], low_back(raw_scores * 0.125), -jnp.inf)
        probs = low(jax.nn.softmax(scores, axis=-1))
        context = jnp.einsum('hqk,khd->qhd', probs, v_block, precision=highest)
        return context.reshape(row_count, D)
    blocks = lax.map(jax.checkpoint(block), jnp.arange(N_FSDP, dtype=jnp.int32))
    return blocks.reshape(TOKENS, D)

def forward(segment_ids, pad_mask, tokens, w_qkv, bias_query, bias_value, w_out, bias_out, gain_one, shift_one, w_up, bias_up, w_down, bias_down, gain_two, shift_two):
    mixed = jnp.dot(tokens, w_qkv, precision=highest)
    queries = round_both(mixed[:, :D] + bias_query)
    key_rows = round_both(mixed[:, D:2 * D])
    values = round_both(mixed[:, 2 * D:] + bias_value)
    context = round_both(attention(queries, key_rows, values, segment_ids, pad_mask))
    branch = low_back(jnp.dot(context, w_out, precision=highest) + bias_out)
    first = norm_rows(tokens + branch, gain_one, shift_one)
    up_in = low(first)
    pre_act = low_back(jnp.dot(up_in, w_up, precision=highest) + bias_up)
    hidden = low(gelu_exact(pre_act))
    ffn = low_back(jnp.dot(hidden, w_down, precision=highest) + bias_down)
    return norm_rows(first + ffn, gain_two, shift_two)

def reference(tokens, segment_ids, pad_mask, w_qkv, bias_query, bias_value, w_out, bias_out, gain_one, shift_one, w_up, bias_up, w_down, bias_down, gain_two, shift_two, cotangent):
    inputs = [tokens, w_qkv, bias_query, bias_value, w_out, bias_out, gain_one, shift_one, w_up, bias_up, w_down, bias_down, gain_two, shift_two]
    inputs = [item.astype(jnp.float32) for item in inputs]

    def layer(*arrays):
        return forward(segment_ids, pad_mask, *arrays)
    result, pullback = jax.vjp(layer, *inputs)
    grads = pullback(cotangent.astype(jnp.float32))
    return (result.astype(jnp.bfloat16), grads[0], grads[1], grads[2], grads[3], grads[4], grads[5], grads[6], grads[7], grads[8], grads[9], grads[10], grads[11], grads[12], grads[13])
```

```python
import functools

import jax
import jax.numpy as jnp
from jax import lax
from jax.experimental import pallas as pl
from jax.experimental.pallas import tpu as pltpu
from jax.sharding import PartitionSpec as P

D = 768
HEADS = 12
HEAD_DIM = 64
LEN_MAX = 2048
GROUP = 4
OWN_HEADS = HEADS // GROUP
Q_ROWS = OWN_HEADS * HEAD_DIM
KV_ROWS = 2 * Q_ROWS
MIX_ROWS = Q_ROWS + KV_ROWS
BQ = 256
BK = 256
NEG = -1e30

bf16 = jnp.bfloat16
f32 = jnp.float32
eps_norm = 1e-12
score_scale = 0.125

NN = (((1,), (0,)), ((), ()))
NT = (((1,), (1,)), ((), ()))


def mm(a, b, dims=NN):
    return lax.dot_general(a, b, dims, preferred_element_type=f32)


def norm_rows(hidden, gain_row, shift_row):
    centre = hidden - jnp.mean(hidden, axis=-1, keepdims=True)
    spread = jnp.mean(centre * centre, axis=-1, keepdims=True)
    return centre * lax.rsqrt(spread + eps_norm) * gain_row + shift_row


def gelu_exact(pre_act):
    return 0.5 * pre_act * (1.0 + jax.scipy.special.erf(pre_act * 0.7071067811865476))


def head_rows(block, h, upper):
    zero = jnp.zeros_like(block[:HEAD_DIM])
    rows = block[h * HEAD_DIM : (h + 1) * HEAD_DIM]
    return jnp.concatenate([zero, rows] if upper else [rows, zero], axis=0)


def attend_kernel(
    span, qtag_ref, ktag_ref, qt_ref, kv_ref, kvt_ref, ot_ref, lse_ref, m_sc, l_sc, acc_sc
):
    i = pl.program_id(0)
    m_sc[...] = jnp.full_like(m_sc, NEG)
    l_sc[...] = jnp.zeros_like(l_sc)
    acc_sc[...] = jnp.zeros_like(acc_sc)
    qtag = qtag_ref[...]
    qt = qt_ref[...]
    q_pad = [head_rows(qt, h, False) for h in range(OWN_HEADS)]

    def step(kb, carry):
        rows = pl.ds(pl.multiple_of(kb * BK, BK), BK)
        seen = ktag_ref[rows, :] == qtag
        for h in range(OWN_HEADS):
            s = mm(kv_ref[rows, 128 * h : 128 * (h + 1)], q_pad[h])
            s = jnp.where(seen, s, NEG)
            m_old = m_sc[h : h + 1, :]
            m_new = jnp.maximum(m_old, jnp.max(s, axis=0, keepdims=True))
            p = jnp.exp(s - m_new)
            fade = jnp.exp(m_old - m_new)
            l_sc[h : h + 1, :] = fade * l_sc[h : h + 1, :] + jnp.sum(p, axis=0, keepdims=True)
            m_sc[h : h + 1, :] = m_new
            own = slice(HEAD_DIM * h, HEAD_DIM * (h + 1))
            v_t = kvt_ref[128 * h + HEAD_DIM : 128 * (h + 1), rows]
            acc_sc[own, :] = acc_sc[own, :] * fade + mm(v_t, p.astype(bf16))
        return carry

    lax.fori_loop(span[i, 0], span[i, 1], step, 0)
    for h in range(OWN_HEADS):
        own = slice(HEAD_DIM * h, HEAD_DIM * (h + 1))
        total = l_sc[h : h + 1, :]
        ot_ref[own, :] = (acc_sc[own, :] / total).astype(bf16)
        lse_ref[h : h + 1, :] = m_sc[h : h + 1, :] + jnp.log(total)
    lse_ref[OWN_HEADS:, :] = jnp.zeros_like(lse_ref[OWN_HEADS:, :])


def attend(span, qtag, ktag, qt, kv, kvt):
    own = qt.shape[1]
    window = kv.shape[0]
    whole = lambda shape: pl.BlockSpec(shape, lambda i, s: (0, 0), pipeline_mode=pl.Buffered(1))
    cols = lambda rows: pl.BlockSpec((rows, BQ), lambda i, s: (0, i))
    return pl.pallas_call(
        attend_kernel,
        grid_spec=pltpu.PrefetchScalarGridSpec(
            num_scalar_prefetch=1,
            grid=(own // BQ,),
            in_specs=[
                cols(1),
                whole((window, 1)),
                cols(Q_ROWS),
                whole((window, KV_ROWS)),
                whole((KV_ROWS, window)),
            ],
            out_specs=[cols(Q_ROWS), cols(8)],
            scratch_shapes=[
                pltpu.VMEM((8, BQ), f32),
                pltpu.VMEM((8, BQ), f32),
                pltpu.VMEM((Q_ROWS, BQ), f32),
            ],
        ),
        out_shape=[
            jax.ShapeDtypeStruct((Q_ROWS, own), bf16),
            jax.ShapeDtypeStruct((8, own), f32),
        ],
        compiler_params=pltpu.CompilerParams(vmem_limit_bytes=60 << 20),
        cost_estimate=pl.CostEstimate(
            flops=4 * own * 2048 * Q_ROWS, bytes_accessed=20 << 20, transcendentals=own * 6144
        ),
        name="attend",
    )(span, qtag, ktag, qt, kv, kvt)


def grad_kernel(
    parts, final, span, qtag_ref, ktag_ref, qt_ref, dot_ref, ot_ref, lse_ref, kv_ref, kvt_ref, *rest
):
    if final:
        dq_in, dq_ref, *rest = rest
    else:
        dq_in, (dq_ref, *rest) = None, rest
    outs, (dq_sc, dkv_sc) = rest[: len(parts)], rest[len(parts) :]
    i = pl.program_id(0)

    @pl.when(i == 0)
    def _():
        dkv_sc[...] = jnp.zeros_like(dkv_sc)

    if final:
        dq_sc[...] = dq_in[...]
    else:
        dq_sc[...] = jnp.zeros_like(dq_sc)
    qtag = qtag_ref[...]
    qt, d_out, out = qt_ref[...], dot_ref[...], ot_ref[...]
    q_pad = [head_rows(qt, h, False) for h in range(OWN_HEADS)]
    d_pad = [head_rows(d_out, h, True) for h in range(OWN_HEADS)]
    both = [jnp.concatenate([q_pad[h], d_pad[h]], axis=1) for h in range(OWN_HEADS)]
    product = d_out.astype(f32) * out.astype(f32)
    inner = [
        jnp.sum(product[HEAD_DIM * h : HEAD_DIM * (h + 1)], axis=0, keepdims=True)
        for h in range(OWN_HEADS)
    ]
    log_row = [lse_ref[h : h + 1, :] for h in range(OWN_HEADS)]

    def step(shift, kb, carry):
        rows = pl.ds(pl.multiple_of(kb * BK, BK), BK)
        place = pl.ds(pl.multiple_of((kb - shift) * BK, BK), BK)
        seen = ktag_ref[rows, :] == qtag
        for h in range(OWN_HEADS):
            kv_h = kv_ref[rows, 128 * h : 128 * (h + 1)]
            s = mm(kv_h, q_pad[h])
            p = jnp.where(seen, jnp.exp(s - log_row[h]), 0.0)
            d_p = mm(kv_h, d_pad[h])
            d_s = (p * (d_p - inner[h])).astype(bf16)
            pair = jnp.concatenate([d_s, p.astype(bf16)], axis=1)
            span_rows = slice(128 * h, 128 * (h + 1))
            dkv_sc[span_rows, place] += mm(both[h], pair, NT)
            own = slice(HEAD_DIM * h, HEAD_DIM * (h + 1))
            dq_sc[own, :] += mm(kvt_ref[128 * h : 128 * h + HEAD_DIM, rows], d_s)
        return carry

    base = 0
    for n, (first, last) in enumerate(parts):
        low = jnp.maximum(span[i, 0], first)
        high = jnp.minimum(span[i, 1], last)
        lax.fori_loop(low, high, functools.partial(step, first - base), 0)
        base += last - first
    if final:
        dq_ref[...] = (dq_sc[...] * score_scale).astype(bf16)
    else:
        dq_ref[...] = dq_sc[...]

    @pl.when(i == pl.num_programs(0) - 1)
    def _():
        base = 0
        for (first, last), ref in zip(parts, outs):
            width = (last - first) * BK
            ref[...] = dkv_sc[:, base : base + width].astype(ref.dtype)
            base += width


def attend_grad(parts, final, span, qtag, ktag, qt, d_out, out, lse, kv, kvt, dq_in=None):
    own = qt.shape[1]
    window = kv.shape[0]
    whole = lambda shape: pl.BlockSpec(shape, lambda i, s: (0, 0), pipeline_mode=pl.Buffered(1))
    cols = lambda rows: pl.BlockSpec((rows, BQ), lambda i, s: (0, i))
    widths = [(last - first) * BK for first, last in parts]
    dtype = f32 if final else bf16
    args = [span, qtag, ktag, qt, d_out, out, lse, kv, kvt] + ([dq_in] if final else [])
    return pl.pallas_call(
        functools.partial(grad_kernel, parts, final),
        grid_spec=pltpu.PrefetchScalarGridSpec(
            num_scalar_prefetch=1,
            grid=(own // BQ,),
            in_specs=[
                cols(1),
                whole((window, 1)),
                cols(Q_ROWS),
                cols(Q_ROWS),
                cols(Q_ROWS),
                cols(8),
                whole((window, KV_ROWS)),
                whole((KV_ROWS, window)),
            ]
            + ([cols(Q_ROWS)] if final else []),
            out_specs=[cols(Q_ROWS)] + [whole((KV_ROWS, w)) for w in widths],
            scratch_shapes=[
                pltpu.VMEM((Q_ROWS, BQ), f32),
                pltpu.VMEM((KV_ROWS, sum(widths)), f32),
            ],
        ),
        out_shape=[jax.ShapeDtypeStruct((Q_ROWS, own), bf16 if final else f32)]
        + [jax.ShapeDtypeStruct((KV_ROWS, w), dtype) for w in widths],
        compiler_params=pltpu.CompilerParams(vmem_limit_bytes=60 << 20),
        cost_estimate=pl.CostEstimate(
            flops=(10 if final else 2) * own * 1536 * Q_ROWS,
            bytes_accessed=20 << 20,
            transcendentals=own * 4096,
        ),
        name="grad_own" if final else "grad_far",
    )(*args)


def body(
    n_dev,
    tokens,
    segment_ids,
    pad_mask,
    w_qkv,
    bias_query,
    bias_value,
    w_out,
    bias_out,
    gain_one,
    shift_one,
    w_up,
    bias_up,
    w_down,
    bias_down,
    gain_two,
    shift_two,
    cotangent,
):
    row_count = tokens.shape[0]
    rows_w = w_qkv.shape[0]
    own = GROUP * row_count
    window = own + 2 * LEN_MAX
    me = lax.axis_index("fsdp")
    place = me % GROUP
    group_id = me // GROUP
    n_group = n_dev // GROUP
    groups = [[GROUP * g + j for j in range(GROUP)] for g in range(n_group)]

    wq = w_qkv[:, :D].reshape(rows_w, GROUP, Q_ROWS)
    wk = w_qkv[:, D : 2 * D].reshape(rows_w, GROUP, OWN_HEADS, 1, HEAD_DIM)
    wv = w_qkv[:, 2 * D :].reshape(rows_w, GROUP, OWN_HEADS, 1, HEAD_DIM)
    wkv = jnp.concatenate([wk, wv], axis=3).reshape(rows_w, GROUP, KV_ROWS)
    w_cut = jnp.concatenate([wq, wkv], axis=2).transpose(1, 0, 2)
    w_send = jnp.tile(w_cut, (n_group, 1, 1))
    w_mix = lax.all_to_all(w_send, "fsdp", 0, 0, tiled=True).reshape(D, MIX_ROWS)
    small = jnp.concatenate(
        [bias_query, bias_value, bias_out, gain_one, shift_one, bias_down, gain_two, shift_two, bias_up]
    )
    small_all = lax.all_gather(small, "fsdp", axis=0, tiled=False)
    rows8 = small_all[:, : 8 * rows_w].reshape(n_dev, 8, rows_w).transpose(1, 0, 2).reshape(8, D)
    rows8 = rows8.astype(f32)
    bu_full = small_all[:, 8 * rows_w :].reshape(-1).astype(f32)
    bq_full, bv_full, bo_full, g1_full, s1_full, bd_full, g2_full, s2_full = [
        rows8[j] for j in range(8)
    ]
    big = jnp.concatenate([w_out, w_up, w_down.reshape(rows_w, -1)], axis=1)
    big_all = lax.all_gather(big, "fsdp", axis=0, tiled=True)
    ff = w_up.shape[1]
    wo_full = big_all[:, :D]
    wu_full = big_all[:, D : D + ff]
    wd_full = big_all[:, D + ff :].reshape(ff, D)

    code = segment_ids * 2 + pad_mask
    x_own = lax.all_gather(tokens, "fsdp", axis=0, tiled=True, axis_index_groups=groups)
    code_own = lax.all_gather(code, "fsdp", axis=0, tiled=True, axis_index_groups=groups)
    up = [(i, i + GROUP) for i in range(n_dev - GROUP)]
    down = [(i + GROUP, i) for i in range(n_dev - GROUP)]
    x_left, c_left = lax.ppermute((x_own[own - LEN_MAX :], code_own[own - LEN_MAX :]), "fsdp", up)
    x_right, c_right = lax.ppermute((x_own[:LEN_MAX], code_own[:LEN_MAX]), "fsdp", down)
    x_win = jnp.concatenate([x_left, x_own, x_right], axis=0)
    c_left = jnp.where(group_id == 0, -2, c_left)
    c_right = jnp.where(group_id == n_group - 1, 2 * n_dev * row_count, c_right)
    code_win = jnp.concatenate([c_left, code_own, c_right])
    seg_win = code_win >> 1
    ktag = jnp.where((code_win & 1) == 1, seg_win + 1, 0).reshape(window, 1)
    seg_own = code_own >> 1
    qtag = (seg_own + 1).reshape(1, own)
    first_seg = seg_own[::BQ]
    last_seg = seg_own[BQ - 1 :: BQ]
    low = jnp.sum((seg_win[None, :] < first_seg[:, None]).astype(jnp.int32), axis=1)
    high = jnp.sum((seg_win[None, :] <= last_seg[:, None]).astype(jnp.int32), axis=1)
    span = jnp.stack([low // BK, (high + BK - 1) // BK], axis=1)

    bq = lax.dynamic_slice(bq_full, (place * Q_ROWS,), (Q_ROWS,))
    bv = lax.dynamic_slice(bv_full, (place * Q_ROWS,), (Q_ROWS,)).reshape(OWN_HEADS, 1, HEAD_DIM)
    bkv = jnp.concatenate([jnp.zeros_like(bv), bv], axis=1).reshape(KV_ROWS)
    w_q, w_kv = w_mix[:, :Q_ROWS], w_mix[:, Q_ROWS:]
    qt = jnp.einsum("dc,td->ct", w_q, x_own, preferred_element_type=f32) + bq[:, None]
    qt = qt.astype(bf16) * jnp.asarray(score_scale, bf16)
    kv = (jnp.dot(x_win, w_kv, preferred_element_type=f32) + bkv).astype(bf16)
    kvt = jnp.einsum("dc,td->ct", w_kv, x_win, preferred_element_type=f32) + bkv[:, None]
    kvt = kvt.astype(bf16)

    ot, lse = attend(span, qtag, ktag, qt, kv, kvt)
    ctx_t = lax.all_to_all(
        ot.reshape(Q_ROWS, GROUP, row_count), "fsdp", 1, 0, axis_index_groups=groups, tiled=True
    ).reshape(D, row_count)

    tokens_f = tokens.astype(f32)
    branch = jnp.einsum("ir,io->ro", ctx_t, wo_full, preferred_element_type=f32) + bo_full
    first, norm_one_back = jax.vjp(norm_rows, tokens_f + branch, g1_full, s1_full)
    up_in = first.astype(bf16)
    pre_act = jnp.dot(up_in, wu_full, preferred_element_type=f32) + bu_full
    gelu_val, gelu_back = jax.vjp(gelu_exact, pre_act)
    hidden = gelu_val.astype(bf16)
    ffn = jnp.dot(hidden, wd_full, preferred_element_type=f32) + bd_full
    result, norm_two_back = jax.vjp(norm_rows, first + ffn, g2_full, s2_full)
    layer_out = result.astype(bf16)
    d_second, d_gain_two, d_shift_two = norm_two_back(cotangent.astype(f32))
    d_ffn = d_second.astype(bf16)
    d_bias_down = jnp.sum(d_ffn.astype(f32), axis=0)
    d_w_down = jnp.einsum("rf,rd->fd", hidden, d_ffn, preferred_element_type=f32)
    d_hidden = jnp.einsum("rd,fd->rf", d_ffn, wd_full, preferred_element_type=f32)
    d_pre = gelu_back(d_hidden)[0].astype(bf16)
    d_bias_up = jnp.sum(d_pre.astype(f32), axis=0)
    d_w_up = jnp.einsum("rd,rf->df", up_in, d_pre, preferred_element_type=f32)
    d_first = d_second + jnp.einsum("rf,df->rd", d_pre, wu_full, preferred_element_type=f32)
    d_mid, d_gain_one, d_shift_one = norm_one_back(d_first)
    d_branch = d_mid.astype(bf16)
    d_bias_out = jnp.sum(d_branch.astype(f32), axis=0)
    d_w_out = jnp.einsum("ir,ro->io", ctx_t, d_branch, preferred_element_type=f32)
    dctx_t = jnp.einsum("ro,io->ir", d_branch, wo_full, preferred_element_type=f32).astype(bf16)
    big_grad = jnp.concatenate(
        [d_w_out.astype(bf16), d_w_up.astype(bf16), d_w_down.astype(bf16).reshape(D, ff)], axis=1
    )
    big_owned = lax.psum_scatter(big_grad, "fsdp", scatter_dimension=0, tiled=True).astype(f32)

    d_out = lax.all_to_all(
        dctx_t.reshape(GROUP, Q_ROWS, row_count), "fsdp", 0, 2, axis_index_groups=groups, tiled=True
    ).reshape(Q_ROWS, own)
    edge, inside = LEN_MAX // BK, own // BK
    far_parts = ((0, edge), (edge + inside, 2 * edge + inside))
    own_parts = ((edge, edge + inside),)
    dq_far, dkv_left, dkv_right = attend_grad(
        far_parts, False, span, qtag, ktag, qt, d_out, ot, lse, kv, kvt
    )
    from_right = lax.ppermute(dkv_left, "fsdp", down)
    from_left = lax.ppermute(dkv_right, "fsdp", up)
    dq_t, dkv_own = attend_grad(
        own_parts, True, span, qtag, ktag, qt, d_out, ot, lse, kv, kvt, dq_far
    )
    dkv = jnp.concatenate(
        [
            dkv_own[:, :LEN_MAX] + from_left.astype(f32),
            dkv_own[:, LEN_MAX : own - LEN_MAX],
            dkv_own[:, own - LEN_MAX :] + from_right.astype(f32),
        ],
        axis=1,
    ).astype(bf16)
    dmix_t = jnp.concatenate([dq_t, dkv], axis=0)
    dmix_sum = jnp.sum(dmix_t.astype(f32), axis=1)
    d_w_mix = jnp.einsum("td,ct->dc", x_own, dmix_t, preferred_element_type=f32)
    d_x = jnp.einsum("ct,dc->td", dmix_t, w_mix, preferred_element_type=f32)
    grad_tokens = d_mid + lax.psum_scatter(
        d_x, "fsdp", scatter_dimension=0, tiled=True, axis_index_groups=groups
    )
    got = lax.all_to_all(
        d_w_mix.reshape(n_dev, rows_w, MIX_ROWS), "fsdp", 0, 0, tiled=True
    ).reshape(n_group, GROUP, rows_w, MIX_ROWS)
    got = jnp.sum(got, axis=0).transpose(1, 0, 2)
    g_q = got[:, :, :Q_ROWS].reshape(rows_w, D)
    g_kv = got[:, :, Q_ROWS:].reshape(rows_w, GROUP, OWN_HEADS, 2, HEAD_DIM)
    g_k = g_kv[:, :, :, 0].reshape(rows_w, D)
    g_v = g_kv[:, :, :, 1].reshape(rows_w, D)
    grad_w_qkv = jnp.concatenate([g_q, g_k, g_v], axis=1)

    pad_vec = lambda v: lax.dynamic_update_slice(jnp.zeros((D,), f32), v, (place * Q_ROWS,))
    d_bq = pad_vec(dmix_sum[:Q_ROWS])
    d_bv = pad_vec(dmix_sum[Q_ROWS:].reshape(OWN_HEADS, 2, HEAD_DIM)[:, 1].reshape(Q_ROWS))
    vecs = jnp.stack(
        [d_bq, d_bv, d_bias_out, d_gain_one, d_shift_one, d_bias_down, d_gain_two, d_shift_two]
    )
    vec_send = jnp.concatenate(
        [
            vecs.reshape(8, n_dev, rows_w).transpose(1, 0, 2).reshape(n_dev, 8 * rows_w),
            d_bias_up.reshape(n_dev, 4 * rows_w),
        ],
        axis=1,
    )
    vec = lax.psum_scatter(vec_send, "fsdp", scatter_dimension=0, tiled=True)[0]
    own_vec = [vec[j * rows_w : (j + 1) * rows_w] for j in range(8)]
    return (
        layer_out,
        grad_tokens,
        grad_w_qkv,
        own_vec[0],
        own_vec[1],
        big_owned[:, :D],
        own_vec[2],
        own_vec[3],
        own_vec[4],
        big_owned[:, D : D + ff],
        vec[8 * rows_w :],
        big_owned[:, D + ff :].reshape(4 * rows_w, D),
        own_vec[5],
        own_vec[6],
        own_vec[7],
    )


def solution(mesh):
    rows, flat = P("fsdp", None), P("fsdp")
    return jax.shard_map(
        functools.partial(body, mesh.shape["fsdp"]),
        mesh=mesh,
        in_specs=(
            rows, flat, flat, rows, flat, flat, rows, flat, flat, flat, rows, flat, rows, flat,
            flat, flat, rows,
        ),
        out_specs=(
            rows, rows, rows, flat, flat, rows, flat, flat, flat, rows, flat, rows, flat, flat,
            flat,
        ),
        check_vma=False,
    )
```

```python
import functools

import jax
import jax.numpy as jnp
from jax import lax
from jax.experimental import pallas as pl
from jax.experimental.pallas import tpu as pltpu
from jax.sharding import PartitionSpec as P

D = 768
HEADS = 12
HEAD_DIM = 64
LEN_MAX = 2048
GROUP = 4
OWN_HEADS = HEADS // GROUP
Q_ROWS = OWN_HEADS * HEAD_DIM
KV_ROWS = 2 * Q_ROWS
MIX_ROWS = Q_ROWS + KV_ROWS
BQ = 256
BK = 256
NEG = -1e30

bf16 = jnp.bfloat16
f32 = jnp.float32
eps_norm = 1e-12
score_scale = 0.125

NN = (((1,), (0,)), ((), ()))
NT = (((1,), (1,)), ((), ()))


def mm(a, b, dims=NN):
    return lax.dot_general(a, b, dims, preferred_element_type=f32)


def norm_rows(hidden, gain_row, shift_row):
    centre = hidden - jnp.mean(hidden, axis=-1, keepdims=True)
    spread = jnp.mean(centre * centre, axis=-1, keepdims=True)
    return centre * lax.rsqrt(spread + eps_norm) * gain_row + shift_row


def gelu_exact(pre_act):
    return 0.5 * pre_act * (1.0 + jax.scipy.special.erf(pre_act * 0.7071067811865476))


def head_rows(block, h, upper):
    zero = jnp.zeros_like(block[:HEAD_DIM])
    rows = block[h * HEAD_DIM : (h + 1) * HEAD_DIM]
    return jnp.concatenate([zero, rows] if upper else [rows, zero], axis=0)


def attend_kernel(
    span, qtag_ref, ktag_ref, qt_ref, kv_ref, kvt_ref, ot_ref, lse_ref, m_sc, l_sc, acc_sc
):
    i = pl.program_id(0)
    m_sc[...] = jnp.full_like(m_sc, NEG)
    l_sc[...] = jnp.zeros_like(l_sc)
    acc_sc[...] = jnp.zeros_like(acc_sc)
    qtag = qtag_ref[...]
    qt = qt_ref[...]
    q_pad = [head_rows(qt, h, False) for h in range(OWN_HEADS)]

    def step(kb, carry):
        rows = pl.ds(pl.multiple_of(kb * BK, BK), BK)
        seen = ktag_ref[rows, :] == qtag
        for h in range(OWN_HEADS):
            s = mm(kv_ref[rows, 128 * h : 128 * (h + 1)], q_pad[h])
            s = jnp.where(seen, s, NEG)
            m_old = m_sc[h : h + 1, :]
            m_new = jnp.maximum(m_old, jnp.max(s, axis=0, keepdims=True))
            p = jnp.exp(s - m_new)
            fade = jnp.exp(m_old - m_new)
            l_sc[h : h + 1, :] = fade * l_sc[h : h + 1, :] + jnp.sum(p, axis=0, keepdims=True)
            m_sc[h : h + 1, :] = m_new
            own = slice(HEAD_DIM * h, HEAD_DIM * (h + 1))
            v_t = kvt_ref[128 * h + HEAD_DIM : 128 * (h + 1), rows]
            acc_sc[own, :] = acc_sc[own, :] * fade + mm(v_t, p.astype(bf16))
        return carry

    lax.fori_loop(span[i, 0], span[i, 1], step, 0)
    for h in range(OWN_HEADS):
        own = slice(HEAD_DIM * h, HEAD_DIM * (h + 1))
        total = l_sc[h : h + 1, :]
        ot_ref[own, :] = (acc_sc[own, :] / total).astype(bf16)
        lse_ref[h : h + 1, :] = m_sc[h : h + 1, :] + jnp.log(total)
    lse_ref[OWN_HEADS:, :] = jnp.zeros_like(lse_ref[OWN_HEADS:, :])


def attend(span, qtag, ktag, qt, kv, kvt):
    own = qt.shape[1]
    window = kv.shape[0]
    whole = lambda shape: pl.BlockSpec(shape, lambda i, s: (0, 0), pipeline_mode=pl.Buffered(1))
    cols = lambda rows: pl.BlockSpec((rows, BQ), lambda i, s: (0, i))
    return pl.pallas_call(
        attend_kernel,
        grid_spec=pltpu.PrefetchScalarGridSpec(
            num_scalar_prefetch=1,
            grid=(own // BQ,),
            in_specs=[
                cols(1),
                whole((window, 1)),
                cols(Q_ROWS),
                whole((window, KV_ROWS)),
                whole((KV_ROWS, window)),
            ],
            out_specs=[cols(Q_ROWS), cols(8)],
            scratch_shapes=[
                pltpu.VMEM((8, BQ), f32),
                pltpu.VMEM((8, BQ), f32),
                pltpu.VMEM((Q_ROWS, BQ), f32),
            ],
        ),
        out_shape=[
            jax.ShapeDtypeStruct((Q_ROWS, own), bf16),
            jax.ShapeDtypeStruct((8, own), f32),
        ],
        compiler_params=pltpu.CompilerParams(vmem_limit_bytes=60 << 20),
        cost_estimate=pl.CostEstimate(
            flops=4 * own * 2048 * Q_ROWS, bytes_accessed=20 << 20, transcendentals=own * 6144
        ),
        name="attend",
    )(span, qtag, ktag, qt, kv, kvt)


def grad_kernel(
    parts, final, span, qtag_ref, ktag_ref, qt_ref, dot_ref, ot_ref, lse_ref, kv_ref, kvt_ref, *rest
):
    if final:
        dq_in, dq_ref, *rest = rest
    else:
        dq_in, (dq_ref, *rest) = None, rest
    outs, (dq_sc, dkv_sc) = rest[: len(parts)], rest[len(parts) :]
    i = pl.program_id(0)

    @pl.when(i == 0)
    def _():
        dkv_sc[...] = jnp.zeros_like(dkv_sc)

    if final:
        dq_sc[...] = dq_in[...]
    else:
        dq_sc[...] = jnp.zeros_like(dq_sc)
    qtag = qtag_ref[...]
    qt, d_out, out = qt_ref[...], dot_ref[...], ot_ref[...]
    q_pad = [head_rows(qt, h, False) for h in range(OWN_HEADS)]
    d_pad = [head_rows(d_out, h, True) for h in range(OWN_HEADS)]
    both = [jnp.concatenate([q_pad[h], d_pad[h]], axis=1) for h in range(OWN_HEADS)]
    product = d_out.astype(f32) * out.astype(f32)
    inner = [
        jnp.sum(product[HEAD_DIM * h : HEAD_DIM * (h + 1)], axis=0, keepdims=True)
        for h in range(OWN_HEADS)
    ]
    log_row = [lse_ref[h : h + 1, :] for h in range(OWN_HEADS)]

    def step(shift, kb, carry):
        rows = pl.ds(pl.multiple_of(kb * BK, BK), BK)
        place = pl.ds(pl.multiple_of((kb - shift) * BK, BK), BK)
        seen = ktag_ref[rows, :] == qtag
        for h in range(OWN_HEADS):
            kv_h = kv_ref[rows, 128 * h : 128 * (h + 1)]
            s = mm(kv_h, q_pad[h])
            p = jnp.where(seen, jnp.exp(s - log_row[h]), 0.0)
            d_p = mm(kv_h, d_pad[h])
            d_s = (p * (d_p - inner[h])).astype(bf16)
            pair = jnp.concatenate([d_s, p.astype(bf16)], axis=1)
            span_rows = slice(128 * h, 128 * (h + 1))
            dkv_sc[span_rows, place] += mm(both[h], pair, NT)
            own = slice(HEAD_DIM * h, HEAD_DIM * (h + 1))
            dq_sc[own, :] += mm(kvt_ref[128 * h : 128 * h + HEAD_DIM, rows], d_s)
        return carry

    base = 0
    for n, (first, last) in enumerate(parts):
        low = jnp.maximum(span[i, 0], first)
        high = jnp.minimum(span[i, 1], last)
        lax.fori_loop(low, high, functools.partial(step, first - base), 0)
        base += last - first
    if final:
        dq_ref[...] = (dq_sc[...] * score_scale).astype(bf16)
    else:
        dq_ref[...] = dq_sc[...]

    @pl.when(i == pl.num_programs(0) - 1)
    def _():
        base = 0
        for (first, last), ref in zip(parts, outs):
            width = (last - first) * BK
            ref[...] = dkv_sc[:, base : base + width].astype(ref.dtype)
            base += width


def attend_grad(parts, final, span, qtag, ktag, qt, d_out, out, lse, kv, kvt, dq_in=None):
    own = qt.shape[1]
    window = kv.shape[0]
    whole = lambda shape: pl.BlockSpec(shape, lambda i, s: (0, 0), pipeline_mode=pl.Buffered(1))
    cols = lambda rows: pl.BlockSpec((rows, BQ), lambda i, s: (0, i))
    widths = [(last - first) * BK for first, last in parts]
    dtype = f32 if final else bf16
    args = [span, qtag, ktag, qt, d_out, out, lse, kv, kvt] + ([dq_in] if final else [])
    return pl.pallas_call(
        functools.partial(grad_kernel, parts, final),
        grid_spec=pltpu.PrefetchScalarGridSpec(
            num_scalar_prefetch=1,
            grid=(own // BQ,),
            in_specs=[
                cols(1),
                whole((window, 1)),
                cols(Q_ROWS),
                cols(Q_ROWS),
                cols(Q_ROWS),
                cols(8),
                whole((window, KV_ROWS)),
                whole((KV_ROWS, window)),
            ]
            + ([cols(Q_ROWS)] if final else []),
            out_specs=[cols(Q_ROWS)] + [whole((KV_ROWS, w)) for w in widths],
            scratch_shapes=[
                pltpu.VMEM((Q_ROWS, BQ), f32),
                pltpu.VMEM((KV_ROWS, sum(widths)), f32),
            ],
        ),
        out_shape=[jax.ShapeDtypeStruct((Q_ROWS, own), bf16 if final else f32)]
        + [jax.ShapeDtypeStruct((KV_ROWS, w), dtype) for w in widths],
        compiler_params=pltpu.CompilerParams(vmem_limit_bytes=60 << 20),
        cost_estimate=pl.CostEstimate(
            flops=(10 if final else 2) * own * 1536 * Q_ROWS,
            bytes_accessed=20 << 20,
            transcendentals=own * 4096,
        ),
        name="grad_own" if final else "grad_far",
    )(*args)


MESH = pl.DeviceIdType.MESH
CHUNKS = 4
MESSAGE_ROWS = 32
W_LANES = 640
KV_AT = 256


def remote(src, dst, send, recv, target):
    return pltpu.make_async_remote_copy(
        src_ref=src,
        dst_ref=dst,
        send_sem=send,
        recv_sem=recv,
        device_id=(target,),
        device_id_type=MESH,
    )


def share_kernel(
    n_dev, tok_ref, code_ref, w_ref, x_out, c_out, w_out,
    w_send, w_recv, c_send, c_recv, part_send, part_recv, mate_send, mate_recv,
    up_send, up_recv, down_send, down_recv, cross_send, cross_recv,
    fwd_send, fwd_recv, keep_sem,
):
    n_group = n_dev // GROUP
    me = lax.axis_index("fsdp")
    g = me // GROUP
    s = me % GROUP
    k = s % 2
    hi = s // 2
    partner = me + 1 - 2 * k
    mate = me + 2 - 4 * hi
    mate_block = 4 + k - 2 * hi
    has_up = g < n_group - 1
    has_down = g > 0
    rows = tok_ref.shape[0] // CHUNKS
    half = CHUNKS // 2

    barrier = pltpu.get_barrier_semaphore()

    def greet(r, carry):
        pl.semaphore_signal(
            barrier, inc=1, device_id=(lax.rem(me + r, n_dev),), device_id_type=MESH
        )
        return carry

    lax.fori_loop(1, n_dev, greet, 0)
    pl.semaphore_wait(barrier, n_dev - 1)

    def chunk(ref, c):
        return ref.at[pl.ds(pl.multiple_of(c * rows, rows), rows)]

    def spot(b, c):
        return x_out.at[b, pl.ds(pl.multiple_of(c * rows, rows), rows)]

    def to_partner(c):
        return remote(chunk(tok_ref, c), spot(2 + s, c), part_send.at[c], part_recv.at[c], partner)

    def to_mate(c):
        return remote(chunk(tok_ref, c), spot(2 + s, c), mate_send.at[c], mate_recv.at[c], mate)

    def up_own(c):
        return remote(chunk(tok_ref, c), spot(k, c), up_send.at[c], up_recv.at[c], me + GROUP)

    def up_mate(c):
        return remote(spot(mate_block, c), spot(k, c), up_send.at[c], up_recv.at[c], me + GROUP)

    def down_own(c):
        return remote(
            chunk(tok_ref, c), spot(6 + k, c), down_send.at[c], down_recv.at[c], me - GROUP
        )

    def down_mate(c):
        return remote(
            spot(mate_block, c + half), spot(6 + k, c + half), down_send.at[c], down_recv.at[c],
            me - GROUP,
        )

    def cross(c):
        at = c + half * hi
        return remote(spot(6 + k, at), spot(6 + k, at), cross_send.at[c], cross_recv.at[c], mate)

    def forward(b, c, slot):
        return remote(spot(b, c), spot(b, c), fwd_send.at[slot], fwd_recv.at[slot], partner)

    keep_x = pltpu.make_async_copy(tok_ref, x_out.at[2 + s], keep_sem.at[0])
    keep_c = pltpu.make_async_copy(code_ref, c_out.at[2 + s], keep_sem.at[1])
    keep_w = pltpu.make_async_copy(w_ref.at[s], w_out.at[me], keep_sem.at[2])
    keep_x.start()
    keep_c.start()
    keep_w.start()

    def w_copy(r):
        target = lax.rem(me + r, n_dev)
        return remote(
            w_ref.at[lax.rem(target, GROUP)], w_out.at[me], w_send.at[r], w_recv.at[r], target
        )

    def w_start(r, carry):
        w_copy(r).start()
        return carry

    def c_group(j):
        target = GROUP * g + lax.rem(s + j, GROUP)
        return remote(code_ref, c_out.at[2 + s], c_send.at[j], c_recv.at[2 + s], target)

    def c_far(j):
        step = GROUP * (2 * hi - 1)
        b = 6 + s - 8 * hi
        target = GROUP * g + step + j
        return remote(code_ref, c_out.at[b], c_send.at[GROUP + j], c_recv.at[b], target)

    sends_far = jnp.where(hi == 1, g < n_group - 1, g > 0)
    for j in range(1, GROUP):
        c_group(j).start()

    @pl.when(sends_far)
    def _():
        for j in range(GROUP):
            c_far(j).start()

    for c in range(CHUNKS):
        to_mate(c).start()
        to_partner(c).start()

        @pl.when((hi == 1) & has_up)
        def _():
            up_own(c).start()

        if c < half:

            @pl.when((hi == 0) & has_down)
            def _():
                down_own(c).start()

    lax.fori_loop(1, n_dev, w_start, 0)

    for c in range(CHUNKS):
        to_mate(c).wait_recv()
        forward(mate_block, c, c).start()

        @pl.when((hi == 0) & has_up)
        def _():
            up_mate(c).start()

        if c >= half:

            @pl.when((hi == 1) & has_down)
            def _():
                down_mate(c - half).start()

    @pl.when(has_up)
    def _():
        for c in range(half):
            down_own(c).wait_recv()
            cross(c).start()
            forward(6 + k, c + half * hi, 2 * CHUNKS + c).start()

    @pl.when(has_down)
    def _():
        for c in range(CHUNKS):
            up_own(c).wait_recv()
            forward(k, c, CHUNKS + c).start()

    @pl.when(has_up)
    def _():
        for c in range(half):
            cross(c).wait_recv()
            forward(6 + k, c + half * (1 - hi), 2 * CHUNKS + half + c).start()

    for c in range(CHUNKS):
        to_partner(c).wait()
        to_mate(c).wait_send()
        forward(mate_block, c, c).wait()

    @pl.when(has_down)
    def _():
        for c in range(CHUNKS):
            forward(k, c, CHUNKS + c).wait()
        for c in range(half):
            down_own(c).wait_send()

    @pl.when(has_up)
    def _():
        for c in range(half):
            cross(c).wait_send()
            forward(6 + k, c, 2 * CHUNKS + c).wait()
            forward(6 + k, c, 2 * CHUNKS + half + c).wait()
        for c in range(CHUNKS):
            up_own(c).wait_send()

    for j in range(1, GROUP):
        c_group(j).wait_send()
        remote(
            code_ref, c_out.at[0], c_send.at[j], c_recv.at[2 + lax.rem(s + j, GROUP)], partner
        ).wait_recv()

    @pl.when(sends_far)
    def _():
        for j in range(GROUP):
            c_far(j).wait_send()

    @pl.when(has_down)
    def _():
        for b in range(2):
            remote(code_ref, c_out.at[b], c_send.at[0], c_recv.at[b], partner).wait_recv()

    @pl.when(has_up)
    def _():
        for b in range(6, 8):
            remote(code_ref, c_out.at[b], c_send.at[0], c_recv.at[b], partner).wait_recv()

    def w_wait(r, carry):
        w_copy(r).wait()
        return carry

    lax.fori_loop(1, n_dev, w_wait, 0)
    keep_x.wait()
    keep_c.wait()
    keep_w.wait()


def share(n_dev, tokens, code, w_send):
    vmem = pl.BlockSpec(memory_space=pltpu.VMEM)
    anywhere = pl.BlockSpec(memory_space=pl.ANY)
    dma = lambda n: pltpu.SemaphoreType.DMA((n,))
    half = CHUNKS // 2
    return pl.pallas_call(
        functools.partial(share_kernel, n_dev),
        in_specs=[vmem] * 3,
        out_specs=[anywhere] * 3,
        out_shape=[
            jax.ShapeDtypeStruct((8,) + tokens.shape, tokens.dtype),
            jax.ShapeDtypeStruct((8,) + code.shape, code.dtype),
            jax.ShapeDtypeStruct((n_dev,) + w_send.shape[1:], w_send.dtype),
        ],
        scratch_shapes=[
            dma(n_dev), dma(n_dev), dma(2 * GROUP), dma(8),
            dma(CHUNKS), dma(CHUNKS), dma(CHUNKS), dma(CHUNKS),
            dma(CHUNKS), dma(CHUNKS), dma(half), dma(half), dma(half), dma(half),
            dma(3 * CHUNKS), dma(3 * CHUNKS), dma(3),
        ],
        compiler_params=pltpu.CompilerParams(collective_id=0, has_side_effects=True),
        name="share",
    )(tokens, code, w_send)


def body(
    n_dev,
    tokens,
    segment_ids,
    pad_mask,
    w_qkv,
    bias_query,
    bias_value,
    w_out,
    bias_out,
    gain_one,
    shift_one,
    w_up,
    bias_up,
    w_down,
    bias_down,
    gain_two,
    shift_two,
    cotangent,
):
    row_count = tokens.shape[0]
    rows_w = w_qkv.shape[0]
    own = GROUP * row_count
    window = own + 2 * LEN_MAX
    me = lax.axis_index("fsdp")
    place = me % GROUP
    group_id = me // GROUP
    n_group = n_dev // GROUP
    up = [(i, i + GROUP) for i in range(n_dev - GROUP)]
    down = [(i + GROUP, i) for i in range(n_dev - GROUP)]
    groups = [[GROUP * g + j for j in range(GROUP)] for g in range(n_group)]

    wq = w_qkv[:, :D].reshape(rows_w, GROUP, Q_ROWS)
    wk = w_qkv[:, D : 2 * D].reshape(rows_w, GROUP, OWN_HEADS, 1, HEAD_DIM)
    wv = w_qkv[:, 2 * D :].reshape(rows_w, GROUP, OWN_HEADS, 1, HEAD_DIM)
    wkv = jnp.concatenate([wk, wv], axis=3).reshape(rows_w, GROUP, KV_ROWS)
    gap = jnp.zeros((rows_w, GROUP, KV_AT - Q_ROWS), bf16)
    w_cut = jnp.concatenate([wq, gap, wkv], axis=2).transpose(1, 0, 2)
    small = jnp.concatenate(
        [bias_query, bias_value, bias_out, gain_one, shift_one, bias_down, gain_two, shift_two, bias_up]
    )
    n_small = small.shape[0]
    small_rows = jnp.pad(small[None], ((0, MESSAGE_ROWS - rows_w - 1), (0, W_LANES - n_small)))
    small_rows = jnp.broadcast_to(small_rows[None], (GROUP,) + small_rows.shape)
    w_send = jnp.concatenate([w_cut, small_rows], axis=1)
    big = jnp.concatenate([w_out, w_up, w_down.reshape(rows_w, -1)], axis=1)
    big_all = lax.all_gather(big, "fsdp", axis=0, tiled=True)
    ff = w_up.shape[1]
    wo_full = big_all[:, :D]
    wu_full = big_all[:, D : D + ff]
    wd_full = big_all[:, D + ff :].reshape(ff, D)

    code = (segment_ids * 2 + pad_mask).reshape(8, row_count // 8)
    x_win, code_win, w_got = share(n_dev, tokens, code, w_send)
    x_win = x_win.reshape(window, D)
    x_own = x_win[LEN_MAX : LEN_MAX + own]
    code_win = code_win.reshape(window)
    at = jnp.arange(window)
    code_win = jnp.where((group_id == 0) & (at < LEN_MAX), -2, code_win)
    code_win = jnp.where(
        (group_id == n_group - 1) & (at >= LEN_MAX + own), 2 * n_dev * row_count, code_win
    )
    code_own = code_win[LEN_MAX : LEN_MAX + own]
    w_mix = w_got[:, :rows_w].reshape(D, W_LANES)
    small_all = w_got[:, rows_w, :n_small]
    rows8 = small_all[:, : 8 * rows_w].reshape(n_dev, 8, rows_w).transpose(1, 0, 2).reshape(8, D)
    rows8 = rows8.astype(f32)
    bu_full = small_all[:, 8 * rows_w :].reshape(-1).astype(f32)
    bq_full, bv_full, bo_full, g1_full, s1_full, bd_full, g2_full, s2_full = [
        rows8[j] for j in range(8)
    ]
    seg_win = code_win >> 1
    ktag = jnp.where((code_win & 1) == 1, seg_win + 1, 0).reshape(window, 1)
    seg_own = code_own >> 1
    qtag = (seg_own + 1).reshape(1, own)
    first_seg = seg_own[::BQ]
    last_seg = seg_own[BQ - 1 :: BQ]
    low = jnp.sum((seg_win[None, :] < first_seg[:, None]).astype(jnp.int32), axis=1)
    high = jnp.sum((seg_win[None, :] <= last_seg[:, None]).astype(jnp.int32), axis=1)
    span = jnp.stack([low // BK, (high + BK - 1) // BK], axis=1)

    bq = lax.dynamic_slice(bq_full, (place * Q_ROWS,), (Q_ROWS,))
    bv = lax.dynamic_slice(bv_full, (place * Q_ROWS,), (Q_ROWS,)).reshape(OWN_HEADS, 1, HEAD_DIM)
    bkv = jnp.concatenate([jnp.zeros_like(bv), bv], axis=1).reshape(KV_ROWS)
    w_q, w_kv = w_mix[:, :Q_ROWS], w_mix[:, KV_AT:]
    w_mix = jnp.concatenate([w_q, w_kv], axis=1)
    qt = jnp.einsum("dc,td->ct", w_q, x_own, preferred_element_type=f32) + bq[:, None]
    qt = qt.astype(bf16) * jnp.asarray(score_scale, bf16)
    kv = (jnp.dot(x_win, w_kv, preferred_element_type=f32) + bkv).astype(bf16)
    kvt = jnp.einsum("dc,td->ct", w_kv, x_win, preferred_element_type=f32) + bkv[:, None]
    kvt = kvt.astype(bf16)

    ot, lse = attend(span, qtag, ktag, qt, kv, kvt)
    ctx_t = lax.all_to_all(
        ot.reshape(Q_ROWS, GROUP, row_count), "fsdp", 1, 0, axis_index_groups=groups, tiled=True
    ).reshape(D, row_count)

    tokens_f = tokens.astype(f32)
    branch = jnp.einsum("ir,io->ro", ctx_t, wo_full, preferred_element_type=f32) + bo_full
    first, norm_one_back = jax.vjp(norm_rows, tokens_f + branch, g1_full, s1_full)
    up_in = first.astype(bf16)
    pre_act = jnp.dot(up_in, wu_full, preferred_element_type=f32) + bu_full
    gelu_val, gelu_back = jax.vjp(gelu_exact, pre_act)
    hidden = gelu_val.astype(bf16)
    ffn = jnp.dot(hidden, wd_full, preferred_element_type=f32) + bd_full
    result, norm_two_back = jax.vjp(norm_rows, first + ffn, g2_full, s2_full)
    layer_out = result.astype(bf16)
    d_second, d_gain_two, d_shift_two = norm_two_back(cotangent.astype(f32))
    d_ffn = d_second.astype(bf16)
    d_bias_down = jnp.sum(d_ffn.astype(f32), axis=0)
    d_w_down = jnp.einsum("rf,rd->fd", hidden, d_ffn, preferred_element_type=f32)
    d_hidden = jnp.einsum("rd,fd->rf", d_ffn, wd_full, preferred_element_type=f32)
    d_pre = gelu_back(d_hidden)[0].astype(bf16)
    d_bias_up = jnp.sum(d_pre.astype(f32), axis=0)
    d_w_up = jnp.einsum("rd,rf->df", up_in, d_pre, preferred_element_type=f32)
    d_first = d_second + jnp.einsum("rf,df->rd", d_pre, wu_full, preferred_element_type=f32)
    d_mid, d_gain_one, d_shift_one = norm_one_back(d_first)
    d_branch = d_mid.astype(bf16)
    d_bias_out = jnp.sum(d_branch.astype(f32), axis=0)
    d_w_out = jnp.einsum("ir,ro->io", ctx_t, d_branch, preferred_element_type=f32)
    dctx_t = jnp.einsum("ro,io->ir", d_branch, wo_full, preferred_element_type=f32).astype(bf16)
    big_grad = jnp.concatenate(
        [d_w_out.astype(bf16), d_w_up.astype(bf16), d_w_down.astype(bf16).reshape(D, ff)], axis=1
    )
    big_owned = lax.psum_scatter(big_grad, "fsdp", scatter_dimension=0, tiled=True).astype(f32)

    d_out = lax.all_to_all(
        dctx_t.reshape(GROUP, Q_ROWS, row_count), "fsdp", 0, 2, axis_index_groups=groups, tiled=True
    ).reshape(Q_ROWS, own)
    edge, inside = LEN_MAX // BK, own // BK
    far_parts = ((0, edge), (edge + inside, 2 * edge + inside))
    own_parts = ((edge, edge + inside),)
    dq_far, dkv_left, dkv_right = attend_grad(
        far_parts, False, span, qtag, ktag, qt, d_out, ot, lse, kv, kvt
    )
    from_right = lax.ppermute(dkv_left, "fsdp", down)
    from_left = lax.ppermute(dkv_right, "fsdp", up)
    dq_t, dkv_own = attend_grad(
        own_parts, True, span, qtag, ktag, qt, d_out, ot, lse, kv, kvt, dq_far
    )
    dkv = jnp.concatenate(
        [
            dkv_own[:, :LEN_MAX] + from_left.astype(f32),
            dkv_own[:, LEN_MAX : own - LEN_MAX],
            dkv_own[:, own - LEN_MAX :] + from_right.astype(f32),
        ],
        axis=1,
    ).astype(bf16)
    dmix_t = jnp.concatenate([dq_t, dkv], axis=0)
    dmix_sum = jnp.sum(dmix_t.astype(f32), axis=1)
    d_w_mix = jnp.einsum("td,ct->dc", x_own, dmix_t, preferred_element_type=f32)
    d_x = jnp.einsum("ct,dc->td", dmix_t, w_mix, preferred_element_type=f32)
    grad_tokens = d_mid + lax.psum_scatter(
        d_x, "fsdp", scatter_dimension=0, tiled=True, axis_index_groups=groups
    )
    got = lax.all_to_all(
        d_w_mix.reshape(n_dev, rows_w, MIX_ROWS), "fsdp", 0, 0, tiled=True
    ).reshape(n_group, GROUP, rows_w, MIX_ROWS)
    got = jnp.sum(got, axis=0).transpose(1, 0, 2)
    g_q = got[:, :, :Q_ROWS].reshape(rows_w, D)
    g_kv = got[:, :, Q_ROWS:].reshape(rows_w, GROUP, OWN_HEADS, 2, HEAD_DIM)
    g_k = g_kv[:, :, :, 0].reshape(rows_w, D)
    g_v = g_kv[:, :, :, 1].reshape(rows_w, D)
    grad_w_qkv = jnp.concatenate([g_q, g_k, g_v], axis=1)

    pad_vec = lambda v: lax.dynamic_update_slice(jnp.zeros((D,), f32), v, (place * Q_ROWS,))
    d_bq = pad_vec(dmix_sum[:Q_ROWS])
    d_bv = pad_vec(dmix_sum[Q_ROWS:].reshape(OWN_HEADS, 2, HEAD_DIM)[:, 1].reshape(Q_ROWS))
    vecs = jnp.stack(
        [d_bq, d_bv, d_bias_out, d_gain_one, d_shift_one, d_bias_down, d_gain_two, d_shift_two]
    )
    vec_send = jnp.concatenate(
        [
            vecs.reshape(8, n_dev, rows_w).transpose(1, 0, 2).reshape(n_dev, 8 * rows_w),
            d_bias_up.reshape(n_dev, 4 * rows_w),
        ],
        axis=1,
    )
    vec = lax.psum_scatter(vec_send, "fsdp", scatter_dimension=0, tiled=True)[0]
    own_vec = [vec[j * rows_w : (j + 1) * rows_w] for j in range(8)]
    return (
        layer_out,
        grad_tokens,
        grad_w_qkv,
        own_vec[0],
        own_vec[1],
        big_owned[:, :D],
        own_vec[2],
        own_vec[3],
        own_vec[4],
        big_owned[:, D : D + ff],
        vec[8 * rows_w :],
        big_owned[:, D + ff :].reshape(4 * rows_w, D),
        own_vec[5],
        own_vec[6],
        own_vec[7],
    )


def solution(mesh):
    rows, flat = P("fsdp", None), P("fsdp")
    return jax.shard_map(
        functools.partial(body, mesh.shape["fsdp"]),
        mesh=mesh,
        in_specs=(
            rows, flat, flat, rows, flat, flat, rows, flat, flat, flat, rows, flat, rows, flat,
            flat, flat, rows,
        ),
        out_specs=(
            rows, rows, rows, flat, flat, rows, flat, flat, flat, rows, flat, rows, flat, flat,
            flat,
        ),
        check_vma=False,
    )
```

```python
import functools

import jax
import jax.numpy as jnp
from jax import lax
from jax.experimental import pallas as pl
from jax.experimental.pallas import tpu as pltpu
from jax.sharding import PartitionSpec as P

D = 768
HEADS = 12
HEAD_DIM = 64
LEN_MAX = 2048
GROUP = 4
OWN_HEADS = HEADS // GROUP
Q_ROWS = OWN_HEADS * HEAD_DIM
KV_ROWS = 2 * Q_ROWS
MIX_ROWS = Q_ROWS + KV_ROWS
BQ = 512
FK = 512
BK = 256
NEG = -1e30

bf16 = jnp.bfloat16
f32 = jnp.float32
eps_norm = 1e-12
score_scale = 0.125

NN = (((1,), (0,)), ((), ()))
NT = (((1,), (1,)), ((), ()))


def mm(a, b, dims=NN):
    return lax.dot_general(a, b, dims, preferred_element_type=f32)


def norm_rows(hidden, gain_row, shift_row):
    centre = hidden - jnp.mean(hidden, axis=-1, keepdims=True)
    spread = jnp.mean(centre * centre, axis=-1, keepdims=True)
    return centre * lax.rsqrt(spread + eps_norm) * gain_row + shift_row


def gelu_exact(pre_act):
    return 0.5 * pre_act * (1.0 + jax.scipy.special.erf(pre_act * 0.7071067811865476))


def head_rows(block, h, upper):
    zero = jnp.zeros_like(block[:HEAD_DIM])
    rows = block[h * HEAD_DIM : (h + 1) * HEAD_DIM]
    return jnp.concatenate([zero, rows] if upper else [rows, zero], axis=0)


def attend_kernel(
    span, qtag_ref, ktag_ref, qt_ref, kv_ref, kvt_ref, ot_ref, lse_ref, m_sc, l_sc, acc_sc
):
    i = pl.program_id(0)
    m_sc[...] = jnp.full_like(m_sc, NEG)
    l_sc[...] = jnp.zeros_like(l_sc)
    acc_sc[...] = jnp.zeros_like(acc_sc)
    qtag = qtag_ref[...]
    qt = qt_ref[...]
    q_pad = [head_rows(qt, h, False) for h in range(OWN_HEADS)]

    def step(kb, carry):
        rows = pl.ds(pl.multiple_of(kb * FK, FK), FK)
        seen = ktag_ref[rows, :] == qtag
        hs = range(OWN_HEADS)
        s = [mm(kv_ref[rows, 128 * h : 128 * (h + 1)], q_pad[h]) for h in hs]
        s = [jnp.where(seen, v, NEG) for v in s]
        m_old = [m_sc[h : h + 1, :] for h in hs]
        l_old = [l_sc[h : h + 1, :] for h in hs]
        m_new = [jnp.maximum(m_old[h], jnp.max(s[h], axis=0, keepdims=True)) for h in hs]
        p = [jnp.exp(s[h] - m_new[h]).astype(bf16) for h in hs]
        fade = [jnp.exp(m_old[h] - m_new[h]) for h in hs]
        one = jnp.ones((16, FK), bf16)
        v_one = [
            jnp.concatenate([kvt_ref[128 * h + HEAD_DIM : 128 * (h + 1), rows], one], axis=0)
            for h in hs
        ]
        out = [mm(v_one[h], p[h]) for h in hs]
        for h in hs:
            own = slice(HEAD_DIM * h, HEAD_DIM * (h + 1))
            acc_sc[own, :] = acc_sc[own, :] * fade[h] + out[h][:HEAD_DIM]
            l_sc[h : h + 1, :] = fade[h] * l_old[h] + out[h][HEAD_DIM : HEAD_DIM + 1]
            m_sc[h : h + 1, :] = m_new[h]
        return carry

    lax.fori_loop(span[i, 0], span[i, 1], step, 0)
    for h in range(OWN_HEADS):
        own = slice(HEAD_DIM * h, HEAD_DIM * (h + 1))
        total = l_sc[h : h + 1, :]
        ot_ref[own, :] = (acc_sc[own, :] / total).astype(bf16)
        lse_ref[h : h + 1, :] = m_sc[h : h + 1, :] + jnp.log(total)
    lse_ref[OWN_HEADS:, :] = jnp.zeros_like(lse_ref[OWN_HEADS:, :])


def attend(span, qtag, ktag, qt, kv, kvt):
    own = qt.shape[1]
    window = kv.shape[0]
    whole = lambda shape: pl.BlockSpec(shape, lambda i, s: (0, 0), pipeline_mode=pl.Buffered(1))
    cols = lambda rows: pl.BlockSpec((rows, BQ), lambda i, s: (0, i))
    return pl.pallas_call(
        attend_kernel,
        grid_spec=pltpu.PrefetchScalarGridSpec(
            num_scalar_prefetch=1,
            grid=(own // BQ,),
            in_specs=[
                cols(1),
                whole((window, 1)),
                cols(Q_ROWS),
                whole((window, KV_ROWS)),
                whole((KV_ROWS, window)),
            ],
            out_specs=[cols(Q_ROWS), cols(8)],
            scratch_shapes=[
                pltpu.VMEM((8, BQ), f32),
                pltpu.VMEM((8, BQ), f32),
                pltpu.VMEM((Q_ROWS, BQ), f32),
            ],
        ),
        out_shape=[
            jax.ShapeDtypeStruct((Q_ROWS, own), bf16),
            jax.ShapeDtypeStruct((8, own), f32),
        ],
        compiler_params=pltpu.CompilerParams(vmem_limit_bytes=60 << 20),
        cost_estimate=pl.CostEstimate(
            flops=4 * own * 2048 * Q_ROWS, bytes_accessed=20 << 20, transcendentals=own * 6144
        ),
        name="attend",
    )(span, qtag, ktag, qt, kv, kvt)


def grad_kernel(
    parts, final, span, qtag_ref, ktag_ref, qt_ref, dot_ref, ot_ref, lse_ref, kv_ref, kvt_ref, *rest
):
    if final:
        dq_in, dq_ref, *rest = rest
    else:
        dq_in, (dq_ref, *rest) = None, rest
    outs, (dq_sc, dkv_sc) = rest[: len(parts)], rest[len(parts) :]
    i = pl.program_id(0)

    @pl.when(i == 0)
    def _():
        dkv_sc[...] = jnp.zeros_like(dkv_sc)

    if final:
        dq_sc[...] = dq_in[...]
    else:
        dq_sc[...] = jnp.zeros_like(dq_sc)
    qtag = qtag_ref[...]
    qt, d_out, out = qt_ref[...], dot_ref[...], ot_ref[...]
    q_pad = [head_rows(qt, h, False) for h in range(OWN_HEADS)]
    d_pad = [head_rows(d_out, h, True) for h in range(OWN_HEADS)]
    product = d_out.astype(f32) * out.astype(f32)
    inner = [
        jnp.sum(product[HEAD_DIM * h : HEAD_DIM * (h + 1)], axis=0, keepdims=True)
        for h in range(OWN_HEADS)
    ]
    log_row = [lse_ref[h : h + 1, :] for h in range(OWN_HEADS)]

    def step(shift, kb, carry):
        rows = pl.ds(pl.multiple_of(kb * BK, BK), BK)
        place = pl.ds(pl.multiple_of((kb - shift) * BK, BK), BK)
        seen = ktag_ref[rows, :] == qtag
        hs = range(OWN_HEADS)
        kv = [kv_ref[rows, 128 * h : 128 * (h + 1)] for h in hs]
        s = [mm(kv[h], q_pad[h]) for h in hs]
        d_p = [mm(kv[h], d_pad[h]) for h in hs]
        p = [jnp.where(seen, jnp.exp(s[h] - log_row[h]), 0.0) for h in hs]
        d_s = [(p[h] * (d_p[h] - inner[h])).astype(bf16) for h in hs]
        p = [v.astype(bf16) for v in p]
        g_kv = [mm(q_pad[h], d_s[h], NT) + mm(d_pad[h], p[h], NT) for h in hs]
        g_q = [mm(kvt_ref[128 * h : 128 * h + HEAD_DIM, rows], d_s[h]) for h in hs]
        for h in hs:
            dkv_sc[128 * h : 128 * (h + 1), place] += g_kv[h]
            own = slice(HEAD_DIM * h, HEAD_DIM * (h + 1))
            dq_sc[own, :] += g_q[h]
        return carry

    base = 0
    for n, (first, last) in enumerate(parts):
        low = jnp.maximum(span[i, 0], first)
        high = jnp.minimum(span[i, 1], last)
        lax.fori_loop(low, high, functools.partial(step, first - base), 0)
        base += last - first
    if final:
        dq_ref[...] = (dq_sc[...] * score_scale).astype(bf16)
    else:
        dq_ref[...] = dq_sc[...]

    @pl.when(i == pl.num_programs(0) - 1)
    def _():
        base = 0
        for (first, last), ref in zip(parts, outs):
            width = (last - first) * BK
            ref[...] = dkv_sc[:, base : base + width].astype(ref.dtype)
            base += width


def attend_grad(parts, final, span, qtag, ktag, qt, d_out, out, lse, kv, kvt, dq_in=None):
    own = qt.shape[1]
    window = kv.shape[0]
    whole = lambda shape: pl.BlockSpec(shape, lambda i, s: (0, 0), pipeline_mode=pl.Buffered(1))
    cols = lambda rows: pl.BlockSpec((rows, BQ), lambda i, s: (0, i))
    widths = [(last - first) * BK for first, last in parts]
    dtype = f32 if final else bf16
    args = [span, qtag, ktag, qt, d_out, out, lse, kv, kvt] + ([dq_in] if final else [])
    return pl.pallas_call(
        functools.partial(grad_kernel, parts, final),
        grid_spec=pltpu.PrefetchScalarGridSpec(
            num_scalar_prefetch=1,
            grid=(own // BQ,),
            in_specs=[
                cols(1),
                whole((window, 1)),
                cols(Q_ROWS),
                cols(Q_ROWS),
                cols(Q_ROWS),
                cols(8),
                whole((window, KV_ROWS)),
                whole((KV_ROWS, window)),
            ]
            + ([cols(Q_ROWS)] if final else []),
            out_specs=[cols(Q_ROWS)] + [whole((KV_ROWS, w)) for w in widths],
            scratch_shapes=[
                pltpu.VMEM((Q_ROWS, BQ), f32),
                pltpu.VMEM((KV_ROWS, sum(widths)), f32),
            ],
        ),
        out_shape=[jax.ShapeDtypeStruct((Q_ROWS, own), bf16 if final else f32)]
        + [jax.ShapeDtypeStruct((KV_ROWS, w), dtype) for w in widths],
        compiler_params=pltpu.CompilerParams(vmem_limit_bytes=60 << 20),
        cost_estimate=pl.CostEstimate(
            flops=(10 if final else 2) * own * 1536 * Q_ROWS,
            bytes_accessed=20 << 20,
            transcendentals=own * 4096,
        ),
        name="grad_own" if final else "grad_far",
    )(*args)


MESH = pl.DeviceIdType.MESH
CHUNKS = 4
MESSAGE_ROWS = 32
W_LANES = 640
KV_AT = 256


def remote(src, dst, send, recv, target):
    return pltpu.make_async_remote_copy(
        src_ref=src,
        dst_ref=dst,
        send_sem=send,
        recv_sem=recv,
        device_id=(target,),
        device_id_type=MESH,
    )


def share_kernel(
    n_dev, tok_ref, code_ref, w_ref, x_out, c_out, w_out,
    w_send, w_recv, c_send, c_recv, part_send, part_recv, mate_send, mate_recv,
    up_send, up_recv, down_send, down_recv, cross_send, cross_recv,
    fwd_send, fwd_recv, keep_sem,
):
    n_group = n_dev // GROUP
    me = lax.axis_index("fsdp")
    g = me // GROUP
    s = me % GROUP
    k = s % 2
    hi = s // 2
    partner = me + 1 - 2 * k
    mate = me + 2 - 4 * hi
    mate_block = 4 + k - 2 * hi
    has_up = g < n_group - 1
    has_down = g > 0
    rows = tok_ref.shape[0] // CHUNKS
    half = CHUNKS // 2

    barrier = pltpu.get_barrier_semaphore()

    def greet(r, carry):
        pl.semaphore_signal(
            barrier, inc=1, device_id=(lax.rem(me + r, n_dev),), device_id_type=MESH
        )
        return carry

    lax.fori_loop(1, n_dev, greet, 0)
    pl.semaphore_wait(barrier, n_dev - 1)

    def chunk(ref, c):
        return ref.at[pl.ds(pl.multiple_of(c * rows, rows), rows)]

    def spot(b, c):
        return x_out.at[b, pl.ds(pl.multiple_of(c * rows, rows), rows)]

    def to_partner(c):
        return remote(chunk(tok_ref, c), spot(2 + s, c), part_send.at[c], part_recv.at[c], partner)

    def to_mate(c):
        return remote(chunk(tok_ref, c), spot(2 + s, c), mate_send.at[c], mate_recv.at[c], mate)

    def up_own(c):
        return remote(chunk(tok_ref, c), spot(k, c), up_send.at[c], up_recv.at[c], me + GROUP)

    def up_mate(c):
        return remote(spot(mate_block, c), spot(k, c), up_send.at[c], up_recv.at[c], me + GROUP)

    def down_own(c):
        return remote(
            chunk(tok_ref, c), spot(6 + k, c), down_send.at[c], down_recv.at[c], me - GROUP
        )

    def down_mate(c):
        return remote(
            spot(mate_block, c + half), spot(6 + k, c + half), down_send.at[c], down_recv.at[c],
            me - GROUP,
        )

    def cross(c):
        at = c + half * hi
        return remote(spot(6 + k, at), spot(6 + k, at), cross_send.at[c], cross_recv.at[c], mate)

    def forward(b, c, slot):
        return remote(spot(b, c), spot(b, c), fwd_send.at[slot], fwd_recv.at[slot], partner)

    keep_x = pltpu.make_async_copy(tok_ref, x_out.at[2 + s], keep_sem.at[0])
    keep_c = pltpu.make_async_copy(code_ref, c_out.at[2 + s], keep_sem.at[1])
    keep_w = pltpu.make_async_copy(w_ref.at[s], w_out.at[me], keep_sem.at[2])
    keep_x.start()
    keep_c.start()
    keep_w.start()

    def w_copy(r):
        target = lax.rem(me + r, n_dev)
        return remote(
            w_ref.at[lax.rem(target, GROUP)], w_out.at[me], w_send.at[r], w_recv.at[r], target
        )

    def w_start(r, carry):
        w_copy(r).start()
        return carry

    def c_group(j):
        target = GROUP * g + lax.rem(s + j, GROUP)
        return remote(code_ref, c_out.at[2 + s], c_send.at[j], c_recv.at[2 + s], target)

    def c_far(j):
        step = GROUP * (2 * hi - 1)
        b = 6 + s - 8 * hi
        target = GROUP * g + step + j
        return remote(code_ref, c_out.at[b], c_send.at[GROUP + j], c_recv.at[b], target)

    sends_far = jnp.where(hi == 1, g < n_group - 1, g > 0)
    for j in range(1, GROUP):
        c_group(j).start()

    @pl.when(sends_far)
    def _():
        for j in range(GROUP):
            c_far(j).start()

    for c in range(CHUNKS):
        to_mate(c).start()
        to_partner(c).start()

        @pl.when((hi == 1) & has_up)
        def _():
            up_own(c).start()

        if c < half:

            @pl.when((hi == 0) & has_down)
            def _():
                down_own(c).start()

    lax.fori_loop(1, n_dev, w_start, 0)

    for c in range(CHUNKS):
        to_mate(c).wait_recv()
        forward(mate_block, c, c).start()

        @pl.when((hi == 0) & has_up)
        def _():
            up_mate(c).start()

        if c >= half:

            @pl.when((hi == 1) & has_down)
            def _():
                down_mate(c - half).start()

    @pl.when(has_up)
    def _():
        for c in range(half):
            down_own(c).wait_recv()
            cross(c).start()
            forward(6 + k, c + half * hi, 2 * CHUNKS + c).start()

    @pl.when(has_down)
    def _():
        for c in range(CHUNKS):
            up_own(c).wait_recv()
            forward(k, c, CHUNKS + c).start()

    @pl.when(has_up)
    def _():
        for c in range(half):
            cross(c).wait_recv()
            forward(6 + k, c + half * (1 - hi), 2 * CHUNKS + half + c).start()

    for c in range(CHUNKS):
        to_partner(c).wait()
        to_mate(c).wait_send()
        forward(mate_block, c, c).wait()

    @pl.when(has_down)
    def _():
        for c in range(CHUNKS):
            forward(k, c, CHUNKS + c).wait()
        for c in range(half):
            down_own(c).wait_send()

    @pl.when(has_up)
    def _():
        for c in range(half):
            cross(c).wait_send()
            forward(6 + k, c, 2 * CHUNKS + c).wait()
            forward(6 + k, c, 2 * CHUNKS + half + c).wait()
        for c in range(CHUNKS):
            up_own(c).wait_send()

    for j in range(1, GROUP):
        c_group(j).wait_send()
        remote(
            code_ref, c_out.at[0], c_send.at[j], c_recv.at[2 + lax.rem(s + j, GROUP)], partner
        ).wait_recv()

    @pl.when(sends_far)
    def _():
        for j in range(GROUP):
            c_far(j).wait_send()

    @pl.when(has_down)
    def _():
        for b in range(2):
            remote(code_ref, c_out.at[b], c_send.at[0], c_recv.at[b], partner).wait_recv()

    @pl.when(has_up)
    def _():
        for b in range(6, 8):
            remote(code_ref, c_out.at[b], c_send.at[0], c_recv.at[b], partner).wait_recv()

    def w_wait(r, carry):
        w_copy(r).wait()
        return carry

    lax.fori_loop(1, n_dev, w_wait, 0)
    keep_x.wait()
    keep_c.wait()
    keep_w.wait()


def share(n_dev, tokens, code, w_send):
    vmem = pl.BlockSpec(memory_space=pltpu.VMEM)
    anywhere = pl.BlockSpec(memory_space=pl.ANY)
    dma = lambda n: pltpu.SemaphoreType.DMA((n,))
    half = CHUNKS // 2
    return pl.pallas_call(
        functools.partial(share_kernel, n_dev),
        in_specs=[vmem] * 3,
        out_specs=[anywhere] * 3,
        out_shape=[
            jax.ShapeDtypeStruct((8,) + tokens.shape, tokens.dtype),
            jax.ShapeDtypeStruct((8,) + code.shape, code.dtype),
            jax.ShapeDtypeStruct((n_dev,) + w_send.shape[1:], w_send.dtype),
        ],
        scratch_shapes=[
            dma(n_dev), dma(n_dev), dma(2 * GROUP), dma(8),
            dma(CHUNKS), dma(CHUNKS), dma(CHUNKS), dma(CHUNKS),
            dma(CHUNKS), dma(CHUNKS), dma(half), dma(half), dma(half), dma(half),
            dma(3 * CHUNKS), dma(3 * CHUNKS), dma(3),
        ],
        compiler_params=pltpu.CompilerParams(collective_id=0, has_side_effects=True),
        name="share",
    )(tokens, code, w_send)


def body(
    n_dev,
    tokens,
    segment_ids,
    pad_mask,
    w_qkv,
    bias_query,
    bias_value,
    w_out,
    bias_out,
    gain_one,
    shift_one,
    w_up,
    bias_up,
    w_down,
    bias_down,
    gain_two,
    shift_two,
    cotangent,
):
    row_count = tokens.shape[0]
    rows_w = w_qkv.shape[0]
    own = GROUP * row_count
    window = own + 2 * LEN_MAX
    me = lax.axis_index("fsdp")
    place = me % GROUP
    group_id = me // GROUP
    n_group = n_dev // GROUP
    up = [(i, i + GROUP) for i in range(n_dev - GROUP)]
    down = [(i + GROUP, i) for i in range(n_dev - GROUP)]
    groups = [[GROUP * g + j for j in range(GROUP)] for g in range(n_group)]

    wq = w_qkv[:, :D].reshape(rows_w, GROUP, Q_ROWS)
    wk = w_qkv[:, D : 2 * D].reshape(rows_w, GROUP, OWN_HEADS, 1, HEAD_DIM)
    wv = w_qkv[:, 2 * D :].reshape(rows_w, GROUP, OWN_HEADS, 1, HEAD_DIM)
    wkv = jnp.concatenate([wk, wv], axis=3).reshape(rows_w, GROUP, KV_ROWS)
    gap = jnp.zeros((rows_w, GROUP, KV_AT - Q_ROWS), bf16)
    w_cut = jnp.concatenate([wq, gap, wkv], axis=2).transpose(1, 0, 2)
    small = jnp.concatenate(
        [bias_query, bias_value, bias_out, gain_one, shift_one, bias_down, gain_two, shift_two, bias_up]
    )
    n_small = small.shape[0]
    small_rows = jnp.pad(small[None], ((0, MESSAGE_ROWS - rows_w - 1), (0, W_LANES - n_small)))
    small_rows = jnp.broadcast_to(small_rows[None], (GROUP,) + small_rows.shape)
    w_send = jnp.concatenate([w_cut, small_rows], axis=1)
    ff = w_up.shape[1]
    wo_full = lax.all_gather(w_out, "fsdp", axis=0, tiled=True)
    wu_full = lax.all_gather(w_up, "fsdp", axis=0, tiled=True)
    wd_full = lax.all_gather(w_down, "fsdp", axis=0, tiled=True)

    code = (segment_ids * 2 + pad_mask).reshape(8, row_count // 8)
    x_win, code_win, w_got = share(n_dev, tokens, code, w_send)
    x_win = x_win.reshape(window, D)
    x_own = x_win[LEN_MAX : LEN_MAX + own]
    code_win = code_win.reshape(window)
    at = jnp.arange(window)
    code_win = jnp.where((group_id == 0) & (at < LEN_MAX), -2, code_win)
    code_win = jnp.where(
        (group_id == n_group - 1) & (at >= LEN_MAX + own), 2 * n_dev * row_count, code_win
    )
    code_own = code_win[LEN_MAX : LEN_MAX + own]
    w_mix = w_got[:, :rows_w].reshape(D, W_LANES)
    small_all = w_got[:, rows_w, :n_small]
    rows8 = small_all[:, : 8 * rows_w].reshape(n_dev, 8, rows_w).transpose(1, 0, 2).reshape(8, D)
    rows8 = rows8.astype(f32)
    bu_full = small_all[:, 8 * rows_w :].reshape(-1).astype(f32)
    bq_full, bv_full, bo_full, g1_full, s1_full, bd_full, g2_full, s2_full = [
        rows8[j] for j in range(8)
    ]
    seg_win = code_win >> 1
    ktag = jnp.where((code_win & 1) == 1, seg_win + 1, 0).reshape(window, 1)
    seg_own = code_own >> 1
    qtag = (seg_own + 1).reshape(1, own)
    first_seg = seg_own[::BQ]
    last_seg = seg_own[BQ - 1 :: BQ]
    low = jnp.sum((seg_win[None, :] < first_seg[:, None]).astype(jnp.int32), axis=1)
    high = jnp.sum((seg_win[None, :] <= last_seg[:, None]).astype(jnp.int32), axis=1)
    spans = [jnp.stack([low // b, (high + b - 1) // b], axis=1) for b in (FK, BK)]

    bq = lax.dynamic_slice(bq_full, (place * Q_ROWS,), (Q_ROWS,))
    bv = lax.dynamic_slice(bv_full, (place * Q_ROWS,), (Q_ROWS,)).reshape(OWN_HEADS, 1, HEAD_DIM)
    bkv = jnp.concatenate([jnp.zeros_like(bv), bv], axis=1).reshape(KV_ROWS)
    w_q, w_kv = w_mix[:, :Q_ROWS], w_mix[:, KV_AT:]
    w_mix = jnp.concatenate([w_q, w_kv], axis=1)
    qt = jnp.einsum("dc,td->ct", w_q, x_own, preferred_element_type=f32) + bq[:, None]
    qt = qt.astype(bf16) * jnp.asarray(score_scale, bf16)
    kv = (jnp.dot(x_win, w_kv, preferred_element_type=f32) + bkv).astype(bf16)
    kvt = jnp.einsum("dc,td->ct", w_kv, x_win, preferred_element_type=f32) + bkv[:, None]
    kvt = kvt.astype(bf16)

    ot, lse = attend(spans[0], qtag, ktag, qt, kv, kvt)
    ctx_t = lax.all_to_all(
        ot.reshape(Q_ROWS, GROUP, row_count), "fsdp", 1, 0, axis_index_groups=groups, tiled=True
    ).reshape(D, row_count)

    tokens_f = tokens.astype(f32)
    branch = jnp.einsum("ir,io->ro", ctx_t, wo_full, preferred_element_type=f32) + bo_full
    first, norm_one_back = jax.vjp(norm_rows, tokens_f + branch, g1_full, s1_full)
    up_in = first.astype(bf16)
    pre_act = jnp.dot(up_in, wu_full, preferred_element_type=f32) + bu_full
    gelu_val, gelu_back = jax.vjp(gelu_exact, pre_act)
    hidden = gelu_val.astype(bf16)
    ffn = jnp.dot(hidden, wd_full, preferred_element_type=f32) + bd_full
    result, norm_two_back = jax.vjp(norm_rows, first + ffn, g2_full, s2_full)
    layer_out = result.astype(bf16)
    d_second, d_gain_two, d_shift_two = norm_two_back(cotangent.astype(f32))
    d_ffn = d_second.astype(bf16)
    d_bias_down = jnp.sum(d_ffn.astype(f32), axis=0)
    d_w_down = jnp.einsum("rf,rd->fd", hidden, d_ffn, preferred_element_type=f32)
    d_hidden = jnp.einsum("rd,fd->rf", d_ffn, wd_full, preferred_element_type=f32)
    d_pre = gelu_back(d_hidden)[0].astype(bf16)
    d_bias_up = jnp.sum(d_pre.astype(f32), axis=0)
    d_w_up = jnp.einsum("rd,rf->df", up_in, d_pre, preferred_element_type=f32)
    d_first = d_second + jnp.einsum("rf,df->rd", d_pre, wu_full, preferred_element_type=f32)
    d_mid, d_gain_one, d_shift_one = norm_one_back(d_first)
    d_branch = d_mid.astype(bf16)
    d_bias_out = jnp.sum(d_branch.astype(f32), axis=0)
    d_w_out = jnp.einsum("ir,ro->io", ctx_t, d_branch, preferred_element_type=f32)
    dctx_t = jnp.einsum("ro,io->ir", d_branch, wo_full, preferred_element_type=f32).astype(bf16)
    n_up = ff // D
    big_grad = jnp.concatenate(
        [
            d_w_down.astype(bf16).reshape(n_dev, -1, D),
            d_w_out.astype(bf16).reshape(n_dev, rows_w, D),
        ]
        + [d_w_up[:, D * j : D * (j + 1)].astype(bf16).reshape(n_dev, rows_w, D) for j in range(n_up)],
        axis=1,
    )
    big_owned = lax.psum_scatter(big_grad, "fsdp", scatter_dimension=0).astype(f32)
    rows_d = w_down.shape[0]
    g_down, g_out = big_owned[:rows_d], big_owned[rows_d : rows_d + rows_w]
    g_up = jnp.concatenate(
        [big_owned[rows_d + rows_w * (j + 1) : rows_d + rows_w * (j + 2)] for j in range(n_up)], axis=1
    )

    d_out = lax.all_to_all(
        dctx_t.reshape(GROUP, Q_ROWS, row_count), "fsdp", 0, 2, axis_index_groups=groups, tiled=True
    ).reshape(Q_ROWS, own)
    edge, inside = LEN_MAX // BK, own // BK
    far_parts = ((0, edge), (edge + inside, 2 * edge + inside))
    own_parts = ((edge, edge + inside),)
    dq_far, dkv_left, dkv_right = attend_grad(
        far_parts, False, spans[1], qtag, ktag, qt, d_out, ot, lse, kv, kvt
    )
    from_right = lax.ppermute(dkv_left, "fsdp", down)
    from_left = lax.ppermute(dkv_right, "fsdp", up)
    dq_t, dkv_own = attend_grad(
        own_parts, True, spans[1], qtag, ktag, qt, d_out, ot, lse, kv, kvt, dq_far
    )
    dkv = jnp.concatenate(
        [
            dkv_own[:, :LEN_MAX] + from_left.astype(f32),
            dkv_own[:, LEN_MAX : own - LEN_MAX],
            dkv_own[:, own - LEN_MAX :] + from_right.astype(f32),
        ],
        axis=1,
    ).astype(bf16)
    dmix_t = jnp.concatenate([dq_t, dkv], axis=0)
    dmix_sum = jnp.sum(dmix_t.astype(f32), axis=1)
    d_w_mix = jnp.einsum("td,ct->dc", x_own, dmix_t, preferred_element_type=f32)
    d_x = jnp.einsum("ct,dc->td", dmix_t, w_mix, preferred_element_type=f32)
    grad_tokens = d_mid + lax.psum_scatter(
        d_x, "fsdp", scatter_dimension=0, tiled=True, axis_index_groups=groups
    )
    got = lax.all_to_all(
        d_w_mix.reshape(n_dev, rows_w, MIX_ROWS), "fsdp", 0, 0, tiled=True
    ).reshape(n_group, GROUP, rows_w, MIX_ROWS)
    got = jnp.sum(got, axis=0).transpose(1, 0, 2)
    g_q = got[:, :, :Q_ROWS].reshape(rows_w, D)
    g_kv = got[:, :, Q_ROWS:].reshape(rows_w, GROUP, OWN_HEADS, 2, HEAD_DIM)
    g_k = g_kv[:, :, :, 0].reshape(rows_w, D)
    g_v = g_kv[:, :, :, 1].reshape(rows_w, D)
    grad_w_qkv = jnp.concatenate([g_q, g_k, g_v], axis=1)

    pad_vec = lambda v: lax.dynamic_update_slice(jnp.zeros((D,), f32), v, (place * Q_ROWS,))
    d_bq = pad_vec(dmix_sum[:Q_ROWS])
    d_bv = pad_vec(dmix_sum[Q_ROWS:].reshape(OWN_HEADS, 2, HEAD_DIM)[:, 1].reshape(Q_ROWS))
    vecs = jnp.stack(
        [d_bq, d_bv, d_bias_out, d_gain_one, d_shift_one, d_bias_down, d_gain_two, d_shift_two]
    )
    vec_send = jnp.concatenate(
        [
            vecs.reshape(8, n_dev, rows_w).transpose(1, 0, 2).reshape(n_dev, 8 * rows_w),
            d_bias_up.reshape(n_dev, 4 * rows_w),
        ],
        axis=1,
    )
    vec = lax.psum_scatter(vec_send, "fsdp", scatter_dimension=0, tiled=True)[0]
    own_vec = [vec[j * rows_w : (j + 1) * rows_w] for j in range(8)]
    return (
        layer_out,
        grad_tokens,
        grad_w_qkv,
        own_vec[0],
        own_vec[1],
        g_out,
        own_vec[2],
        own_vec[3],
        own_vec[4],
        g_up,
        vec[8 * rows_w :],
        g_down,
        own_vec[5],
        own_vec[6],
        own_vec[7],
    )


def solution(mesh):
    rows, flat = P("fsdp", None), P("fsdp")
    return jax.shard_map(
        functools.partial(body, mesh.shape["fsdp"]),
        mesh=mesh,
        in_specs=(
            rows, flat, flat, rows, flat, flat, rows, flat, flat, flat, rows, flat, rows, flat,
            flat, flat, rows,
        ),
        out_specs=(
            rows, rows, rows, flat, flat, rows, flat, flat, flat, rows, flat, rows, flat, flat,
            flat,
        ),
        check_vma=False,
    )
```

```python
import functools

import jax
import jax.numpy as jnp
from jax import lax
from jax.experimental import pallas as pl
from jax.experimental.pallas import tpu as pltpu
from jax.sharding import PartitionSpec as P

D = 768
HEADS = 12
HEAD_DIM = 64
LEN_MAX = 2048
GROUP = 4
OWN_HEADS = HEADS // GROUP
Q_ROWS = OWN_HEADS * HEAD_DIM
KV_ROWS = 2 * Q_ROWS
MIX_ROWS = Q_ROWS + KV_ROWS
BQ = 512
FK = 512
BK = 256
NEG = -1e30

bf16 = jnp.bfloat16
f32 = jnp.float32
eps_norm = 1e-12
score_scale = 0.125

NN = (((1,), (0,)), ((), ()))
NT = (((1,), (1,)), ((), ()))


def mm(a, b, dims=NN):
    return lax.dot_general(a, b, dims, preferred_element_type=f32)


def norm_rows(hidden, gain_row, shift_row):
    centre = hidden - jnp.mean(hidden, axis=-1, keepdims=True)
    spread = jnp.mean(centre * centre, axis=-1, keepdims=True)
    return centre * lax.rsqrt(spread + eps_norm) * gain_row + shift_row


def gelu_exact(pre_act):
    return 0.5 * pre_act * (1.0 + jax.scipy.special.erf(pre_act * 0.7071067811865476))


def head_rows(block, h, upper):
    zero = jnp.zeros_like(block[:HEAD_DIM])
    rows = block[h * HEAD_DIM : (h + 1) * HEAD_DIM]
    return jnp.concatenate([zero, rows] if upper else [rows, zero], axis=0)


def attend_kernel(
    span, qtag_ref, ktag_ref, qt_ref, kv_ref, kvt_ref, ot_ref, lse_ref, m_sc, l_sc, acc_sc
):
    i = pl.program_id(0)
    m_sc[...] = jnp.full_like(m_sc, NEG)
    l_sc[...] = jnp.zeros_like(l_sc)
    acc_sc[...] = jnp.zeros_like(acc_sc)
    qtag = qtag_ref[...]
    qt = qt_ref[...]
    q_pad = [head_rows(qt, h, False) for h in range(OWN_HEADS)]

    def step(kb, carry):
        rows = pl.ds(pl.multiple_of(kb * FK, FK), FK)
        seen = ktag_ref[rows, :] == qtag
        hs = range(OWN_HEADS)
        s = [mm(kv_ref[rows, 128 * h : 128 * (h + 1)], q_pad[h]) for h in hs]
        s = [jnp.where(seen, v, NEG) for v in s]
        m_old = [m_sc[h : h + 1, :] for h in hs]
        l_old = [l_sc[h : h + 1, :] for h in hs]
        m_new = [jnp.maximum(m_old[h], jnp.max(s[h], axis=0, keepdims=True)) for h in hs]
        p = [jnp.exp(s[h] - m_new[h]).astype(bf16) for h in hs]
        fade = [jnp.exp(m_old[h] - m_new[h]) for h in hs]
        one = jnp.ones((16, FK), bf16)
        v_one = [
            jnp.concatenate([kvt_ref[128 * h + HEAD_DIM : 128 * (h + 1), rows], one], axis=0)
            for h in hs
        ]
        out = [mm(v_one[h], p[h]) for h in hs]
        for h in hs:
            own = slice(HEAD_DIM * h, HEAD_DIM * (h + 1))
            acc_sc[own, :] = acc_sc[own, :] * fade[h] + out[h][:HEAD_DIM]
            l_sc[h : h + 1, :] = fade[h] * l_old[h] + out[h][HEAD_DIM : HEAD_DIM + 1]
            m_sc[h : h + 1, :] = m_new[h]
        return carry

    lax.fori_loop(span[i, 0], span[i, 1], step, 0)
    for h in range(OWN_HEADS):
        own = slice(HEAD_DIM * h, HEAD_DIM * (h + 1))
        total = l_sc[h : h + 1, :]
        ot_ref[own, :] = (acc_sc[own, :] / total).astype(bf16)
        lse_ref[h : h + 1, :] = m_sc[h : h + 1, :] + jnp.log(total)
    lse_ref[OWN_HEADS:, :] = jnp.zeros_like(lse_ref[OWN_HEADS:, :])


def attend(span, qtag, ktag, qt, kv, kvt):
    own = qt.shape[1]
    window = kv.shape[0]
    whole = lambda shape: pl.BlockSpec(shape, lambda i, s: (0, 0), pipeline_mode=pl.Buffered(1))
    cols = lambda rows: pl.BlockSpec((rows, BQ), lambda i, s: (0, i))
    return pl.pallas_call(
        attend_kernel,
        grid_spec=pltpu.PrefetchScalarGridSpec(
            num_scalar_prefetch=1,
            grid=(own // BQ,),
            in_specs=[
                cols(1),
                whole((window, 1)),
                cols(Q_ROWS),
                whole((window, KV_ROWS)),
                whole((KV_ROWS, window)),
            ],
            out_specs=[cols(Q_ROWS), cols(8)],
            scratch_shapes=[
                pltpu.VMEM((8, BQ), f32),
                pltpu.VMEM((8, BQ), f32),
                pltpu.VMEM((Q_ROWS, BQ), f32),
            ],
        ),
        out_shape=[
            jax.ShapeDtypeStruct((Q_ROWS, own), bf16),
            jax.ShapeDtypeStruct((8, own), f32),
        ],
        compiler_params=pltpu.CompilerParams(vmem_limit_bytes=60 << 20),
        cost_estimate=pl.CostEstimate(
            flops=4 * own * 2048 * Q_ROWS, bytes_accessed=20 << 20, transcendentals=own * 6144
        ),
        name="attend",
    )(span, qtag, ktag, qt, kv, kvt)


def grad_kernel(
    parts, final, span, qtag_ref, ktag_ref, qt_ref, dot_ref, ot_ref, lse_ref, kv_ref, kvt_ref, *rest
):
    if final:
        dq_in, dq_ref, *rest = rest
    else:
        dq_in, (dq_ref, *rest) = None, rest
    outs, (dq_sc, dkv_sc) = rest[: len(parts)], rest[len(parts) :]
    i = pl.program_id(0)

    @pl.when(i == 0)
    def _():
        dkv_sc[...] = jnp.zeros_like(dkv_sc)

    if final:
        dq_sc[...] = dq_in[...]
    else:
        dq_sc[...] = jnp.zeros_like(dq_sc)
    qtag = qtag_ref[...]
    qt, d_out, out = qt_ref[...], dot_ref[...], ot_ref[...]
    q_pad = [head_rows(qt, h, False) for h in range(OWN_HEADS)]
    d_pad = [head_rows(d_out, h, True) for h in range(OWN_HEADS)]
    product = d_out.astype(f32) * out.astype(f32)
    inner = [
        jnp.sum(product[HEAD_DIM * h : HEAD_DIM * (h + 1)], axis=0, keepdims=True)
        for h in range(OWN_HEADS)
    ]
    log_row = [lse_ref[h : h + 1, :] for h in range(OWN_HEADS)]

    def step(shift, kb, carry):
        rows = pl.ds(pl.multiple_of(kb * BK, BK), BK)
        place = pl.ds(pl.multiple_of((kb - shift) * BK, BK), BK)
        seen = ktag_ref[rows, :] == qtag
        hs = range(OWN_HEADS)
        kv = [kv_ref[rows, 128 * h : 128 * (h + 1)] for h in hs]
        s = [mm(kv[h], q_pad[h]) for h in hs]
        d_p = [mm(kv[h], d_pad[h]) for h in hs]
        p = [jnp.where(seen, jnp.exp(s[h] - log_row[h]), 0.0) for h in hs]
        d_s = [(p[h] * (d_p[h] - inner[h])).astype(bf16) for h in hs]
        p = [v.astype(bf16) for v in p]
        g_kv = [mm(q_pad[h], d_s[h], NT) + mm(d_pad[h], p[h], NT) for h in hs]
        g_q = [mm(kvt_ref[128 * h : 128 * h + HEAD_DIM, rows], d_s[h]) for h in hs]
        for h in hs:
            dkv_sc[128 * h : 128 * (h + 1), place] += g_kv[h]
            own = slice(HEAD_DIM * h, HEAD_DIM * (h + 1))
            dq_sc[own, :] += g_q[h]
        return carry

    base = 0
    for n, (first, last) in enumerate(parts):
        low = jnp.maximum(span[i, 0], first)
        high = jnp.minimum(span[i, 1], last)
        lax.fori_loop(low, high, functools.partial(step, first - base), 0)
        base += last - first
    if final:
        dq_ref[...] = (dq_sc[...] * score_scale).astype(bf16)
    else:
        dq_ref[...] = dq_sc[...]

    @pl.when(i == pl.num_programs(0) - 1)
    def _():
        base = 0
        for (first, last), ref in zip(parts, outs):
            width = (last - first) * BK
            ref[...] = dkv_sc[:, base : base + width].astype(ref.dtype)
            base += width


def attend_grad(parts, final, span, qtag, ktag, qt, d_out, out, lse, kv, kvt, dq_in=None):
    own = qt.shape[1]
    window = kv.shape[0]
    whole = lambda shape: pl.BlockSpec(shape, lambda i, s: (0, 0), pipeline_mode=pl.Buffered(1))
    cols = lambda rows: pl.BlockSpec((rows, BQ), lambda i, s: (0, i))
    widths = [(last - first) * BK for first, last in parts]
    dtype = f32 if final else bf16
    args = [span, qtag, ktag, qt, d_out, out, lse, kv, kvt] + ([dq_in] if final else [])
    return pl.pallas_call(
        functools.partial(grad_kernel, parts, final),
        grid_spec=pltpu.PrefetchScalarGridSpec(
            num_scalar_prefetch=1,
            grid=(own // BQ,),
            in_specs=[
                cols(1),
                whole((window, 1)),
                cols(Q_ROWS),
                cols(Q_ROWS),
                cols(Q_ROWS),
                cols(8),
                whole((window, KV_ROWS)),
                whole((KV_ROWS, window)),
            ]
            + ([cols(Q_ROWS)] if final else []),
            out_specs=[cols(Q_ROWS)] + [whole((KV_ROWS, w)) for w in widths],
            scratch_shapes=[
                pltpu.VMEM((Q_ROWS, BQ), f32),
                pltpu.VMEM((KV_ROWS, sum(widths)), f32),
            ],
        ),
        out_shape=[jax.ShapeDtypeStruct((Q_ROWS, own), bf16 if final else f32)]
        + [jax.ShapeDtypeStruct((KV_ROWS, w), dtype) for w in widths],
        compiler_params=pltpu.CompilerParams(vmem_limit_bytes=60 << 20),
        cost_estimate=pl.CostEstimate(
            flops=(10 if final else 2) * own * 1536 * Q_ROWS,
            bytes_accessed=20 << 20,
            transcendentals=own * 4096,
        ),
        name="grad_own" if final else "grad_far",
    )(*args)


MESH = pl.DeviceIdType.MESH
CHUNKS = 8
W_LANES = 640
KV_AT = 256


def remote(src, dst, send, recv, target):
    return pltpu.make_async_remote_copy(
        src_ref=src,
        dst_ref=dst,
        send_sem=send,
        recv_sem=recv,
        device_id=(target,),
        device_id_type=MESH,
    )


def share_kernel(
    n_dev, tok_ref, code_ref, w_ref, x_out, c_out, w_out,
    w_send, w_recv, c_send, c_recv, part_send, part_recv, mate_send, mate_recv,
    up_send, up_recv, down_send, down_recv, cross_send, cross_recv,
    fwd_send, fwd_recv, keep_sem,
):
    n_group = n_dev // GROUP
    me = lax.axis_index("fsdp")
    g = me // GROUP
    s = me % GROUP
    k = s % 2
    hi = s // 2
    partner = me + 1 - 2 * k
    mate = me + 2 - 4 * hi
    mate_block = 4 + k - 2 * hi
    has_up = g < n_group - 1
    has_down = g > 0
    rows = tok_ref.shape[0] // CHUNKS
    half = CHUNKS // 2

    barrier = pltpu.get_barrier_semaphore()

    def greet(r, carry):
        pl.semaphore_signal(
            barrier, inc=1, device_id=(lax.rem(me + r, n_dev),), device_id_type=MESH
        )
        return carry

    lax.fori_loop(1, n_dev, greet, 0)
    pl.semaphore_wait(barrier, n_dev - 1)

    def chunk(ref, c):
        return ref.at[pl.ds(pl.multiple_of(c * rows, rows), rows)]

    def spot(b, c):
        return x_out.at[b, pl.ds(pl.multiple_of(c * rows, rows), rows)]

    def to_partner(c):
        return remote(chunk(tok_ref, c), spot(2 + s, c), part_send.at[c], part_recv.at[c], partner)

    def to_mate(c):
        return remote(chunk(tok_ref, c), spot(2 + s, c), mate_send.at[c], mate_recv.at[c], mate)

    def up_own(c):
        return remote(chunk(tok_ref, c), spot(k, c), up_send.at[c], up_recv.at[c], me + GROUP)

    def up_mate(c):
        return remote(spot(mate_block, c), spot(k, c), up_send.at[c], up_recv.at[c], me + GROUP)

    def down_own(c):
        return remote(
            chunk(tok_ref, c), spot(6 + k, c), down_send.at[c], down_recv.at[c], me - GROUP
        )

    def down_mate(c):
        return remote(
            spot(mate_block, c + half), spot(6 + k, c + half), down_send.at[c], down_recv.at[c],
            me - GROUP,
        )

    def cross(c):
        at = c + half * hi
        return remote(spot(6 + k, at), spot(6 + k, at), cross_send.at[c], cross_recv.at[c], mate)

    def forward(b, c, slot):
        return remote(spot(b, c), spot(b, c), fwd_send.at[slot], fwd_recv.at[slot], partner)

    keep_x = pltpu.make_async_copy(tok_ref, x_out.at[2 + s], keep_sem.at[0])
    keep_c = pltpu.make_async_copy(code_ref, c_out.at[2 + s], keep_sem.at[1])
    keep_w = pltpu.make_async_copy(w_ref.at[s], w_out.at[me], keep_sem.at[2])
    keep_x.start()
    keep_c.start()
    keep_w.start()

    def w_copy(r):
        target = lax.rem(me + r, n_dev)
        return remote(
            w_ref.at[lax.rem(target, GROUP)], w_out.at[me], w_send.at[r], w_recv.at[r], target
        )

    def w_start(r, carry):
        w_copy(r).start()
        return carry

    def c_group(j):
        target = GROUP * g + lax.rem(s + j, GROUP)
        return remote(code_ref, c_out.at[2 + s], c_send.at[j], c_recv.at[2 + s], target)

    def c_far(j):
        step = GROUP * (2 * hi - 1)
        b = 6 + s - 8 * hi
        target = GROUP * g + step + j
        return remote(code_ref, c_out.at[b], c_send.at[GROUP + j], c_recv.at[b], target)

    sends_far = jnp.where(hi == 1, g < n_group - 1, g > 0)
    for j in range(1, GROUP):
        c_group(j).start()

    @pl.when(sends_far)
    def _():
        for j in range(GROUP):
            c_far(j).start()

    order = list(range(half, CHUNKS)) + list(range(half))

    @pl.when((hi == 0) & has_down)
    def _():
        for c in range(half):
            down_own(c).start()

    for n, c in enumerate(order):
        to_mate(c).start()
        to_partner(c).start()
        if n < half:

            @pl.when((hi == 1) & has_up)
            def _():
                up_own(c).start()

    lax.fori_loop(1, n_dev, w_start, 0)

    for n, c in enumerate(order):
        to_mate(c).wait_recv()
        forward(mate_block, c, c).start()

        @pl.when((hi == 0) & has_up)
        def _():
            up_mate(c).start()

        if n < half:

            @pl.when((hi == 1) & has_down)
            def _():
                down_mate(c - half).start()

        else:

            @pl.when((hi == 1) & has_up)
            def _():
                up_own(c).start()

    @pl.when(has_up)
    def _():
        for c in range(half):
            down_own(c).wait_recv()
            cross(c).start()
            forward(6 + k, c + half * hi, 2 * CHUNKS + c).start()

    @pl.when(has_down)
    def _():
        for c in order:
            up_own(c).wait_recv()
            forward(k, c, CHUNKS + c).start()

    @pl.when(has_up)
    def _():
        for c in range(half):
            cross(c).wait_recv()
            forward(6 + k, c + half * (1 - hi), 2 * CHUNKS + half + c).start()

    for c in range(CHUNKS):
        to_partner(c).wait()
        to_mate(c).wait_send()
        forward(mate_block, c, c).wait()

    @pl.when(has_down)
    def _():
        for c in range(CHUNKS):
            forward(k, c, CHUNKS + c).wait()
        for c in range(half):
            down_own(c).wait_send()

    @pl.when(has_up)
    def _():
        for c in range(half):
            cross(c).wait_send()
            forward(6 + k, c, 2 * CHUNKS + c).wait()
            forward(6 + k, c, 2 * CHUNKS + half + c).wait()
        for c in range(CHUNKS):
            up_own(c).wait_send()

    for j in range(1, GROUP):
        c_group(j).wait_send()
        remote(
            code_ref, c_out.at[0], c_send.at[j], c_recv.at[2 + lax.rem(s + j, GROUP)], partner
        ).wait_recv()

    @pl.when(sends_far)
    def _():
        for j in range(GROUP):
            c_far(j).wait_send()

    @pl.when(has_down)
    def _():
        for b in range(2):
            remote(code_ref, c_out.at[b], c_send.at[0], c_recv.at[b], partner).wait_recv()

    @pl.when(has_up)
    def _():
        for b in range(6, 8):
            remote(code_ref, c_out.at[b], c_send.at[0], c_recv.at[b], partner).wait_recv()

    def w_wait(r, carry):
        w_copy(r).wait()
        return carry

    lax.fori_loop(1, n_dev, w_wait, 0)
    keep_x.wait()
    keep_c.wait()
    keep_w.wait()


def share(n_dev, tokens, code, w_send):
    vmem = pl.BlockSpec(memory_space=pltpu.VMEM)
    anywhere = pl.BlockSpec(memory_space=pl.ANY)
    dma = lambda n: pltpu.SemaphoreType.DMA((n,))
    half = CHUNKS // 2
    return pl.pallas_call(
        functools.partial(share_kernel, n_dev),
        in_specs=[vmem] * 3,
        out_specs=[anywhere] * 3,
        out_shape=[
            jax.ShapeDtypeStruct((8,) + tokens.shape, tokens.dtype),
            jax.ShapeDtypeStruct((8,) + code.shape, code.dtype),
            jax.ShapeDtypeStruct((n_dev,) + w_send.shape[1:], w_send.dtype),
        ],
        scratch_shapes=[
            dma(n_dev), dma(n_dev), dma(2 * GROUP), dma(8),
            dma(CHUNKS), dma(CHUNKS), dma(CHUNKS), dma(CHUNKS),
            dma(CHUNKS), dma(CHUNKS), dma(half), dma(half), dma(half), dma(half),
            dma(3 * CHUNKS), dma(3 * CHUNKS), dma(3),
        ],
        compiler_params=pltpu.CompilerParams(collective_id=0, has_side_effects=True),
        name="share",
    )(tokens, code, w_send)


def settle_kernel(
    n_dev, dx_ref, w_ref, vec_ref, near_out, far_out, w_out, vec_out,
    relay, total,
    w_send, w_recv, vec_send, vec_recv, near_send, near_recv, relay_send, relay_recv,
    far_send, far_recv, keep_sem,
):
    me = lax.axis_index("fsdp")
    s = me % GROUP
    k = s % 2
    hi = s // 2
    partner = me + 1 - 2 * k
    mate = me + 2 - 4 * hi
    s_partner = s + 1 - 2 * k
    s_mate = s + 2 - 4 * hi
    s_across = 3 - s
    rows = dx_ref.shape[1] // CHUNKS

    barrier = pltpu.get_barrier_semaphore()

    def greet(r, carry):
        pl.semaphore_signal(
            barrier, inc=1, device_id=(lax.rem(me + r, n_dev),), device_id_type=MESH
        )
        return carry

    lax.fori_loop(1, n_dev, greet, 0)
    pl.semaphore_wait(barrier, n_dev - 1)

    def part(c):
        return pl.ds(c * rows, rows)

    def to_relay(c):
        return remote(
            dx_ref.at[s_across, part(c)], relay.at[part(c)], relay_send.at[c], relay_recv.at[c], partner
        )

    def to_near(c):
        return remote(
            dx_ref.at[s_partner, part(c)], near_out.at[part(c)], near_send.at[c], near_recv.at[c], partner
        )

    def to_far(c):
        return remote(total.at[part(c)], far_out.at[part(c)], far_send.at[c], far_recv.at[c], mate)

    def w_copy(r):
        target = lax.rem(me + r, n_dev)
        return remote(w_ref.at[target], w_out.at[me], w_send.at[r], w_recv.at[r], target)

    def vec_copy(r):
        target = lax.rem(me + r, n_dev)
        return remote(vec_ref.at[target], vec_out.at[me], vec_send.at[r], vec_recv.at[r], target)

    for c in range(CHUNKS):
        to_relay(c).start()

    def start(r, carry):
        w_copy(r).start()
        vec_copy(r).start()
        return carry

    lax.fori_loop(1, n_dev, start, 0)
    keep_w = pltpu.make_async_copy(w_ref.at[me], w_out.at[me], keep_sem.at[0])
    keep_vec = pltpu.make_async_copy(vec_ref.at[me], vec_out.at[me], keep_sem.at[1])
    keep_w.start()
    keep_vec.start()
    for c in range(CHUNKS):
        to_relay(c).wait_recv()
        mine = dx_ref[s_mate, c * rows : (c + 1) * rows, :].astype(f32)
        other = relay[c * rows : (c + 1) * rows, :].astype(f32)
        total[c * rows : (c + 1) * rows, :] = (mine + other).astype(bf16)
        if c > 0:
            to_far(c - 1).start()
    for c in range(CHUNKS):
        to_near(c).start()
    to_far(CHUNKS - 1).start()
    for c in range(CHUNKS):
        to_relay(c).wait_send()
        to_near(c).wait()
        to_far(c).wait()

    def finish(r, carry):
        w_copy(r).wait()
        vec_copy(r).wait()
        return carry

    lax.fori_loop(1, n_dev, finish, 0)
    keep_w.wait()
    keep_vec.wait()


def settle(n_dev, dx, w, vec):
    vmem = pl.BlockSpec(memory_space=pltpu.VMEM)
    anywhere = pl.BlockSpec(memory_space=pl.ANY)
    dma = lambda n: pltpu.SemaphoreType.DMA((n,))
    block = dx.shape[1:]
    return pl.pallas_call(
        functools.partial(settle_kernel, n_dev),
        in_specs=[vmem] * 3,
        out_specs=[anywhere] * 4,
        out_shape=[
            jax.ShapeDtypeStruct(block, dx.dtype),
            jax.ShapeDtypeStruct(block, dx.dtype),
            jax.ShapeDtypeStruct(w.shape, w.dtype),
            jax.ShapeDtypeStruct(vec.shape, vec.dtype),
        ],
        scratch_shapes=[
            pltpu.VMEM(block, dx.dtype), pltpu.VMEM(block, dx.dtype),
            dma(n_dev), dma(n_dev), dma(n_dev), dma(n_dev),
            dma(CHUNKS), dma(CHUNKS), dma(CHUNKS), dma(CHUNKS), dma(CHUNKS), dma(CHUNKS), dma(2),
        ],
        compiler_params=pltpu.CompilerParams(collective_id=1, has_side_effects=True),
        name="settle",
    )(dx, w, vec)


def body(
    n_dev,
    tokens,
    segment_ids,
    pad_mask,
    w_qkv,
    bias_query,
    bias_value,
    w_out,
    bias_out,
    gain_one,
    shift_one,
    w_up,
    bias_up,
    w_down,
    bias_down,
    gain_two,
    shift_two,
    cotangent,
):
    row_count = tokens.shape[0]
    rows_w = w_qkv.shape[0]
    own = GROUP * row_count
    window = own + 2 * LEN_MAX
    me = lax.axis_index("fsdp")
    place = me % GROUP
    group_id = me // GROUP
    n_group = n_dev // GROUP
    up = [(i, i + GROUP) for i in range(n_dev - GROUP)]
    down = [(i + GROUP, i) for i in range(n_dev - GROUP)]
    groups = [[GROUP * g + j for j in range(GROUP)] for g in range(n_group)]

    wq = w_qkv[:, :D].reshape(rows_w, GROUP, Q_ROWS)
    wk = w_qkv[:, D : 2 * D].reshape(rows_w, GROUP, OWN_HEADS, 1, HEAD_DIM)
    wv = w_qkv[:, 2 * D :].reshape(rows_w, GROUP, OWN_HEADS, 1, HEAD_DIM)
    wkv = jnp.concatenate([wk, wv], axis=3).reshape(rows_w, GROUP, KV_ROWS)
    small = jnp.concatenate(
        [bias_query, bias_value, bias_out, gain_one, shift_one, bias_down, gain_two, shift_two, bias_up]
    )
    n_small = small.shape[0]
    gap = KV_AT - Q_ROWS
    small_cols = jnp.pad(small.reshape(rows_w, -1), ((0, 0), (0, gap - n_small // rows_w)))
    small_cols = jnp.broadcast_to(small_cols[:, None], (rows_w, GROUP, gap))
    w_send = jnp.concatenate([wq, small_cols, wkv], axis=2).transpose(1, 0, 2)
    ff = w_up.shape[1]
    wo_full = lax.all_gather(w_out, "fsdp", axis=0, tiled=True)
    wu_full = lax.all_gather(w_up, "fsdp", axis=0, tiled=True)
    wd_full = lax.all_gather(w_down, "fsdp", axis=0, tiled=True)

    code = (segment_ids * 2 + pad_mask).reshape(8, row_count // 8)
    x_win, code_win, w_got = share(n_dev, tokens, code, w_send)
    x_win = x_win.reshape(window, D)
    x_own = x_win[LEN_MAX : LEN_MAX + own]
    code_win = code_win.reshape(window)
    at = jnp.arange(window)
    code_win = jnp.where((group_id == 0) & (at < LEN_MAX), -2, code_win)
    code_win = jnp.where(
        (group_id == n_group - 1) & (at >= LEN_MAX + own), 2 * n_dev * row_count, code_win
    )
    code_own = code_win[LEN_MAX : LEN_MAX + own]
    w_mix = w_got.reshape(D, W_LANES)
    small_all = w_got[:, :, Q_ROWS : Q_ROWS + n_small // rows_w].reshape(n_dev, n_small)
    rows8 = small_all[:, : 8 * rows_w].reshape(n_dev, 8, rows_w).transpose(1, 0, 2).reshape(8, D)
    rows8 = rows8.astype(f32)
    bu_full = small_all[:, 8 * rows_w :].reshape(-1).astype(f32)
    bq_full, bv_full, bo_full, g1_full, s1_full, bd_full, g2_full, s2_full = [
        rows8[j] for j in range(8)
    ]
    seg_win = code_win >> 1
    ktag = jnp.where((code_win & 1) == 1, seg_win + 1, 0).reshape(window, 1)
    seg_own = code_own >> 1
    qtag = (seg_own + 1).reshape(1, own)
    first_seg = seg_own[::BQ]
    last_seg = seg_own[BQ - 1 :: BQ]
    low = jnp.sum((seg_win[None, :] < first_seg[:, None]).astype(jnp.int32), axis=1)
    high = jnp.sum((seg_win[None, :] <= last_seg[:, None]).astype(jnp.int32), axis=1)
    spans = [jnp.stack([low // b, (high + b - 1) // b], axis=1) for b in (FK, BK)]

    bq = lax.dynamic_slice(bq_full, (place * Q_ROWS,), (Q_ROWS,))
    bv = lax.dynamic_slice(bv_full, (place * Q_ROWS,), (Q_ROWS,)).reshape(OWN_HEADS, 1, HEAD_DIM)
    bkv = jnp.concatenate([jnp.zeros_like(bv), bv], axis=1).reshape(KV_ROWS)
    w_q, w_kv = w_mix[:, :Q_ROWS], w_mix[:, KV_AT:]
    w_mix = jnp.concatenate([w_q, w_kv], axis=1)
    qt = jnp.einsum("dc,td->ct", w_q, x_own, preferred_element_type=f32) + bq[:, None]
    qt = qt.astype(bf16) * jnp.asarray(score_scale, bf16)
    kv = (jnp.dot(x_win, w_kv, preferred_element_type=f32) + bkv).astype(bf16)
    kvt = jnp.einsum("dc,td->ct", w_kv, x_win, preferred_element_type=f32) + bkv[:, None]
    kvt = kvt.astype(bf16)

    ot, lse = attend(spans[0], qtag, ktag, qt, kv, kvt)
    ctx_t = lax.all_to_all(
        ot.reshape(Q_ROWS, GROUP, row_count), "fsdp", 1, 0, axis_index_groups=groups, tiled=True
    ).reshape(D, row_count)

    tokens_f = tokens.astype(f32)
    branch = jnp.einsum("ir,io->ro", ctx_t, wo_full, preferred_element_type=f32) + bo_full
    first, norm_one_back = jax.vjp(norm_rows, tokens_f + branch, g1_full, s1_full)
    up_in = first.astype(bf16)
    pre_act = jnp.dot(up_in, wu_full, preferred_element_type=f32) + bu_full
    gelu_val, gelu_back = jax.vjp(gelu_exact, pre_act)
    hidden = gelu_val.astype(bf16)
    ffn = jnp.dot(hidden, wd_full, preferred_element_type=f32) + bd_full
    result, norm_two_back = jax.vjp(norm_rows, first + ffn, g2_full, s2_full)
    layer_out = result.astype(bf16)
    d_second, d_gain_two, d_shift_two = norm_two_back(cotangent.astype(f32))
    d_ffn = d_second.astype(bf16)
    d_bias_down = jnp.sum(d_ffn.astype(f32), axis=0)
    d_w_down = jnp.einsum("rf,rd->fd", hidden, d_ffn, preferred_element_type=f32)
    d_hidden = jnp.einsum("rd,fd->rf", d_ffn, wd_full, preferred_element_type=f32)
    d_pre = gelu_back(d_hidden)[0].astype(bf16)
    d_bias_up = jnp.sum(d_pre.astype(f32), axis=0)
    d_w_up = jnp.einsum("rd,rf->df", up_in, d_pre, preferred_element_type=f32)
    d_first = d_second + jnp.einsum("rf,df->rd", d_pre, wu_full, preferred_element_type=f32)
    d_mid, d_gain_one, d_shift_one = norm_one_back(d_first)
    d_branch = d_mid.astype(bf16)
    d_bias_out = jnp.sum(d_branch.astype(f32), axis=0)
    d_w_out = jnp.einsum("ir,ro->io", ctx_t, d_branch, preferred_element_type=f32)
    dctx_t = jnp.einsum("ro,io->ir", d_branch, wo_full, preferred_element_type=f32).astype(bf16)
    n_up = ff // D
    big_grad = jnp.concatenate(
        [
            d_w_down.astype(bf16).reshape(n_dev, -1, D),
            d_w_out.astype(bf16).reshape(n_dev, rows_w, D),
        ]
        + [d_w_up[:, D * j : D * (j + 1)].astype(bf16).reshape(n_dev, rows_w, D) for j in range(n_up)],
        axis=1,
    )
    big_owned = lax.psum_scatter(big_grad, "fsdp", scatter_dimension=0).astype(f32)
    rows_d = w_down.shape[0]
    g_down, g_out = big_owned[:rows_d], big_owned[rows_d : rows_d + rows_w]
    g_up = jnp.concatenate(
        [big_owned[rows_d + rows_w * (j + 1) : rows_d + rows_w * (j + 2)] for j in range(n_up)], axis=1
    )

    d_out = lax.all_to_all(
        dctx_t.reshape(GROUP, Q_ROWS, row_count), "fsdp", 0, 2, axis_index_groups=groups, tiled=True
    ).reshape(Q_ROWS, own)
    edge, inside = LEN_MAX // BK, own // BK
    far_parts = ((0, edge), (edge + inside, 2 * edge + inside))
    own_parts = ((edge, edge + inside),)
    dq_far, dkv_left, dkv_right = attend_grad(
        far_parts, False, spans[1], qtag, ktag, qt, d_out, ot, lse, kv, kvt
    )
    from_right = lax.ppermute(dkv_left, "fsdp", down)
    from_left = lax.ppermute(dkv_right, "fsdp", up)
    dq_t, dkv_own = attend_grad(
        own_parts, True, spans[1], qtag, ktag, qt, d_out, ot, lse, kv, kvt, dq_far
    )
    dkv = jnp.concatenate(
        [
            dkv_own[:, :LEN_MAX] + from_left.astype(f32),
            dkv_own[:, LEN_MAX : own - LEN_MAX],
            dkv_own[:, own - LEN_MAX :] + from_right.astype(f32),
        ],
        axis=1,
    ).astype(bf16)
    dmix_t = jnp.concatenate([dq_t, dkv], axis=0)
    dmix_sum = jnp.sum(dmix_t.astype(f32), axis=1)
    d_w_rows = lax.optimization_barrier(jnp.dot(dmix_t, x_own, preferred_element_type=f32).astype(bf16))
    d_x = jnp.einsum("ct,dc->td", dmix_t, w_mix, preferred_element_type=f32).astype(bf16)
    d_x = d_x.reshape(GROUP, row_count, D)

    pad_vec = lambda v: lax.dynamic_update_slice(jnp.zeros((D,), f32), v, (place * Q_ROWS,))
    d_bq = pad_vec(dmix_sum[:Q_ROWS])
    d_bv = pad_vec(dmix_sum[Q_ROWS:].reshape(OWN_HEADS, 2, HEAD_DIM)[:, 1].reshape(Q_ROWS))
    vecs = jnp.stack(
        [d_bq, d_bv, d_bias_out, d_gain_one, d_shift_one, d_bias_down, d_gain_two, d_shift_two]
    )
    vec_send = jnp.concatenate(
        [
            vecs.reshape(8, n_dev, rows_w).transpose(1, 0, 2).reshape(n_dev, 8 * rows_w),
            d_bias_up.reshape(n_dev, 4 * rows_w),
        ],
        axis=1,
    )
    vec_send = jnp.pad(vec_send, ((0, 0), (0, 1024 - vec_send.shape[1]))).reshape(n_dev, 8, 128)
    near, far, w_got, vec_got = settle(
        n_dev, d_x, d_w_rows.T.reshape(n_dev, rows_w, MIX_ROWS), vec_send
    )
    own_x = lax.dynamic_index_in_dim(d_x, place, 0, keepdims=False)
    grad_tokens = d_mid + ((own_x.astype(f32) + near.astype(f32)) + far.astype(f32))
    got = jnp.sum(w_got.astype(f32).reshape(n_group, GROUP, rows_w, MIX_ROWS), axis=0)
    got = got.transpose(1, 0, 2)
    g_q = got[:, :, :Q_ROWS].reshape(rows_w, D)
    g_kv = got[:, :, Q_ROWS:].reshape(rows_w, GROUP, OWN_HEADS, 2, HEAD_DIM)
    g_k = g_kv[:, :, :, 0].reshape(rows_w, D)
    g_v = g_kv[:, :, :, 1].reshape(rows_w, D)
    grad_w_qkv = jnp.concatenate([g_q, g_k, g_v], axis=1)
    vec = jnp.sum(vec_got, axis=0).reshape(-1)[: 12 * rows_w]
    own_vec = [vec[j * rows_w : (j + 1) * rows_w] for j in range(8)]
    return (
        layer_out,
        grad_tokens,
        grad_w_qkv,
        own_vec[0],
        own_vec[1],
        g_out,
        own_vec[2],
        own_vec[3],
        own_vec[4],
        g_up,
        vec[8 * rows_w :],
        g_down,
        own_vec[5],
        own_vec[6],
        own_vec[7],
    )


def solution(mesh):
    rows, flat = P("fsdp", None), P("fsdp")
    return jax.shard_map(
        functools.partial(body, mesh.shape["fsdp"]),
        mesh=mesh,
        in_specs=(
            rows, flat, flat, rows, flat, flat, rows, flat, flat, flat, rows, flat, rows, flat,
            flat, flat, rows,
        ),
        out_specs=(
            rows, rows, rows, flat, flat, rows, flat, flat, flat, rows, flat, rows, flat, flat,
            flat,
        ),
        check_vma=False,
    )
```

```python
import functools

import jax
import jax.numpy as jnp
from jax import lax
from jax.experimental import pallas as pl
from jax.experimental.pallas import tpu as pltpu
from jax.sharding import PartitionSpec as P

D = 768
HEADS = 12
HEAD_DIM = 64
LEN_MAX = 2048
GROUP = 4
OWN_HEADS = HEADS // GROUP
Q_ROWS = OWN_HEADS * HEAD_DIM
KV_ROWS = 2 * Q_ROWS
MIX_ROWS = Q_ROWS + KV_ROWS
BQ = 512
FK = 512
BK = 256
NEG = -1e30

bf16 = jnp.bfloat16
f32 = jnp.float32
eps_norm = 1e-12
score_scale = 0.125

NN = (((1,), (0,)), ((), ()))
NT = (((1,), (1,)), ((), ()))


def mm(a, b, dims=NN):
    return lax.dot_general(a, b, dims, preferred_element_type=f32)


def norm_rows(hidden, gain_row, shift_row):
    centre = hidden - jnp.mean(hidden, axis=-1, keepdims=True)
    spread = jnp.mean(centre * centre, axis=-1, keepdims=True)
    return centre * lax.rsqrt(spread + eps_norm) * gain_row + shift_row


def gelu_exact(pre_act):
    return 0.5 * pre_act * (1.0 + jax.scipy.special.erf(pre_act * 0.7071067811865476))


def head_rows(block, h, upper):
    zero = jnp.zeros_like(block[:HEAD_DIM])
    rows = block[h * HEAD_DIM : (h + 1) * HEAD_DIM]
    return jnp.concatenate([zero, rows] if upper else [rows, zero], axis=0)


def attend_kernel(
    span, qtag_ref, ktag_ref, qt_ref, kv_ref, kvt_ref, ot_ref, lse_ref, m_sc, l_sc, acc_sc
):
    i = pl.program_id(0)
    m_sc[...] = jnp.full_like(m_sc, NEG)
    l_sc[...] = jnp.zeros_like(l_sc)
    acc_sc[...] = jnp.zeros_like(acc_sc)
    qtag = qtag_ref[...]
    qt = qt_ref[...]
    q_pad = [head_rows(qt, h, False) for h in range(OWN_HEADS)]

    def step(kb, carry):
        rows = pl.ds(pl.multiple_of(kb * FK, FK), FK)
        seen = ktag_ref[rows, :] == qtag
        hs = range(OWN_HEADS)
        s = [mm(kv_ref[rows, 128 * h : 128 * (h + 1)], q_pad[h]) for h in hs]
        s = [jnp.where(seen, v, NEG) for v in s]
        m_old = [m_sc[h : h + 1, :] for h in hs]
        l_old = [l_sc[h : h + 1, :] for h in hs]
        m_new = [jnp.maximum(m_old[h], jnp.max(s[h], axis=0, keepdims=True)) for h in hs]
        p = [jnp.exp(s[h] - m_new[h]).astype(bf16) for h in hs]
        fade = [jnp.exp(m_old[h] - m_new[h]) for h in hs]
        one = jnp.ones((16, FK), bf16)
        v_one = [
            jnp.concatenate([kvt_ref[128 * h + HEAD_DIM : 128 * (h + 1), rows], one], axis=0)
            for h in hs
        ]
        out = [mm(v_one[h], p[h]) for h in hs]
        for h in hs:
            own = slice(HEAD_DIM * h, HEAD_DIM * (h + 1))
            acc_sc[own, :] = acc_sc[own, :] * fade[h] + out[h][:HEAD_DIM]
            l_sc[h : h + 1, :] = fade[h] * l_old[h] + out[h][HEAD_DIM : HEAD_DIM + 1]
            m_sc[h : h + 1, :] = m_new[h]
        return carry

    lax.fori_loop(span[i, 0], span[i, 1], step, 0)
    for h in range(OWN_HEADS):
        own = slice(HEAD_DIM * h, HEAD_DIM * (h + 1))
        total = l_sc[h : h + 1, :]
        ot_ref[own, :] = (acc_sc[own, :] / total).astype(bf16)
        lse_ref[h : h + 1, :] = m_sc[h : h + 1, :] + jnp.log(total)
    lse_ref[OWN_HEADS:, :] = jnp.zeros_like(lse_ref[OWN_HEADS:, :])


def attend(span, qtag, ktag, qt, kv, kvt):
    own = qt.shape[1]
    window = kv.shape[0]
    whole = lambda shape: pl.BlockSpec(shape, lambda i, s: (0, 0), pipeline_mode=pl.Buffered(1))
    cols = lambda rows: pl.BlockSpec((rows, BQ), lambda i, s: (0, i))
    return pl.pallas_call(
        attend_kernel,
        grid_spec=pltpu.PrefetchScalarGridSpec(
            num_scalar_prefetch=1,
            grid=(own // BQ,),
            in_specs=[
                cols(1),
                whole((window, 1)),
                cols(Q_ROWS),
                whole((window, KV_ROWS)),
                whole((KV_ROWS, window)),
            ],
            out_specs=[cols(Q_ROWS), cols(8)],
            scratch_shapes=[
                pltpu.VMEM((8, BQ), f32),
                pltpu.VMEM((8, BQ), f32),
                pltpu.VMEM((Q_ROWS, BQ), f32),
            ],
        ),
        out_shape=[
            jax.ShapeDtypeStruct((Q_ROWS, own), bf16),
            jax.ShapeDtypeStruct((8, own), f32),
        ],
        compiler_params=pltpu.CompilerParams(vmem_limit_bytes=60 << 20),
        cost_estimate=pl.CostEstimate(
            flops=4 * own * 2048 * Q_ROWS, bytes_accessed=20 << 20, transcendentals=own * 6144
        ),
        name="attend",
    )(span, qtag, ktag, qt, kv, kvt)


def grad_kernel(
    parts, final, span, qtag_ref, ktag_ref, qt_ref, dot_ref, ot_ref, lse_ref, kv_ref, kvt_ref, *rest
):
    if final:
        dq_in, dq_ref, *rest = rest
    else:
        dq_in, (dq_ref, *rest) = None, rest
    outs, (dq_sc, dkv_sc) = rest[: len(parts)], rest[len(parts) :]
    i = pl.program_id(0)

    @pl.when(i == 0)
    def _():
        dkv_sc[...] = jnp.zeros_like(dkv_sc)

    if final:
        dq_sc[...] = dq_in[...]
    else:
        dq_sc[...] = jnp.zeros_like(dq_sc)
    qtag = qtag_ref[...]
    qt, d_out, out = qt_ref[...], dot_ref[...], ot_ref[...]
    q_pad = [head_rows(qt, h, False) for h in range(OWN_HEADS)]
    d_pad = [head_rows(d_out, h, True) for h in range(OWN_HEADS)]
    product = d_out.astype(f32) * out.astype(f32)
    inner = [
        jnp.sum(product[HEAD_DIM * h : HEAD_DIM * (h + 1)], axis=0, keepdims=True)
        for h in range(OWN_HEADS)
    ]
    log_row = [lse_ref[h : h + 1, :] for h in range(OWN_HEADS)]

    def step(shift, kb, carry):
        rows = pl.ds(pl.multiple_of(kb * BK, BK), BK)
        place = pl.ds(pl.multiple_of((kb - shift) * BK, BK), BK)
        seen = ktag_ref[rows, :] == qtag
        hs = range(OWN_HEADS)
        kv = [kv_ref[rows, 128 * h : 128 * (h + 1)] for h in hs]
        s = [mm(kv[h], q_pad[h]) for h in hs]
        d_p = [mm(kv[h], d_pad[h]) for h in hs]
        p = [jnp.where(seen, jnp.exp(s[h] - log_row[h]), 0.0) for h in hs]
        d_s = [(p[h] * (d_p[h] - inner[h])).astype(bf16) for h in hs]
        p = [v.astype(bf16) for v in p]
        g_kv = [mm(q_pad[h], d_s[h], NT) + mm(d_pad[h], p[h], NT) for h in hs]
        g_q = [mm(kvt_ref[128 * h : 128 * h + HEAD_DIM, rows], d_s[h]) for h in hs]
        for h in hs:
            dkv_sc[128 * h : 128 * (h + 1), place] += g_kv[h]
            own = slice(HEAD_DIM * h, HEAD_DIM * (h + 1))
            dq_sc[own, :] += g_q[h]
        return carry

    base = 0
    for n, (first, last) in enumerate(parts):
        low = jnp.maximum(span[i, 0], first)
        high = jnp.minimum(span[i, 1], last)
        lax.fori_loop(low, high, functools.partial(step, first - base), 0)
        base += last - first
    if final:
        dq_ref[...] = (dq_sc[...] * score_scale).astype(bf16)
    else:
        dq_ref[...] = dq_sc[...]

    @pl.when(i == pl.num_programs(0) - 1)
    def _():
        base = 0
        for (first, last), ref in zip(parts, outs):
            width = (last - first) * BK
            ref[...] = dkv_sc[:, base : base + width].astype(ref.dtype)
            base += width


def attend_grad(parts, final, span, qtag, ktag, qt, d_out, out, lse, kv, kvt, dq_in=None):
    own = qt.shape[1]
    window = kv.shape[0]
    whole = lambda shape: pl.BlockSpec(shape, lambda i, s: (0, 0), pipeline_mode=pl.Buffered(1))
    cols = lambda rows: pl.BlockSpec((rows, BQ), lambda i, s: (0, i))
    widths = [(last - first) * BK for first, last in parts]
    dtype = f32 if final else bf16
    args = [span, qtag, ktag, qt, d_out, out, lse, kv, kvt] + ([dq_in] if final else [])
    return pl.pallas_call(
        functools.partial(grad_kernel, parts, final),
        grid_spec=pltpu.PrefetchScalarGridSpec(
            num_scalar_prefetch=1,
            grid=(own // BQ,),
            in_specs=[
                cols(1),
                whole((window, 1)),
                cols(Q_ROWS),
                cols(Q_ROWS),
                cols(Q_ROWS),
                cols(8),
                whole((window, KV_ROWS)),
                whole((KV_ROWS, window)),
            ]
            + ([cols(Q_ROWS)] if final else []),
            out_specs=[cols(Q_ROWS)] + [whole((KV_ROWS, w)) for w in widths],
            scratch_shapes=[
                pltpu.VMEM((Q_ROWS, BQ), f32),
                pltpu.VMEM((KV_ROWS, sum(widths)), f32),
            ],
        ),
        out_shape=[jax.ShapeDtypeStruct((Q_ROWS, own), bf16 if final else f32)]
        + [jax.ShapeDtypeStruct((KV_ROWS, w), dtype) for w in widths],
        compiler_params=pltpu.CompilerParams(vmem_limit_bytes=60 << 20),
        cost_estimate=pl.CostEstimate(
            flops=(10 if final else 2) * own * 1536 * Q_ROWS,
            bytes_accessed=20 << 20,
            transcendentals=own * 4096,
        ),
        name="grad_own" if final else "grad_far",
    )(*args)


MESH = pl.DeviceIdType.MESH
CHUNKS = 8
W_LANES = 640
KV_AT = 256


def remote(src, dst, send, recv, target):
    return pltpu.make_async_remote_copy(
        src_ref=src,
        dst_ref=dst,
        send_sem=send,
        recv_sem=recv,
        device_id=(target,),
        device_id_type=MESH,
    )


def share_kernel(
    n_dev, rows_w, tok_ref, code_ref, w_ref, x_own, c_out, w_full, qt_out, kv_out, kvt_out,
    x_out, w_out, w_wide, w_turn, qt_sc, kv_sc, kvt_sc,
    w_send, w_recv, c_send, c_recv, part_send, part_recv, mate_send, mate_recv,
    up_send, up_recv, down_send, down_recv, cross_send, cross_recv,
    fwd_send, fwd_recv, keep_sem, x_sem, q_sem, kv_sem, kvt_sem,
):
    n_group = n_dev // GROUP
    me = lax.axis_index("fsdp")
    g = me // GROUP
    s = me % GROUP
    k = s % 2
    hi = s // 2
    partner = me + 1 - 2 * k
    mate = me + 2 - 4 * hi
    mate_block = 4 + k - 2 * hi
    has_up = g < n_group - 1
    has_down = g > 0
    rows = tok_ref.shape[0] // CHUNKS
    half = CHUNKS // 2

    barrier = pltpu.get_barrier_semaphore()

    def greet(r, carry):
        pl.semaphore_signal(
            barrier, inc=1, device_id=(lax.rem(me + r, n_dev),), device_id_type=MESH
        )
        return carry

    lax.fori_loop(1, n_dev, greet, 0)
    pl.semaphore_wait(barrier, n_dev - 1)

    def chunk(ref, c):
        return ref.at[pl.ds(pl.multiple_of(c * rows, rows), rows)]

    def spot(b, c):
        return x_out.at[b, pl.ds(pl.multiple_of(c * rows, rows), rows)]

    def to_partner(c):
        return remote(chunk(tok_ref, c), spot(2 + s, c), part_send.at[c], part_recv.at[c], partner)

    def to_mate(c):
        return remote(chunk(tok_ref, c), spot(2 + s, c), mate_send.at[c], mate_recv.at[c], mate)

    def up_own(c):
        return remote(chunk(tok_ref, c), spot(k, c), up_send.at[c], up_recv.at[c], me + GROUP)

    def up_mate(c):
        return remote(spot(mate_block, c), spot(k, c), up_send.at[c], up_recv.at[c], me + GROUP)

    def down_own(c):
        return remote(
            chunk(tok_ref, c), spot(6 + k, c), down_send.at[c], down_recv.at[c], me - GROUP
        )

    def down_mate(c):
        return remote(
            spot(mate_block, c + half), spot(6 + k, c + half), down_send.at[c], down_recv.at[c],
            me - GROUP,
        )

    def cross(c):
        at = c + half * hi
        return remote(spot(6 + k, at), spot(6 + k, at), cross_send.at[c], cross_recv.at[c], mate)

    def forward(b, c, slot):
        return remote(spot(b, c), spot(b, c), fwd_send.at[slot], fwd_recv.at[slot], partner)

    keep_x = pltpu.make_async_copy(tok_ref, x_out.at[2 + s], keep_sem.at[0])
    keep_c = pltpu.make_async_copy(code_ref, c_out.at[2 + s], keep_sem.at[1])
    keep_w = pltpu.make_async_copy(w_ref.at[s], w_out.at[me], keep_sem.at[2])
    keep_x.start()
    keep_c.start()
    keep_w.start()

    def w_copy(r):
        target = lax.rem(me + r, n_dev)
        return remote(
            w_ref.at[lax.rem(target, GROUP)], w_out.at[me], w_send.at[r], w_recv.at[r], target
        )

    def w_start(r, carry):
        w_copy(r).start()
        return carry

    def c_group(j):
        target = GROUP * g + lax.rem(s + j, GROUP)
        return remote(code_ref, c_out.at[2 + s], c_send.at[j], c_recv.at[2 + s], target)

    def c_far(j):
        step = GROUP * (2 * hi - 1)
        b = 6 + s - 8 * hi
        target = GROUP * g + step + j
        return remote(code_ref, c_out.at[b], c_send.at[GROUP + j], c_recv.at[b], target)

    sends_far = jnp.where(hi == 1, g < n_group - 1, g > 0)
    for j in range(1, GROUP):
        c_group(j).start()

    @pl.when(sends_far)
    def _():
        for j in range(GROUP):
            c_far(j).start()

    order = list(range(half, CHUNKS)) + list(range(half))
    lax.fori_loop(1, n_dev, w_start, 0)

    @pl.when((hi == 0) & has_down)
    def _():
        for c in range(half):
            down_own(c).start()

    for n, c in enumerate(order):
        to_mate(c).start()
        to_partner(c).start()
        if n < half:

            @pl.when((hi == 1) & has_up)
            def _():
                up_own(c).start()

    for n, c in enumerate(order):
        to_mate(c).wait_recv()
        forward(mate_block, c, c).start()

        @pl.when((hi == 0) & has_up)
        def _():
            up_mate(c).start()

        if n < half:

            @pl.when((hi == 1) & has_down)
            def _():
                down_mate(c - half).start()

        else:

            @pl.when((hi == 1) & has_up)
            def _():
                up_own(c).start()

    def w_wait(r, carry):
        w_copy(r).wait_recv()
        return carry

    lax.fori_loop(1, n_dev, w_wait, 0)
    keep_w.wait()
    keep_x.wait()
    bias_row = jnp.zeros((8, W_LANES), f32)
    bias_at = w_ref.shape[1] - 8
    for j in range(n_dev):
        w_wide[rows_w * j : rows_w * (j + 1), :] = w_out[j, :rows_w, :].astype(f32)
        bias_row = bias_row + w_out[j, bias_at:, :].astype(f32)
    bias_row = jnp.sum(bias_row, axis=0, keepdims=True)
    bias_col = jnp.broadcast_to(bias_row, (128, W_LANES)).T[:, :1]
    w_full[...] = w_wide[...].astype(bf16)
    w_turn[...] = w_wide[...].T.astype(bf16)
    piece = 512
    pieces = tok_ref.shape[0] // piece

    def project(b, inside):
        def one(j, carry):
            x = x_out[b, pl.ds(pl.multiple_of(j * piece, piece), piece), :]
            at = pl.ds(pl.multiple_of((b * pieces + j) * piece, piece), piece)
            kv = mm(x, w_full[:, KV_AT:]) + bias_row[:, KV_AT:]
            kv_sc[at, :] = kv.astype(bf16)
            kvt_sc[:, at] = (mm(w_turn[KV_AT:, :], x, NT) + bias_col[KV_AT:]).astype(bf16)
            if inside:
                to = pl.ds(pl.multiple_of(((b - 2) * pieces + j) * piece, piece), piece)
                q = (mm(w_turn[:Q_ROWS, :], x, NT) + bias_col[:Q_ROWS]).astype(bf16)
                qt_sc[:, to] = q * jnp.asarray(score_scale, bf16)
            return carry

        lax.fori_loop(0, pieces, one, 0)

    def outs(b, inside):
        whole = tok_ref.shape[0]
        at = pl.ds(pl.multiple_of(b * whole, whole), whole)
        copies = [
            pltpu.make_async_copy(kv_sc.at[at], kv_out.at[at], kv_sem.at[b]),
            pltpu.make_async_copy(kvt_sc.at[:, at], kvt_out.at[:, at], kvt_sem.at[b]),
        ]
        if inside:
            to = pl.ds(pl.multiple_of((b - 2) * whole, whole), whole)
            copies.append(pltpu.make_async_copy(qt_sc.at[:, to], qt_out.at[:, to], q_sem.at[b - 2]))
            copies.append(pltpu.make_async_copy(x_out.at[b], x_own.at[b - 2], x_sem.at[b - 2]))
        return copies

    def put(b, inside):
        for copy in outs(b, inside):
            copy.start()

    own_block = 2 + s
    near_block = own_block + 1 - 2 * k
    across_block = mate_block + 1 - 2 * k
    project(own_block, True)

    @pl.when(has_up)
    def _():
        for c in range(half):
            down_own(c).wait_recv()
            cross(c).start()
            forward(6 + k, c + half * hi, 2 * CHUNKS + c).start()

    project(mate_block, True)
    put(own_block, True)

    @pl.when(has_down)
    def _():
        for c in order:
            up_own(c).wait_recv()
            forward(k, c, CHUNKS + c).start()

    for c in range(CHUNKS):
        to_partner(c).wait_recv()
    project(near_block, True)
    put(mate_block, True)

    @pl.when(has_up)
    def _():
        for c in range(half):
            cross(c).wait_recv()
            forward(6 + k, c + half * (1 - hi), 2 * CHUNKS + half + c).start()

    for c in range(CHUNKS):
        forward(mate_block, c, c).wait_recv()
    project(across_block, True)
    put(near_block, True)

    @pl.when(has_down)
    def _():
        project(k, False)
        for c in range(CHUNKS):
            forward(k, c, CHUNKS + c).wait_recv()
        project(1 - k, False)
        put(k, False)

    put(across_block, True)

    @pl.when(has_up)
    def _():
        project(6 + k, False)
        for c in range(half):
            forward(6 + k, c, 2 * CHUNKS + c).wait_recv()
            forward(6 + k, c, 2 * CHUNKS + half + c).wait_recv()
        project(7 - k, False)
        put(6 + k, False)

    for c in range(CHUNKS):
        to_partner(c).wait_send()
        to_mate(c).wait_send()
        forward(mate_block, c, c).wait_send()

    @pl.when(has_down)
    def _():
        put(1 - k, False)
        for c in range(CHUNKS):
            forward(k, c, CHUNKS + c).wait_send()
        for c in range(half):
            down_own(c).wait_send()

    @pl.when(has_up)
    def _():
        for c in range(half):
            cross(c).wait_send()
            forward(6 + k, c, 2 * CHUNKS + c).wait_send()
            forward(6 + k, c, 2 * CHUNKS + half + c).wait_send()
        for c in range(CHUNKS):
            up_own(c).wait_send()
        put(7 - k, False)

    for j in range(1, GROUP):
        c_group(j).wait_send()
        remote(
            code_ref, c_out.at[0], c_send.at[j], c_recv.at[2 + lax.rem(s + j, GROUP)], partner
        ).wait_recv()

    @pl.when(sends_far)
    def _():
        for j in range(GROUP):
            c_far(j).wait_send()

    @pl.when(has_down)
    def _():
        for b in range(2):
            remote(code_ref, c_out.at[b], c_send.at[0], c_recv.at[b], partner).wait_recv()

    @pl.when(has_up)
    def _():
        for b in range(6, 8):
            remote(code_ref, c_out.at[b], c_send.at[0], c_recv.at[b], partner).wait_recv()

    def w_sent(r, carry):
        w_copy(r).wait_send()
        return carry

    lax.fori_loop(1, n_dev, w_sent, 0)
    keep_c.wait()
    for b in range(2, 6):
        for copy in outs(b, True):
            copy.wait()

    @pl.when(has_down)
    def _():
        for b in range(2):
            for copy in outs(b, False):
                copy.wait()

    @pl.when(has_up)
    def _():
        for b in range(6, 8):
            for copy in outs(b, False):
                copy.wait()


def share(n_dev, rows_w, tokens, code, w_send):
    vmem = pl.BlockSpec(memory_space=pltpu.VMEM)
    anywhere = pl.BlockSpec(memory_space=pl.ANY)
    dma = lambda n: pltpu.SemaphoreType.DMA((n,))
    half = CHUNKS // 2
    rows, width = tokens.shape
    own, window = GROUP * rows, 8 * rows
    return pl.pallas_call(
        functools.partial(share_kernel, n_dev, rows_w),
        in_specs=[vmem] * 3,
        out_specs=[anywhere, anywhere, vmem, anywhere, anywhere, anywhere],
        out_shape=[
            jax.ShapeDtypeStruct((GROUP, rows, width), bf16),
            jax.ShapeDtypeStruct((8,) + code.shape, code.dtype),
            jax.ShapeDtypeStruct((width, W_LANES), bf16),
            jax.ShapeDtypeStruct((Q_ROWS, own), bf16),
            jax.ShapeDtypeStruct((window, KV_ROWS), bf16),
            jax.ShapeDtypeStruct((KV_ROWS, window), bf16),
        ],
        scratch_shapes=[
            pltpu.VMEM((8, rows, width), bf16),
            pltpu.VMEM((n_dev,) + w_send.shape[1:], bf16),
            pltpu.VMEM((width, W_LANES), f32),
            pltpu.VMEM((W_LANES, width), bf16),
            pltpu.VMEM((Q_ROWS, own), bf16),
            pltpu.VMEM((window, KV_ROWS), bf16),
            pltpu.VMEM((KV_ROWS, window), bf16),
            dma(n_dev), dma(n_dev), dma(2 * GROUP), dma(8),
            dma(CHUNKS), dma(CHUNKS), dma(CHUNKS), dma(CHUNKS),
            dma(CHUNKS), dma(CHUNKS), dma(half), dma(half), dma(half), dma(half),
            dma(3 * CHUNKS), dma(3 * CHUNKS), dma(3), dma(GROUP), dma(GROUP), dma(8), dma(8),
        ],
        compiler_params=pltpu.CompilerParams(
            collective_id=0, has_side_effects=True, vmem_limit_bytes=60 << 20
        ),
        name="share",
    )(tokens, code, w_send)


def settle_kernel(
    n_dev, dx_ref, w_ref, vec_ref, near_out, far_out, w_out, vec_out,
    relay, total,
    w_send, w_recv, vec_send, vec_recv, near_send, near_recv, relay_send, relay_recv,
    far_send, far_recv, keep_sem,
):
    me = lax.axis_index("fsdp")
    s = me % GROUP
    k = s % 2
    hi = s // 2
    partner = me + 1 - 2 * k
    mate = me + 2 - 4 * hi
    s_partner = s + 1 - 2 * k
    s_mate = s + 2 - 4 * hi
    s_across = 3 - s
    rows = dx_ref.shape[1] // CHUNKS

    barrier = pltpu.get_barrier_semaphore()

    def greet(r, carry):
        pl.semaphore_signal(
            barrier, inc=1, device_id=(lax.rem(me + r, n_dev),), device_id_type=MESH
        )
        return carry

    lax.fori_loop(1, n_dev, greet, 0)
    pl.semaphore_wait(barrier, n_dev - 1)

    def part(c):
        return pl.ds(c * rows, rows)

    def to_relay(c):
        return remote(
            dx_ref.at[s_across, part(c)], relay.at[part(c)], relay_send.at[c], relay_recv.at[c], partner
        )

    def to_near(c):
        return remote(
            dx_ref.at[s_partner, part(c)], near_out.at[part(c)], near_send.at[c], near_recv.at[c], partner
        )

    def to_far(c):
        return remote(total.at[part(c)], far_out.at[part(c)], far_send.at[c], far_recv.at[c], mate)

    def w_copy(r):
        target = lax.rem(me + r, n_dev)
        return remote(w_ref.at[target], w_out.at[me], w_send.at[r], w_recv.at[r], target)

    def vec_copy(r):
        target = lax.rem(me + r, n_dev)
        return remote(vec_ref.at[target], vec_out.at[me], vec_send.at[r], vec_recv.at[r], target)

    for c in range(CHUNKS):
        to_relay(c).start()

    def start(r, carry):
        w_copy(r).start()
        vec_copy(r).start()
        return carry

    lax.fori_loop(1, n_dev, start, 0)
    keep_w = pltpu.make_async_copy(w_ref.at[me], w_out.at[me], keep_sem.at[0])
    keep_vec = pltpu.make_async_copy(vec_ref.at[me], vec_out.at[me], keep_sem.at[1])
    keep_w.start()
    keep_vec.start()
    for c in range(CHUNKS):
        to_relay(c).wait_recv()
        mine = dx_ref[s_mate, c * rows : (c + 1) * rows, :].astype(f32)
        other = relay[c * rows : (c + 1) * rows, :].astype(f32)
        total[c * rows : (c + 1) * rows, :] = (mine + other).astype(bf16)
        if c > 0:
            to_far(c - 1).start()
    for c in range(CHUNKS):
        to_near(c).start()
    to_far(CHUNKS - 1).start()
    for c in range(CHUNKS):
        to_relay(c).wait_send()
        to_near(c).wait()
        to_far(c).wait()

    def finish(r, carry):
        w_copy(r).wait()
        vec_copy(r).wait()
        return carry

    lax.fori_loop(1, n_dev, finish, 0)
    keep_w.wait()
    keep_vec.wait()


def settle(n_dev, dx, w, vec):
    vmem = pl.BlockSpec(memory_space=pltpu.VMEM)
    anywhere = pl.BlockSpec(memory_space=pl.ANY)
    dma = lambda n: pltpu.SemaphoreType.DMA((n,))
    block = dx.shape[1:]
    return pl.pallas_call(
        functools.partial(settle_kernel, n_dev),
        in_specs=[vmem] * 3,
        out_specs=[anywhere] * 4,
        out_shape=[
            jax.ShapeDtypeStruct(block, dx.dtype),
            jax.ShapeDtypeStruct(block, dx.dtype),
            jax.ShapeDtypeStruct(w.shape, w.dtype),
            jax.ShapeDtypeStruct(vec.shape, vec.dtype),
        ],
        scratch_shapes=[
            pltpu.VMEM(block, dx.dtype), pltpu.VMEM(block, dx.dtype),
            dma(n_dev), dma(n_dev), dma(n_dev), dma(n_dev),
            dma(CHUNKS), dma(CHUNKS), dma(CHUNKS), dma(CHUNKS), dma(CHUNKS), dma(CHUNKS), dma(2),
        ],
        compiler_params=pltpu.CompilerParams(collective_id=1, has_side_effects=True),
        name="settle",
    )(dx, w, vec)


def body(
    n_dev,
    tokens,
    segment_ids,
    pad_mask,
    w_qkv,
    bias_query,
    bias_value,
    w_out,
    bias_out,
    gain_one,
    shift_one,
    w_up,
    bias_up,
    w_down,
    bias_down,
    gain_two,
    shift_two,
    cotangent,
):
    row_count = tokens.shape[0]
    rows_w = w_qkv.shape[0]
    own = GROUP * row_count
    window = own + 2 * LEN_MAX
    me = lax.axis_index("fsdp")
    place = me % GROUP
    group_id = me // GROUP
    n_group = n_dev // GROUP
    up = [(i, i + GROUP) for i in range(n_dev - GROUP)]
    down = [(i + GROUP, i) for i in range(n_dev - GROUP)]
    groups = [[GROUP * g + j for j in range(GROUP)] for g in range(n_group)]

    wq = w_qkv[:, :D].reshape(rows_w, GROUP, Q_ROWS)
    wk = w_qkv[:, D : 2 * D].reshape(rows_w, GROUP, OWN_HEADS, 1, HEAD_DIM)
    wv = w_qkv[:, 2 * D :].reshape(rows_w, GROUP, OWN_HEADS, 1, HEAD_DIM)
    wkv = jnp.concatenate([wk, wv], axis=3).reshape(rows_w, GROUP, KV_ROWS)
    small = jnp.concatenate(
        [bias_query, bias_value, bias_out, gain_one, shift_one, bias_down, gain_two, shift_two, bias_up]
    )
    n_small = small.shape[0]
    gap = KV_AT - Q_ROWS
    small_cols = jnp.pad(small.reshape(rows_w, -1), ((0, 0), (0, gap - n_small // rows_w)))
    small_cols = jnp.broadcast_to(small_cols[:, None], (rows_w, GROUP, gap))
    w_cut = jnp.concatenate([wq, small_cols, wkv], axis=2).transpose(1, 0, 2)
    column = me * rows_w + jnp.arange(rows_w)
    feature = jnp.arange(D)
    spread = lambda bias: jnp.sum(
        jnp.where(feature[None] == column[:, None], bias.astype(f32)[:, None], 0.0), axis=0
    )
    bias_q = spread(bias_query).reshape(GROUP, Q_ROWS)
    bias_v = spread(bias_value).reshape(GROUP, OWN_HEADS, 1, HEAD_DIM)
    bias_kv = jnp.concatenate([jnp.zeros_like(bias_v), bias_v], axis=2).reshape(GROUP, KV_ROWS)
    bias_cut = jnp.concatenate([bias_q, jnp.zeros((GROUP, gap), f32), bias_kv], axis=1)
    fill = -rows_w % 8
    bias_cut = jnp.pad(bias_cut.astype(bf16)[:, None], ((0, 0), (fill, 7), (0, 0)))
    w_send = jnp.concatenate([w_cut, bias_cut], axis=1)
    ff = w_up.shape[1]
    wo_full = lax.all_gather(w_out, "fsdp", axis=0, tiled=True)
    wu_full = lax.all_gather(w_up, "fsdp", axis=0, tiled=True)
    wd_full = lax.all_gather(w_down, "fsdp", axis=0, tiled=True)

    code = (segment_ids * 2 + pad_mask).reshape(8, row_count // 8)
    x_own, code_win, w_got, qt, kv, kvt = share(n_dev, rows_w, tokens, code, w_send)
    x_own = x_own.reshape(own, D)
    code_win = code_win.reshape(window)
    at = jnp.arange(window)
    code_win = jnp.where((group_id == 0) & (at < LEN_MAX), -2, code_win)
    code_win = jnp.where(
        (group_id == n_group - 1) & (at >= LEN_MAX + own), 2 * n_dev * row_count, code_win
    )
    code_own = code_win[LEN_MAX : LEN_MAX + own]
    w_mix = jnp.concatenate([w_got[:, :Q_ROWS], w_got[:, KV_AT:]], axis=1)
    small_all = w_got.reshape(n_dev, rows_w, W_LANES)[:, :, Q_ROWS : Q_ROWS + n_small // rows_w].reshape(n_dev, n_small)
    rows8 = small_all[:, : 8 * rows_w].reshape(n_dev, 8, rows_w).transpose(1, 0, 2).reshape(8, D)
    rows8 = rows8.astype(f32)
    bu_full = small_all[:, 8 * rows_w :].reshape(-1).astype(f32)
    bo_full, g1_full, s1_full, bd_full, g2_full, s2_full = [rows8[j] for j in range(2, 8)]
    seg_win = code_win >> 1
    ktag = jnp.where((code_win & 1) == 1, seg_win + 1, 0).reshape(window, 1)
    seg_own = code_own >> 1
    qtag = (seg_own + 1).reshape(1, own)
    first_seg = seg_own[::BQ]
    last_seg = seg_own[BQ - 1 :: BQ]
    low = jnp.sum((seg_win[None, :] < first_seg[:, None]).astype(jnp.int32), axis=1)
    high = jnp.sum((seg_win[None, :] <= last_seg[:, None]).astype(jnp.int32), axis=1)
    spans = [jnp.stack([low // b, (high + b - 1) // b], axis=1) for b in (FK, BK)]

    ot, lse = attend(spans[0], qtag, ktag, qt, kv, kvt)
    ctx_t = lax.all_to_all(
        ot.reshape(Q_ROWS, GROUP, row_count), "fsdp", 1, 0, axis_index_groups=groups, tiled=True
    ).reshape(D, row_count)

    tokens_f = tokens.astype(f32)
    branch = jnp.einsum("ir,io->ro", ctx_t, wo_full, preferred_element_type=f32) + bo_full
    first, norm_one_back = jax.vjp(norm_rows, tokens_f + branch, g1_full, s1_full)
    up_in = first.astype(bf16)
    pre_act = jnp.dot(up_in, wu_full, preferred_element_type=f32) + bu_full
    gelu_val, gelu_back = jax.vjp(gelu_exact, pre_act)
    hidden = gelu_val.astype(bf16)
    ffn = jnp.dot(hidden, wd_full, preferred_element_type=f32) + bd_full
    result, norm_two_back = jax.vjp(norm_rows, first + ffn, g2_full, s2_full)
    layer_out = result.astype(bf16)
    d_second, d_gain_two, d_shift_two = norm_two_back(cotangent.astype(f32))
    d_ffn = d_second.astype(bf16)
    d_bias_down = jnp.sum(d_ffn.astype(f32), axis=0)
    d_w_down = jnp.einsum("rf,rd->fd", hidden, d_ffn, preferred_element_type=f32)
    d_hidden = jnp.einsum("rd,fd->rf", d_ffn, wd_full, preferred_element_type=f32)
    d_pre = gelu_back(d_hidden)[0].astype(bf16)
    d_bias_up = jnp.sum(d_pre.astype(f32), axis=0)
    d_w_up = jnp.einsum("rd,rf->df", up_in, d_pre, preferred_element_type=f32)
    d_first = d_second + jnp.einsum("rf,df->rd", d_pre, wu_full, preferred_element_type=f32)
    d_mid, d_gain_one, d_shift_one = norm_one_back(d_first)
    d_branch = d_mid.astype(bf16)
    d_bias_out = jnp.sum(d_branch.astype(f32), axis=0)
    d_w_out = jnp.einsum("ir,ro->io", ctx_t, d_branch, preferred_element_type=f32)
    dctx_t = jnp.einsum("ro,io->ir", d_branch, wo_full, preferred_element_type=f32).astype(bf16)
    n_up = ff // D
    big_grad = jnp.concatenate(
        [
            d_w_down.astype(bf16).reshape(n_dev, -1, D),
            d_w_out.astype(bf16).reshape(n_dev, rows_w, D),
        ]
        + [d_w_up[:, D * j : D * (j + 1)].astype(bf16).reshape(n_dev, rows_w, D) for j in range(n_up)],
        axis=1,
    )
    big_owned = lax.psum_scatter(big_grad, "fsdp", scatter_dimension=0).astype(f32)
    rows_d = w_down.shape[0]
    g_down, g_out = big_owned[:rows_d], big_owned[rows_d : rows_d + rows_w]
    g_up = jnp.concatenate(
        [big_owned[rows_d + rows_w * (j + 1) : rows_d + rows_w * (j + 2)] for j in range(n_up)], axis=1
    )

    d_out = lax.all_to_all(
        dctx_t.reshape(GROUP, Q_ROWS, row_count), "fsdp", 0, 2, axis_index_groups=groups, tiled=True
    ).reshape(Q_ROWS, own)
    edge, inside = LEN_MAX // BK, own // BK
    far_parts = ((0, edge), (edge + inside, 2 * edge + inside))
    own_parts = ((edge, edge + inside),)
    dq_far, dkv_left, dkv_right = attend_grad(
        far_parts, False, spans[1], qtag, ktag, qt, d_out, ot, lse, kv, kvt
    )
    from_right = lax.ppermute(dkv_left, "fsdp", down)
    from_left = lax.ppermute(dkv_right, "fsdp", up)
    dq_t, dkv_own = attend_grad(
        own_parts, True, spans[1], qtag, ktag, qt, d_out, ot, lse, kv, kvt, dq_far
    )
    dkv = jnp.concatenate(
        [
            dkv_own[:, :LEN_MAX] + from_left.astype(f32),
            dkv_own[:, LEN_MAX : own - LEN_MAX],
            dkv_own[:, own - LEN_MAX :] + from_right.astype(f32),
        ],
        axis=1,
    ).astype(bf16)
    dmix_t = jnp.concatenate([dq_t, dkv], axis=0)
    dmix_sum = jnp.sum(dmix_t.astype(f32), axis=1)
    d_w_rows = lax.optimization_barrier(jnp.dot(dmix_t, x_own, preferred_element_type=f32).astype(bf16))
    d_x = jnp.einsum("ct,dc->td", dmix_t, w_mix, preferred_element_type=f32).astype(bf16)
    d_x = d_x.reshape(GROUP, row_count, D)

    pad_vec = lambda v: lax.dynamic_update_slice(jnp.zeros((D,), f32), v, (place * Q_ROWS,))
    d_bq = pad_vec(dmix_sum[:Q_ROWS])
    d_bv = pad_vec(dmix_sum[Q_ROWS:].reshape(OWN_HEADS, 2, HEAD_DIM)[:, 1].reshape(Q_ROWS))
    vecs = jnp.stack(
        [d_bq, d_bv, d_bias_out, d_gain_one, d_shift_one, d_bias_down, d_gain_two, d_shift_two]
    )
    vec_send = jnp.concatenate(
        [
            vecs.reshape(8, n_dev, rows_w).transpose(1, 0, 2).reshape(n_dev, 8 * rows_w),
            d_bias_up.reshape(n_dev, 4 * rows_w),
        ],
        axis=1,
    )
    vec_send = jnp.pad(vec_send, ((0, 0), (0, 1024 - vec_send.shape[1]))).reshape(n_dev, 8, 128)
    near, far, w_got, vec_got = settle(
        n_dev, d_x, d_w_rows.T.reshape(n_dev, rows_w, MIX_ROWS), vec_send
    )
    own_x = lax.dynamic_index_in_dim(d_x, place, 0, keepdims=False)
    grad_tokens = d_mid + ((own_x.astype(f32) + near.astype(f32)) + far.astype(f32))
    got = jnp.sum(w_got.astype(f32).reshape(n_group, GROUP, rows_w, MIX_ROWS), axis=0)
    got = got.transpose(1, 0, 2)
    g_q = got[:, :, :Q_ROWS].reshape(rows_w, D)
    g_kv = got[:, :, Q_ROWS:].reshape(rows_w, GROUP, OWN_HEADS, 2, HEAD_DIM)
    g_k = g_kv[:, :, :, 0].reshape(rows_w, D)
    g_v = g_kv[:, :, :, 1].reshape(rows_w, D)
    grad_w_qkv = jnp.concatenate([g_q, g_k, g_v], axis=1)
    vec = jnp.sum(vec_got, axis=0).reshape(-1)[: 12 * rows_w]
    own_vec = [vec[j * rows_w : (j + 1) * rows_w] for j in range(8)]
    return (
        layer_out,
        grad_tokens,
        grad_w_qkv,
        own_vec[0],
        own_vec[1],
        g_out,
        own_vec[2],
        own_vec[3],
        own_vec[4],
        g_up,
        vec[8 * rows_w :],
        g_down,
        own_vec[5],
        own_vec[6],
        own_vec[7],
    )


def solution(mesh):
    rows, flat = P("fsdp", None), P("fsdp")
    return jax.shard_map(
        functools.partial(body, mesh.shape["fsdp"]),
        mesh=mesh,
        in_specs=(
            rows, flat, flat, rows, flat, flat, rows, flat, flat, flat, rows, flat, rows, flat,
            flat, flat, rows,
        ),
        out_specs=(
            rows, rows, rows, flat, flat, rows, flat, flat, flat, rows, flat, rows, flat, flat,
            flat,
        ),
        check_vma=False,
    )
```

```python
import functools

import jax
import jax.numpy as jnp
from jax import lax
from jax.experimental import pallas as pl
from jax.experimental.pallas import tpu as pltpu
from jax.sharding import PartitionSpec as P

D = 768
HEADS = 12
HEAD_DIM = 64
LEN_MAX = 2048
GROUP = 4
OWN_HEADS = HEADS // GROUP
Q_ROWS = OWN_HEADS * HEAD_DIM
KV_ROWS = 2 * Q_ROWS
MIX_ROWS = Q_ROWS + KV_ROWS
BQ = 512
FK = 512
BK = 256
NEG = -1e30

bf16 = jnp.bfloat16
f32 = jnp.float32
eps_norm = 1e-12
score_scale = 0.125

NN = (((1,), (0,)), ((), ()))
NT = (((1,), (1,)), ((), ()))


def mm(a, b, dims=NN):
    return lax.dot_general(a, b, dims, preferred_element_type=f32)


def norm_rows(hidden, gain_row, shift_row):
    centre = hidden - jnp.mean(hidden, axis=-1, keepdims=True)
    spread = jnp.mean(centre * centre, axis=-1, keepdims=True)
    return centre * lax.rsqrt(spread + eps_norm) * gain_row + shift_row


def gelu_exact(pre_act):
    return 0.5 * pre_act * (1.0 + jax.scipy.special.erf(pre_act * 0.7071067811865476))


def head_rows(block, h, upper):
    zero = jnp.zeros_like(block[:HEAD_DIM])
    rows = block[h * HEAD_DIM : (h + 1) * HEAD_DIM]
    return jnp.concatenate([zero, rows] if upper else [rows, zero], axis=0)


def attend_kernel(
    span, qtag_ref, ktag_ref, qt_ref, kv_ref, kvt_ref, ot_ref, lse_ref, m_sc, l_sc, acc_sc
):
    i = pl.program_id(0)
    m_sc[...] = jnp.full_like(m_sc, NEG)
    l_sc[...] = jnp.zeros_like(l_sc)
    acc_sc[...] = jnp.zeros_like(acc_sc)
    qtag = qtag_ref[...]
    qt = qt_ref[...]
    q_pad = [head_rows(qt, h, False) for h in range(OWN_HEADS)]

    def step(kb, carry):
        rows = pl.ds(pl.multiple_of(kb * FK, FK), FK)
        seen = ktag_ref[rows, :] == qtag
        hs = range(OWN_HEADS)
        s = [mm(kv_ref[rows, 128 * h : 128 * (h + 1)], q_pad[h]) for h in hs]
        s = [jnp.where(seen, v, NEG) for v in s]
        m_old = [m_sc[h : h + 1, :] for h in hs]
        l_old = [l_sc[h : h + 1, :] for h in hs]
        m_new = [jnp.maximum(m_old[h], jnp.max(s[h], axis=0, keepdims=True)) for h in hs]
        p = [jnp.exp(s[h] - m_new[h]).astype(bf16) for h in hs]
        fade = [jnp.exp(m_old[h] - m_new[h]) for h in hs]
        one = jnp.ones((16, FK), bf16)
        v_one = [
            jnp.concatenate([kvt_ref[128 * h + HEAD_DIM : 128 * (h + 1), rows], one], axis=0)
            for h in hs
        ]
        out = [mm(v_one[h], p[h]) for h in hs]
        for h in hs:
            own = slice(HEAD_DIM * h, HEAD_DIM * (h + 1))
            acc_sc[own, :] = acc_sc[own, :] * fade[h] + out[h][:HEAD_DIM]
            l_sc[h : h + 1, :] = fade[h] * l_old[h] + out[h][HEAD_DIM : HEAD_DIM + 1]
            m_sc[h : h + 1, :] = m_new[h]
        return carry

    lax.fori_loop(span[i, 0], span[i, 1], step, 0)
    for h in range(OWN_HEADS):
        own = slice(HEAD_DIM * h, HEAD_DIM * (h + 1))
        total = l_sc[h : h + 1, :]
        ot_ref[own, :] = (acc_sc[own, :] / total).astype(bf16)
        lse_ref[h : h + 1, :] = m_sc[h : h + 1, :] + jnp.log(total)
    lse_ref[OWN_HEADS:, :] = jnp.zeros_like(lse_ref[OWN_HEADS:, :])


def attend(span, qtag, ktag, qt, kv, kvt):
    own = qt.shape[1]
    window = kv.shape[0]
    whole = lambda shape: pl.BlockSpec(shape, lambda i, s: (0, 0), pipeline_mode=pl.Buffered(1))
    cols = lambda rows: pl.BlockSpec((rows, BQ), lambda i, s: (0, i))
    return pl.pallas_call(
        attend_kernel,
        grid_spec=pltpu.PrefetchScalarGridSpec(
            num_scalar_prefetch=1,
            grid=(own // BQ,),
            in_specs=[
                cols(1),
                whole((window, 1)),
                cols(Q_ROWS),
                whole((window, KV_ROWS)),
                whole((KV_ROWS, window)),
            ],
            out_specs=[cols(Q_ROWS), cols(8)],
            scratch_shapes=[
                pltpu.VMEM((8, BQ), f32),
                pltpu.VMEM((8, BQ), f32),
                pltpu.VMEM((Q_ROWS, BQ), f32),
            ],
        ),
        out_shape=[
            jax.ShapeDtypeStruct((Q_ROWS, own), bf16),
            jax.ShapeDtypeStruct((8, own), f32),
        ],
        compiler_params=pltpu.CompilerParams(vmem_limit_bytes=60 << 20),
        cost_estimate=pl.CostEstimate(
            flops=4 * own * 2048 * Q_ROWS, bytes_accessed=20 << 20, transcendentals=own * 6144
        ),
        name="attend",
    )(span, qtag, ktag, qt, kv, kvt)


def grad_kernel(
    parts, final, span, qtag_ref, ktag_ref, qt_ref, dot_ref, ot_ref, lse_ref, kv_ref, kvt_ref, *rest
):
    if final:
        dq_in, dq_ref, *rest = rest
    else:
        dq_in, (dq_ref, *rest) = None, rest
    outs, (dq_sc, dkv_sc) = rest[: len(parts)], rest[len(parts) :]
    i = pl.program_id(0)

    @pl.when(i == 0)
    def _():
        dkv_sc[...] = jnp.zeros_like(dkv_sc)

    if final:
        dq_sc[...] = dq_in[...]
    else:
        dq_sc[...] = jnp.zeros_like(dq_sc)
    qtag = qtag_ref[...]
    qt, d_out, out = qt_ref[...], dot_ref[...], ot_ref[...]
    q_pad = [head_rows(qt, h, False) for h in range(OWN_HEADS)]
    d_pad = [head_rows(d_out, h, True) for h in range(OWN_HEADS)]
    product = d_out.astype(f32) * out.astype(f32)
    inner = [
        jnp.sum(product[HEAD_DIM * h : HEAD_DIM * (h + 1)], axis=0, keepdims=True)
        for h in range(OWN_HEADS)
    ]
    log_row = [lse_ref[h : h + 1, :] for h in range(OWN_HEADS)]

    def step(shift, kb, carry):
        rows = pl.ds(pl.multiple_of(kb * BK, BK), BK)
        place = pl.ds(pl.multiple_of((kb - shift) * BK, BK), BK)
        seen = ktag_ref[rows, :] == qtag
        hs = range(OWN_HEADS)
        kv = [kv_ref[rows, 128 * h : 128 * (h + 1)] for h in hs]
        s = [mm(kv[h], q_pad[h]) for h in hs]
        d_p = [mm(kv[h], d_pad[h]) for h in hs]
        p = [jnp.where(seen, jnp.exp(s[h] - log_row[h]), 0.0) for h in hs]
        d_s = [(p[h] * (d_p[h] - inner[h])).astype(bf16) for h in hs]
        p = [v.astype(bf16) for v in p]
        g_kv = [mm(q_pad[h], d_s[h], NT) + mm(d_pad[h], p[h], NT) for h in hs]
        g_q = [mm(kvt_ref[128 * h : 128 * h + HEAD_DIM, rows], d_s[h]) for h in hs]
        for h in hs:
            dkv_sc[128 * h : 128 * (h + 1), place] += g_kv[h]
            own = slice(HEAD_DIM * h, HEAD_DIM * (h + 1))
            dq_sc[own, :] += g_q[h]
        return carry

    base = 0
    for n, (first, last) in enumerate(parts):
        low = jnp.maximum(span[i, 0], first)
        high = jnp.minimum(span[i, 1], last)
        lax.fori_loop(low, high, functools.partial(step, first - base), 0)
        base += last - first
    if final:
        dq_ref[...] = (dq_sc[...] * score_scale).astype(bf16)
    else:
        dq_ref[...] = dq_sc[...]

    @pl.when(i == pl.num_programs(0) - 1)
    def _():
        base = 0
        for (first, last), ref in zip(parts, outs):
            width = (last - first) * BK
            ref[...] = dkv_sc[:, base : base + width].astype(ref.dtype)
            base += width


def attend_grad(parts, final, span, qtag, ktag, qt, d_out, out, lse, kv, kvt, dq_in=None):
    own = qt.shape[1]
    window = kv.shape[0]
    whole = lambda shape: pl.BlockSpec(shape, lambda i, s: (0, 0), pipeline_mode=pl.Buffered(1))
    cols = lambda rows: pl.BlockSpec((rows, BQ), lambda i, s: (0, i))
    widths = [(last - first) * BK for first, last in parts]
    dtype = f32 if final else bf16
    args = [span, qtag, ktag, qt, d_out, out, lse, kv, kvt] + ([dq_in] if final else [])
    return pl.pallas_call(
        functools.partial(grad_kernel, parts, final),
        grid_spec=pltpu.PrefetchScalarGridSpec(
            num_scalar_prefetch=1,
            grid=(own // BQ,),
            in_specs=[
                cols(1),
                whole((window, 1)),
                cols(Q_ROWS),
                cols(Q_ROWS),
                cols(Q_ROWS),
                cols(8),
                whole((window, KV_ROWS)),
                whole((KV_ROWS, window)),
            ]
            + ([cols(Q_ROWS)] if final else []),
            out_specs=[cols(Q_ROWS)] + [whole((KV_ROWS, w)) for w in widths],
            scratch_shapes=[
                pltpu.VMEM((Q_ROWS, BQ), f32),
                pltpu.VMEM((KV_ROWS, sum(widths)), f32),
            ],
        ),
        out_shape=[jax.ShapeDtypeStruct((Q_ROWS, own), bf16 if final else f32)]
        + [jax.ShapeDtypeStruct((KV_ROWS, w), dtype) for w in widths],
        compiler_params=pltpu.CompilerParams(vmem_limit_bytes=60 << 20),
        cost_estimate=pl.CostEstimate(
            flops=(10 if final else 2) * own * 1536 * Q_ROWS,
            bytes_accessed=20 << 20,
            transcendentals=own * 4096,
        ),
        name="grad_own" if final else "grad_far",
    )(*args)


MESH = pl.DeviceIdType.MESH
CHUNKS = 8
W_LANES = 640
KV_AT = 256


def remote(src, dst, send, recv, target):
    return pltpu.make_async_remote_copy(
        src_ref=src,
        dst_ref=dst,
        send_sem=send,
        recv_sem=recv,
        device_id=(target,),
        device_id_type=MESH,
    )


def share_kernel(
    n_dev, rows_w, tok_ref, code_ref, w_ref, x_own, c_out, w_turn, qt_out, kv_out, kvt_out,
    x_out, w_out, w_wide, w_full, qt_sc, kv_sc, kvt_sc,
    w_send, w_recv, c_send, c_recv, part_send, part_recv, mate_send, mate_recv,
    up_send, up_recv, down_send, down_recv, cross_send, cross_recv,
    fwd_send, fwd_recv, keep_sem, x_sem, q_sem, kv_sem, kvt_sem,
):
    n_group = n_dev // GROUP
    me = lax.axis_index("fsdp")
    g = me // GROUP
    s = me % GROUP
    k = s % 2
    hi = s // 2
    partner = me + 1 - 2 * k
    mate = me + 2 - 4 * hi
    mate_block = 4 + k - 2 * hi
    has_up = g < n_group - 1
    has_down = g > 0
    rows = tok_ref.shape[0] // CHUNKS
    half = CHUNKS // 2

    barrier = pltpu.get_barrier_semaphore()

    def greet(r, carry):
        pl.semaphore_signal(
            barrier, inc=1, device_id=(lax.rem(me + r, n_dev),), device_id_type=MESH
        )
        return carry

    lax.fori_loop(1, n_dev, greet, 0)
    pl.semaphore_wait(barrier, n_dev - 1)

    def chunk(ref, c):
        return ref.at[pl.ds(pl.multiple_of(c * rows, rows), rows)]

    def spot(b, c):
        return x_out.at[b, pl.ds(pl.multiple_of(c * rows, rows), rows)]

    def to_partner(c):
        return remote(chunk(tok_ref, c), spot(2 + s, c), part_send.at[c], part_recv.at[c], partner)

    def to_mate(c):
        return remote(chunk(tok_ref, c), spot(2 + s, c), mate_send.at[c], mate_recv.at[c], mate)

    def up_own(c):
        return remote(chunk(tok_ref, c), spot(k, c), up_send.at[c], up_recv.at[c], me + GROUP)

    def up_mate(c):
        return remote(spot(mate_block, c), spot(k, c), up_send.at[c], up_recv.at[c], me + GROUP)

    def down_own(c):
        return remote(
            chunk(tok_ref, c), spot(6 + k, c), down_send.at[c], down_recv.at[c], me - GROUP
        )

    def down_mate(c):
        return remote(
            spot(mate_block, c + half), spot(6 + k, c + half), down_send.at[c], down_recv.at[c],
            me - GROUP,
        )

    def cross(c):
        at = c + half * hi
        return remote(spot(6 + k, at), spot(6 + k, at), cross_send.at[c], cross_recv.at[c], mate)

    def forward(b, c, slot):
        return remote(spot(b, c), spot(b, c), fwd_send.at[slot], fwd_recv.at[slot], partner)

    keep_x = pltpu.make_async_copy(tok_ref, x_out.at[2 + s], keep_sem.at[0])
    keep_c = pltpu.make_async_copy(code_ref, c_out.at[2 + s], keep_sem.at[1])
    keep_w = pltpu.make_async_copy(w_ref.at[s], w_out.at[me], keep_sem.at[2])
    keep_x.start()
    keep_c.start()
    keep_w.start()

    def w_copy(r):
        target = lax.rem(me + r, n_dev)
        return remote(
            w_ref.at[lax.rem(target, GROUP)], w_out.at[me], w_send.at[r], w_recv.at[r], target
        )

    def w_start(r, carry):
        w_copy(r).start()
        return carry

    def c_group(j):
        target = GROUP * g + lax.rem(s + j, GROUP)
        return remote(code_ref, c_out.at[2 + s], c_send.at[j], c_recv.at[2 + s], target)

    def c_far(j):
        step = GROUP * (2 * hi - 1)
        b = 6 + s - 8 * hi
        target = GROUP * g + step + j
        return remote(code_ref, c_out.at[b], c_send.at[GROUP + j], c_recv.at[b], target)

    sends_far = jnp.where(hi == 1, g < n_group - 1, g > 0)
    for j in range(1, GROUP):
        c_group(j).start()

    @pl.when(sends_far)
    def _():
        for j in range(GROUP):
            c_far(j).start()

    order = list(range(half, CHUNKS)) + list(range(half))
    lax.fori_loop(1, n_dev, w_start, 0)

    @pl.when((hi == 0) & has_down)
    def _():
        for c in range(half):
            down_own(c).start()

    for n, c in enumerate(order):
        to_mate(c).start()
        to_partner(c).start()
        if n < half:

            @pl.when((hi == 1) & has_up)
            def _():
                up_own(c).start()

    for n, c in enumerate(order):
        to_mate(c).wait_recv()
        forward(mate_block, c, c).start()

        @pl.when((hi == 0) & has_up)
        def _():
            up_mate(c).start()

        if n < half:

            @pl.when((hi == 1) & has_down)
            def _():
                down_mate(c - half).start()

        else:

            @pl.when((hi == 1) & has_up)
            def _():
                up_own(c).start()

    def w_wait(r, carry):
        w_copy(r).wait_recv()
        return carry

    lax.fori_loop(1, n_dev, w_wait, 0)
    keep_w.wait()
    keep_x.wait()
    bias_row = jnp.zeros((8, W_LANES), f32)
    bias_at = w_ref.shape[1] - 8
    for j in range(n_dev):
        w_wide[rows_w * j : rows_w * (j + 1), :] = w_out[j, :rows_w, :].astype(f32)
        bias_row = bias_row + w_out[j, bias_at:, :].astype(f32)
    bias_row = jnp.sum(bias_row, axis=0, keepdims=True)
    bias_col = jnp.broadcast_to(bias_row, (128, W_LANES)).T[:, :1]
    w_full[...] = w_wide[...].astype(bf16)
    w_turn[...] = w_wide[...].T.astype(bf16)
    piece = 512
    pieces = tok_ref.shape[0] // piece

    def project(b, inside):
        def one(j, carry):
            x = x_out[b, pl.ds(pl.multiple_of(j * piece, piece), piece), :]
            at = pl.ds(pl.multiple_of((b * pieces + j) * piece, piece), piece)
            kv = mm(x, w_full[:, KV_AT:]) + bias_row[:, KV_AT:]
            kv_sc[at, :] = kv.astype(bf16)
            kvt_sc[:, at] = (mm(w_turn[KV_AT:, :], x, NT) + bias_col[KV_AT:]).astype(bf16)
            if inside:
                to = pl.ds(pl.multiple_of(((b - 2) * pieces + j) * piece, piece), piece)
                q = (mm(w_turn[:Q_ROWS, :], x, NT) + bias_col[:Q_ROWS]).astype(bf16)
                qt_sc[:, to] = q * jnp.asarray(score_scale, bf16)
            return carry

        lax.fori_loop(0, pieces, one, 0)

    def outs(b, inside):
        whole = tok_ref.shape[0]
        at = pl.ds(pl.multiple_of(b * whole, whole), whole)
        copies = [
            pltpu.make_async_copy(kv_sc.at[at], kv_out.at[at], kv_sem.at[b]),
            pltpu.make_async_copy(kvt_sc.at[:, at], kvt_out.at[:, at], kvt_sem.at[b]),
        ]
        if inside:
            to = pl.ds(pl.multiple_of((b - 2) * whole, whole), whole)
            copies.append(pltpu.make_async_copy(qt_sc.at[:, to], qt_out.at[:, to], q_sem.at[b - 2]))
            copies.append(pltpu.make_async_copy(x_out.at[b], x_own.at[b - 2], x_sem.at[b - 2]))
        return copies

    def put(b, inside):
        for copy in outs(b, inside):
            copy.start()

    own_block = 2 + s
    near_block = own_block + 1 - 2 * k
    across_block = mate_block + 1 - 2 * k
    project(own_block, True)

    @pl.when(has_up)
    def _():
        for c in range(half):
            down_own(c).wait_recv()
            cross(c).start()
            forward(6 + k, c + half * hi, 2 * CHUNKS + c).start()

    project(mate_block, True)
    put(own_block, True)

    @pl.when(has_down)
    def _():
        for c in order:
            up_own(c).wait_recv()
            forward(k, c, CHUNKS + c).start()

    for c in range(CHUNKS):
        to_partner(c).wait_recv()
    project(near_block, True)
    put(mate_block, True)

    @pl.when(has_up)
    def _():
        for c in range(half):
            cross(c).wait_recv()
            forward(6 + k, c + half * (1 - hi), 2 * CHUNKS + half + c).start()

    for c in range(CHUNKS):
        forward(mate_block, c, c).wait_recv()
    project(across_block, True)
    put(near_block, True)

    @pl.when(has_down)
    def _():
        project(k, False)
        for c in range(CHUNKS):
            forward(k, c, CHUNKS + c).wait_recv()
        project(1 - k, False)
        put(k, False)

    put(across_block, True)

    @pl.when(has_up)
    def _():
        project(6 + k, False)
        for c in range(half):
            forward(6 + k, c, 2 * CHUNKS + c).wait_recv()
            forward(6 + k, c, 2 * CHUNKS + half + c).wait_recv()
        project(7 - k, False)
        put(6 + k, False)

    for c in range(CHUNKS):
        to_partner(c).wait_send()
        to_mate(c).wait_send()
        forward(mate_block, c, c).wait_send()

    @pl.when(has_down)
    def _():
        put(1 - k, False)
        for c in range(CHUNKS):
            forward(k, c, CHUNKS + c).wait_send()
        for c in range(half):
            down_own(c).wait_send()

    @pl.when(has_up)
    def _():
        for c in range(half):
            cross(c).wait_send()
            forward(6 + k, c, 2 * CHUNKS + c).wait_send()
            forward(6 + k, c, 2 * CHUNKS + half + c).wait_send()
        for c in range(CHUNKS):
            up_own(c).wait_send()
        put(7 - k, False)

    for j in range(1, GROUP):
        c_group(j).wait_send()
        remote(
            code_ref, c_out.at[0], c_send.at[j], c_recv.at[2 + lax.rem(s + j, GROUP)], partner
        ).wait_recv()

    @pl.when(sends_far)
    def _():
        for j in range(GROUP):
            c_far(j).wait_send()

    @pl.when(has_down)
    def _():
        for b in range(2):
            remote(code_ref, c_out.at[b], c_send.at[0], c_recv.at[b], partner).wait_recv()

    @pl.when(has_up)
    def _():
        for b in range(6, 8):
            remote(code_ref, c_out.at[b], c_send.at[0], c_recv.at[b], partner).wait_recv()

    def w_sent(r, carry):
        w_copy(r).wait_send()
        return carry

    lax.fori_loop(1, n_dev, w_sent, 0)
    keep_c.wait()
    for b in range(2, 6):
        for copy in outs(b, True):
            copy.wait()

    @pl.when(has_down)
    def _():
        for b in range(2):
            for copy in outs(b, False):
                copy.wait()

    @pl.when(has_up)
    def _():
        for b in range(6, 8):
            for copy in outs(b, False):
                copy.wait()


def share(n_dev, rows_w, tokens, code, w_send):
    vmem = pl.BlockSpec(memory_space=pltpu.VMEM)
    anywhere = pl.BlockSpec(memory_space=pl.ANY)
    dma = lambda n: pltpu.SemaphoreType.DMA((n,))
    half = CHUNKS // 2
    rows, width = tokens.shape
    own, window = GROUP * rows, 8 * rows
    return pl.pallas_call(
        functools.partial(share_kernel, n_dev, rows_w),
        in_specs=[vmem] * 3,
        out_specs=[anywhere, anywhere, vmem, anywhere, anywhere, anywhere],
        out_shape=[
            jax.ShapeDtypeStruct((GROUP, rows, width), bf16),
            jax.ShapeDtypeStruct((8,) + code.shape, code.dtype),
            jax.ShapeDtypeStruct((W_LANES, width), bf16),
            jax.ShapeDtypeStruct((Q_ROWS, own), bf16),
            jax.ShapeDtypeStruct((window, KV_ROWS), bf16),
            jax.ShapeDtypeStruct((KV_ROWS, window), bf16),
        ],
        scratch_shapes=[
            pltpu.VMEM((8, rows, width), bf16),
            pltpu.VMEM((n_dev,) + w_send.shape[1:], bf16),
            pltpu.VMEM((width, W_LANES), f32),
            pltpu.VMEM((width, W_LANES), bf16),
            pltpu.VMEM((Q_ROWS, own), bf16),
            pltpu.VMEM((window, KV_ROWS), bf16),
            pltpu.VMEM((KV_ROWS, window), bf16),
            dma(n_dev), dma(n_dev), dma(2 * GROUP), dma(8),
            dma(CHUNKS), dma(CHUNKS), dma(CHUNKS), dma(CHUNKS),
            dma(CHUNKS), dma(CHUNKS), dma(half), dma(half), dma(half), dma(half),
            dma(3 * CHUNKS), dma(3 * CHUNKS), dma(3), dma(GROUP), dma(GROUP), dma(8), dma(8),
        ],
        compiler_params=pltpu.CompilerParams(
            collective_id=0, has_side_effects=True, vmem_limit_bytes=60 << 20
        ),
        name="share",
    )(tokens, code, w_send)


PARTS = 4
TN = (((0,), (0,)), ((), ()))


def settle_kernel(
    n_dev, rows_w, mix_ref, x_ref, w_ref, vec_ref, own_out, near_out, far_out, w_out, vec_out,
    wide, slabs, across, near, relay, total,
    w_send, w_recv, vec_send, vec_recv, near_send, near_recv, relay_send, relay_recv,
    far_send, far_recv, keep_sem,
):
    me = lax.axis_index("fsdp")
    s = me % GROUP
    k = s % 2
    hi = s // 2
    partner = me + 1 - 2 * k
    mate = me + 2 - 4 * hi
    s_partner = s + 1 - 2 * k
    s_mate = s + 2 - 4 * hi
    s_across = 3 - s
    block = own_out.shape[0]
    rows = block // PARTS

    barrier = pltpu.get_barrier_semaphore()

    def greet(r, carry):
        pl.semaphore_signal(
            barrier, inc=1, device_id=(lax.rem(me + r, n_dev),), device_id_type=MESH
        )
        return carry

    lax.fori_loop(1, n_dev, greet, 0)
    pl.semaphore_wait(barrier, n_dev - 1)

    def part(c):
        return pl.ds(c * rows, rows)

    def to_relay(c):
        return remote(
            across.at[part(c)], relay.at[part(c)], relay_send.at[c], relay_recv.at[c], partner
        )

    def to_near(c):
        return remote(
            near.at[part(c)], near_out.at[part(c)], near_send.at[c], near_recv.at[c], partner
        )

    def to_far(c):
        return remote(total.at[part(c)], far_out.at[part(c)], far_send.at[c], far_recv.at[c], mate)

    def w_copy(r):
        target = lax.rem(me + r, n_dev)
        return remote(slabs.at[target], w_out.at[me], w_send.at[r], w_recv.at[r], target)

    def vec_copy(r):
        target = lax.rem(me + r, n_dev)
        return remote(vec_ref.at[target], vec_out.at[me], vec_send.at[r], vec_recv.at[r], target)

    def vec_start(r, carry):
        vec_copy(r).start()
        return carry

    lax.fori_loop(1, n_dev, vec_start, 0)
    keep_vec = pltpu.make_async_copy(vec_ref.at[me], vec_out.at[me], keep_sem.at[1])
    keep_vec.start()

    wide[...] = jnp.zeros_like(wide)

    def add_rows(j, carry):
        at = pl.ds(pl.multiple_of(j * block, block), block)
        wide[:MIX_ROWS, :] += mm(mix_ref[:, at], x_ref[at, :])
        return carry

    lax.fori_loop(0, GROUP, add_rows, 0)
    turned = wide[...].T.astype(bf16).astype(f32)
    bias = mm(jnp.ones((8, GROUP * block), bf16), mix_ref[...], NT).astype(bf16)
    bias_at = slabs.shape[1] - 8
    for j in range(n_dev):
        slabs[j, :rows_w, :] = turned[rows_w * j : rows_w * (j + 1), :].astype(bf16)
        slabs[j, bias_at:, :MIX_ROWS] = bias

    def back(t, c):
        at = pl.ds(pl.multiple_of(t * block + c * rows, rows), rows)
        return mm(mix_ref[:, at], w_ref[...], TN)

    for c in range(PARTS):
        across[c * rows : (c + 1) * rows, :] = back(s_across, c).astype(bf16)
        if c > 0:
            to_relay(c - 1).start()

    def w_start(r, carry):
        w_copy(r).start()
        return carry

    lax.fori_loop(1, n_dev, w_start, 0)
    keep_w = pltpu.make_async_copy(slabs.at[me], w_out.at[me], keep_sem.at[0])
    keep_w.start()
    mine = back(s_mate, 0)
    to_relay(PARTS - 1).start()
    for c in range(PARTS):
        to_relay(c).wait_recv()
        other = relay[c * rows : (c + 1) * rows, :].astype(f32)
        total[c * rows : (c + 1) * rows, :] = (mine + other).astype(bf16)
        if c + 1 < PARTS:
            mine = back(s_mate, c + 1)
        else:
            near[:rows, :] = back(s_partner, 0).astype(bf16)
        to_far(c).start()
    for c in range(1, PARTS):
        near[c * rows : (c + 1) * rows, :] = back(s_partner, c).astype(bf16)
        to_near(c - 1).start()
    for c in range(PARTS):
        own_out[c * rows : (c + 1) * rows, :] = back(s, c)
        if c == 0:
            to_near(PARTS - 1).start()
    for c in range(PARTS):
        to_relay(c).wait_send()
        to_near(c).wait()
        to_far(c).wait()

    def finish(r, carry):
        w_copy(r).wait()
        vec_copy(r).wait()
        return carry

    lax.fori_loop(1, n_dev, finish, 0)
    keep_w.wait()
    keep_vec.wait()


def settle(n_dev, rows_w, mix, x, w, vec):
    vmem = pl.BlockSpec(memory_space=pltpu.VMEM)
    anywhere = pl.BlockSpec(memory_space=pl.ANY)
    dma = lambda n: pltpu.SemaphoreType.DMA((n,))
    block = (x.shape[0] // GROUP, x.shape[1])
    slabs = (n_dev, rows_w + -rows_w % 8 + 8, W_LANES)
    return pl.pallas_call(
        functools.partial(settle_kernel, n_dev, rows_w),
        in_specs=[vmem] * 4,
        out_specs=[vmem] + [anywhere] * 4,
        out_shape=[
            jax.ShapeDtypeStruct(block, f32),
            jax.ShapeDtypeStruct(block, bf16),
            jax.ShapeDtypeStruct(block, bf16),
            jax.ShapeDtypeStruct(slabs, bf16),
            jax.ShapeDtypeStruct(vec.shape, vec.dtype),
        ],
        scratch_shapes=[
            pltpu.VMEM((W_LANES, x.shape[1]), f32),
            pltpu.VMEM(slabs, bf16),
            pltpu.VMEM(block, bf16), pltpu.VMEM(block, bf16),
            pltpu.VMEM(block, bf16), pltpu.VMEM(block, bf16),
            dma(n_dev), dma(n_dev), dma(n_dev), dma(n_dev),
            dma(PARTS), dma(PARTS), dma(PARTS), dma(PARTS), dma(PARTS), dma(PARTS), dma(2),
        ],
        compiler_params=pltpu.CompilerParams(
            collective_id=1, has_side_effects=True, vmem_limit_bytes=60 << 20
        ),
        name="settle",
    )(mix, x, w, vec)


def body(
    n_dev,
    tokens,
    segment_ids,
    pad_mask,
    w_qkv,
    bias_query,
    bias_value,
    w_out,
    bias_out,
    gain_one,
    shift_one,
    w_up,
    bias_up,
    w_down,
    bias_down,
    gain_two,
    shift_two,
    cotangent,
):
    row_count = tokens.shape[0]
    rows_w = w_qkv.shape[0]
    own = GROUP * row_count
    window = own + 2 * LEN_MAX
    me = lax.axis_index("fsdp")
    place = me % GROUP
    group_id = me // GROUP
    n_group = n_dev // GROUP
    up = [(i, i + GROUP) for i in range(n_dev - GROUP)]
    down = [(i + GROUP, i) for i in range(n_dev - GROUP)]
    groups = [[GROUP * g + j for j in range(GROUP)] for g in range(n_group)]

    wq = w_qkv[:, :D].reshape(rows_w, GROUP, Q_ROWS)
    wk = w_qkv[:, D : 2 * D].reshape(rows_w, GROUP, OWN_HEADS, 1, HEAD_DIM)
    wv = w_qkv[:, 2 * D :].reshape(rows_w, GROUP, OWN_HEADS, 1, HEAD_DIM)
    wkv = jnp.concatenate([wk, wv], axis=3).reshape(rows_w, GROUP, KV_ROWS)
    gap = KV_AT - Q_ROWS
    lane = jnp.arange(gap)[None, :]
    small_cols = jnp.pad(bias_up.reshape(rows_w, -1), ((0, 0), (6, gap - 10)))
    for j, v in enumerate([bias_out, gain_one, shift_one, bias_down, gain_two, shift_two]):
        small_cols = jnp.where(lane == j, v[:, None], small_cols)
    small_cols = jnp.broadcast_to(small_cols[:, None], (rows_w, GROUP, gap))
    w_cut = jnp.concatenate([wq, small_cols, wkv], axis=2).transpose(1, 0, 2)
    column = me * rows_w + jnp.arange(rows_w)
    feature = jnp.arange(D)
    spread = lambda bias: jnp.sum(
        jnp.where(feature[None] == column[:, None], bias.astype(f32)[:, None], 0.0), axis=0
    )
    bias_q = spread(bias_query).reshape(GROUP, Q_ROWS)
    bias_v = spread(bias_value).reshape(GROUP, OWN_HEADS, 1, HEAD_DIM)
    bias_kv = jnp.concatenate([jnp.zeros_like(bias_v), bias_v], axis=2).reshape(GROUP, KV_ROWS)
    bias_cut = jnp.concatenate([bias_q, jnp.zeros((GROUP, gap), f32), bias_kv], axis=1)
    fill = -rows_w % 8
    bias_cut = jnp.pad(bias_cut.astype(bf16)[:, None], ((0, 0), (fill, 7), (0, 0)))
    w_send = jnp.concatenate([w_cut, bias_cut], axis=1)
    ff = w_up.shape[1]
    wo_full = lax.all_gather(w_out, "fsdp", axis=0, tiled=True)
    wu_full = lax.all_gather(w_up, "fsdp", axis=0, tiled=True)
    wd_full = lax.all_gather(w_down, "fsdp", axis=0, tiled=True)

    code = (segment_ids * 2 + pad_mask).reshape(8, row_count // 8)
    x_own, code_win, w_turn, qt, kv, kvt = share(n_dev, rows_w, tokens, code, w_send)
    x_own = x_own.reshape(own, D)
    code_win = code_win.reshape(window)
    at = jnp.arange(window)
    code_win = jnp.where((group_id == 0) & (at < LEN_MAX), -2, code_win)
    code_win = jnp.where(
        (group_id == n_group - 1) & (at >= LEN_MAX + own), 2 * n_dev * row_count, code_win
    )
    code_own = code_win[LEN_MAX : LEN_MAX + own]
    w_back = jnp.concatenate([w_turn[:Q_ROWS], w_turn[KV_AT:]], axis=0)
    small_all = w_turn[Q_ROWS : Q_ROWS + 10].astype(f32)
    bu_full = small_all[6:].T.reshape(-1)
    bo_full, g1_full, s1_full, bd_full, g2_full, s2_full = [small_all[j] for j in range(6)]
    seg_win = code_win >> 1
    ktag = jnp.where((code_win & 1) == 1, seg_win + 1, 0).reshape(window, 1)
    seg_own = code_own >> 1
    qtag = (seg_own + 1).reshape(1, own)
    first_seg = seg_own[::BQ]
    last_seg = seg_own[BQ - 1 :: BQ]
    low = jnp.sum((seg_win[None, :] < first_seg[:, None]).astype(jnp.int32), axis=1)
    high = jnp.sum((seg_win[None, :] <= last_seg[:, None]).astype(jnp.int32), axis=1)
    spans = [jnp.stack([low // b, (high + b - 1) // b], axis=1) for b in (FK, BK)]

    ot, lse = attend(spans[0], qtag, ktag, qt, kv, kvt)
    ctx_t = lax.all_to_all(
        ot.reshape(Q_ROWS, GROUP, row_count), "fsdp", 1, 0, axis_index_groups=groups, tiled=True
    ).reshape(D, row_count)

    tokens_f = tokens.astype(f32)
    branch = jnp.einsum("ir,io->ro", ctx_t, wo_full, preferred_element_type=f32) + bo_full
    first, norm_one_back = jax.vjp(norm_rows, tokens_f + branch, g1_full, s1_full)
    up_in = first.astype(bf16)
    pre_act = jnp.dot(up_in, wu_full, preferred_element_type=f32) + bu_full
    gelu_val, gelu_back = jax.vjp(gelu_exact, pre_act)
    hidden = gelu_val.astype(bf16)
    ffn = jnp.dot(hidden, wd_full, preferred_element_type=f32) + bd_full
    result, norm_two_back = jax.vjp(norm_rows, first + ffn, g2_full, s2_full)
    layer_out = result.astype(bf16)
    d_second, d_gain_two, d_shift_two = norm_two_back(cotangent.astype(f32))
    d_ffn = d_second.astype(bf16)
    d_bias_down = jnp.sum(d_ffn.astype(f32), axis=0)
    d_w_down = jnp.einsum("rf,rd->fd", hidden, d_ffn, preferred_element_type=f32)
    d_hidden = jnp.einsum("rd,fd->rf", d_ffn, wd_full, preferred_element_type=f32)
    d_pre = gelu_back(d_hidden)[0].astype(bf16)
    d_bias_up = jnp.sum(d_pre.astype(f32), axis=0)
    d_w_up = [
        jnp.einsum("rd,rf->df", up_in, d_pre[:, D * j : D * (j + 1)], preferred_element_type=f32)
        for j in range(ff // D)
    ]
    d_first = d_second + jnp.einsum("rf,df->rd", d_pre, wu_full, preferred_element_type=f32)
    d_mid, d_gain_one, d_shift_one = norm_one_back(d_first)
    d_branch = d_mid.astype(bf16)
    d_bias_out = jnp.sum(d_branch.astype(f32), axis=0)
    d_w_out = jnp.einsum("ir,ro->io", ctx_t, d_branch, preferred_element_type=f32)
    dctx_t = jnp.einsum("ro,io->ir", d_branch, wo_full, preferred_element_type=f32).astype(bf16)
    n_up = ff // D
    big_grad = jnp.concatenate(
        [
            d_w_down.astype(bf16).reshape(n_dev, -1, D),
            d_w_out.astype(bf16).reshape(n_dev, rows_w, D),
        ]
        + [v.astype(bf16).reshape(n_dev, rows_w, D) for v in d_w_up],
        axis=1,
    )
    big_owned = lax.psum_scatter(big_grad, "fsdp", scatter_dimension=0).astype(f32)
    rows_d = w_down.shape[0]
    g_down, g_out = big_owned[:rows_d], big_owned[rows_d : rows_d + rows_w]
    g_up = jnp.concatenate(
        [big_owned[rows_d + rows_w * (j + 1) : rows_d + rows_w * (j + 2)] for j in range(n_up)], axis=1
    )

    d_out = lax.all_to_all(
        dctx_t.reshape(GROUP, Q_ROWS, row_count), "fsdp", 0, 2, axis_index_groups=groups, tiled=True
    ).reshape(Q_ROWS, own)
    edge, inside = LEN_MAX // BK, own // BK
    far_parts = ((0, edge), (edge + inside, 2 * edge + inside))
    own_parts = ((edge, edge + inside),)
    dq_far, dkv_left, dkv_right = attend_grad(
        far_parts, False, spans[1], qtag, ktag, qt, d_out, ot, lse, kv, kvt
    )
    from_right = lax.ppermute(dkv_left, "fsdp", down)
    from_left = lax.ppermute(dkv_right, "fsdp", up)
    dq_t, dkv_own = attend_grad(
        own_parts, True, spans[1], qtag, ktag, qt, d_out, ot, lse, kv, kvt, dq_far
    )
    dkv = jnp.concatenate(
        [
            dkv_own[:, :LEN_MAX] + from_left.astype(f32),
            dkv_own[:, LEN_MAX : own - LEN_MAX],
            dkv_own[:, own - LEN_MAX :] + from_right.astype(f32),
        ],
        axis=1,
    ).astype(bf16)
    dmix_t = jnp.concatenate([dq_t, dkv], axis=0)
    vecs = jnp.stack([d_bias_out, d_gain_one, d_shift_one, d_bias_down, d_gain_two, d_shift_two])
    vec_send = jnp.concatenate(
        [
            vecs.reshape(6, n_dev, rows_w).transpose(1, 0, 2).reshape(n_dev, 6 * rows_w),
            d_bias_up.reshape(n_dev, 4 * rows_w),
        ],
        axis=1,
    )
    vec_send = jnp.pad(vec_send, ((0, 0), (0, 1024 - vec_send.shape[1]))).reshape(n_dev, 8, 128)
    own_x, near, far, w_got, vec_got = settle(n_dev, rows_w, dmix_t, x_own, w_back, vec_send)
    grad_tokens = d_mid + ((own_x + near.astype(f32)) + far.astype(f32))
    got = jnp.sum(w_got.astype(f32).reshape(n_group, GROUP, -1, W_LANES), axis=0)
    got_q = got[:, :, :Q_ROWS].transpose(1, 0, 2).reshape(-1, D)
    got_kv = got[:, :, Q_ROWS:MIX_ROWS].transpose(1, 0, 2)
    got_kv = got_kv.reshape(-1, GROUP, OWN_HEADS, 2, HEAD_DIM)
    got_k = got_kv[:, :, :, 0].reshape(-1, D)
    got_v = got_kv[:, :, :, 1].reshape(-1, D)
    grad_w_qkv = jnp.concatenate([got_q[:rows_w], got_k[:rows_w], got_v[:rows_w]], axis=1)
    mine = lambda rows: lax.dynamic_slice(rows[-1], (me * rows_w,), (rows_w,))
    vec = jnp.sum(vec_got, axis=0).reshape(-1)[: 10 * rows_w]
    own_vec = [mine(got_q), mine(got_v)] + [vec[j * rows_w : (j + 1) * rows_w] for j in range(6)]
    return (
        layer_out,
        grad_tokens,
        grad_w_qkv,
        own_vec[0],
        own_vec[1],
        g_out,
        own_vec[2],
        own_vec[3],
        own_vec[4],
        g_up,
        vec[6 * rows_w :],
        g_down,
        own_vec[5],
        own_vec[6],
        own_vec[7],
    )


def solution(mesh):
    rows, flat = P("fsdp", None), P("fsdp")
    return jax.shard_map(
        functools.partial(body, mesh.shape["fsdp"]),
        mesh=mesh,
        in_specs=(
            rows, flat, flat, rows, flat, flat, rows, flat, flat, flat, rows, flat, rows, flat,
            flat, flat, rows,
        ),
        out_specs=(
            rows, rows, rows, flat, flat, rows, flat, flat, flat, rows, flat, rows, flat, flat,
            flat,
        ),
        check_vma=False,
    )
```

```python
import functools

import jax
import jax.numpy as jnp
from jax import lax
from jax.experimental import pallas as pl
from jax.experimental.pallas import tpu as pltpu
from jax.sharding import PartitionSpec as P

D = 768
HEADS = 12
HEAD_DIM = 64
LEN_MAX = 2048
GROUP = 4
OWN_HEADS = HEADS // GROUP
Q_ROWS = OWN_HEADS * HEAD_DIM
KV_ROWS = 2 * Q_ROWS
MIX_ROWS = Q_ROWS + KV_ROWS
BQ = 512
FK = 512
BK = 256
NEG = -1e30

bf16 = jnp.bfloat16
f32 = jnp.float32
eps_norm = 1e-12
score_scale = 0.125

NN = (((1,), (0,)), ((), ()))
NT = (((1,), (1,)), ((), ()))


def mm(a, b, dims=NN):
    return lax.dot_general(a, b, dims, preferred_element_type=f32)


def norm_rows(hidden, gain_row, shift_row):
    centre = hidden - jnp.mean(hidden, axis=-1, keepdims=True)
    spread = jnp.mean(centre * centre, axis=-1, keepdims=True)
    return centre * lax.rsqrt(spread + eps_norm) * gain_row + shift_row


def gelu_exact(pre_act):
    return 0.5 * pre_act * (1.0 + jax.scipy.special.erf(pre_act * 0.7071067811865476))


def head_rows(block, h, upper):
    zero = jnp.zeros_like(block[:HEAD_DIM])
    rows = block[h * HEAD_DIM : (h + 1) * HEAD_DIM]
    return jnp.concatenate([zero, rows] if upper else [rows, zero], axis=0)


def attend_kernel(
    span, qtag_ref, ktag_ref, qt_ref, kv_ref, kvt_ref, ot_ref, lse_ref, m_sc, l_sc, acc_sc
):
    i = pl.program_id(0)
    m_sc[...] = jnp.full_like(m_sc, NEG)
    l_sc[...] = jnp.zeros_like(l_sc)
    acc_sc[...] = jnp.zeros_like(acc_sc)
    qtag = qtag_ref[...]
    qt = qt_ref[...]
    q_pad = [head_rows(qt, h, False) for h in range(OWN_HEADS)]

    def step(kb, carry):
        rows = pl.ds(pl.multiple_of(kb * FK, FK), FK)
        seen = ktag_ref[rows, :] == qtag
        hs = range(OWN_HEADS)
        s = [mm(kv_ref[rows, 128 * h : 128 * (h + 1)], q_pad[h]) for h in hs]
        s = [jnp.where(seen, v, NEG) for v in s]
        m_old = [m_sc[h : h + 1, :] for h in hs]
        l_old = [l_sc[h : h + 1, :] for h in hs]
        m_new = [jnp.maximum(m_old[h], jnp.max(s[h], axis=0, keepdims=True)) for h in hs]
        p = [jnp.exp(s[h] - m_new[h]).astype(bf16) for h in hs]
        fade = [jnp.exp(m_old[h] - m_new[h]) for h in hs]
        one = jnp.ones((16, FK), bf16)
        v_one = [
            jnp.concatenate([kvt_ref[128 * h + HEAD_DIM : 128 * (h + 1), rows], one], axis=0)
            for h in hs
        ]
        out = [mm(v_one[h], p[h]) for h in hs]
        for h in hs:
            own = slice(HEAD_DIM * h, HEAD_DIM * (h + 1))
            acc_sc[own, :] = acc_sc[own, :] * fade[h] + out[h][:HEAD_DIM]
            l_sc[h : h + 1, :] = fade[h] * l_old[h] + out[h][HEAD_DIM : HEAD_DIM + 1]
            m_sc[h : h + 1, :] = m_new[h]
        return carry

    lax.fori_loop(span[i, 0], span[i, 1], step, 0)
    for h in range(OWN_HEADS):
        own = slice(HEAD_DIM * h, HEAD_DIM * (h + 1))
        total = l_sc[h : h + 1, :]
        ot_ref[own, :] = (acc_sc[own, :] / total).astype(bf16)
        lse_ref[h : h + 1, :] = m_sc[h : h + 1, :] + jnp.log(total)
    lse_ref[OWN_HEADS:, :] = jnp.zeros_like(lse_ref[OWN_HEADS:, :])


def attend(span, qtag, ktag, qt, kv, kvt):
    own = qt.shape[1]
    window = kv.shape[0]
    whole = lambda shape: pl.BlockSpec(shape, lambda i, s: (0, 0), pipeline_mode=pl.Buffered(1))
    cols = lambda rows: pl.BlockSpec((rows, BQ), lambda i, s: (0, i))
    return pl.pallas_call(
        attend_kernel,
        grid_spec=pltpu.PrefetchScalarGridSpec(
            num_scalar_prefetch=1,
            grid=(own // BQ,),
            in_specs=[
                cols(1),
                whole((window, 1)),
                cols(Q_ROWS),
                whole((window, KV_ROWS)),
                whole((KV_ROWS, window)),
            ],
            out_specs=[cols(Q_ROWS), cols(8)],
            scratch_shapes=[
                pltpu.VMEM((8, BQ), f32),
                pltpu.VMEM((8, BQ), f32),
                pltpu.VMEM((Q_ROWS, BQ), f32),
            ],
        ),
        out_shape=[
            jax.ShapeDtypeStruct((Q_ROWS, own), bf16),
            jax.ShapeDtypeStruct((8, own), f32),
        ],
        compiler_params=pltpu.CompilerParams(vmem_limit_bytes=60 << 20),
        cost_estimate=pl.CostEstimate(
            flops=4 * own * 2048 * Q_ROWS, bytes_accessed=20 << 20, transcendentals=own * 6144
        ),
        name="attend",
    )(span, qtag, ktag, qt, kv, kvt)


def grad_kernel(
    parts, final, span, qtag_ref, ktag_ref, qt_ref, dot_ref, ot_ref, lse_ref, kv_ref, kvt_ref, *rest
):
    if final:
        dq_in, dq_ref, *rest = rest
    else:
        dq_in, (dq_ref, *rest) = None, rest
    outs, (dq_sc, dkv_sc) = rest[: len(parts)], rest[len(parts) :]
    i = pl.program_id(0)

    @pl.when(i == 0)
    def _():
        dkv_sc[...] = jnp.zeros_like(dkv_sc)

    if final:
        dq_sc[...] = dq_in[...]
    else:
        dq_sc[...] = jnp.zeros_like(dq_sc)
    qtag = qtag_ref[...]
    qt, d_out, out = qt_ref[...], dot_ref[...], ot_ref[...]
    q_pad = [head_rows(qt, h, False) for h in range(OWN_HEADS)]
    d_pad = [head_rows(d_out, h, True) for h in range(OWN_HEADS)]
    product = d_out.astype(f32) * out.astype(f32)
    inner = [
        jnp.sum(product[HEAD_DIM * h : HEAD_DIM * (h + 1)], axis=0, keepdims=True)
        for h in range(OWN_HEADS)
    ]
    log_row = [lse_ref[h : h + 1, :] for h in range(OWN_HEADS)]

    def step(shift, kb, carry):
        rows = pl.ds(pl.multiple_of(kb * BK, BK), BK)
        place = pl.ds(pl.multiple_of((kb - shift) * BK, BK), BK)
        seen = ktag_ref[rows, :] == qtag
        hs = range(OWN_HEADS)
        kv = [kv_ref[rows, 128 * h : 128 * (h + 1)] for h in hs]
        s = [mm(kv[h], q_pad[h]) for h in hs]
        d_p = [mm(kv[h], d_pad[h]) for h in hs]
        p = [jnp.where(seen, jnp.exp(s[h] - log_row[h]), 0.0) for h in hs]
        d_s = [(p[h] * (d_p[h] - inner[h])).astype(bf16) for h in hs]
        p = [v.astype(bf16) for v in p]
        g_kv = [mm(q_pad[h], d_s[h], NT) + mm(d_pad[h], p[h], NT) for h in hs]
        g_q = [mm(kvt_ref[128 * h : 128 * h + HEAD_DIM, rows], d_s[h]) for h in hs]
        for h in hs:
            dkv_sc[128 * h : 128 * (h + 1), place] += g_kv[h]
            own = slice(HEAD_DIM * h, HEAD_DIM * (h + 1))
            dq_sc[own, :] += g_q[h]
        return carry

    base = 0
    for n, (first, last) in enumerate(parts):
        low = jnp.maximum(span[i, 0], first)
        high = jnp.minimum(span[i, 1], last)
        lax.fori_loop(low, high, functools.partial(step, first - base), 0)
        base += last - first
    if final:
        dq_ref[...] = (dq_sc[...] * score_scale).astype(bf16)
    else:
        dq_ref[...] = dq_sc[...]

    @pl.when(i == pl.num_programs(0) - 1)
    def _():
        base = 0
        for (first, last), ref in zip(parts, outs):
            width = (last - first) * BK
            ref[...] = dkv_sc[:, base : base + width].astype(ref.dtype)
            base += width


def attend_grad(parts, final, span, qtag, ktag, qt, d_out, out, lse, kv, kvt, dq_in=None):
    own = qt.shape[1]
    window = kv.shape[0]
    whole = lambda shape: pl.BlockSpec(shape, lambda i, s: (0, 0), pipeline_mode=pl.Buffered(1))
    cols = lambda rows: pl.BlockSpec((rows, BQ), lambda i, s: (0, i))
    widths = [(last - first) * BK for first, last in parts]
    dtype = f32 if final else bf16
    args = [span, qtag, ktag, qt, d_out, out, lse, kv, kvt] + ([dq_in] if final else [])
    return pl.pallas_call(
        functools.partial(grad_kernel, parts, final),
        grid_spec=pltpu.PrefetchScalarGridSpec(
            num_scalar_prefetch=1,
            grid=(own // BQ,),
            in_specs=[
                cols(1),
                whole((window, 1)),
                cols(Q_ROWS),
                cols(Q_ROWS),
                cols(Q_ROWS),
                cols(8),
                whole((window, KV_ROWS)),
                whole((KV_ROWS, window)),
            ]
            + ([cols(Q_ROWS)] if final else []),
            out_specs=[cols(Q_ROWS)] + [whole((KV_ROWS, w)) for w in widths],
            scratch_shapes=[
                pltpu.VMEM((Q_ROWS, BQ), f32),
                pltpu.VMEM((KV_ROWS, sum(widths)), f32),
            ],
        ),
        out_shape=[jax.ShapeDtypeStruct((Q_ROWS, own), bf16 if final else f32)]
        + [jax.ShapeDtypeStruct((KV_ROWS, w), dtype) for w in widths],
        compiler_params=pltpu.CompilerParams(vmem_limit_bytes=60 << 20),
        cost_estimate=pl.CostEstimate(
            flops=(10 if final else 2) * own * 1536 * Q_ROWS,
            bytes_accessed=20 << 20,
            transcendentals=own * 4096,
        ),
        name="grad_own" if final else "grad_far",
    )(*args)


MESH = pl.DeviceIdType.MESH
CHUNKS = 8
W_LANES = 640
KV_AT = 256


def remote(src, dst, send, recv, target):
    return pltpu.make_async_remote_copy(
        src_ref=src,
        dst_ref=dst,
        send_sem=send,
        recv_sem=recv,
        device_id=(target,),
        device_id_type=MESH,
    )


def share_kernel(
    n_dev, rows_w, tok_ref, code_ref, w_ref, x_own, code_out, ktag_out, w_turn, qt_out, kv_out, kvt_out,
    c_out, x_out, w_out, w_wide, w_full, qt_sc, kv_sc, kvt_sc,
    w_send, w_recv, c_send, c_recv, part_send, part_recv, mate_send, mate_recv,
    up_send, up_recv, down_send, down_recv, cross_send, cross_recv,
    fwd_send, fwd_recv, keep_sem, x_sem, q_sem, kv_sem, kvt_sem,
):
    n_group = n_dev // GROUP
    me = lax.axis_index("fsdp")
    g = me // GROUP
    s = me % GROUP
    k = s % 2
    hi = s // 2
    partner = me + 1 - 2 * k
    mate = me + 2 - 4 * hi
    mate_block = 4 + k - 2 * hi
    has_up = g < n_group - 1
    has_down = g > 0
    rows = tok_ref.shape[0] // CHUNKS
    half = CHUNKS // 2

    barrier = pltpu.get_barrier_semaphore()

    def greet(r, carry):
        pl.semaphore_signal(
            barrier, inc=1, device_id=(lax.rem(me + r, n_dev),), device_id_type=MESH
        )
        return carry

    lax.fori_loop(1, n_dev, greet, 0)
    pl.semaphore_wait(barrier, n_dev - 1)

    def chunk(ref, c):
        return ref.at[pl.ds(pl.multiple_of(c * rows, rows), rows)]

    def spot(b, c):
        return x_out.at[b, pl.ds(pl.multiple_of(c * rows, rows), rows)]

    def to_partner(c):
        return remote(chunk(tok_ref, c), spot(2 + s, c), part_send.at[c], part_recv.at[c], partner)

    def to_mate(c):
        return remote(chunk(tok_ref, c), spot(2 + s, c), mate_send.at[c], mate_recv.at[c], mate)

    def up_own(c):
        return remote(chunk(tok_ref, c), spot(k, c), up_send.at[c], up_recv.at[c], me + GROUP)

    def up_mate(c):
        return remote(spot(mate_block, c), spot(k, c), up_send.at[c], up_recv.at[c], me + GROUP)

    def down_own(c):
        return remote(
            chunk(tok_ref, c), spot(6 + k, c), down_send.at[c], down_recv.at[c], me - GROUP
        )

    def down_mate(c):
        return remote(
            spot(mate_block, c + half), spot(6 + k, c + half), down_send.at[c], down_recv.at[c],
            me - GROUP,
        )

    def cross(c):
        at = c + half * hi
        return remote(spot(6 + k, at), spot(6 + k, at), cross_send.at[c], cross_recv.at[c], mate)

    def forward(b, c, slot):
        return remote(spot(b, c), spot(b, c), fwd_send.at[slot], fwd_recv.at[slot], partner)

    keep_x = pltpu.make_async_copy(tok_ref, x_out.at[2 + s], keep_sem.at[0])
    keep_c = pltpu.make_async_copy(code_ref, c_out.at[2 + s], keep_sem.at[1])
    keep_w = pltpu.make_async_copy(w_ref.at[s], w_out.at[me], keep_sem.at[2])
    keep_x.start()
    keep_c.start()
    keep_w.start()

    def w_copy(r):
        target = lax.rem(me + r, n_dev)
        return remote(
            w_ref.at[lax.rem(target, GROUP)], w_out.at[me], w_send.at[r], w_recv.at[r], target
        )

    def w_start(r, carry):
        w_copy(r).start()
        return carry

    def c_group(j):
        target = GROUP * g + lax.rem(s + j, GROUP)
        return remote(code_ref, c_out.at[2 + s], c_send.at[j], c_recv.at[2 + s], target)

    def c_far(j):
        step = GROUP * (2 * hi - 1)
        b = 6 + s - 8 * hi
        target = GROUP * g + step + j
        return remote(code_ref, c_out.at[b], c_send.at[GROUP + j], c_recv.at[b], target)

    sends_far = jnp.where(hi == 1, g < n_group - 1, g > 0)
    for j in range(1, GROUP):
        c_group(j).start()

    @pl.when(sends_far)
    def _():
        for j in range(GROUP):
            c_far(j).start()

    order = list(range(half, CHUNKS)) + list(range(half))

    @pl.when((hi == 0) & has_down)
    def _():
        for c in range(half):
            down_own(c).start()

    for n, c in enumerate(order):
        to_mate(c).start()
        to_partner(c).start()
        if n < half:

            @pl.when((hi == 1) & has_up)
            def _():
                up_own(c).start()

        if n == half - 1:
            lax.fori_loop(1, n_dev, w_start, 0)

    for n, c in enumerate(order):
        to_mate(c).wait_recv()
        forward(mate_block, c, c).start()

        @pl.when((hi == 0) & has_up)
        def _():
            up_mate(c).start()

        if n < half:

            @pl.when((hi == 1) & has_down)
            def _():
                down_mate(c - half).start()

        else:

            @pl.when((hi == 1) & has_up)
            def _():
                up_own(c).start()

    def w_wait(r, carry):
        w_copy(r).wait_recv()
        return carry

    lax.fori_loop(1, n_dev, w_wait, 0)
    keep_w.wait()
    keep_x.wait()
    bias_row = jnp.zeros((8, W_LANES), f32)
    bias_at = w_ref.shape[1] - 8
    for j in range(n_dev):
        w_wide[rows_w * j : rows_w * (j + 1), :] = w_out[j, :rows_w, :].astype(f32)
        bias_row = bias_row + w_out[j, bias_at:, :].astype(f32)
    bias_row = jnp.sum(bias_row, axis=0, keepdims=True)
    bias_col = jnp.broadcast_to(bias_row, (128, W_LANES)).T[:, :1]
    w_full[...] = w_wide[...].astype(bf16)
    w_turn[...] = w_wide[...].T.astype(bf16)
    piece = 512
    pieces = tok_ref.shape[0] // piece

    def project(b, inside):
        def one(j, carry):
            x = x_out[b, pl.ds(pl.multiple_of(j * piece, piece), piece), :]
            at = pl.ds(pl.multiple_of((b * pieces + j) * piece, piece), piece)
            kv = mm(x, w_full[:, KV_AT:]) + bias_row[:, KV_AT:]
            kv_sc[at, :] = kv.astype(bf16)
            kvt_sc[:, at] = (mm(w_turn[KV_AT:, :], x, NT) + bias_col[KV_AT:]).astype(bf16)
            if inside:
                to = pl.ds(pl.multiple_of(((b - 2) * pieces + j) * piece, piece), piece)
                q = (mm(w_turn[:Q_ROWS, :], x, NT) + bias_col[:Q_ROWS]).astype(bf16)
                qt_sc[:, to] = q * jnp.asarray(score_scale, bf16)
            return carry

        lax.fori_loop(0, pieces, one, 0)

    def outs(b, inside):
        whole = tok_ref.shape[0]
        at = pl.ds(pl.multiple_of(b * whole, whole), whole)
        copies = [
            pltpu.make_async_copy(kv_sc.at[at], kv_out.at[at], kv_sem.at[b]),
            pltpu.make_async_copy(kvt_sc.at[:, at], kvt_out.at[:, at], kvt_sem.at[b]),
        ]
        if inside:
            to = pl.ds(pl.multiple_of((b - 2) * whole, whole), whole)
            copies.append(pltpu.make_async_copy(qt_sc.at[:, to], qt_out.at[:, to], q_sem.at[b - 2]))
            copies.append(pltpu.make_async_copy(x_out.at[b], x_own.at[b - 2], x_sem.at[b - 2]))
        return copies

    def put(b, inside):
        for copy in outs(b, inside):
            copy.start()

    keep_c.wait()
    for j in range(1, GROUP):
        remote(
            code_ref, c_out.at[0], c_send.at[j], c_recv.at[2 + lax.rem(s + j, GROUP)], partner
        ).wait_recv()

    @pl.when(has_down)
    def _():
        for b in range(2):
            remote(code_ref, c_out.at[b], c_send.at[0], c_recv.at[b], partner).wait_recv()

    @pl.when(has_up)
    def _():
        for b in range(6, 8):
            remote(code_ref, c_out.at[b], c_send.at[0], c_recv.at[b], partner).wait_recv()

    for b in range(8):
        code = c_out[b]
        if b < 2:
            code = jnp.where(has_down, code, -2)
        if b >= 6:
            code = jnp.where(has_up, code, 2 * n_dev * tok_ref.shape[0])
        code_out[b] = code
        tag = jnp.where((code & 1) == 1, (code >> 1) + 1, 0)
        lanes = tag.shape[1]
        for r in range(8):
            turned = jnp.broadcast_to(tag[r : r + 1, :], (lanes, lanes)).T
            at = (8 * b + r) * lanes
            ktag_out[at : at + lanes, :] = turned[:, :1]

    own_block = 2 + s
    near_block = own_block + 1 - 2 * k
    across_block = mate_block + 1 - 2 * k
    project(own_block, True)

    @pl.when(has_up)
    def _():
        for c in range(half):
            down_own(c).wait_recv()
            cross(c).start()
            forward(6 + k, c + half * hi, 2 * CHUNKS + c).start()

    project(mate_block, True)
    put(own_block, True)

    @pl.when(has_down)
    def _():
        for c in order:
            up_own(c).wait_recv()
            forward(k, c, CHUNKS + c).start()

    for c in range(CHUNKS):
        to_partner(c).wait_recv()
    project(near_block, True)
    put(mate_block, True)

    @pl.when(has_up)
    def _():
        for c in range(half):
            cross(c).wait_recv()
            forward(6 + k, c + half * (1 - hi), 2 * CHUNKS + half + c).start()

    for c in range(CHUNKS):
        forward(mate_block, c, c).wait_recv()
    project(across_block, True)
    put(near_block, True)

    @pl.when(has_down)
    def _():
        project(k, False)
        for c in range(CHUNKS):
            forward(k, c, CHUNKS + c).wait_recv()
        project(1 - k, False)
        put(k, False)

    put(across_block, True)

    @pl.when(has_up)
    def _():
        project(6 + k, False)
        for c in range(half):
            forward(6 + k, c, 2 * CHUNKS + c).wait_recv()
            forward(6 + k, c, 2 * CHUNKS + half + c).wait_recv()
        project(7 - k, False)
        put(6 + k, False)

    for c in range(CHUNKS):
        to_partner(c).wait_send()
        to_mate(c).wait_send()
        forward(mate_block, c, c).wait_send()

    @pl.when(has_down)
    def _():
        put(1 - k, False)
        for c in range(CHUNKS):
            forward(k, c, CHUNKS + c).wait_send()
        for c in range(half):
            down_own(c).wait_send()

    @pl.when(has_up)
    def _():
        for c in range(half):
            cross(c).wait_send()
            forward(6 + k, c, 2 * CHUNKS + c).wait_send()
            forward(6 + k, c, 2 * CHUNKS + half + c).wait_send()
        for c in range(CHUNKS):
            up_own(c).wait_send()
        put(7 - k, False)

    for j in range(1, GROUP):
        c_group(j).wait_send()

    @pl.when(sends_far)
    def _():
        for j in range(GROUP):
            c_far(j).wait_send()

    def w_sent(r, carry):
        w_copy(r).wait_send()
        return carry

    lax.fori_loop(1, n_dev, w_sent, 0)
    for b in range(2, 6):
        for copy in outs(b, True):
            copy.wait()

    @pl.when(has_down)
    def _():
        for b in range(2):
            for copy in outs(b, False):
                copy.wait()

    @pl.when(has_up)
    def _():
        for b in range(6, 8):
            for copy in outs(b, False):
                copy.wait()


def share(n_dev, rows_w, tokens, code, w_send):
    vmem = pl.BlockSpec(memory_space=pltpu.VMEM)
    anywhere = pl.BlockSpec(memory_space=pl.ANY)
    dma = lambda n: pltpu.SemaphoreType.DMA((n,))
    half = CHUNKS // 2
    rows, width = tokens.shape
    own, window = GROUP * rows, 8 * rows
    return pl.pallas_call(
        functools.partial(share_kernel, n_dev, rows_w),
        in_specs=[vmem] * 3,
        out_specs=[anywhere, vmem, vmem, vmem, anywhere, anywhere, anywhere],
        out_shape=[
            jax.ShapeDtypeStruct((GROUP, rows, width), bf16),
            jax.ShapeDtypeStruct((8,) + code.shape, code.dtype),
            jax.ShapeDtypeStruct((window, 1), code.dtype),
            jax.ShapeDtypeStruct((W_LANES, width), bf16),
            jax.ShapeDtypeStruct((Q_ROWS, own), bf16),
            jax.ShapeDtypeStruct((window, KV_ROWS), bf16),
            jax.ShapeDtypeStruct((KV_ROWS, window), bf16),
        ],
        scratch_shapes=[
            pltpu.VMEM((8,) + code.shape, code.dtype),
            pltpu.VMEM((8, rows, width), bf16),
            pltpu.VMEM((n_dev,) + w_send.shape[1:], bf16),
            pltpu.VMEM((width, W_LANES), f32),
            pltpu.VMEM((width, W_LANES), bf16),
            pltpu.VMEM((Q_ROWS, own), bf16),
            pltpu.VMEM((window, KV_ROWS), bf16),
            pltpu.VMEM((KV_ROWS, window), bf16),
            dma(n_dev), dma(n_dev), dma(2 * GROUP), dma(8),
            dma(CHUNKS), dma(CHUNKS), dma(CHUNKS), dma(CHUNKS),
            dma(CHUNKS), dma(CHUNKS), dma(half), dma(half), dma(half), dma(half),
            dma(3 * CHUNKS), dma(3 * CHUNKS), dma(3), dma(GROUP), dma(GROUP), dma(8), dma(8),
        ],
        compiler_params=pltpu.CompilerParams(
            collective_id=0, has_side_effects=True, vmem_limit_bytes=60 << 20
        ),
        name="share",
    )(tokens, code, w_send)


PARTS = 4
TN = (((0,), (0,)), ((), ()))


def settle_kernel(
    n_dev, rows_w, q_ref, kv_ref, x_ref, w_ref, vec_ref, own_out, near_out, far_out, w_out, vec_out,
    wide, slabs, across, near, relay, total,
    w_send, w_recv, vec_send, vec_recv, near_send, near_recv, relay_send, relay_recv,
    far_send, far_recv, keep_sem,
):
    me = lax.axis_index("fsdp")
    s = me % GROUP
    k = s % 2
    hi = s // 2
    partner = me + 1 - 2 * k
    mate = me + 2 - 4 * hi
    s_partner = s + 1 - 2 * k
    s_mate = s + 2 - 4 * hi
    s_across = 3 - s
    block = own_out.shape[0]
    rows = block // PARTS

    barrier = pltpu.get_barrier_semaphore()

    def greet(r, carry):
        pl.semaphore_signal(
            barrier, inc=1, device_id=(lax.rem(me + r, n_dev),), device_id_type=MESH
        )
        return carry

    lax.fori_loop(1, n_dev, greet, 0)
    pl.semaphore_wait(barrier, n_dev - 1)

    def part(c):
        return pl.ds(c * rows, rows)

    def to_relay(c):
        return remote(
            across.at[part(c)], relay.at[part(c)], relay_send.at[c], relay_recv.at[c], partner
        )

    def to_near(c):
        return remote(
            near.at[part(c)], near_out.at[part(c)], near_send.at[c], near_recv.at[c], partner
        )

    def to_far(c):
        return remote(total.at[part(c)], far_out.at[part(c)], far_send.at[c], far_recv.at[c], mate)

    def w_copy(r):
        target = lax.rem(me + r, n_dev)
        return remote(slabs.at[target], w_out.at[me], w_send.at[r], w_recv.at[r], target)

    def vec_copy(r):
        target = lax.rem(me + r, n_dev)
        return remote(vec_ref.at[target], vec_out.at[me], vec_send.at[r], vec_recv.at[r], target)

    def vec_start(r, carry):
        vec_copy(r).start()
        return carry

    lax.fori_loop(1, n_dev, vec_start, 0)
    keep_vec = pltpu.make_async_copy(vec_ref.at[me], vec_out.at[me], keep_sem.at[1])
    keep_vec.start()

    def back(t, c):
        at = pl.ds(pl.multiple_of(t * block + c * rows, rows), rows)
        return mm(q_ref[:, at], w_ref[:Q_ROWS, :], TN) + mm(kv_ref[:, at], w_ref[KV_AT:, :], TN)

    def add_rows(j):
        at = slice(j * block, (j + 1) * block)
        wide[:Q_ROWS, :] += mm(q_ref[:, at], x_ref[at, :])
        wide[Q_ROWS:MIX_ROWS, :] += mm(kv_ref[:, at], x_ref[at, :])

    def w_start(r, carry):
        w_copy(r).start()
        return carry

    for c in range(PARTS):
        across[c * rows : (c + 1) * rows, :] = back(s_across, c).astype(bf16)
        if c > 0:
            to_relay(c - 1).start()
    mine = back(s_mate, 0)
    to_relay(PARTS - 1).start()
    wide[...] = jnp.zeros_like(wide)
    for c in range(PARTS):
        to_relay(c).wait_recv()
        other = relay[c * rows : (c + 1) * rows, :].astype(f32)
        total[c * rows : (c + 1) * rows, :] = (mine + other).astype(bf16)
        if c + 1 < PARTS:
            mine = back(s_mate, c + 1)
        else:
            add_rows(0)
        to_far(c).start()
    for j in range(1, GROUP):
        add_rows(j)
    turned = wide[...].T
    one = jnp.ones((8, GROUP * block), bf16)
    bias_q = mm(one, q_ref[...], NT).astype(bf16)
    bias_kv = mm(one, kv_ref[...], NT).astype(bf16)
    bias_at = slabs.shape[1] - 8
    for j in range(n_dev):
        slabs[j, :rows_w, :] = turned[rows_w * j : rows_w * (j + 1), :].astype(bf16)
        slabs[j, bias_at:, :Q_ROWS] = bias_q
        slabs[j, bias_at:, Q_ROWS:MIX_ROWS] = bias_kv
    near[:rows, :] = back(s_partner, 0).astype(bf16)
    lax.fori_loop(1, n_dev, w_start, 0)
    keep_w = pltpu.make_async_copy(slabs.at[me], w_out.at[me], keep_sem.at[0])
    keep_w.start()
    for c in range(1, PARTS):
        near[c * rows : (c + 1) * rows, :] = back(s_partner, c).astype(bf16)
        to_near(c - 1).start()
    for c in range(PARTS):
        own_out[c * rows : (c + 1) * rows, :] = back(s, c)
        if c == 0:
            to_near(PARTS - 1).start()
    for c in range(PARTS):
        to_relay(c).wait_send()
        to_near(c).wait()
        to_far(c).wait()

    def finish(r, carry):
        w_copy(r).wait()
        vec_copy(r).wait()
        return carry

    lax.fori_loop(1, n_dev, finish, 0)
    keep_w.wait()
    keep_vec.wait()


def settle(n_dev, rows_w, d_q, d_kv, x, w, vec):
    vmem = pl.BlockSpec(memory_space=pltpu.VMEM)
    anywhere = pl.BlockSpec(memory_space=pl.ANY)
    dma = lambda n: pltpu.SemaphoreType.DMA((n,))
    block = (x.shape[0] // GROUP, x.shape[1])
    slabs = (n_dev, rows_w + -rows_w % 8 + 8, W_LANES)
    return pl.pallas_call(
        functools.partial(settle_kernel, n_dev, rows_w),
        in_specs=[vmem] * 5,
        out_specs=[vmem] + [anywhere] * 4,
        out_shape=[
            jax.ShapeDtypeStruct(block, f32),
            jax.ShapeDtypeStruct(block, bf16),
            jax.ShapeDtypeStruct(block, bf16),
            jax.ShapeDtypeStruct(slabs, bf16),
            jax.ShapeDtypeStruct(vec.shape, vec.dtype),
        ],
        scratch_shapes=[
            pltpu.VMEM((W_LANES, x.shape[1]), f32),
            pltpu.VMEM(slabs, bf16),
            pltpu.VMEM(block, bf16), pltpu.VMEM(block, bf16),
            pltpu.VMEM(block, bf16), pltpu.VMEM(block, bf16),
            dma(n_dev), dma(n_dev), dma(n_dev), dma(n_dev),
            dma(PARTS), dma(PARTS), dma(PARTS), dma(PARTS), dma(PARTS), dma(PARTS), dma(2),
        ],
        compiler_params=pltpu.CompilerParams(
            collective_id=1, has_side_effects=True, vmem_limit_bytes=60 << 20
        ),
        name="settle",
    )(d_q, d_kv, x, w, vec)


def body(
    n_dev,
    tokens,
    segment_ids,
    pad_mask,
    w_qkv,
    bias_query,
    bias_value,
    w_out,
    bias_out,
    gain_one,
    shift_one,
    w_up,
    bias_up,
    w_down,
    bias_down,
    gain_two,
    shift_two,
    cotangent,
):
    row_count = tokens.shape[0]
    rows_w = w_qkv.shape[0]
    own = GROUP * row_count
    window = own + 2 * LEN_MAX
    me = lax.axis_index("fsdp")
    place = me % GROUP
    group_id = me // GROUP
    n_group = n_dev // GROUP
    up = [(i, i + GROUP) for i in range(n_dev - GROUP)]
    down = [(i + GROUP, i) for i in range(n_dev - GROUP)]
    groups = [[GROUP * g + j for j in range(GROUP)] for g in range(n_group)]

    wq = w_qkv[:, :D].reshape(rows_w, GROUP, Q_ROWS)
    wk = w_qkv[:, D : 2 * D].reshape(rows_w, GROUP, OWN_HEADS, 1, HEAD_DIM)
    wv = w_qkv[:, 2 * D :].reshape(rows_w, GROUP, OWN_HEADS, 1, HEAD_DIM)
    wkv = jnp.concatenate([wk, wv], axis=3).reshape(rows_w, GROUP, KV_ROWS)
    gap = KV_AT - Q_ROWS
    lane = jnp.arange(gap)[None, :]
    small_cols = jnp.pad(bias_up.reshape(rows_w, -1), ((0, 0), (6, gap - 10)))
    for j, v in enumerate([bias_out, gain_one, shift_one, bias_down, gain_two, shift_two]):
        small_cols = jnp.where(lane == j, v[:, None], small_cols)
    small_cols = jnp.broadcast_to(small_cols[:, None], (rows_w, GROUP, gap))
    w_cut = jnp.concatenate([wq, small_cols, wkv], axis=2).transpose(1, 0, 2)
    column = me * rows_w + jnp.arange(rows_w)
    feature = jnp.arange(D)
    spread = lambda bias: jnp.sum(
        jnp.where(feature[None] == column[:, None], bias.astype(f32)[:, None], 0.0), axis=0
    )
    bias_q = spread(bias_query).reshape(GROUP, Q_ROWS)
    bias_v = spread(bias_value).reshape(GROUP, OWN_HEADS, 1, HEAD_DIM)
    bias_kv = jnp.concatenate([jnp.zeros_like(bias_v), bias_v], axis=2).reshape(GROUP, KV_ROWS)
    bias_cut = jnp.concatenate([bias_q, jnp.zeros((GROUP, gap), f32), bias_kv], axis=1)
    fill = -rows_w % 8
    bias_cut = jnp.pad(bias_cut.astype(bf16)[:, None], ((0, 0), (fill, 7), (0, 0)))
    w_send = jnp.concatenate([w_cut, bias_cut], axis=1)
    ff = w_up.shape[1]
    wo_full = lax.all_gather(w_out, "fsdp", axis=0, tiled=True)
    wu_full = lax.all_gather(w_up, "fsdp", axis=0, tiled=True)
    wd_full = lax.all_gather(w_down, "fsdp", axis=0, tiled=True)

    code = (segment_ids * 2 + pad_mask).reshape(8, row_count // 8)
    x_own, code_win, ktag, w_turn, qt, kv, kvt = share(n_dev, rows_w, tokens, code, w_send)
    x_own = x_own.reshape(own, D)
    code_win = code_win.reshape(window)
    code_own = code_win[LEN_MAX : LEN_MAX + own]
    small_all = w_turn[Q_ROWS : Q_ROWS + 10].astype(f32)
    bu_full = small_all[6:].T.reshape(-1)
    bo_full, g1_full, s1_full, bd_full, g2_full, s2_full = [small_all[j] for j in range(6)]
    seg_win = code_win >> 1
    seg_own = code_own >> 1
    qtag = (seg_own + 1).reshape(1, own)
    first_seg = seg_own[::BQ]
    last_seg = seg_own[BQ - 1 :: BQ]
    low = jnp.sum((seg_win[None, :] < first_seg[:, None]).astype(jnp.int32), axis=1)
    high = jnp.sum((seg_win[None, :] <= last_seg[:, None]).astype(jnp.int32), axis=1)
    spans = [jnp.stack([low // b, (high + b - 1) // b], axis=1) for b in (FK, BK)]

    ot, lse = attend(spans[0], qtag, ktag, qt, kv, kvt)
    ctx_t = lax.all_to_all(
        ot.reshape(Q_ROWS, GROUP, row_count), "fsdp", 1, 0, axis_index_groups=groups, tiled=True
    ).reshape(D, row_count)

    tokens_f = tokens.astype(f32)
    branch = jnp.einsum("ir,io->ro", ctx_t, wo_full, preferred_element_type=f32) + bo_full
    first, norm_one_back = jax.vjp(norm_rows, tokens_f + branch, g1_full, s1_full)
    up_in = first.astype(bf16)
    pre_act = jnp.dot(up_in, wu_full, preferred_element_type=f32) + bu_full
    gelu_val, gelu_back = jax.vjp(gelu_exact, pre_act)
    hidden = gelu_val.astype(bf16)
    ffn = jnp.dot(hidden, wd_full, preferred_element_type=f32) + bd_full
    result, norm_two_back = jax.vjp(norm_rows, first + ffn, g2_full, s2_full)
    layer_out = result.astype(bf16)
    d_second, d_gain_two, d_shift_two = norm_two_back(cotangent.astype(f32))
    d_ffn = d_second.astype(bf16)
    d_bias_down = jnp.sum(d_ffn.astype(f32), axis=0)
    d_w_down = jnp.einsum("rf,rd->fd", hidden, d_ffn, preferred_element_type=f32)
    d_hidden = jnp.einsum("rd,fd->rf", d_ffn, wd_full, preferred_element_type=f32)
    d_pre = gelu_back(d_hidden)[0].astype(bf16)
    d_bias_up = jnp.sum(d_pre.astype(f32), axis=0)
    d_w_up = jnp.einsum("rd,rf->df", up_in, d_pre, preferred_element_type=f32).astype(bf16)
    d_w_up = lax.optimization_barrier(d_w_up)
    d_first = d_second + jnp.einsum("rf,df->rd", d_pre, wu_full, preferred_element_type=f32)
    d_mid, d_gain_one, d_shift_one = norm_one_back(d_first)
    d_branch = d_mid.astype(bf16)
    d_bias_out = jnp.sum(d_branch.astype(f32), axis=0)
    d_w_out = jnp.einsum("ir,ro->io", ctx_t, d_branch, preferred_element_type=f32)
    dctx_t = jnp.einsum("ro,io->ir", d_branch, wo_full, preferred_element_type=f32).astype(bf16)
    n_up = ff // D
    big_grad = jnp.concatenate(
        [
            d_w_down.astype(bf16).reshape(n_dev, -1, D),
            d_w_out.astype(bf16).reshape(n_dev, rows_w, D),
        ]
        + [d_w_up[:, D * j : D * (j + 1)].reshape(n_dev, rows_w, D) for j in range(n_up)],
        axis=1,
    )
    big_owned = lax.psum_scatter(big_grad, "fsdp", scatter_dimension=0).astype(f32)
    rows_d = w_down.shape[0]
    g_down, g_out = big_owned[:rows_d], big_owned[rows_d : rows_d + rows_w]
    g_up = jnp.concatenate(
        [big_owned[rows_d + rows_w * (j + 1) : rows_d + rows_w * (j + 2)] for j in range(n_up)], axis=1
    )

    d_out = lax.all_to_all(
        dctx_t.reshape(GROUP, Q_ROWS, row_count), "fsdp", 0, 2, axis_index_groups=groups, tiled=True
    ).reshape(Q_ROWS, own)
    edge, inside = LEN_MAX // BK, own // BK
    far_parts = ((0, edge), (edge + inside, 2 * edge + inside))
    own_parts = ((edge, edge + inside),)
    dq_far, dkv_left, dkv_right = attend_grad(
        far_parts, False, spans[1], qtag, ktag, qt, d_out, ot, lse, kv, kvt
    )
    from_right = lax.ppermute(dkv_left, "fsdp", down)
    from_left = lax.ppermute(dkv_right, "fsdp", up)
    dq_t, dkv_own = attend_grad(
        own_parts, True, spans[1], qtag, ktag, qt, d_out, ot, lse, kv, kvt, dq_far
    )
    dkv = jnp.concatenate(
        [
            dkv_own[:, :LEN_MAX] + from_left.astype(f32),
            dkv_own[:, LEN_MAX : own - LEN_MAX],
            dkv_own[:, own - LEN_MAX :] + from_right.astype(f32),
        ],
        axis=1,
    ).astype(bf16)
    vecs = jnp.stack([d_bias_out, d_gain_one, d_shift_one, d_bias_down, d_gain_two, d_shift_two])
    vec_send = jnp.concatenate(
        [
            vecs.reshape(6, n_dev, rows_w).transpose(1, 0, 2).reshape(n_dev, 6 * rows_w),
            d_bias_up.reshape(n_dev, 4 * rows_w),
        ],
        axis=1,
    )
    vec_send = jnp.pad(vec_send, ((0, 0), (0, 1024 - vec_send.shape[1]))).reshape(n_dev, 8, 128)
    own_x, near, far, w_got, vec_got = settle(n_dev, rows_w, dq_t, dkv, x_own, w_turn, vec_send)
    grad_tokens = d_mid + ((own_x + near.astype(f32)) + far.astype(f32))
    got = jnp.sum(w_got.astype(f32).reshape(n_group, GROUP, -1, W_LANES), axis=0)
    got_q = got[:, :, :Q_ROWS].transpose(1, 0, 2).reshape(-1, D)
    got_kv = got[:, :, Q_ROWS:MIX_ROWS].transpose(1, 0, 2)
    got_kv = got_kv.reshape(-1, GROUP, OWN_HEADS, 2, HEAD_DIM)
    got_k = got_kv[:, :, :, 0].reshape(-1, D)
    got_v = got_kv[:, :, :, 1].reshape(-1, D)
    grad_w_qkv = jnp.concatenate([got_q[:rows_w], got_k[:rows_w], got_v[:rows_w]], axis=1)
    bias_rows = jnp.stack([got_q[-1], got_v[-1]])
    bias_own = lax.dynamic_slice(bias_rows, (0, me * rows_w), (2, rows_w))
    vec = jnp.sum(vec_got, axis=0).reshape(-1)[: 10 * rows_w]
    own_vec = [bias_own[0], bias_own[1]] + [vec[j * rows_w : (j + 1) * rows_w] for j in range(6)]
    return (
        layer_out,
        grad_tokens,
        grad_w_qkv,
        own_vec[0],
        own_vec[1],
        g_out,
        own_vec[2],
        own_vec[3],
        own_vec[4],
        g_up,
        vec[6 * rows_w :],
        g_down,
        own_vec[5],
        own_vec[6],
        own_vec[7],
    )


def solution(mesh):
    rows, flat = P("fsdp", None), P("fsdp")
    return jax.shard_map(
        functools.partial(body, mesh.shape["fsdp"]),
        mesh=mesh,
        in_specs=(
            rows, flat, flat, rows, flat, flat, rows, flat, flat, flat, rows, flat, rows, flat,
            flat, flat, rows,
        ),
        out_specs=(
            rows, rows, rows, flat, flat, rows, flat, flat, flat, rows, flat, rows, flat, flat,
            flat,
        ),
        check_vma=False,
    )
```

```python
import functools

import jax
import jax.numpy as jnp
from jax import lax
from jax.experimental import pallas as pl
from jax.experimental.pallas import tpu as pltpu
from jax.sharding import PartitionSpec as P

D = 768
HEADS = 12
HEAD_DIM = 64
LEN_MAX = 2048
GROUP = 4
OWN_HEADS = HEADS // GROUP
Q_ROWS = OWN_HEADS * HEAD_DIM
KV_ROWS = 2 * Q_ROWS
MIX_ROWS = Q_ROWS + KV_ROWS
BQ = 512
FK = 512
BK = 256
NEG = -1e30

bf16 = jnp.bfloat16
f32 = jnp.float32
eps_norm = 1e-12
score_scale = 0.125

NN = (((1,), (0,)), ((), ()))
NT = (((1,), (1,)), ((), ()))


def mm(a, b, dims=NN):
    return lax.dot_general(a, b, dims, preferred_element_type=f32)


def norm_rows(hidden, gain_row, shift_row):
    centre = hidden - jnp.mean(hidden, axis=-1, keepdims=True)
    spread = jnp.mean(centre * centre, axis=-1, keepdims=True)
    return centre * lax.rsqrt(spread + eps_norm) * gain_row + shift_row


def gelu_exact(pre_act):
    return 0.5 * pre_act * (1.0 + jax.scipy.special.erf(pre_act * 0.7071067811865476))


def head_rows(block, h, upper):
    zero = jnp.zeros_like(block[:HEAD_DIM])
    rows = block[h * HEAD_DIM : (h + 1) * HEAD_DIM]
    return jnp.concatenate([zero, rows] if upper else [rows, zero], axis=0)


def attend_kernel(
    span, qtag_ref, ktag_ref, qt_ref, kv_ref, kvt_ref, ot_ref, lse_ref, m_sc, l_sc, acc_sc
):
    i = pl.program_id(0)
    m_sc[...] = jnp.full_like(m_sc, NEG)
    l_sc[...] = jnp.zeros_like(l_sc)
    acc_sc[...] = jnp.zeros_like(acc_sc)
    qtag = qtag_ref[...]
    qt = qt_ref[...]
    q_pad = [head_rows(qt, h, False) for h in range(OWN_HEADS)]

    def step(kb, carry):
        rows = pl.ds(pl.multiple_of(kb * FK, FK), FK)
        seen = ktag_ref[rows, :] == qtag
        hs = range(OWN_HEADS)
        s = [mm(kv_ref[rows, 128 * h : 128 * (h + 1)], q_pad[h]) for h in hs]
        s = [jnp.where(seen, v, NEG) for v in s]
        m_old = [m_sc[h : h + 1, :] for h in hs]
        l_old = [l_sc[h : h + 1, :] for h in hs]
        m_new = [jnp.maximum(m_old[h], jnp.max(s[h], axis=0, keepdims=True)) for h in hs]
        p = [jnp.exp(s[h] - m_new[h]).astype(bf16) for h in hs]
        fade = [jnp.exp(m_old[h] - m_new[h]) for h in hs]
        one = jnp.ones((16, FK), bf16)
        v_one = [
            jnp.concatenate([kvt_ref[128 * h + HEAD_DIM : 128 * (h + 1), rows], one], axis=0)
            for h in hs
        ]
        out = [mm(v_one[h], p[h]) for h in hs]
        for h in hs:
            own = slice(HEAD_DIM * h, HEAD_DIM * (h + 1))
            acc_sc[own, :] = acc_sc[own, :] * fade[h] + out[h][:HEAD_DIM]
            l_sc[h : h + 1, :] = fade[h] * l_old[h] + out[h][HEAD_DIM : HEAD_DIM + 1]
            m_sc[h : h + 1, :] = m_new[h]
        return carry

    lax.fori_loop(span[i, 0], span[i, 1], step, 0)
    for h in range(OWN_HEADS):
        own = slice(HEAD_DIM * h, HEAD_DIM * (h + 1))
        total = l_sc[h : h + 1, :]
        ot_ref[own, :] = (acc_sc[own, :] / total).astype(bf16)
        lse_ref[h : h + 1, :] = m_sc[h : h + 1, :] + jnp.log(total)
    lse_ref[OWN_HEADS:, :] = jnp.zeros_like(lse_ref[OWN_HEADS:, :])


def attend(span, qtag, ktag, qt, kv, kvt):
    own = qt.shape[1]
    window = kv.shape[0]
    whole = lambda shape: pl.BlockSpec(shape, lambda i, s: (0, 0), pipeline_mode=pl.Buffered(1))
    cols = lambda rows: pl.BlockSpec((rows, BQ), lambda i, s: (0, i))
    return pl.pallas_call(
        attend_kernel,
        grid_spec=pltpu.PrefetchScalarGridSpec(
            num_scalar_prefetch=1,
            grid=(own // BQ,),
            in_specs=[
                cols(1),
                whole((window, 1)),
                cols(Q_ROWS),
                whole((window, KV_ROWS)),
                whole((KV_ROWS, window)),
            ],
            out_specs=[cols(Q_ROWS), cols(8)],
            scratch_shapes=[
                pltpu.VMEM((8, BQ), f32),
                pltpu.VMEM((8, BQ), f32),
                pltpu.VMEM((Q_ROWS, BQ), f32),
            ],
        ),
        out_shape=[
            jax.ShapeDtypeStruct((Q_ROWS, own), bf16),
            jax.ShapeDtypeStruct((8, own), f32),
        ],
        compiler_params=pltpu.CompilerParams(vmem_limit_bytes=60 << 20),
        cost_estimate=pl.CostEstimate(
            flops=4 * own * 2048 * Q_ROWS, bytes_accessed=20 << 20, transcendentals=own * 6144
        ),
        name="attend",
    )(span, qtag, ktag, qt, kv, kvt)


def grad_kernel(
    parts, final, span, qtag_ref, ktag_ref, qt_ref, dot_ref, ot_ref, lse_ref, kv_ref, kvt_ref, *rest
):
    if final:
        dq_in, dq_ref, *rest = rest
    else:
        dq_in, (dq_ref, *rest) = None, rest
    outs, (dq_sc, dkv_sc) = rest[: len(parts)], rest[len(parts) :]
    i = pl.program_id(0)

    @pl.when(i == 0)
    def _():
        dkv_sc[...] = jnp.zeros_like(dkv_sc)

    if final:
        dq_sc[...] = dq_in[...]
    else:
        dq_sc[...] = jnp.zeros_like(dq_sc)
    qtag = qtag_ref[...]
    qt, d_out, out = qt_ref[...], dot_ref[...], ot_ref[...]
    q_pad = [head_rows(qt, h, False) for h in range(OWN_HEADS)]
    d_pad = [head_rows(d_out, h, True) for h in range(OWN_HEADS)]
    product = d_out.astype(f32) * out.astype(f32)
    inner = [
        jnp.sum(product[HEAD_DIM * h : HEAD_DIM * (h + 1)], axis=0, keepdims=True)
        for h in range(OWN_HEADS)
    ]
    log_row = [lse_ref[h : h + 1, :] for h in range(OWN_HEADS)]

    def step(shift, kb, carry):
        rows = pl.ds(pl.multiple_of(kb * BK, BK), BK)
        place = pl.ds(pl.multiple_of((kb - shift) * BK, BK), BK)
        seen = ktag_ref[rows, :] == qtag
        hs = range(OWN_HEADS)
        kv = [kv_ref[rows, 128 * h : 128 * (h + 1)] for h in hs]
        s = [mm(kv[h], q_pad[h]) for h in hs]
        d_p = [mm(kv[h], d_pad[h]) for h in hs]
        p = [jnp.where(seen, jnp.exp(s[h] - log_row[h]), 0.0) for h in hs]
        d_s = [(p[h] * (d_p[h] - inner[h])).astype(bf16) for h in hs]
        p = [v.astype(bf16) for v in p]
        g_kv = [mm(q_pad[h], d_s[h], NT) + mm(d_pad[h], p[h], NT) for h in hs]
        g_q = [mm(kvt_ref[128 * h : 128 * h + HEAD_DIM, rows], d_s[h]) for h in hs]
        for h in hs:
            dkv_sc[128 * h : 128 * (h + 1), place] += g_kv[h]
            own = slice(HEAD_DIM * h, HEAD_DIM * (h + 1))
            dq_sc[own, :] += g_q[h]
        return carry

    base = 0
    for n, (first, last) in enumerate(parts):
        low = jnp.maximum(span[i, 0], first)
        high = jnp.minimum(span[i, 1], last)
        lax.fori_loop(low, high, functools.partial(step, first - base), 0)
        base += last - first
    if final:
        dq_ref[...] = (dq_sc[...] * score_scale).astype(bf16)
    else:
        dq_ref[...] = dq_sc[...]

    @pl.when(i == pl.num_programs(0) - 1)
    def _():
        base = 0
        for (first, last), ref in zip(parts, outs):
            width = (last - first) * BK
            ref[...] = dkv_sc[:, base : base + width].astype(ref.dtype)
            base += width


def attend_grad(parts, final, span, qtag, ktag, qt, d_out, out, lse, kv, kvt, dq_in=None):
    own = qt.shape[1]
    window = kv.shape[0]
    whole = lambda shape: pl.BlockSpec(shape, lambda i, s: (0, 0), pipeline_mode=pl.Buffered(1))
    cols = lambda rows: pl.BlockSpec((rows, BQ), lambda i, s: (0, i))
    widths = [(last - first) * BK for first, last in parts]
    dtype = f32 if final else bf16
    args = [span, qtag, ktag, qt, d_out, out, lse, kv, kvt] + ([dq_in] if final else [])
    return pl.pallas_call(
        functools.partial(grad_kernel, parts, final),
        grid_spec=pltpu.PrefetchScalarGridSpec(
            num_scalar_prefetch=1,
            grid=(own // BQ,),
            in_specs=[
                cols(1),
                whole((window, 1)),
                cols(Q_ROWS),
                cols(Q_ROWS),
                cols(Q_ROWS),
                cols(8),
                whole((window, KV_ROWS)),
                whole((KV_ROWS, window)),
            ]
            + ([cols(Q_ROWS)] if final else []),
            out_specs=[cols(Q_ROWS)] + [whole((KV_ROWS, w)) for w in widths],
            scratch_shapes=[
                pltpu.VMEM((Q_ROWS, BQ), f32),
                pltpu.VMEM((KV_ROWS, sum(widths)), f32),
            ],
        ),
        out_shape=[jax.ShapeDtypeStruct((Q_ROWS, own), bf16 if final else f32)]
        + [jax.ShapeDtypeStruct((KV_ROWS, w), dtype) for w in widths],
        compiler_params=pltpu.CompilerParams(vmem_limit_bytes=60 << 20),
        cost_estimate=pl.CostEstimate(
            flops=(10 if final else 2) * own * 1536 * Q_ROWS,
            bytes_accessed=20 << 20,
            transcendentals=own * 4096,
        ),
        name="grad_own" if final else "grad_far",
    )(*args)


MESH = pl.DeviceIdType.MESH
CHUNKS = 8
W_LANES = 640
KV_AT = 256


def remote(src, dst, send, recv, target):
    return pltpu.make_async_remote_copy(
        src_ref=src,
        dst_ref=dst,
        send_sem=send,
        recv_sem=recv,
        device_id=(target,),
        device_id_type=MESH,
    )


def share_kernel(
    n_dev, rows_w, tok_ref, code_ref, w_ref, x_own, code_out, ktag_out, w_turn, qt_out, kv_out, kvt_out,
    c_out, x_out, w_out, w_wide, w_full, qt_sc, kv_sc, kvt_sc,
    w_send, w_recv, c_send, c_recv, part_send, part_recv, mate_send, mate_recv,
    up_send, up_recv, down_send, down_recv, cross_send, cross_recv,
    fwd_send, fwd_recv, keep_sem, x_sem, q_sem, kv_sem, kvt_sem,
):
    n_group = n_dev // GROUP
    me = lax.axis_index("fsdp")
    g = me // GROUP
    s = me % GROUP
    k = s % 2
    hi = s // 2
    partner = me + 1 - 2 * k
    mate = me + 2 - 4 * hi
    mate_block = 4 + k - 2 * hi
    has_up = g < n_group - 1
    has_down = g > 0
    rows = tok_ref.shape[0] // CHUNKS
    half = CHUNKS // 2

    barrier = pltpu.get_barrier_semaphore()

    def greet(r, carry):
        pl.semaphore_signal(
            barrier, inc=1, device_id=(lax.rem(me + r, n_dev),), device_id_type=MESH
        )
        return carry

    lax.fori_loop(1, n_dev, greet, 0)
    pl.semaphore_wait(barrier, n_dev - 1)

    def chunk(ref, c):
        return ref.at[pl.ds(pl.multiple_of(c * rows, rows), rows)]

    def spot(b, c):
        return x_out.at[b, pl.ds(pl.multiple_of(c * rows, rows), rows)]

    def to_partner(c):
        return remote(chunk(tok_ref, c), spot(2 + s, c), part_send.at[c], part_recv.at[c], partner)

    def to_mate(c):
        return remote(chunk(tok_ref, c), spot(2 + s, c), mate_send.at[c], mate_recv.at[c], mate)

    def up_own(c):
        return remote(chunk(tok_ref, c), spot(k, c), up_send.at[c], up_recv.at[c], me + GROUP)

    def up_mate(c):
        return remote(spot(mate_block, c), spot(k, c), up_send.at[c], up_recv.at[c], me + GROUP)

    def down_own(c):
        return remote(
            chunk(tok_ref, c), spot(6 + k, c), down_send.at[c], down_recv.at[c], me - GROUP
        )

    def down_mate(c):
        return remote(
            spot(mate_block, c + half), spot(6 + k, c + half), down_send.at[c], down_recv.at[c],
            me - GROUP,
        )

    def cross(c):
        at = c + half * hi
        return remote(spot(6 + k, at), spot(6 + k, at), cross_send.at[c], cross_recv.at[c], mate)

    def forward(b, c, slot):
        return remote(spot(b, c), spot(b, c), fwd_send.at[slot], fwd_recv.at[slot], partner)

    keep_x = pltpu.make_async_copy(tok_ref, x_out.at[2 + s], keep_sem.at[0])
    keep_c = pltpu.make_async_copy(code_ref, c_out.at[2 + s], keep_sem.at[1])
    keep_w = pltpu.make_async_copy(w_ref.at[s], w_out.at[me], keep_sem.at[2])
    keep_x.start()
    keep_c.start()
    keep_w.start()

    def w_copy(r):
        target = lax.rem(me + r, n_dev)
        return remote(
            w_ref.at[lax.rem(target, GROUP)], w_out.at[me], w_send.at[r], w_recv.at[r], target
        )

    def w_start(r, carry):
        w_copy(r).start()
        return carry

    def c_group(j):
        target = GROUP * g + lax.rem(s + j, GROUP)
        return remote(code_ref, c_out.at[2 + s], c_send.at[j], c_recv.at[2 + s], target)

    def c_far(j):
        step = GROUP * (2 * hi - 1)
        b = 6 + s - 8 * hi
        target = GROUP * g + step + j
        return remote(code_ref, c_out.at[b], c_send.at[GROUP + j], c_recv.at[b], target)

    sends_far = jnp.where(hi == 1, g < n_group - 1, g > 0)
    for j in range(1, GROUP):
        c_group(j).start()

    @pl.when(sends_far)
    def _():
        for j in range(GROUP):
            c_far(j).start()

    order = list(range(half, CHUNKS)) + list(range(half))

    @pl.when((hi == 0) & has_down)
    def _():
        for c in range(half):
            down_own(c).start()

    for n, c in enumerate(order):
        to_mate(c).start()
        to_partner(c).start()
        if n < half:

            @pl.when((hi == 1) & has_up)
            def _():
                up_own(c).start()

        if n == half - 1:
            lax.fori_loop(1, n_dev, w_start, 0)

    for n, c in enumerate(order):
        to_mate(c).wait_recv()
        forward(mate_block, c, c).start()

        @pl.when((hi == 0) & has_up)
        def _():
            up_mate(c).start()

        if n < half:

            @pl.when((hi == 1) & has_down)
            def _():
                down_mate(c - half).start()

        else:

            @pl.when((hi == 1) & has_up)
            def _():
                up_own(c).start()

    def w_wait(r, carry):
        w_copy(r).wait_recv()
        return carry

    lax.fori_loop(1, n_dev, w_wait, 0)
    keep_w.wait()
    keep_x.wait()
    bias_row = jnp.zeros((8, W_LANES), f32)
    bias_at = w_ref.shape[1] - 8
    for j in range(n_dev):
        w_wide[rows_w * j : rows_w * (j + 1), :] = w_out[j, :rows_w, :].astype(f32)
        bias_row = bias_row + w_out[j, bias_at:, :].astype(f32)
    bias_row = jnp.sum(bias_row, axis=0, keepdims=True)
    bias_col = jnp.broadcast_to(bias_row, (128, W_LANES)).T[:, :1]
    w_full[...] = w_wide[...].astype(bf16)
    w_turn[...] = w_wide[...].T.astype(bf16)
    piece = 512
    pieces = tok_ref.shape[0] // piece

    def project(b, inside):
        def one(j, carry):
            x = x_out[b, pl.ds(pl.multiple_of(j * piece, piece), piece), :]
            at = pl.ds(pl.multiple_of((b * pieces + j) * piece, piece), piece)
            kv = mm(x, w_full[:, KV_AT:]) + bias_row[:, KV_AT:]
            kv_sc[at, :] = kv.astype(bf16)
            kvt_sc[:, at] = (mm(w_turn[KV_AT:, :], x, NT) + bias_col[KV_AT:]).astype(bf16)
            if inside:
                to = pl.ds(pl.multiple_of(((b - 2) * pieces + j) * piece, piece), piece)
                q = (mm(w_turn[:Q_ROWS, :], x, NT) + bias_col[:Q_ROWS]).astype(bf16)
                qt_sc[:, to] = q * jnp.asarray(score_scale, bf16)
            return carry

        lax.fori_loop(0, pieces, one, 0)

    def outs(b, inside):
        whole = tok_ref.shape[0]
        at = pl.ds(pl.multiple_of(b * whole, whole), whole)
        copies = [
            pltpu.make_async_copy(kv_sc.at[at], kv_out.at[at], kv_sem.at[b]),
            pltpu.make_async_copy(kvt_sc.at[:, at], kvt_out.at[:, at], kvt_sem.at[b]),
        ]
        if inside:
            to = pl.ds(pl.multiple_of((b - 2) * whole, whole), whole)
            copies.append(pltpu.make_async_copy(qt_sc.at[:, to], qt_out.at[:, to], q_sem.at[b - 2]))
            copies.append(pltpu.make_async_copy(x_out.at[b], x_own.at[b - 2], x_sem.at[b - 2]))
        return copies

    def put(b, inside):
        for copy in outs(b, inside):
            copy.start()

    keep_c.wait()
    for j in range(1, GROUP):
        remote(
            code_ref, c_out.at[0], c_send.at[j], c_recv.at[2 + lax.rem(s + j, GROUP)], partner
        ).wait_recv()

    @pl.when(has_down)
    def _():
        for b in range(2):
            remote(code_ref, c_out.at[b], c_send.at[0], c_recv.at[b], partner).wait_recv()

    @pl.when(has_up)
    def _():
        for b in range(6, 8):
            remote(code_ref, c_out.at[b], c_send.at[0], c_recv.at[b], partner).wait_recv()

    for b in range(8):
        code = c_out[b]
        if b < 2:
            code = jnp.where(has_down, code, -2)
        if b >= 6:
            code = jnp.where(has_up, code, 2 * n_dev * tok_ref.shape[0])
        code_out[b] = code
        tag = jnp.where((code & 1) == 1, (code >> 1) + 1, 0)
        lanes = tag.shape[1]
        for r in range(8):
            turned = jnp.broadcast_to(tag[r : r + 1, :], (lanes, lanes)).T
            at = (8 * b + r) * lanes
            ktag_out[at : at + lanes, :] = turned[:, :1]

    own_block = 2 + s
    near_block = own_block + 1 - 2 * k
    across_block = mate_block + 1 - 2 * k
    project(own_block, True)

    @pl.when(has_up)
    def _():
        for c in range(half):
            down_own(c).wait_recv()
            cross(c).start()
            forward(6 + k, c + half * hi, 2 * CHUNKS + c).start()

    project(mate_block, True)
    put(own_block, True)

    @pl.when(has_down)
    def _():
        for c in order:
            up_own(c).wait_recv()
            forward(k, c, CHUNKS + c).start()

    for c in range(CHUNKS):
        to_partner(c).wait_recv()
    project(near_block, True)
    put(mate_block, True)

    @pl.when(has_up)
    def _():
        for c in range(half):
            cross(c).wait_recv()
            forward(6 + k, c + half * (1 - hi), 2 * CHUNKS + half + c).start()

    for c in range(CHUNKS):
        forward(mate_block, c, c).wait_recv()
    project(across_block, True)
    put(near_block, True)

    @pl.when(has_down)
    def _():
        project(k, False)
        for c in range(CHUNKS):
            forward(k, c, CHUNKS + c).wait_recv()
        project(1 - k, False)
        put(k, False)

    put(across_block, True)

    @pl.when(has_up)
    def _():
        project(6 + k, False)
        for c in range(half):
            forward(6 + k, c, 2 * CHUNKS + c).wait_recv()
            forward(6 + k, c, 2 * CHUNKS + half + c).wait_recv()
        project(7 - k, False)
        put(6 + k, False)

    for c in range(CHUNKS):
        to_partner(c).wait_send()
        to_mate(c).wait_send()
        forward(mate_block, c, c).wait_send()

    @pl.when(has_down)
    def _():
        put(1 - k, False)
        for c in range(CHUNKS):
            forward(k, c, CHUNKS + c).wait_send()
        for c in range(half):
            down_own(c).wait_send()

    @pl.when(has_up)
    def _():
        for c in range(half):
            cross(c).wait_send()
            forward(6 + k, c, 2 * CHUNKS + c).wait_send()
            forward(6 + k, c, 2 * CHUNKS + half + c).wait_send()
        for c in range(CHUNKS):
            up_own(c).wait_send()
        put(7 - k, False)

    for j in range(1, GROUP):
        c_group(j).wait_send()

    @pl.when(sends_far)
    def _():
        for j in range(GROUP):
            c_far(j).wait_send()

    def w_sent(r, carry):
        w_copy(r).wait_send()
        return carry

    lax.fori_loop(1, n_dev, w_sent, 0)
    for b in range(2, 6):
        for copy in outs(b, True):
            copy.wait()

    @pl.when(has_down)
    def _():
        for b in range(2):
            for copy in outs(b, False):
                copy.wait()

    @pl.when(has_up)
    def _():
        for b in range(6, 8):
            for copy in outs(b, False):
                copy.wait()


def share(n_dev, rows_w, tokens, code, w_send):
    vmem = pl.BlockSpec(memory_space=pltpu.VMEM)
    anywhere = pl.BlockSpec(memory_space=pl.ANY)
    dma = lambda n: pltpu.SemaphoreType.DMA((n,))
    half = CHUNKS // 2
    rows, width = tokens.shape
    own, window = GROUP * rows, 8 * rows
    return pl.pallas_call(
        functools.partial(share_kernel, n_dev, rows_w),
        in_specs=[vmem] * 3,
        out_specs=[anywhere, vmem, vmem, vmem, anywhere, anywhere, anywhere],
        out_shape=[
            jax.ShapeDtypeStruct((GROUP, rows, width), bf16),
            jax.ShapeDtypeStruct((8,) + code.shape, code.dtype),
            jax.ShapeDtypeStruct((window, 1), code.dtype),
            jax.ShapeDtypeStruct((W_LANES, width), bf16),
            jax.ShapeDtypeStruct((Q_ROWS, own), bf16),
            jax.ShapeDtypeStruct((window, KV_ROWS), bf16),
            jax.ShapeDtypeStruct((KV_ROWS, window), bf16),
        ],
        scratch_shapes=[
            pltpu.VMEM((8,) + code.shape, code.dtype),
            pltpu.VMEM((8, rows, width), bf16),
            pltpu.VMEM((n_dev,) + w_send.shape[1:], bf16),
            pltpu.VMEM((width, W_LANES), f32),
            pltpu.VMEM((width, W_LANES), bf16),
            pltpu.VMEM((Q_ROWS, own), bf16),
            pltpu.VMEM((window, KV_ROWS), bf16),
            pltpu.VMEM((KV_ROWS, window), bf16),
            dma(n_dev), dma(n_dev), dma(2 * GROUP), dma(8),
            dma(CHUNKS), dma(CHUNKS), dma(CHUNKS), dma(CHUNKS),
            dma(CHUNKS), dma(CHUNKS), dma(half), dma(half), dma(half), dma(half),
            dma(3 * CHUNKS), dma(3 * CHUNKS), dma(3), dma(GROUP), dma(GROUP), dma(8), dma(8),
        ],
        compiler_params=pltpu.CompilerParams(
            collective_id=0, has_side_effects=True, vmem_limit_bytes=60 << 20
        ),
        name="share",
    )(tokens, code, w_send)


PARTS = 4
TN = (((0,), (0,)), ((), ()))


def settle_kernel(
    n_dev, rows_w, q_ref, kv_ref, x_ref, w_ref, vec_ref, own_out, near_out, far_out, w_out, vec_out,
    wide, slabs, across, near, relay, total,
    w_send, w_recv, vec_send, vec_recv, near_send, near_recv, relay_send, relay_recv,
    far_send, far_recv, keep_sem,
):
    me = lax.axis_index("fsdp")
    s = me % GROUP
    k = s % 2
    hi = s // 2
    partner = me + 1 - 2 * k
    mate = me + 2 - 4 * hi
    s_partner = s + 1 - 2 * k
    s_mate = s + 2 - 4 * hi
    s_across = 3 - s
    block = own_out.shape[0]
    rows = block // PARTS

    barrier = pltpu.get_barrier_semaphore()

    def greet(r, carry):
        pl.semaphore_signal(
            barrier, inc=1, device_id=(lax.rem(me + r, n_dev),), device_id_type=MESH
        )
        return carry

    lax.fori_loop(1, n_dev, greet, 0)
    pl.semaphore_wait(barrier, n_dev - 1)

    def part(c):
        return pl.ds(c * rows, rows)

    def to_relay(c):
        return remote(
            across.at[part(c)], relay.at[part(c)], relay_send.at[c], relay_recv.at[c], partner
        )

    def to_near(c):
        return remote(
            near.at[part(c)], near_out.at[part(c)], near_send.at[c], near_recv.at[c], partner
        )

    def to_far(c):
        return remote(total.at[part(c)], far_out.at[part(c)], far_send.at[c], far_recv.at[c], mate)

    def w_copy(r):
        target = lax.rem(me + r, n_dev)
        return remote(slabs.at[target], w_out.at[me], w_send.at[r], w_recv.at[r], target)

    def vec_copy(r):
        target = lax.rem(me + r, n_dev)
        return remote(vec_ref.at[target], vec_out.at[me], vec_send.at[r], vec_recv.at[r], target)

    def vec_start(r, carry):
        vec_copy(r).start()
        return carry

    lax.fori_loop(1, n_dev, vec_start, 0)
    keep_vec = pltpu.make_async_copy(vec_ref.at[me], vec_out.at[me], keep_sem.at[1])
    keep_vec.start()

    def back(t, c):
        at = pl.ds(pl.multiple_of(t * block + c * rows, rows), rows)
        return mm(q_ref[:, at], w_ref[:Q_ROWS, :], TN) + mm(kv_ref[:, at], w_ref[KV_AT:, :], TN)

    def add_rows(j):
        at = slice(j * block, (j + 1) * block)
        wide[:Q_ROWS, :] += mm(q_ref[:, at], x_ref[at, :])
        wide[Q_ROWS:MIX_ROWS, :] += mm(kv_ref[:, at], x_ref[at, :])

    def w_start(r, carry):
        w_copy(r).start()
        return carry

    for c in range(PARTS):
        across[c * rows : (c + 1) * rows, :] = back(s_across, c).astype(bf16)
        if c > 0:
            to_relay(c - 1).start()
    mine = back(s_mate, 0)
    to_relay(PARTS - 1).start()
    wide[...] = jnp.zeros_like(wide)
    for c in range(PARTS):
        to_relay(c).wait_recv()
        other = relay[c * rows : (c + 1) * rows, :].astype(f32)
        total[c * rows : (c + 1) * rows, :] = (mine + other).astype(bf16)
        if c + 1 < PARTS:
            mine = back(s_mate, c + 1)
        else:
            add_rows(0)
        to_far(c).start()
    for j in range(1, GROUP):
        add_rows(j)
    turned = wide[...].T
    one = jnp.ones((8, GROUP * block), bf16)
    bias_q = mm(one, q_ref[...], NT).astype(bf16)
    bias_kv = mm(one, kv_ref[...], NT).astype(bf16)
    bias_at = slabs.shape[1] - 8
    for j in range(n_dev):
        slabs[j, :rows_w, :] = turned[rows_w * j : rows_w * (j + 1), :].astype(bf16)
        slabs[j, bias_at:, :Q_ROWS] = bias_q
        slabs[j, bias_at:, Q_ROWS:MIX_ROWS] = bias_kv
    near[:rows, :] = back(s_partner, 0).astype(bf16)
    lax.fori_loop(1, n_dev, w_start, 0)
    keep_w = pltpu.make_async_copy(slabs.at[me], w_out.at[me], keep_sem.at[0])
    keep_w.start()
    for c in range(1, PARTS):
        near[c * rows : (c + 1) * rows, :] = back(s_partner, c).astype(bf16)
        to_near(c - 1).start()
    for c in range(PARTS):
        own_out[c * rows : (c + 1) * rows, :] = back(s, c)
        if c == 0:
            to_near(PARTS - 1).start()
    for c in range(PARTS):
        to_relay(c).wait_send()
        to_near(c).wait()
        to_far(c).wait()

    def finish(r, carry):
        w_copy(r).wait()
        vec_copy(r).wait()
        return carry

    lax.fori_loop(1, n_dev, finish, 0)
    keep_w.wait()
    keep_vec.wait()


def settle(n_dev, rows_w, d_q, d_kv, x, w, vec):
    vmem = pl.BlockSpec(memory_space=pltpu.VMEM)
    anywhere = pl.BlockSpec(memory_space=pl.ANY)
    dma = lambda n: pltpu.SemaphoreType.DMA((n,))
    block = (x.shape[0] // GROUP, x.shape[1])
    slabs = (n_dev, rows_w + -rows_w % 8 + 8, W_LANES)
    return pl.pallas_call(
        functools.partial(settle_kernel, n_dev, rows_w),
        in_specs=[vmem] * 5,
        out_specs=[vmem] + [anywhere] * 4,
        out_shape=[
            jax.ShapeDtypeStruct(block, f32),
            jax.ShapeDtypeStruct(block, bf16),
            jax.ShapeDtypeStruct(block, bf16),
            jax.ShapeDtypeStruct(slabs, bf16),
            jax.ShapeDtypeStruct(vec.shape, vec.dtype),
        ],
        scratch_shapes=[
            pltpu.VMEM((W_LANES, x.shape[1]), f32),
            pltpu.VMEM(slabs, bf16),
            pltpu.VMEM(block, bf16), pltpu.VMEM(block, bf16),
            pltpu.VMEM(block, bf16), pltpu.VMEM(block, bf16),
            dma(n_dev), dma(n_dev), dma(n_dev), dma(n_dev),
            dma(PARTS), dma(PARTS), dma(PARTS), dma(PARTS), dma(PARTS), dma(PARTS), dma(2),
        ],
        compiler_params=pltpu.CompilerParams(
            collective_id=1, has_side_effects=True, vmem_limit_bytes=60 << 20
        ),
        name="settle",
    )(d_q, d_kv, x, w, vec)


def swap_kernel(spread, in_ref, out_ref, send, recv, keep_sem):
    me = lax.axis_index("fsdp")
    s = me % GROUP
    start = me - s
    width = (in_ref if spread else out_ref).shape[1] // GROUP

    barrier = pltpu.get_barrier_semaphore()
    for j in range(1, GROUP):
        target = start + lax.rem(s + j, GROUP)
        pl.semaphore_signal(barrier, inc=1, device_id=(target,), device_id_type=MESH)
    pl.semaphore_wait(barrier, GROUP - 1)

    def cols(ref, t):
        return ref.at[:, pl.ds(pl.multiple_of(t * width, width), width)]

    def rows(ref, t):
        return ref.at[pl.ds(pl.multiple_of(t * Q_ROWS, Q_ROWS), Q_ROWS)]

    def ends(t):
        if spread:
            return cols(in_ref, t), rows(out_ref, s)
        return rows(in_ref, t), cols(out_ref, s)

    def copy(j):
        t = lax.rem(s + j, GROUP)
        src, dst = ends(t)
        return remote(src, dst, send.at[j], recv.at[j], start + t)

    for j in (2, 1, 3):
        copy(j).start()
    src, dst = ends(s)
    keep = pltpu.make_async_copy(src, dst, keep_sem.at[0])
    keep.start()
    for j in range(1, GROUP):
        copy(j).wait()
    keep.wait()


def swap(x, spread):
    shape = (x.shape[0] * GROUP, x.shape[1] // GROUP) if spread else (
        x.shape[0] // GROUP, x.shape[1] * GROUP
    )
    dma = lambda n: pltpu.SemaphoreType.DMA((n,))
    return pl.pallas_call(
        functools.partial(swap_kernel, spread),
        in_specs=[pl.BlockSpec(memory_space=pltpu.VMEM)],
        out_specs=pl.BlockSpec(memory_space=pltpu.VMEM),
        out_shape=jax.ShapeDtypeStruct(shape, x.dtype),
        scratch_shapes=[dma(GROUP), dma(GROUP), dma(1)],
        compiler_params=pltpu.CompilerParams(
            collective_id=2 if spread else 3, has_side_effects=True
        ),
        name="swap_out" if spread else "swap_back",
    )(x)


def body(
    n_dev,
    tokens,
    segment_ids,
    pad_mask,
    w_qkv,
    bias_query,
    bias_value,
    w_out,
    bias_out,
    gain_one,
    shift_one,
    w_up,
    bias_up,
    w_down,
    bias_down,
    gain_two,
    shift_two,
    cotangent,
):
    row_count = tokens.shape[0]
    rows_w = w_qkv.shape[0]
    own = GROUP * row_count
    window = own + 2 * LEN_MAX
    me = lax.axis_index("fsdp")
    place = me % GROUP
    group_id = me // GROUP
    n_group = n_dev // GROUP
    up = [(i, i + GROUP) for i in range(n_dev - GROUP)]
    down = [(i + GROUP, i) for i in range(n_dev - GROUP)]

    wq = w_qkv[:, :D].reshape(rows_w, GROUP, Q_ROWS)
    wk = w_qkv[:, D : 2 * D].reshape(rows_w, GROUP, OWN_HEADS, 1, HEAD_DIM)
    wv = w_qkv[:, 2 * D :].reshape(rows_w, GROUP, OWN_HEADS, 1, HEAD_DIM)
    wkv = jnp.concatenate([wk, wv], axis=3).reshape(rows_w, GROUP, KV_ROWS)
    gap = KV_AT - Q_ROWS
    lane = jnp.arange(gap)[None, :]
    small_cols = jnp.pad(bias_up.reshape(rows_w, -1), ((0, 0), (6, gap - 10)))
    for j, v in enumerate([bias_out, gain_one, shift_one, bias_down, gain_two, shift_two]):
        small_cols = jnp.where(lane == j, v[:, None], small_cols)
    small_cols = jnp.broadcast_to(small_cols[:, None], (rows_w, GROUP, gap))
    w_cut = jnp.concatenate([wq, small_cols, wkv], axis=2).transpose(1, 0, 2)
    column = me * rows_w + jnp.arange(rows_w)
    feature = jnp.arange(D)
    spread = lambda bias: jnp.sum(
        jnp.where(feature[None] == column[:, None], bias.astype(f32)[:, None], 0.0), axis=0
    )
    bias_q = spread(bias_query).reshape(GROUP, Q_ROWS)
    bias_v = spread(bias_value).reshape(GROUP, OWN_HEADS, 1, HEAD_DIM)
    bias_kv = jnp.concatenate([jnp.zeros_like(bias_v), bias_v], axis=2).reshape(GROUP, KV_ROWS)
    bias_cut = jnp.concatenate([bias_q, jnp.zeros((GROUP, gap), f32), bias_kv], axis=1)
    fill = -rows_w % 8
    bias_cut = jnp.pad(bias_cut.astype(bf16)[:, None], ((0, 0), (fill, 7), (0, 0)))
    w_send = jnp.concatenate([w_cut, bias_cut], axis=1)
    ff = w_up.shape[1]
    out_down = jnp.concatenate([w_out, w_down], axis=0)
    out_down = lax.all_gather(out_down, "fsdp", axis=0)
    wo_full = out_down[:, :rows_w].reshape(D, D)
    wd_full = lax.optimization_barrier(out_down[:, rows_w:].reshape(ff, D))
    wu_full = lax.all_gather(w_up, "fsdp", axis=0, tiled=True)

    code = (segment_ids * 2 + pad_mask).reshape(8, row_count // 8)
    x_own, code_win, ktag, w_turn, qt, kv, kvt = share(n_dev, rows_w, tokens, code, w_send)
    x_own = x_own.reshape(own, D)
    code_win = code_win.reshape(window)
    code_own = code_win[LEN_MAX : LEN_MAX + own]
    small_all = w_turn[Q_ROWS : Q_ROWS + 10].astype(f32)
    bu_full = small_all[6:].T.reshape(-1)
    bo_full, g1_full, s1_full, bd_full, g2_full, s2_full = [small_all[j] for j in range(6)]
    seg_win = code_win >> 1
    seg_own = code_own >> 1
    qtag = (seg_own + 1).reshape(1, own)
    first_seg = seg_own[::BQ]
    last_seg = seg_own[BQ - 1 :: BQ]
    low = jnp.sum((seg_win[None, :] < first_seg[:, None]).astype(jnp.int32), axis=1)
    high = jnp.sum((seg_win[None, :] <= last_seg[:, None]).astype(jnp.int32), axis=1)
    spans = [jnp.stack([low // b, (high + b - 1) // b], axis=1) for b in (FK, BK)]

    ot, lse = attend(spans[0], qtag, ktag, qt, kv, kvt)
    ctx_t = swap(ot, True)

    tokens_f = tokens.astype(f32)
    branch = jnp.einsum("ir,io->ro", ctx_t, wo_full, preferred_element_type=f32) + bo_full
    first, norm_one_back = jax.vjp(norm_rows, tokens_f + branch, g1_full, s1_full)
    up_in = lax.optimization_barrier(first.astype(bf16))
    pre_act = jnp.dot(up_in, wu_full, preferred_element_type=f32) + bu_full
    gelu_val, gelu_back = jax.vjp(gelu_exact, pre_act)
    hidden = gelu_val.astype(bf16)
    ffn = jnp.dot(hidden, wd_full, preferred_element_type=f32) + bd_full
    result, norm_two_back = jax.vjp(norm_rows, first + ffn, g2_full, s2_full)
    layer_out = result.astype(bf16)
    d_second, d_gain_two, d_shift_two = norm_two_back(cotangent.astype(f32))
    d_ffn = d_second.astype(bf16)
    d_bias_down = jnp.sum(d_ffn.astype(f32), axis=0)
    d_w_down = jnp.einsum("rf,rd->fd", hidden, d_ffn, preferred_element_type=f32)
    d_hidden = jnp.einsum("rd,fd->rf", d_ffn, wd_full, preferred_element_type=f32)
    d_pre = gelu_back(d_hidden)[0].astype(bf16)
    d_bias_up = jnp.sum(d_pre.astype(f32), axis=0)
    d_w_up = jnp.einsum("rd,rf->df", up_in, d_pre, preferred_element_type=f32).astype(bf16)
    d_w_up = lax.optimization_barrier(d_w_up)
    d_first = d_second + jnp.einsum("rf,df->rd", d_pre, wu_full, preferred_element_type=f32)
    d_mid, d_gain_one, d_shift_one = norm_one_back(d_first)
    d_branch = d_mid.astype(bf16)
    d_bias_out = jnp.sum(d_branch.astype(f32), axis=0)
    d_w_out = jnp.einsum("ir,ro->io", ctx_t, d_branch, preferred_element_type=f32)
    dctx_t = jnp.einsum("ro,io->ir", d_branch, wo_full, preferred_element_type=f32).astype(bf16)
    n_up = ff // D
    big_grad = jnp.concatenate(
        [
            d_w_down.astype(bf16).reshape(n_dev, -1, D),
            d_w_out.astype(bf16).reshape(n_dev, rows_w, D),
        ]
        + [d_w_up[:, D * j : D * (j + 1)].reshape(n_dev, rows_w, D) for j in range(n_up)],
        axis=1,
    )
    big_owned = lax.psum_scatter(big_grad, "fsdp", scatter_dimension=0).astype(f32)
    rows_d = w_down.shape[0]
    g_down, g_out = big_owned[:rows_d], big_owned[rows_d : rows_d + rows_w]
    g_up = jnp.concatenate(
        [big_owned[rows_d + rows_w * (j + 1) : rows_d + rows_w * (j + 2)] for j in range(n_up)], axis=1
    )

    d_out = swap(dctx_t, False)
    edge, inside = LEN_MAX // BK, own // BK
    far_parts = ((0, edge), (edge + inside, 2 * edge + inside))
    own_parts = ((edge, edge + inside),)
    dq_far, dkv_left, dkv_right = attend_grad(
        far_parts, False, spans[1], qtag, ktag, qt, d_out, ot, lse, kv, kvt
    )
    from_right = lax.ppermute(dkv_left, "fsdp", down)
    from_left = lax.ppermute(dkv_right, "fsdp", up)
    dq_t, dkv_own = attend_grad(
        own_parts, True, spans[1], qtag, ktag, qt, d_out, ot, lse, kv, kvt, dq_far
    )
    dkv = jnp.concatenate(
        [
            dkv_own[:, :LEN_MAX] + from_left.astype(f32),
            dkv_own[:, LEN_MAX : own - LEN_MAX],
            dkv_own[:, own - LEN_MAX :] + from_right.astype(f32),
        ],
        axis=1,
    ).astype(bf16)
    vecs = jnp.stack([d_bias_out, d_gain_one, d_shift_one, d_bias_down, d_gain_two, d_shift_two])
    vec_send = jnp.concatenate(
        [
            vecs.reshape(6, n_dev, rows_w).transpose(1, 0, 2).reshape(n_dev, 6 * rows_w),
            d_bias_up.reshape(n_dev, 4 * rows_w),
        ],
        axis=1,
    )
    vec_send = jnp.pad(vec_send, ((0, 0), (0, 1024 - vec_send.shape[1]))).reshape(n_dev, 8, 128)
    own_x, near, far, w_got, vec_got = settle(n_dev, rows_w, dq_t, dkv, x_own, w_turn, vec_send)
    grad_tokens = d_mid + ((own_x + near.astype(f32)) + far.astype(f32))
    got = jnp.sum(w_got.astype(f32).reshape(n_group, GROUP, -1, W_LANES), axis=0)
    got_q = got[:, :, :Q_ROWS].transpose(1, 0, 2).reshape(-1, D)
    got_kv = got[:, :, Q_ROWS:MIX_ROWS].transpose(1, 0, 2)
    got_kv = got_kv.reshape(-1, GROUP, OWN_HEADS, 2, HEAD_DIM)
    got_k = got_kv[:, :, :, 0].reshape(-1, D)
    got_v = got_kv[:, :, :, 1].reshape(-1, D)
    grad_w_qkv = jnp.concatenate([got_q[:rows_w], got_k[:rows_w], got_v[:rows_w]], axis=1)
    bias_rows = jnp.stack([got_q[-1], got_v[-1]])
    bias_own = lax.dynamic_slice(bias_rows, (0, me * rows_w), (2, rows_w))
    vec = jnp.sum(vec_got, axis=0).reshape(-1)[: 10 * rows_w]
    own_vec = [bias_own[0], bias_own[1]] + [vec[j * rows_w : (j + 1) * rows_w] for j in range(6)]
    return (
        layer_out,
        grad_tokens,
        grad_w_qkv,
        own_vec[0],
        own_vec[1],
        g_out,
        own_vec[2],
        own_vec[3],
        own_vec[4],
        g_up,
        vec[6 * rows_w :],
        g_down,
        own_vec[5],
        own_vec[6],
        own_vec[7],
    )


def solution(mesh):
    rows, flat = P("fsdp", None), P("fsdp")
    return jax.shard_map(
        functools.partial(body, mesh.shape["fsdp"]),
        mesh=mesh,
        in_specs=(
            rows, flat, flat, rows, flat, flat, rows, flat, flat, flat, rows, flat, rows, flat,
            flat, flat, rows,
        ),
        out_specs=(
            rows, rows, rows, flat, flat, rows, flat, flat, flat, rows, flat, rows, flat, flat,
            flat,
        ),
        check_vma=False,
    )
```

```python
import functools

import jax
import jax.numpy as jnp
from jax import lax
from jax.experimental import pallas as pl
from jax.experimental.pallas import tpu as pltpu
from jax.sharding import PartitionSpec as P

D = 768
HEADS = 12
HEAD_DIM = 64
LEN_MAX = 2048
GROUP = 4
OWN_HEADS = HEADS // GROUP
Q_ROWS = OWN_HEADS * HEAD_DIM
KV_ROWS = 2 * Q_ROWS
MIX_ROWS = Q_ROWS + KV_ROWS
BQ = 512
FK = 512
BK = 256
NEG = -1e30

bf16 = jnp.bfloat16
f32 = jnp.float32
eps_norm = 1e-12
score_scale = 0.125

NN = (((1,), (0,)), ((), ()))
NT = (((1,), (1,)), ((), ()))


def mm(a, b, dims=NN):
    return lax.dot_general(a, b, dims, preferred_element_type=f32)


def norm_rows(hidden, gain_row, shift_row):
    centre = hidden - jnp.mean(hidden, axis=-1, keepdims=True)
    spread = jnp.mean(centre * centre, axis=-1, keepdims=True)
    return centre * lax.rsqrt(spread + eps_norm) * gain_row + shift_row


def gelu_exact(pre_act):
    return 0.5 * pre_act * (1.0 + jax.scipy.special.erf(pre_act * 0.7071067811865476))


def head_rows(block, h, upper):
    zero = jnp.zeros_like(block[:HEAD_DIM])
    rows = block[h * HEAD_DIM : (h + 1) * HEAD_DIM]
    return jnp.concatenate([zero, rows] if upper else [rows, zero], axis=0)


def attend_kernel(
    span, qtag_ref, ktag_ref, qt_ref, kv_ref, kvt_ref, ot_ref, lse_ref, m_sc, l_sc, acc_sc
):
    i = pl.program_id(0)
    m_sc[...] = jnp.full_like(m_sc, NEG)
    l_sc[...] = jnp.zeros_like(l_sc)
    acc_sc[...] = jnp.zeros_like(acc_sc)
    qtag = qtag_ref[...]
    qt = qt_ref[...]
    q_pad = [head_rows(qt, h, False) for h in range(OWN_HEADS)]

    def step(kb, carry):
        rows = pl.ds(pl.multiple_of(kb * FK, FK), FK)
        seen = ktag_ref[rows, :] == qtag
        hs = range(OWN_HEADS)
        s = [mm(kv_ref[rows, 128 * h : 128 * (h + 1)], q_pad[h]) for h in hs]
        s = [jnp.where(seen, v, NEG) for v in s]
        m_old = [m_sc[h : h + 1, :] for h in hs]
        l_old = [l_sc[h : h + 1, :] for h in hs]
        m_new = [jnp.maximum(m_old[h], jnp.max(s[h], axis=0, keepdims=True)) for h in hs]
        p = [jnp.exp(s[h] - m_new[h]).astype(bf16) for h in hs]
        fade = [jnp.exp(m_old[h] - m_new[h]) for h in hs]
        one = jnp.ones((16, FK), bf16)
        v_one = [
            jnp.concatenate([kvt_ref[128 * h + HEAD_DIM : 128 * (h + 1), rows], one], axis=0)
            for h in hs
        ]
        out = [mm(v_one[h], p[h]) for h in hs]
        for h in hs:
            own = slice(HEAD_DIM * h, HEAD_DIM * (h + 1))
            acc_sc[own, :] = acc_sc[own, :] * fade[h] + out[h][:HEAD_DIM]
            l_sc[h : h + 1, :] = fade[h] * l_old[h] + out[h][HEAD_DIM : HEAD_DIM + 1]
            m_sc[h : h + 1, :] = m_new[h]
        return carry

    lax.fori_loop(span[i, 0], span[i, 1], step, 0)
    for h in range(OWN_HEADS):
        own = slice(HEAD_DIM * h, HEAD_DIM * (h + 1))
        total = l_sc[h : h + 1, :]
        ot_ref[own, :] = (acc_sc[own, :] / total).astype(bf16)
        lse_ref[h : h + 1, :] = m_sc[h : h + 1, :] + jnp.log(total)
    lse_ref[OWN_HEADS:, :] = jnp.zeros_like(lse_ref[OWN_HEADS:, :])


def attend(span, qtag, ktag, qt, kv, kvt):
    own = qt.shape[1]
    window = kv.shape[0]
    whole = lambda shape: pl.BlockSpec(shape, lambda i, s: (0, 0), pipeline_mode=pl.Buffered(1))
    cols = lambda rows: pl.BlockSpec((rows, BQ), lambda i, s: (0, i))
    return pl.pallas_call(
        attend_kernel,
        grid_spec=pltpu.PrefetchScalarGridSpec(
            num_scalar_prefetch=1,
            grid=(own // BQ,),
            in_specs=[
                cols(1),
                whole((window, 1)),
                cols(Q_ROWS),
                whole((window, KV_ROWS)),
                whole((KV_ROWS, window)),
            ],
            out_specs=[cols(Q_ROWS), cols(8)],
            scratch_shapes=[
                pltpu.VMEM((8, BQ), f32),
                pltpu.VMEM((8, BQ), f32),
                pltpu.VMEM((Q_ROWS, BQ), f32),
            ],
        ),
        out_shape=[
            jax.ShapeDtypeStruct((Q_ROWS, own), bf16),
            jax.ShapeDtypeStruct((8, own), f32),
        ],
        compiler_params=pltpu.CompilerParams(vmem_limit_bytes=60 << 20),
        cost_estimate=pl.CostEstimate(
            flops=4 * own * 2048 * Q_ROWS, bytes_accessed=20 << 20, transcendentals=own * 6144
        ),
        name="attend",
    )(span, qtag, ktag, qt, kv, kvt)


def grad_kernel(
    parts, final, span, qtag_ref, ktag_ref, qt_ref, dot_ref, ot_ref, lse_ref, kv_ref, kvt_ref, *rest
):
    if final:
        dq_in, dq_ref, *rest = rest
    else:
        dq_in, (dq_ref, *rest) = None, rest
    outs, (dq_sc, dkv_sc) = rest[: len(parts)], rest[len(parts) :]
    i = pl.program_id(0)

    @pl.when(i == 0)
    def _():
        dkv_sc[...] = jnp.zeros_like(dkv_sc)

    if final:
        dq_sc[...] = dq_in[...]
    else:
        dq_sc[...] = jnp.zeros_like(dq_sc)
    qtag = qtag_ref[...]
    qt, d_out, out = qt_ref[...], dot_ref[...], ot_ref[...]
    q_pad = [head_rows(qt, h, False) for h in range(OWN_HEADS)]
    d_pad = [head_rows(d_out, h, True) for h in range(OWN_HEADS)]
    product = d_out.astype(f32) * out.astype(f32)
    inner = [
        jnp.sum(product[HEAD_DIM * h : HEAD_DIM * (h + 1)], axis=0, keepdims=True)
        for h in range(OWN_HEADS)
    ]
    log_row = [lse_ref[h : h + 1, :] for h in range(OWN_HEADS)]

    def step(shift, kb, carry):
        rows = pl.ds(pl.multiple_of(kb * BK, BK), BK)
        place = pl.ds(pl.multiple_of((kb - shift) * BK, BK), BK)
        seen = ktag_ref[rows, :] == qtag
        hs = range(OWN_HEADS)
        kv = [kv_ref[rows, 128 * h : 128 * (h + 1)] for h in hs]
        s = [mm(kv[h], q_pad[h]) for h in hs]
        d_p = [mm(kv[h], d_pad[h]) for h in hs]
        p = [jnp.where(seen, jnp.exp(s[h] - log_row[h]), 0.0) for h in hs]
        d_s = [(p[h] * (d_p[h] - inner[h])).astype(bf16) for h in hs]
        p = [v.astype(bf16) for v in p]
        g_kv = [mm(q_pad[h], d_s[h], NT) + mm(d_pad[h], p[h], NT) for h in hs]
        g_q = [mm(kvt_ref[128 * h : 128 * h + HEAD_DIM, rows], d_s[h]) for h in hs]
        for h in hs:
            dkv_sc[128 * h : 128 * (h + 1), place] += g_kv[h]
            own = slice(HEAD_DIM * h, HEAD_DIM * (h + 1))
            dq_sc[own, :] += g_q[h]
        return carry

    base = 0
    for n, (first, last) in enumerate(parts):
        low = jnp.maximum(span[i, 0], first)
        high = jnp.minimum(span[i, 1], last)
        lax.fori_loop(low, high, functools.partial(step, first - base), 0)
        base += last - first
    if final:
        dq_ref[...] = (dq_sc[...] * score_scale).astype(bf16)
    else:
        dq_ref[...] = dq_sc[...]

    @pl.when(i == pl.num_programs(0) - 1)
    def _():
        base = 0
        for (first, last), ref in zip(parts, outs):
            width = (last - first) * BK
            ref[...] = dkv_sc[:, base : base + width].astype(ref.dtype)
            base += width


def attend_grad(parts, final, span, qtag, ktag, qt, d_out, out, lse, kv, kvt, dq_in=None):
    own = qt.shape[1]
    window = kv.shape[0]
    whole = lambda shape: pl.BlockSpec(shape, lambda i, s: (0, 0), pipeline_mode=pl.Buffered(1))
    cols = lambda rows: pl.BlockSpec((rows, BQ), lambda i, s: (0, i))
    widths = [(last - first) * BK for first, last in parts]
    dtype = f32 if final else bf16
    args = [span, qtag, ktag, qt, d_out, out, lse, kv, kvt] + ([dq_in] if final else [])
    return pl.pallas_call(
        functools.partial(grad_kernel, parts, final),
        grid_spec=pltpu.PrefetchScalarGridSpec(
            num_scalar_prefetch=1,
            grid=(own // BQ,),
            in_specs=[
                cols(1),
                whole((window, 1)),
                cols(Q_ROWS),
                cols(Q_ROWS),
                cols(Q_ROWS),
                cols(8),
                whole((window, KV_ROWS)),
                whole((KV_ROWS, window)),
            ]
            + ([cols(Q_ROWS)] if final else []),
            out_specs=[cols(Q_ROWS)] + [whole((KV_ROWS, w)) for w in widths],
            scratch_shapes=[
                pltpu.VMEM((Q_ROWS, BQ), f32),
                pltpu.VMEM((KV_ROWS, sum(widths)), f32),
            ],
        ),
        out_shape=[jax.ShapeDtypeStruct((Q_ROWS, own), bf16 if final else f32)]
        + [jax.ShapeDtypeStruct((KV_ROWS, w), dtype) for w in widths],
        compiler_params=pltpu.CompilerParams(vmem_limit_bytes=60 << 20),
        cost_estimate=pl.CostEstimate(
            flops=(10 if final else 2) * own * 1536 * Q_ROWS,
            bytes_accessed=20 << 20,
            transcendentals=own * 4096,
        ),
        name="grad_own" if final else "grad_far",
    )(*args)


MESH = pl.DeviceIdType.MESH
CHUNKS = 8
W_LANES = 640
KV_AT = 256


def remote(src, dst, send, recv, target):
    return pltpu.make_async_remote_copy(
        src_ref=src,
        dst_ref=dst,
        send_sem=send,
        recv_sem=recv,
        device_id=(target,),
        device_id_type=MESH,
    )


def share_kernel(
    n_dev, rows_w, tok_ref, code_ref, w_ref, x_own, code_out, ktag_out, w_turn, qt_out, kv_out, kvt_out,
    c_out, x_out, w_out, w_wide, w_full, qt_sc, kv_sc, kvt_sc,
    w_send, w_recv, c_send, c_recv, part_send, part_recv, mate_send, mate_recv,
    up_send, up_recv, down_send, down_recv, cross_send, cross_recv,
    fwd_send, fwd_recv, keep_sem, x_sem, q_sem, kv_sem, kvt_sem,
):
    n_group = n_dev // GROUP
    me = lax.axis_index("fsdp")
    g = me // GROUP
    s = me % GROUP
    k = s % 2
    hi = s // 2
    partner = me + 1 - 2 * k
    mate = me + 2 - 4 * hi
    mate_block = 4 + k - 2 * hi
    has_up = g < n_group - 1
    has_down = g > 0
    rows = tok_ref.shape[0] // CHUNKS
    half = CHUNKS // 2

    barrier = pltpu.get_barrier_semaphore()

    def greet(r, carry):
        pl.semaphore_signal(
            barrier, inc=1, device_id=(lax.rem(me + r, n_dev),), device_id_type=MESH
        )
        return carry

    lax.fori_loop(1, n_dev, greet, 0)
    pl.semaphore_wait(barrier, n_dev - 1)

    def chunk(ref, c):
        return ref.at[pl.ds(pl.multiple_of(c * rows, rows), rows)]

    def spot(b, c):
        return x_out.at[b, pl.ds(pl.multiple_of(c * rows, rows), rows)]

    def to_partner(c):
        return remote(chunk(tok_ref, c), spot(2 + s, c), part_send.at[c], part_recv.at[c], partner)

    def to_mate(c):
        return remote(chunk(tok_ref, c), spot(2 + s, c), mate_send.at[c], mate_recv.at[c], mate)

    def up_own(c):
        return remote(chunk(tok_ref, c), spot(k, c), up_send.at[c], up_recv.at[c], me + GROUP)

    def up_mate(c):
        return remote(spot(mate_block, c), spot(k, c), up_send.at[c], up_recv.at[c], me + GROUP)

    def down_own(c):
        return remote(
            chunk(tok_ref, c), spot(6 + k, c), down_send.at[c], down_recv.at[c], me - GROUP
        )

    def down_mate(c):
        return remote(
            spot(mate_block, c + half), spot(6 + k, c + half), down_send.at[c], down_recv.at[c],
            me - GROUP,
        )

    def cross(c):
        at = c + half * hi
        return remote(spot(6 + k, at), spot(6 + k, at), cross_send.at[c], cross_recv.at[c], mate)

    def forward(b, c, slot):
        return remote(spot(b, c), spot(b, c), fwd_send.at[slot], fwd_recv.at[slot], partner)

    keep_x = pltpu.make_async_copy(tok_ref, x_out.at[2 + s], keep_sem.at[0])
    keep_c = pltpu.make_async_copy(code_ref, c_out.at[2 + s], keep_sem.at[1])
    keep_w = pltpu.make_async_copy(w_ref.at[s], w_out.at[me], keep_sem.at[2])
    keep_x.start()
    keep_c.start()
    keep_w.start()

    def w_copy(r):
        target = lax.rem(me + r, n_dev)
        return remote(
            w_ref.at[lax.rem(target, GROUP)], w_out.at[me], w_send.at[r], w_recv.at[r], target
        )

    def w_start(r, carry):
        w_copy(r).start()
        return carry

    def c_group(j):
        target = GROUP * g + lax.rem(s + j, GROUP)
        return remote(code_ref, c_out.at[2 + s], c_send.at[j], c_recv.at[2 + s], target)

    def c_far(j):
        step = GROUP * (2 * hi - 1)
        b = 6 + s - 8 * hi
        target = GROUP * g + step + j
        return remote(code_ref, c_out.at[b], c_send.at[GROUP + j], c_recv.at[b], target)

    sends_far = jnp.where(hi == 1, g < n_group - 1, g > 0)
    for j in range(1, GROUP):
        c_group(j).start()

    @pl.when(sends_far)
    def _():
        for j in range(GROUP):
            c_far(j).start()

    order = list(range(half, CHUNKS)) + list(range(half))

    @pl.when((hi == 0) & has_down)
    def _():
        for c in range(half):
            down_own(c).start()

    for n, c in enumerate(order):
        to_mate(c).start()
        to_partner(c).start()
        if n < half:

            @pl.when((hi == 1) & has_up)
            def _():
                up_own(c).start()

        if n == half - 1:
            lax.fori_loop(1, n_dev, w_start, 0)

    for n, c in enumerate(order):
        to_mate(c).wait_recv()
        forward(mate_block, c, c).start()

        @pl.when((hi == 0) & has_up)
        def _():
            up_mate(c).start()

        if n < half:

            @pl.when((hi == 1) & has_down)
            def _():
                down_mate(c - half).start()

        else:

            @pl.when((hi == 1) & has_up)
            def _():
                up_own(c).start()

    @pl.when(has_up)
    def _():
        for c in range(half):
            down_own(c).wait_recv()
            cross(c).start()
            forward(6 + k, c + half * hi, 2 * CHUNKS + c).start()

    def w_wait(r, carry):
        w_copy(r).wait_recv()
        return carry

    lax.fori_loop(1, n_dev, w_wait, 0)
    keep_w.wait()
    keep_x.wait()
    bias_row = jnp.zeros((8, W_LANES), f32)
    bias_at = w_ref.shape[1] - 8
    for j in range(n_dev):
        w_wide[rows_w * j : rows_w * (j + 1), :] = w_out[j, :rows_w, :].astype(f32)
        bias_row = bias_row + w_out[j, bias_at:, :].astype(f32)
    bias_row = jnp.sum(bias_row, axis=0, keepdims=True)
    bias_col = jnp.broadcast_to(bias_row, (128, W_LANES)).T[:, :1]
    w_full[...] = w_wide[...].astype(bf16)
    w_turn[...] = w_wide[...].T.astype(bf16)
    piece = 512
    pieces = tok_ref.shape[0] // piece

    def project(b, inside):
        def one(j, carry):
            x = x_out[b, pl.ds(pl.multiple_of(j * piece, piece), piece), :]
            at = pl.ds(pl.multiple_of((b * pieces + j) * piece, piece), piece)
            kv = mm(x, w_full[:, KV_AT:]) + bias_row[:, KV_AT:]
            kv_sc[at, :] = kv.astype(bf16)
            kvt_sc[:, at] = (mm(w_turn[KV_AT:, :], x, NT) + bias_col[KV_AT:]).astype(bf16)
            if inside:
                to = pl.ds(pl.multiple_of(((b - 2) * pieces + j) * piece, piece), piece)
                q = (mm(w_turn[:Q_ROWS, :], x, NT) + bias_col[:Q_ROWS]).astype(bf16)
                qt_sc[:, to] = q * jnp.asarray(score_scale, bf16)
            return carry

        lax.fori_loop(0, pieces, one, 0)

    def outs(b, inside):
        whole = tok_ref.shape[0]
        at = pl.ds(pl.multiple_of(b * whole, whole), whole)
        copies = [
            pltpu.make_async_copy(kv_sc.at[at], kv_out.at[at], kv_sem.at[b]),
            pltpu.make_async_copy(kvt_sc.at[:, at], kvt_out.at[:, at], kvt_sem.at[b]),
        ]
        if inside:
            to = pl.ds(pl.multiple_of((b - 2) * whole, whole), whole)
            copies.append(pltpu.make_async_copy(qt_sc.at[:, to], qt_out.at[:, to], q_sem.at[b - 2]))
            copies.append(pltpu.make_async_copy(x_out.at[b], x_own.at[b - 2], x_sem.at[b - 2]))
        return copies

    def put(b, inside):
        for copy in outs(b, inside):
            copy.start()

    keep_c.wait()
    for j in range(1, GROUP):
        remote(
            code_ref, c_out.at[0], c_send.at[j], c_recv.at[2 + lax.rem(s + j, GROUP)], partner
        ).wait_recv()

    @pl.when(has_down)
    def _():
        for b in range(2):
            remote(code_ref, c_out.at[b], c_send.at[0], c_recv.at[b], partner).wait_recv()

    @pl.when(has_up)
    def _():
        for b in range(6, 8):
            remote(code_ref, c_out.at[b], c_send.at[0], c_recv.at[b], partner).wait_recv()

    for b in range(8):
        code = c_out[b]
        if b < 2:
            code = jnp.where(has_down, code, -2)
        if b >= 6:
            code = jnp.where(has_up, code, 2 * n_dev * tok_ref.shape[0])
        code_out[b] = code
        tag = jnp.where((code & 1) == 1, (code >> 1) + 1, 0)
        lanes = tag.shape[1]
        for r in range(8):
            turned = jnp.broadcast_to(tag[r : r + 1, :], (lanes, lanes)).T
            at = (8 * b + r) * lanes
            ktag_out[at : at + lanes, :] = turned[:, :1]

    own_block = 2 + s
    near_block = own_block + 1 - 2 * k
    across_block = mate_block + 1 - 2 * k
    project(own_block, True)

    project(mate_block, True)
    put(own_block, True)

    @pl.when(has_down)
    def _():
        for c in order:
            up_own(c).wait_recv()
            forward(k, c, CHUNKS + c).start()

    for c in range(CHUNKS):
        to_partner(c).wait_recv()
    project(near_block, True)
    put(mate_block, True)

    @pl.when(has_up)
    def _():
        for c in range(half):
            cross(c).wait_recv()
            forward(6 + k, c + half * (1 - hi), 2 * CHUNKS + half + c).start()

    for c in range(CHUNKS):
        forward(mate_block, c, c).wait_recv()
    project(across_block, True)
    put(near_block, True)

    @pl.when(has_down)
    def _():
        project(k, False)
        for c in range(CHUNKS):
            forward(k, c, CHUNKS + c).wait_recv()
        project(1 - k, False)
        put(k, False)

    put(across_block, True)

    @pl.when(has_up)
    def _():
        project(6 + k, False)
        for c in range(half):
            forward(6 + k, c, 2 * CHUNKS + c).wait_recv()
            forward(6 + k, c, 2 * CHUNKS + half + c).wait_recv()
        project(7 - k, False)
        put(6 + k, False)

    for c in range(CHUNKS):
        to_partner(c).wait_send()
        to_mate(c).wait_send()
        forward(mate_block, c, c).wait_send()

    @pl.when(has_down)
    def _():
        put(1 - k, False)
        for c in range(CHUNKS):
            forward(k, c, CHUNKS + c).wait_send()
        for c in range(half):
            down_own(c).wait_send()

    @pl.when(has_up)
    def _():
        for c in range(half):
            cross(c).wait_send()
            forward(6 + k, c, 2 * CHUNKS + c).wait_send()
            forward(6 + k, c, 2 * CHUNKS + half + c).wait_send()
        for c in range(CHUNKS):
            up_own(c).wait_send()
        put(7 - k, False)

    for j in range(1, GROUP):
        c_group(j).wait_send()

    @pl.when(sends_far)
    def _():
        for j in range(GROUP):
            c_far(j).wait_send()

    def w_sent(r, carry):
        w_copy(r).wait_send()
        return carry

    lax.fori_loop(1, n_dev, w_sent, 0)
    for b in range(2, 6):
        for copy in outs(b, True):
            copy.wait()

    @pl.when(has_down)
    def _():
        for b in range(2):
            for copy in outs(b, False):
                copy.wait()

    @pl.when(has_up)
    def _():
        for b in range(6, 8):
            for copy in outs(b, False):
                copy.wait()


def share(n_dev, rows_w, tokens, code, w_send):
    vmem = pl.BlockSpec(memory_space=pltpu.VMEM)
    anywhere = pl.BlockSpec(memory_space=pl.ANY)
    dma = lambda n: pltpu.SemaphoreType.DMA((n,))
    half = CHUNKS // 2
    rows, width = tokens.shape
    own, window = GROUP * rows, 8 * rows
    return pl.pallas_call(
        functools.partial(share_kernel, n_dev, rows_w),
        in_specs=[vmem] * 3,
        out_specs=[anywhere, vmem, vmem, vmem, anywhere, anywhere, anywhere],
        out_shape=[
            jax.ShapeDtypeStruct((GROUP, rows, width), bf16),
            jax.ShapeDtypeStruct((8,) + code.shape, code.dtype),
            jax.ShapeDtypeStruct((window, 1), code.dtype),
            jax.ShapeDtypeStruct((W_LANES, width), bf16),
            jax.ShapeDtypeStruct((Q_ROWS, own), bf16),
            jax.ShapeDtypeStruct((window, KV_ROWS), bf16),
            jax.ShapeDtypeStruct((KV_ROWS, window), bf16),
        ],
        scratch_shapes=[
            pltpu.VMEM((8,) + code.shape, code.dtype),
            pltpu.VMEM((8, rows, width), bf16),
            pltpu.VMEM((n_dev,) + w_send.shape[1:], bf16),
            pltpu.VMEM((width, W_LANES), f32),
            pltpu.VMEM((width, W_LANES), bf16),
            pltpu.VMEM((Q_ROWS, own), bf16),
            pltpu.VMEM((window, KV_ROWS), bf16),
            pltpu.VMEM((KV_ROWS, window), bf16),
            dma(n_dev), dma(n_dev), dma(2 * GROUP), dma(8),
            dma(CHUNKS), dma(CHUNKS), dma(CHUNKS), dma(CHUNKS),
            dma(CHUNKS), dma(CHUNKS), dma(half), dma(half), dma(half), dma(half),
            dma(3 * CHUNKS), dma(3 * CHUNKS), dma(3), dma(GROUP), dma(GROUP), dma(8), dma(8),
        ],
        compiler_params=pltpu.CompilerParams(
            collective_id=0, has_side_effects=True, vmem_limit_bytes=60 << 20
        ),
        name="share",
    )(tokens, code, w_send)


PARTS = 4
TN = (((0,), (0,)), ((), ()))


def settle_kernel(
    n_dev, rows_w, q_ref, kv_ref, x_ref, w_ref, vec_ref, own_out, near_out, far_out, grad_out, vec_sum,
    w_out, vec_out, wide, slabs, across, near, relay, total,
    w_send, w_recv, vec_send, vec_recv, near_send, near_recv, relay_send, relay_recv,
    far_send, far_recv, keep_sem,
):
    me = lax.axis_index("fsdp")
    s = me % GROUP
    k = s % 2
    hi = s // 2
    partner = me + 1 - 2 * k
    mate = me + 2 - 4 * hi
    s_partner = s + 1 - 2 * k
    s_mate = s + 2 - 4 * hi
    s_across = 3 - s
    block = own_out.shape[0]
    rows = block // PARTS

    barrier = pltpu.get_barrier_semaphore()

    def greet(r, carry):
        pl.semaphore_signal(
            barrier, inc=1, device_id=(lax.rem(me + r, n_dev),), device_id_type=MESH
        )
        return carry

    lax.fori_loop(1, n_dev, greet, 0)
    pl.semaphore_wait(barrier, n_dev - 1)

    def part(c):
        return pl.ds(c * rows, rows)

    def to_relay(c):
        return remote(
            across.at[part(c)], relay.at[part(c)], relay_send.at[c], relay_recv.at[c], partner
        )

    def to_near(c):
        return remote(
            near.at[part(c)], near_out.at[part(c)], near_send.at[c], near_recv.at[c], partner
        )

    def to_far(c):
        return remote(total.at[part(c)], far_out.at[part(c)], far_send.at[c], far_recv.at[c], mate)

    def w_copy(r):
        target = lax.rem(me + r, n_dev)
        return remote(slabs.at[target], w_out.at[me], w_send.at[r], w_recv.at[r], target)

    def vec_copy(r):
        target = lax.rem(me + r, n_dev)
        return remote(vec_ref.at[target], vec_out.at[me], vec_send.at[r], vec_recv.at[r], target)

    def vec_start(r, carry):
        vec_copy(r).start()
        return carry

    lax.fori_loop(1, n_dev, vec_start, 0)
    keep_vec = pltpu.make_async_copy(vec_ref.at[me], vec_out.at[me], keep_sem.at[1])
    keep_vec.start()

    def back(t, c):
        at = pl.ds(pl.multiple_of(t * block + c * rows, rows), rows)
        return mm(q_ref[:, at], w_ref[:Q_ROWS, :], TN) + mm(kv_ref[:, at], w_ref[KV_AT:, :], TN)

    def add_rows(j):
        at = slice(j * block, (j + 1) * block)
        wide[:Q_ROWS, :] += mm(q_ref[:, at], x_ref[at, :])
        wide[Q_ROWS:MIX_ROWS, :] += mm(kv_ref[:, at], x_ref[at, :])

    def w_start(r, carry):
        w_copy(r).start()
        return carry

    for c in range(PARTS):
        across[c * rows : (c + 1) * rows, :] = back(s_across, c).astype(bf16)
        if c > 0:
            to_relay(c - 1).start()
    mine = back(s_mate, 0)
    to_relay(PARTS - 1).start()
    wide[...] = jnp.zeros_like(wide)
    for c in range(PARTS):
        to_relay(c).wait_recv()
        other = relay[c * rows : (c + 1) * rows, :].astype(f32)
        total[c * rows : (c + 1) * rows, :] = (mine + other).astype(bf16)
        if c + 1 < PARTS:
            mine = back(s_mate, c + 1)
        else:
            add_rows(0)
        to_far(c).start()
    for j in range(1, GROUP):
        add_rows(j)
    turned = wide[...].T
    one = jnp.ones((8, GROUP * block), bf16)
    bias_q = mm(one, q_ref[...], NT).astype(bf16)
    bias_kv = mm(one, kv_ref[...], NT).astype(bf16)
    bias_at = slabs.shape[1] - 8
    for j in range(n_dev):
        slabs[j, :rows_w, :] = turned[rows_w * j : rows_w * (j + 1), :].astype(bf16)
        slabs[j, bias_at:, :Q_ROWS] = bias_q
        slabs[j, bias_at:, Q_ROWS:MIX_ROWS] = bias_kv
    near[:rows, :] = back(s_partner, 0).astype(bf16)
    lax.fori_loop(1, n_dev, w_start, 0)
    keep_w = pltpu.make_async_copy(slabs.at[me], w_out.at[me], keep_sem.at[0])
    keep_w.start()
    for c in range(1, PARTS):
        near[c * rows : (c + 1) * rows, :] = back(s_partner, c).astype(bf16)
        to_near(c - 1).start()
    for c in range(PARTS):
        own_out[c * rows : (c + 1) * rows, :] = back(s, c)
        if c == 0:
            to_near(PARTS - 1).start()
    for c in range(PARTS):
        to_relay(c).wait_send()
        to_near(c).wait()
        to_far(c).wait()

    def finish(r, carry):
        w_copy(r).wait()
        vec_copy(r).wait()
        return carry

    lax.fori_loop(1, n_dev, finish, 0)
    keep_w.wait()
    keep_vec.wait()
    vec_sum[...] = jnp.sum(vec_out[...], axis=0)
    for t in range(GROUP):
        got = w_out[t].astype(f32)
        for j in range(1, n_dev // GROUP):
            got = got + w_out[GROUP * j + t].astype(f32)
        grad_out[:, Q_ROWS * t : Q_ROWS * (t + 1)] = got[:, :Q_ROWS]
        for h in range(OWN_HEADS):
            for part_at in range(2):
                at = Q_ROWS + 128 * h + HEAD_DIM * part_at
                to = D * (1 + part_at) + Q_ROWS * t + HEAD_DIM * h
                grad_out[:, to : to + HEAD_DIM] = got[:, at : at + HEAD_DIM]


def settle(n_dev, rows_w, d_q, d_kv, x, w, vec):
    vmem = pl.BlockSpec(memory_space=pltpu.VMEM)
    anywhere = pl.BlockSpec(memory_space=pl.ANY)
    dma = lambda n: pltpu.SemaphoreType.DMA((n,))
    block = (x.shape[0] // GROUP, x.shape[1])
    slabs = (n_dev, rows_w + -rows_w % 8 + 8, W_LANES)
    return pl.pallas_call(
        functools.partial(settle_kernel, n_dev, rows_w),
        in_specs=[vmem] * 5,
        out_specs=[vmem, anywhere, anywhere, vmem, vmem],
        out_shape=[
            jax.ShapeDtypeStruct(block, f32),
            jax.ShapeDtypeStruct(block, bf16),
            jax.ShapeDtypeStruct(block, bf16),
            jax.ShapeDtypeStruct((slabs[1], 3 * D), f32),
            jax.ShapeDtypeStruct(vec.shape[1:], vec.dtype),
        ],
        scratch_shapes=[
            pltpu.VMEM(slabs, bf16),
            pltpu.VMEM(vec.shape, vec.dtype),
            pltpu.VMEM((W_LANES, x.shape[1]), f32),
            pltpu.VMEM(slabs, bf16),
            pltpu.VMEM(block, bf16), pltpu.VMEM(block, bf16),
            pltpu.VMEM(block, bf16), pltpu.VMEM(block, bf16),
            dma(n_dev), dma(n_dev), dma(n_dev), dma(n_dev),
            dma(PARTS), dma(PARTS), dma(PARTS), dma(PARTS), dma(PARTS), dma(PARTS), dma(2),
        ],
        compiler_params=pltpu.CompilerParams(
            collective_id=1, has_side_effects=True, vmem_limit_bytes=60 << 20
        ),
        name="settle",
    )(d_q, d_kv, x, w, vec)


def swap_kernel(spread, in_ref, out_ref, send, recv, keep_sem):
    me = lax.axis_index("fsdp")
    s = me % GROUP
    start = me - s
    width = (in_ref if spread else out_ref).shape[1] // GROUP

    barrier = pltpu.get_barrier_semaphore()
    for j in range(1, GROUP):
        target = start + lax.rem(s + j, GROUP)
        pl.semaphore_signal(barrier, inc=1, device_id=(target,), device_id_type=MESH)
    pl.semaphore_wait(barrier, GROUP - 1)

    def cols(ref, t):
        return ref.at[:, pl.ds(pl.multiple_of(t * width, width), width)]

    def rows(ref, t):
        return ref.at[pl.ds(pl.multiple_of(t * Q_ROWS, Q_ROWS), Q_ROWS)]

    def ends(t):
        if spread:
            return cols(in_ref, t), rows(out_ref, s)
        return rows(in_ref, t), cols(out_ref, s)

    def copy(j):
        t = lax.rem(s + j, GROUP)
        src, dst = ends(t)
        return remote(src, dst, send.at[j], recv.at[j], start + t)

    for j in (2, 1, 3):
        copy(j).start()
    src, dst = ends(s)
    keep = pltpu.make_async_copy(src, dst, keep_sem.at[0])
    keep.start()
    for j in range(1, GROUP):
        copy(j).wait()
    keep.wait()


def swap(x, spread):
    shape = (x.shape[0] * GROUP, x.shape[1] // GROUP) if spread else (
        x.shape[0] // GROUP, x.shape[1] * GROUP
    )
    dma = lambda n: pltpu.SemaphoreType.DMA((n,))
    return pl.pallas_call(
        functools.partial(swap_kernel, spread),
        in_specs=[pl.BlockSpec(memory_space=pltpu.VMEM)],
        out_specs=pl.BlockSpec(memory_space=pltpu.VMEM),
        out_shape=jax.ShapeDtypeStruct(shape, x.dtype),
        scratch_shapes=[dma(GROUP), dma(GROUP), dma(1)],
        compiler_params=pltpu.CompilerParams(
            collective_id=2 if spread else 3, has_side_effects=True
        ),
        name="swap_out" if spread else "swap_back",
    )(x)


def body(
    n_dev,
    tokens,
    segment_ids,
    pad_mask,
    w_qkv,
    bias_query,
    bias_value,
    w_out,
    bias_out,
    gain_one,
    shift_one,
    w_up,
    bias_up,
    w_down,
    bias_down,
    gain_two,
    shift_two,
    cotangent,
):
    row_count = tokens.shape[0]
    rows_w = w_qkv.shape[0]
    own = GROUP * row_count
    window = own + 2 * LEN_MAX
    me = lax.axis_index("fsdp")
    place = me % GROUP
    group_id = me // GROUP
    n_group = n_dev // GROUP
    up = [(i, i + GROUP) for i in range(n_dev - GROUP)]
    down = [(i + GROUP, i) for i in range(n_dev - GROUP)]

    wq = w_qkv[:, :D].reshape(rows_w, GROUP, Q_ROWS)
    wk = w_qkv[:, D : 2 * D].reshape(rows_w, GROUP, OWN_HEADS, 1, HEAD_DIM)
    wv = w_qkv[:, 2 * D :].reshape(rows_w, GROUP, OWN_HEADS, 1, HEAD_DIM)
    wkv = jnp.concatenate([wk, wv], axis=3).reshape(rows_w, GROUP, KV_ROWS)
    gap = KV_AT - Q_ROWS
    lane = jnp.arange(gap)[None, :]
    small_cols = jnp.pad(bias_up.reshape(rows_w, -1), ((0, 0), (6, gap - 10)))
    for j, v in enumerate([bias_out, gain_one, shift_one, bias_down, gain_two, shift_two]):
        small_cols = jnp.where(lane == j, v[:, None], small_cols)
    small_cols = jnp.broadcast_to(small_cols[:, None], (rows_w, GROUP, gap))
    w_cut = jnp.concatenate([wq, small_cols, wkv], axis=2).transpose(1, 0, 2)
    column = me * rows_w + jnp.arange(rows_w)
    feature = jnp.arange(D)
    spread = lambda bias: jnp.sum(
        jnp.where(feature[None] == column[:, None], bias.astype(f32)[:, None], 0.0), axis=0
    )
    bias_q = spread(bias_query).reshape(GROUP, Q_ROWS)
    bias_v = spread(bias_value).reshape(GROUP, OWN_HEADS, 1, HEAD_DIM)
    bias_kv = jnp.concatenate([jnp.zeros_like(bias_v), bias_v], axis=2).reshape(GROUP, KV_ROWS)
    bias_cut = jnp.concatenate([bias_q, jnp.zeros((GROUP, gap), f32), bias_kv], axis=1)
    fill = -rows_w % 8
    bias_cut = jnp.pad(bias_cut.astype(bf16)[:, None], ((0, 0), (fill, 7), (0, 0)))
    w_send = jnp.concatenate([w_cut, bias_cut], axis=1)
    ff = w_up.shape[1]
    out_down = jnp.concatenate([w_out, w_down], axis=0)
    out_down = lax.all_gather(out_down, "fsdp", axis=0)
    wo_full = out_down[:, :rows_w].reshape(D, D)
    wd_full = lax.optimization_barrier(out_down[:, rows_w:].reshape(ff, D))
    wu_full = lax.all_gather(w_up, "fsdp", axis=0, tiled=True)

    code = (segment_ids * 2 + pad_mask).reshape(8, row_count // 8)
    x_own, code_win, ktag, w_turn, qt, kv, kvt = share(n_dev, rows_w, tokens, code, w_send)
    x_own = x_own.reshape(own, D)
    code_win = code_win.reshape(window)
    code_own = code_win[LEN_MAX : LEN_MAX + own]
    small_all = w_turn[Q_ROWS : Q_ROWS + 10].astype(f32)
    bu_full = small_all[6:].T.reshape(-1)
    bo_full, g1_full, s1_full, bd_full, g2_full, s2_full = [small_all[j] for j in range(6)]
    seg_win = code_win >> 1
    seg_own = code_own >> 1
    qtag = (seg_own + 1).reshape(1, own)
    first_seg = seg_own[::BQ]
    last_seg = seg_own[BQ - 1 :: BQ]
    low = jnp.sum((seg_win[None, :] < first_seg[:, None]).astype(jnp.int32), axis=1)
    high = jnp.sum((seg_win[None, :] <= last_seg[:, None]).astype(jnp.int32), axis=1)
    spans = [jnp.stack([low // b, (high + b - 1) // b], axis=1) for b in (FK, BK)]

    ot, lse = attend(spans[0], qtag, ktag, qt, kv, kvt)
    ctx_t = swap(ot, True)

    tokens_f = tokens.astype(f32)
    branch = jnp.einsum("ir,io->ro", ctx_t, wo_full, preferred_element_type=f32) + bo_full
    first, norm_one_back = jax.vjp(norm_rows, tokens_f + branch, g1_full, s1_full)
    up_in = lax.optimization_barrier(first.astype(bf16))
    pre_act = jnp.dot(up_in, wu_full, preferred_element_type=f32) + bu_full
    gelu_val, gelu_back = jax.vjp(gelu_exact, pre_act)
    hidden = gelu_val.astype(bf16)
    ffn = jnp.dot(hidden, wd_full, preferred_element_type=f32) + bd_full
    result, norm_two_back = jax.vjp(norm_rows, first + ffn, g2_full, s2_full)
    layer_out = result.astype(bf16)
    d_second, d_gain_two, d_shift_two = norm_two_back(cotangent.astype(f32))
    d_ffn = d_second.astype(bf16)
    d_bias_down = jnp.sum(d_ffn.astype(f32), axis=0)
    d_w_down = jnp.einsum("rf,rd->fd", hidden, d_ffn, preferred_element_type=f32)
    d_hidden = jnp.einsum("rd,fd->rf", d_ffn, wd_full, preferred_element_type=f32)
    d_pre = gelu_back(d_hidden)[0].astype(bf16)
    d_bias_up = jnp.sum(d_pre.astype(f32), axis=0)
    d_w_up = jnp.einsum("rd,rf->df", up_in, d_pre, preferred_element_type=f32).astype(bf16)
    d_w_up = lax.optimization_barrier(d_w_up)
    d_first = d_second + jnp.einsum("rf,df->rd", d_pre, wu_full, preferred_element_type=f32)
    d_mid, d_gain_one, d_shift_one = norm_one_back(d_first)
    d_branch = d_mid.astype(bf16)
    d_bias_out = jnp.sum(d_branch.astype(f32), axis=0)
    d_w_out = jnp.einsum("ir,ro->io", ctx_t, d_branch, preferred_element_type=f32)
    dctx_t = jnp.einsum("ro,io->ir", d_branch, wo_full, preferred_element_type=f32).astype(bf16)
    n_up = ff // D
    big_grad = jnp.concatenate(
        [
            d_w_down.astype(bf16).reshape(n_dev, -1, D),
            d_w_out.astype(bf16).reshape(n_dev, rows_w, D),
        ]
        + [d_w_up[:, D * j : D * (j + 1)].reshape(n_dev, rows_w, D) for j in range(n_up)],
        axis=1,
    )
    big_owned = lax.psum_scatter(big_grad, "fsdp", scatter_dimension=0).astype(f32)
    rows_d = w_down.shape[0]
    g_down, g_out = big_owned[:rows_d], big_owned[rows_d : rows_d + rows_w]
    g_up = jnp.concatenate(
        [big_owned[rows_d + rows_w * (j + 1) : rows_d + rows_w * (j + 2)] for j in range(n_up)], axis=1
    )

    d_out = swap(dctx_t, False)
    edge, inside = LEN_MAX // BK, own // BK
    far_parts = ((0, edge), (edge + inside, 2 * edge + inside))
    own_parts = ((edge, edge + inside),)
    dq_far, dkv_left, dkv_right = attend_grad(
        far_parts, False, spans[1], qtag, ktag, qt, d_out, ot, lse, kv, kvt
    )
    from_right = lax.ppermute(dkv_left, "fsdp", down)
    from_left = lax.ppermute(dkv_right, "fsdp", up)
    dq_t, dkv_own = attend_grad(
        own_parts, True, spans[1], qtag, ktag, qt, d_out, ot, lse, kv, kvt, dq_far
    )
    dkv = jnp.concatenate(
        [
            dkv_own[:, :LEN_MAX] + from_left.astype(f32),
            dkv_own[:, LEN_MAX : own - LEN_MAX],
            dkv_own[:, own - LEN_MAX :] + from_right.astype(f32),
        ],
        axis=1,
    ).astype(bf16)
    vecs = jnp.stack([d_bias_out, d_gain_one, d_shift_one, d_bias_down, d_gain_two, d_shift_two])
    vec_send = jnp.concatenate(
        [
            vecs.reshape(6, n_dev, rows_w).transpose(1, 0, 2).reshape(n_dev, 6 * rows_w),
            d_bias_up.reshape(n_dev, 4 * rows_w),
        ],
        axis=1,
    )
    vec_send = jnp.pad(vec_send, ((0, 0), (0, 1024 - vec_send.shape[1]))).reshape(n_dev, 8, 128)
    own_x, near, far, got, vec = settle(n_dev, rows_w, dq_t, dkv, x_own, w_turn, vec_send)
    grad_tokens = d_mid + ((own_x + near.astype(f32)) + far.astype(f32))
    grad_w_qkv = got[:rows_w]
    bias_rows = got[-8].reshape(3, D)
    bias_own = lax.dynamic_slice(bias_rows, (0, me * rows_w), (3, rows_w))
    vec = vec.reshape(-1)[: 10 * rows_w]
    own_vec = [bias_own[0], bias_own[2]] + [vec[j * rows_w : (j + 1) * rows_w] for j in range(6)]
    return (
        layer_out,
        grad_tokens,
        grad_w_qkv,
        own_vec[0],
        own_vec[1],
        g_out,
        own_vec[2],
        own_vec[3],
        own_vec[4],
        g_up,
        vec[6 * rows_w :],
        g_down,
        own_vec[5],
        own_vec[6],
        own_vec[7],
    )


def solution(mesh):
    rows, flat = P("fsdp", None), P("fsdp")
    return jax.shard_map(
        functools.partial(body, mesh.shape["fsdp"]),
        mesh=mesh,
        in_specs=(
            rows, flat, flat, rows, flat, flat, rows, flat, flat, flat, rows, flat, rows, flat,
            flat, flat, rows,
        ),
        out_specs=(
            rows, rows, rows, flat, flat, rows, flat, flat, flat, rows, flat, rows, flat, flat,
            flat,
        ),
        check_vma=False,
    )
```

```python
import functools

import jax
import jax.numpy as jnp
from jax import lax
from jax.experimental import pallas as pl
from jax.experimental.pallas import tpu as pltpu
from jax.sharding import PartitionSpec as P

D = 768
HEADS = 12
HEAD_DIM = 64
LEN_MAX = 2048
GROUP = 4
OWN_HEADS = HEADS // GROUP
Q_ROWS = OWN_HEADS * HEAD_DIM
KV_ROWS = 2 * Q_ROWS
MIX_ROWS = Q_ROWS + KV_ROWS
BQ = 512
FK = 512
BK = 256
NEG = -1e30

bf16 = jnp.bfloat16
f32 = jnp.float32
eps_norm = 1e-12
score_scale = 0.125

NN = (((1,), (0,)), ((), ()))
NT = (((1,), (1,)), ((), ()))


def mm(a, b, dims=NN):
    return lax.dot_general(a, b, dims, preferred_element_type=f32)


def norm_rows(hidden, gain_row, shift_row):
    centre = hidden - jnp.mean(hidden, axis=-1, keepdims=True)
    spread = jnp.mean(centre * centre, axis=-1, keepdims=True)
    return centre * lax.rsqrt(spread + eps_norm) * gain_row + shift_row


def gelu_exact(pre_act):
    return 0.5 * pre_act * (1.0 + jax.scipy.special.erf(pre_act * 0.7071067811865476))


def head_rows(block, h, upper):
    zero = jnp.zeros_like(block[:HEAD_DIM])
    rows = block[h * HEAD_DIM : (h + 1) * HEAD_DIM]
    return jnp.concatenate([zero, rows] if upper else [rows, zero], axis=0)


def attend_kernel(
    span, qtag_ref, ktag_ref, qt_ref, kv_ref, kvt_ref, ot_ref, lse_ref, m_sc, l_sc, acc_sc
):
    i = pl.program_id(0)
    m_sc[...] = jnp.full_like(m_sc, NEG)
    l_sc[...] = jnp.zeros_like(l_sc)
    acc_sc[...] = jnp.zeros_like(acc_sc)
    qtag = qtag_ref[...]
    qt = qt_ref[...]
    q_pad = [head_rows(qt, h, False) for h in range(OWN_HEADS)]

    def step(kb, carry):
        rows = pl.ds(pl.multiple_of(kb * FK, FK), FK)
        seen = ktag_ref[rows, :] == qtag
        hs = range(OWN_HEADS)
        s = [mm(kv_ref[rows, 128 * h : 128 * (h + 1)], q_pad[h]) for h in hs]
        s = [jnp.where(seen, v, NEG) for v in s]
        m_old = [m_sc[h : h + 1, :] for h in hs]
        l_old = [l_sc[h : h + 1, :] for h in hs]
        m_new = [jnp.maximum(m_old[h], jnp.max(s[h], axis=0, keepdims=True)) for h in hs]
        p = [jnp.exp(s[h] - m_new[h]).astype(bf16) for h in hs]
        fade = [jnp.exp(m_old[h] - m_new[h]) for h in hs]
        one = jnp.ones((16, FK), bf16)
        v_one = [
            jnp.concatenate([kvt_ref[128 * h + HEAD_DIM : 128 * (h + 1), rows], one], axis=0)
            for h in hs
        ]
        out = [mm(v_one[h], p[h]) for h in hs]
        for h in hs:
            own = slice(HEAD_DIM * h, HEAD_DIM * (h + 1))
            acc_sc[own, :] = acc_sc[own, :] * fade[h] + out[h][:HEAD_DIM]
            l_sc[h : h + 1, :] = fade[h] * l_old[h] + out[h][HEAD_DIM : HEAD_DIM + 1]
            m_sc[h : h + 1, :] = m_new[h]
        return carry

    lax.fori_loop(span[i, 0], span[i, 1], step, 0)
    for h in range(OWN_HEADS):
        own = slice(HEAD_DIM * h, HEAD_DIM * (h + 1))
        total = l_sc[h : h + 1, :]
        ot_ref[own, :] = (acc_sc[own, :] / total).astype(bf16)
        lse_ref[h : h + 1, :] = m_sc[h : h + 1, :] + jnp.log(total)
    lse_ref[OWN_HEADS:, :] = jnp.zeros_like(lse_ref[OWN_HEADS:, :])


def attend(span, qtag, ktag, qt, kv, kvt):
    own = qt.shape[1]
    window = kv.shape[0]
    whole = lambda shape: pl.BlockSpec(shape, lambda i, s: (0, 0), pipeline_mode=pl.Buffered(1))
    cols = lambda rows: pl.BlockSpec((rows, BQ), lambda i, s: (0, i))
    return pl.pallas_call(
        attend_kernel,
        grid_spec=pltpu.PrefetchScalarGridSpec(
            num_scalar_prefetch=1,
            grid=(own // BQ,),
            in_specs=[
                cols(1),
                whole((window, 1)),
                cols(Q_ROWS),
                whole((window, KV_ROWS)),
                whole((KV_ROWS, window)),
            ],
            out_specs=[cols(Q_ROWS), cols(8)],
            scratch_shapes=[
                pltpu.VMEM((8, BQ), f32),
                pltpu.VMEM((8, BQ), f32),
                pltpu.VMEM((Q_ROWS, BQ), f32),
            ],
        ),
        out_shape=[
            jax.ShapeDtypeStruct((Q_ROWS, own), bf16),
            jax.ShapeDtypeStruct((8, own), f32),
        ],
        compiler_params=pltpu.CompilerParams(vmem_limit_bytes=60 << 20),
        cost_estimate=pl.CostEstimate(
            flops=4 * own * 2048 * Q_ROWS, bytes_accessed=20 << 20, transcendentals=own * 6144
        ),
        name="attend",
    )(span, qtag, ktag, qt, kv, kvt)


def grad_kernel(
    parts, final, span, qtag_ref, ktag_ref, qt_ref, dot_ref, ot_ref, lse_ref, kv_ref, kvt_ref, *rest
):
    if final:
        dq_in, dq_ref, *rest = rest
    else:
        dq_in, (dq_ref, *rest) = None, rest
    outs, (dq_sc, dkv_sc) = rest[: len(parts)], rest[len(parts) :]
    i = pl.program_id(0)

    @pl.when(i == 0)
    def _():
        dkv_sc[...] = jnp.zeros_like(dkv_sc)

    if final:
        dq_sc[...] = dq_in[...]
    else:
        dq_sc[...] = jnp.zeros_like(dq_sc)
    qtag = qtag_ref[...]
    qt, d_out, out = qt_ref[...], dot_ref[...], ot_ref[...]
    q_pad = [head_rows(qt, h, False) for h in range(OWN_HEADS)]
    d_pad = [head_rows(d_out, h, True) for h in range(OWN_HEADS)]
    product = d_out.astype(f32) * out.astype(f32)
    inner = [
        jnp.sum(product[HEAD_DIM * h : HEAD_DIM * (h + 1)], axis=0, keepdims=True)
        for h in range(OWN_HEADS)
    ]
    log_row = [lse_ref[h : h + 1, :] for h in range(OWN_HEADS)]

    def step(shift, kb, carry):
        rows = pl.ds(pl.multiple_of(kb * BK, BK), BK)
        place = pl.ds(pl.multiple_of((kb - shift) * BK, BK), BK)
        seen = ktag_ref[rows, :] == qtag
        hs = range(OWN_HEADS)
        kv = [kv_ref[rows, 128 * h : 128 * (h + 1)] for h in hs]
        s = [mm(kv[h], q_pad[h]) for h in hs]
        d_p = [mm(kv[h], d_pad[h]) for h in hs]
        p = [jnp.where(seen, jnp.exp(s[h] - log_row[h]), 0.0) for h in hs]
        d_s = [(p[h] * (d_p[h] - inner[h])).astype(bf16) for h in hs]
        p = [v.astype(bf16) for v in p]
        g_kv = [mm(q_pad[h], d_s[h], NT) + mm(d_pad[h], p[h], NT) for h in hs]
        g_q = [mm(kvt_ref[128 * h : 128 * h + HEAD_DIM, rows], d_s[h]) for h in hs]
        for h in hs:
            dkv_sc[128 * h : 128 * (h + 1), place] += g_kv[h]
            own = slice(HEAD_DIM * h, HEAD_DIM * (h + 1))
            dq_sc[own, :] += g_q[h]
        return carry

    (first, last), (first_b, last_b) = parts[0], parts[-1]
    low = jnp.maximum(span[i, 0], first)
    count = jnp.maximum(jnp.minimum(span[i, 1], last) - low, 0)
    if len(parts) == 1:
        lax.fori_loop(0, count, lambda n, c: step(first, low + n, c), 0)
    else:
        low_b = jnp.maximum(span[i, 0], first_b)
        count_b = jnp.maximum(jnp.minimum(span[i, 1], last_b) - low_b, 0)

        def either(n, c):
            right = n >= count
            kb = jnp.where(right, low_b + n - count, low + n)
            return step(jnp.where(right, first_b - (last - first), first), kb, c)

        lax.fori_loop(0, count + count_b, either, 0)
    if final:
        dq_ref[...] = (dq_sc[...] * score_scale).astype(bf16)
    else:
        dq_ref[...] = dq_sc[...]

    @pl.when(i == pl.num_programs(0) - 1)
    def _():
        base = 0
        for (first, last), ref in zip(parts, outs):
            width = (last - first) * BK
            ref[...] = dkv_sc[:, base : base + width].astype(ref.dtype)
            base += width


def attend_grad(parts, final, span, qtag, ktag, qt, d_out, out, lse, kv, kvt, dq_in=None):
    own = qt.shape[1]
    window = kv.shape[0]
    whole = lambda shape: pl.BlockSpec(shape, lambda i, s: (0, 0), pipeline_mode=pl.Buffered(1))
    cols = lambda rows: pl.BlockSpec((rows, BQ), lambda i, s: (0, i))
    widths = [(last - first) * BK for first, last in parts]
    dtype = f32 if final else bf16
    args = [span, qtag, ktag, qt, d_out, out, lse, kv, kvt] + ([dq_in] if final else [])
    return pl.pallas_call(
        functools.partial(grad_kernel, parts, final),
        grid_spec=pltpu.PrefetchScalarGridSpec(
            num_scalar_prefetch=1,
            grid=(own // BQ,),
            in_specs=[
                cols(1),
                whole((window, 1)),
                cols(Q_ROWS),
                cols(Q_ROWS),
                cols(Q_ROWS),
                cols(8),
                whole((window, KV_ROWS)),
                whole((KV_ROWS, window)),
            ]
            + ([cols(Q_ROWS)] if final else []),
            out_specs=[cols(Q_ROWS)] + [whole((KV_ROWS, w)) for w in widths],
            scratch_shapes=[
                pltpu.VMEM((Q_ROWS, BQ), f32),
                pltpu.VMEM((KV_ROWS, sum(widths)), f32),
            ],
        ),
        out_shape=[jax.ShapeDtypeStruct((Q_ROWS, own), bf16 if final else f32)]
        + [jax.ShapeDtypeStruct((KV_ROWS, w), dtype) for w in widths],
        compiler_params=pltpu.CompilerParams(vmem_limit_bytes=60 << 20),
        cost_estimate=pl.CostEstimate(
            flops=(10 if final else 2) * own * 1536 * Q_ROWS,
            bytes_accessed=20 << 20,
            transcendentals=own * 4096,
        ),
        name="grad_own" if final else "grad_far",
    )(*args)


MESH = pl.DeviceIdType.MESH
CHUNKS = 8
W_LANES = 640
KV_AT = 256


def remote(src, dst, send, recv, target):
    return pltpu.make_async_remote_copy(
        src_ref=src,
        dst_ref=dst,
        send_sem=send,
        recv_sem=recv,
        device_id=(target,),
        device_id_type=MESH,
    )


def share_kernel(
    n_dev, rows_w, tok_ref, code_ref, w_ref, x_own, code_out, ktag_out, w_turn, qt_out, kv_out, kvt_out,
    c_out, x_out, w_out, w_wide, w_full, qt_sc, kv_sc, kvt_sc,
    w_send, w_recv, c_send, c_recv, part_send, part_recv, mate_send, mate_recv,
    up_send, up_recv, down_send, down_recv, cross_send, cross_recv,
    fwd_send, fwd_recv, keep_sem, x_sem, q_sem, kv_sem, kvt_sem,
):
    n_group = n_dev // GROUP
    me = lax.axis_index("fsdp")
    g = me // GROUP
    s = me % GROUP
    k = s % 2
    hi = s // 2
    partner = me + 1 - 2 * k
    mate = me + 2 - 4 * hi
    mate_block = 4 + k - 2 * hi
    has_up = g < n_group - 1
    has_down = g > 0
    rows = tok_ref.shape[0] // CHUNKS
    half = CHUNKS // 2

    barrier = pltpu.get_barrier_semaphore()

    def greet(r, carry):
        pl.semaphore_signal(
            barrier, inc=1, device_id=(lax.rem(me + r, n_dev),), device_id_type=MESH
        )
        return carry

    lax.fori_loop(1, n_dev, greet, 0)
    pl.semaphore_wait(barrier, n_dev - 1)

    def chunk(ref, c):
        return ref.at[pl.ds(pl.multiple_of(c * rows, rows), rows)]

    def spot(b, c):
        return x_out.at[b, pl.ds(pl.multiple_of(c * rows, rows), rows)]

    def to_partner(c):
        return remote(chunk(tok_ref, c), spot(2 + s, c), part_send.at[c], part_recv.at[c], partner)

    def to_mate(c):
        return remote(chunk(tok_ref, c), spot(2 + s, c), mate_send.at[c], mate_recv.at[c], mate)

    def up_own(c):
        return remote(chunk(tok_ref, c), spot(k, c), up_send.at[c], up_recv.at[c], me + GROUP)

    def up_mate(c):
        return remote(spot(mate_block, c), spot(k, c), up_send.at[c], up_recv.at[c], me + GROUP)

    def down_own(c):
        return remote(
            chunk(tok_ref, c), spot(6 + k, c), down_send.at[c], down_recv.at[c], me - GROUP
        )

    def down_mate(c):
        return remote(
            spot(mate_block, c + half), spot(6 + k, c + half), down_send.at[c], down_recv.at[c],
            me - GROUP,
        )

    def cross(c):
        at = c + half * hi
        return remote(spot(6 + k, at), spot(6 + k, at), cross_send.at[c], cross_recv.at[c], mate)

    def forward(b, c, slot):
        return remote(spot(b, c), spot(b, c), fwd_send.at[slot], fwd_recv.at[slot], partner)

    keep_x = pltpu.make_async_copy(tok_ref, x_out.at[2 + s], keep_sem.at[0])
    keep_c = pltpu.make_async_copy(code_ref, c_out.at[2 + s], keep_sem.at[1])
    keep_w = pltpu.make_async_copy(w_ref.at[s], w_out.at[me], keep_sem.at[2])
    keep_x.start()
    keep_c.start()
    keep_w.start()

    def w_copy(r):
        target = lax.rem(me + r, n_dev)
        return remote(
            w_ref.at[lax.rem(target, GROUP)], w_out.at[me], w_send.at[r], w_recv.at[r], target
        )

    def w_start(r, carry):
        w_copy(r).start()
        return carry

    def c_group(j):
        target = GROUP * g + lax.rem(s + j, GROUP)
        return remote(code_ref, c_out.at[2 + s], c_send.at[j], c_recv.at[2 + s], target)

    def c_far(j):
        step = GROUP * (2 * hi - 1)
        b = 6 + s - 8 * hi
        target = GROUP * g + step + j
        return remote(code_ref, c_out.at[b], c_send.at[GROUP + j], c_recv.at[b], target)

    sends_far = jnp.where(hi == 1, g < n_group - 1, g > 0)
    for j in range(1, GROUP):
        c_group(j).start()

    @pl.when(sends_far)
    def _():
        for j in range(GROUP):
            c_far(j).start()

    order = list(range(half, CHUNKS)) + list(range(half))

    @pl.when((hi == 0) & has_down)
    def _():
        for c in range(half):
            down_own(c).start()

    for n, c in enumerate(order):
        to_mate(c).start()
        to_partner(c).start()
        if n < half:

            @pl.when((hi == 1) & has_up)
            def _():
                up_own(c).start()

        if n == half - 1:
            lax.fori_loop(1, n_dev, w_start, 0)

    for n, c in enumerate(order):
        to_mate(c).wait_recv()
        forward(mate_block, c, c).start()

        @pl.when((hi == 0) & has_up)
        def _():
            up_mate(c).start()

        if n < half:

            @pl.when((hi == 1) & has_down)
            def _():
                down_mate(c - half).start()

        else:

            @pl.when((hi == 1) & has_up)
            def _():
                up_own(c).start()

    @pl.when(has_up)
    def _():
        for c in range(half):
            down_own(c).wait_recv()
            cross(c).start()
            forward(6 + k, c + half * hi, 2 * CHUNKS + c).start()

    def w_wait(r, carry):
        w_copy(r).wait_recv()
        return carry

    lax.fori_loop(1, n_dev, w_wait, 0)
    keep_w.wait()
    keep_x.wait()
    bias_row = jnp.zeros((8, W_LANES), f32)
    bias_at = w_ref.shape[1] - 8
    for j in range(n_dev):
        w_wide[rows_w * j : rows_w * (j + 1), :] = w_out[j, :rows_w, :].astype(f32)
        bias_row = bias_row + w_out[j, bias_at:, :].astype(f32)
    bias_row = jnp.sum(bias_row, axis=0, keepdims=True)
    bias_col = jnp.broadcast_to(bias_row, (128, W_LANES)).T[:, :1]
    w_full[...] = w_wide[...].astype(bf16)
    w_turn[...] = w_wide[...].T.astype(bf16)
    piece = 512
    pieces = tok_ref.shape[0] // piece

    def project(b, inside):
        def one(j, carry):
            x = x_out[b, pl.ds(pl.multiple_of(j * piece, piece), piece), :]
            at = pl.ds(pl.multiple_of((b * pieces + j) * piece, piece), piece)
            kv = mm(x, w_full[:, KV_AT:]) + bias_row[:, KV_AT:]
            kv_sc[at, :] = kv.astype(bf16)
            kvt_sc[:, at] = (mm(w_turn[KV_AT:, :], x, NT) + bias_col[KV_AT:]).astype(bf16)
            if inside:
                to = pl.ds(pl.multiple_of(((b - 2) * pieces + j) * piece, piece), piece)
                q = (mm(w_turn[:Q_ROWS, :], x, NT) + bias_col[:Q_ROWS]).astype(bf16)
                qt_sc[:, to] = q * jnp.asarray(score_scale, bf16)
            return carry

        lax.fori_loop(0, pieces, one, 0)

    def outs(b, inside):
        whole = tok_ref.shape[0]
        at = pl.ds(pl.multiple_of(b * whole, whole), whole)
        copies = [
            pltpu.make_async_copy(kv_sc.at[at], kv_out.at[at], kv_sem.at[b]),
            pltpu.make_async_copy(kvt_sc.at[:, at], kvt_out.at[:, at], kvt_sem.at[b]),
        ]
        if inside:
            to = pl.ds(pl.multiple_of((b - 2) * whole, whole), whole)
            copies.append(pltpu.make_async_copy(qt_sc.at[:, to], qt_out.at[:, to], q_sem.at[b - 2]))
            copies.append(pltpu.make_async_copy(x_out.at[b], x_own.at[b - 2], x_sem.at[b - 2]))
        return copies

    def put(b, inside):
        for copy in outs(b, inside):
            copy.start()

    keep_c.wait()
    for j in range(1, GROUP):
        remote(
            code_ref, c_out.at[0], c_send.at[j], c_recv.at[2 + lax.rem(s + j, GROUP)], partner
        ).wait_recv()

    @pl.when(has_down)
    def _():
        for b in range(2):
            remote(code_ref, c_out.at[b], c_send.at[0], c_recv.at[b], partner).wait_recv()

    @pl.when(has_up)
    def _():
        for b in range(6, 8):
            remote(code_ref, c_out.at[b], c_send.at[0], c_recv.at[b], partner).wait_recv()

    for b in range(8):
        code = c_out[b]
        if b < 2:
            code = jnp.where(has_down, code, -2)
        if b >= 6:
            code = jnp.where(has_up, code, 2 * n_dev * tok_ref.shape[0])
        code_out[b] = code
        tag = jnp.where((code & 1) == 1, (code >> 1) + 1, 0)
        lanes = tag.shape[1]
        for r in range(8):
            turned = jnp.broadcast_to(tag[r : r + 1, :], (lanes, lanes)).T
            at = (8 * b + r) * lanes
            ktag_out[at : at + lanes, :] = turned[:, :1]

    own_block = 2 + s
    near_block = own_block + 1 - 2 * k
    across_block = mate_block + 1 - 2 * k
    project(own_block, True)

    project(mate_block, True)
    put(own_block, True)

    @pl.when(has_down)
    def _():
        for c in order:
            up_own(c).wait_recv()
            forward(k, c, CHUNKS + c).start()

    for c in range(CHUNKS):
        to_partner(c).wait_recv()
    project(near_block, True)
    put(mate_block, True)

    @pl.when(has_up)
    def _():
        for c in range(half):
            cross(c).wait_recv()
            forward(6 + k, c + half * (1 - hi), 2 * CHUNKS + half + c).start()

    for c in range(CHUNKS):
        forward(mate_block, c, c).wait_recv()
    project(across_block, True)
    put(near_block, True)

    @pl.when(has_down)
    def _():
        project(k, False)
        for c in range(CHUNKS):
            forward(k, c, CHUNKS + c).wait_recv()
        project(1 - k, False)
        put(k, False)

    put(across_block, True)

    @pl.when(has_up)
    def _():
        project(6 + k, False)
        for c in range(half):
            forward(6 + k, c, 2 * CHUNKS + c).wait_recv()
            forward(6 + k, c, 2 * CHUNKS + half + c).wait_recv()
        project(7 - k, False)
        put(6 + k, False)

    for c in range(CHUNKS):
        to_partner(c).wait_send()
        to_mate(c).wait_send()
        forward(mate_block, c, c).wait_send()

    @pl.when(has_down)
    def _():
        put(1 - k, False)
        for c in range(CHUNKS):
            forward(k, c, CHUNKS + c).wait_send()
        for c in range(half):
            down_own(c).wait_send()

    @pl.when(has_up)
    def _():
        for c in range(half):
            cross(c).wait_send()
            forward(6 + k, c, 2 * CHUNKS + c).wait_send()
            forward(6 + k, c, 2 * CHUNKS + half + c).wait_send()
        for c in range(CHUNKS):
            up_own(c).wait_send()
        put(7 - k, False)

    for j in range(1, GROUP):
        c_group(j).wait_send()

    @pl.when(sends_far)
    def _():
        for j in range(GROUP):
            c_far(j).wait_send()

    def w_sent(r, carry):
        w_copy(r).wait_send()
        return carry

    lax.fori_loop(1, n_dev, w_sent, 0)
    for b in range(2, 6):
        for copy in outs(b, True):
            copy.wait()

    @pl.when(has_down)
    def _():
        for b in range(2):
            for copy in outs(b, False):
                copy.wait()

    @pl.when(has_up)
    def _():
        for b in range(6, 8):
            for copy in outs(b, False):
                copy.wait()


def share(n_dev, rows_w, tokens, code, w_send):
    vmem = pl.BlockSpec(memory_space=pltpu.VMEM)
    anywhere = pl.BlockSpec(memory_space=pl.ANY)
    dma = lambda n: pltpu.SemaphoreType.DMA((n,))
    half = CHUNKS // 2
    rows, width = tokens.shape
    own, window = GROUP * rows, 8 * rows
    return pl.pallas_call(
        functools.partial(share_kernel, n_dev, rows_w),
        in_specs=[vmem] * 3,
        out_specs=[anywhere, vmem, vmem, vmem, anywhere, anywhere, anywhere],
        out_shape=[
            jax.ShapeDtypeStruct((GROUP, rows, width), bf16),
            jax.ShapeDtypeStruct((8,) + code.shape, code.dtype),
            jax.ShapeDtypeStruct((window, 1), code.dtype),
            jax.ShapeDtypeStruct((W_LANES, width), bf16),
            jax.ShapeDtypeStruct((Q_ROWS, own), bf16),
            jax.ShapeDtypeStruct((window, KV_ROWS), bf16),
            jax.ShapeDtypeStruct((KV_ROWS, window), bf16),
        ],
        scratch_shapes=[
            pltpu.VMEM((8,) + code.shape, code.dtype),
            pltpu.VMEM((8, rows, width), bf16),
            pltpu.VMEM((n_dev,) + w_send.shape[1:], bf16),
            pltpu.VMEM((width, W_LANES), f32),
            pltpu.VMEM((width, W_LANES), bf16),
            pltpu.VMEM((Q_ROWS, own), bf16),
            pltpu.VMEM((window, KV_ROWS), bf16),
            pltpu.VMEM((KV_ROWS, window), bf16),
            dma(n_dev), dma(n_dev), dma(2 * GROUP), dma(8),
            dma(CHUNKS), dma(CHUNKS), dma(CHUNKS), dma(CHUNKS),
            dma(CHUNKS), dma(CHUNKS), dma(half), dma(half), dma(half), dma(half),
            dma(3 * CHUNKS), dma(3 * CHUNKS), dma(3), dma(GROUP), dma(GROUP), dma(8), dma(8),
        ],
        compiler_params=pltpu.CompilerParams(
            collective_id=0, has_side_effects=True, vmem_limit_bytes=60 << 20
        ),
        name="share",
    )(tokens, code, w_send)


PARTS = 4
TN = (((0,), (0,)), ((), ()))


def settle_kernel(
    n_dev, rows_w, q_ref, kv_ref, x_ref, w_ref, vec_ref, own_out, near_out, far_out, grad_out, vec_sum,
    w_out, vec_out, wide, slabs, across, near, relay, total,
    w_send, w_recv, vec_send, vec_recv, near_send, near_recv, relay_send, relay_recv,
    far_send, far_recv, keep_sem,
):
    me = lax.axis_index("fsdp")
    s = me % GROUP
    k = s % 2
    hi = s // 2
    partner = me + 1 - 2 * k
    mate = me + 2 - 4 * hi
    s_partner = s + 1 - 2 * k
    s_mate = s + 2 - 4 * hi
    s_across = 3 - s
    block = own_out.shape[0]
    rows = block // PARTS

    barrier = pltpu.get_barrier_semaphore()

    def greet(r, carry):
        pl.semaphore_signal(
            barrier, inc=1, device_id=(lax.rem(me + r, n_dev),), device_id_type=MESH
        )
        return carry

    lax.fori_loop(1, n_dev, greet, 0)
    pl.semaphore_wait(barrier, n_dev - 1)

    def part(c):
        return pl.ds(pl.multiple_of(c * rows, rows), rows)

    def to_relay(c):
        return remote(
            across.at[part(c)], relay.at[part(c)], relay_send.at[c], relay_recv.at[c], partner
        )

    def to_near(c):
        return remote(
            near.at[part(c)], near_out.at[part(c)], near_send.at[c], near_recv.at[c], partner
        )

    def to_far(c):
        return remote(total.at[part(c)], far_out.at[part(c)], far_send.at[c], far_recv.at[c], mate)

    def w_copy(r):
        target = lax.rem(me + r, n_dev)
        return remote(slabs.at[target], w_out.at[me], w_send.at[r], w_recv.at[r], target)

    def vec_copy(r):
        target = lax.rem(me + r, n_dev)
        return remote(vec_ref.at[target], vec_out.at[me], vec_send.at[r], vec_recv.at[r], target)

    def vec_start(r, carry):
        vec_copy(r).start()
        return carry

    lax.fori_loop(1, n_dev, vec_start, 0)
    keep_vec = pltpu.make_async_copy(vec_ref.at[me], vec_out.at[me], keep_sem.at[1])
    keep_vec.start()

    def back(t, c):
        at = pl.ds(pl.multiple_of(t * block + c * rows, rows), rows)
        return mm(q_ref[:, at], w_ref[:Q_ROWS, :], TN) + mm(kv_ref[:, at], w_ref[KV_AT:, :], TN)

    def add_rows(j, carry):
        at = pl.ds(pl.multiple_of(j * block, block), block)
        wide[:Q_ROWS, :] += mm(q_ref[:, at], x_ref[at, :])
        wide[Q_ROWS:MIX_ROWS, :] += mm(kv_ref[:, at], x_ref[at, :])

        @pl.when(j == 0)
        def _():
            to_far(PARTS - 1).start()

        return carry

    def w_start(r, carry):
        w_copy(r).start()
        return carry

    def make_across(c, carry):
        across[part(c), :] = back(s_across, c).astype(bf16)

        @pl.when(c > 0)
        def _():
            to_relay(c - 1).start()

        return carry

    def make_far(c, carry):
        mine = back(s_mate, c)

        @pl.when(c == 0)
        def _():
            to_relay(PARTS - 1).start()

        to_relay(c).wait_recv()
        total[part(c), :] = (mine + relay[part(c), :].astype(f32)).astype(bf16)

        @pl.when(c > 0)
        def _():
            to_far(c - 1).start()

        return carry

    def make_near(c, carry):
        near[part(c), :] = back(s_partner, c).astype(bf16)

        @pl.when(c == 0)
        def _():
            lax.fori_loop(1, n_dev, w_start, 0)

        @pl.when(c > 0)
        def _():
            to_near(c - 1).start()

        return carry

    def make_own(c, carry):
        own_out[part(c), :] = back(s, c)

        @pl.when(c == 0)
        def _():
            to_near(PARTS - 1).start()

        return carry

    lax.fori_loop(0, PARTS, make_across, 0)
    wide[...] = jnp.zeros_like(wide)
    lax.fori_loop(0, PARTS, make_far, 0)
    lax.fori_loop(0, GROUP, add_rows, 0)
    turned = wide[...].T
    one = jnp.ones((8, GROUP * block), bf16)
    bias_q = mm(one, q_ref[...], NT).astype(bf16)
    bias_kv = mm(one, kv_ref[...], NT).astype(bf16)
    bias_at = slabs.shape[1] - 8
    for j in range(n_dev):
        slabs[j, :rows_w, :] = turned[rows_w * j : rows_w * (j + 1), :].astype(bf16)
        slabs[j, bias_at:, :Q_ROWS] = bias_q
        slabs[j, bias_at:, Q_ROWS:MIX_ROWS] = bias_kv
    lax.fori_loop(0, PARTS, make_near, 0)
    keep_w = pltpu.make_async_copy(slabs.at[me], w_out.at[me], keep_sem.at[0])
    keep_w.start()
    lax.fori_loop(0, PARTS, make_own, 0)
    for c in range(PARTS):
        to_relay(c).wait_send()
        to_near(c).wait()
        to_far(c).wait()

    def finish(r, carry):
        w_copy(r).wait()
        vec_copy(r).wait()
        return carry

    lax.fori_loop(1, n_dev, finish, 0)
    keep_w.wait()
    keep_vec.wait()
    vec_sum[...] = jnp.sum(vec_out[...], axis=0)
    for t in range(GROUP):
        got = w_out[t].astype(f32)
        for j in range(1, n_dev // GROUP):
            got = got + w_out[GROUP * j + t].astype(f32)
        grad_out[:, Q_ROWS * t : Q_ROWS * (t + 1)] = got[:, :Q_ROWS]
        for h in range(OWN_HEADS):
            for part_at in range(2):
                at = Q_ROWS + 128 * h + HEAD_DIM * part_at
                to = D * (1 + part_at) + Q_ROWS * t + HEAD_DIM * h
                grad_out[:, to : to + HEAD_DIM] = got[:, at : at + HEAD_DIM]


def settle(n_dev, rows_w, d_q, d_kv, x, w, vec):
    vmem = pl.BlockSpec(memory_space=pltpu.VMEM)
    anywhere = pl.BlockSpec(memory_space=pl.ANY)
    dma = lambda n: pltpu.SemaphoreType.DMA((n,))
    block = (x.shape[0] // GROUP, x.shape[1])
    slabs = (n_dev, rows_w + -rows_w % 8 + 8, W_LANES)
    return pl.pallas_call(
        functools.partial(settle_kernel, n_dev, rows_w),
        in_specs=[vmem] * 5,
        out_specs=[vmem, anywhere, anywhere, vmem, vmem],
        out_shape=[
            jax.ShapeDtypeStruct(block, f32),
            jax.ShapeDtypeStruct(block, bf16),
            jax.ShapeDtypeStruct(block, bf16),
            jax.ShapeDtypeStruct((slabs[1], 3 * D), f32),
            jax.ShapeDtypeStruct(vec.shape[1:], vec.dtype),
        ],
        scratch_shapes=[
            pltpu.VMEM(slabs, bf16),
            pltpu.VMEM(vec.shape, vec.dtype),
            pltpu.VMEM((W_LANES, x.shape[1]), f32),
            pltpu.VMEM(slabs, bf16),
            pltpu.VMEM(block, bf16), pltpu.VMEM(block, bf16),
            pltpu.VMEM(block, bf16), pltpu.VMEM(block, bf16),
            dma(n_dev), dma(n_dev), dma(n_dev), dma(n_dev),
            dma(PARTS), dma(PARTS), dma(PARTS), dma(PARTS), dma(PARTS), dma(PARTS), dma(2),
        ],
        compiler_params=pltpu.CompilerParams(
            collective_id=1, has_side_effects=True, vmem_limit_bytes=60 << 20
        ),
        name="settle",
    )(d_q, d_kv, x, w, vec)


def swap_kernel(spread, in_ref, out_ref, send, recv, keep_sem):
    me = lax.axis_index("fsdp")
    s = me % GROUP
    start = me - s
    width = (in_ref if spread else out_ref).shape[1] // GROUP

    barrier = pltpu.get_barrier_semaphore()
    for j in range(1, GROUP):
        target = start + lax.rem(s + j, GROUP)
        pl.semaphore_signal(barrier, inc=1, device_id=(target,), device_id_type=MESH)
    pl.semaphore_wait(barrier, GROUP - 1)

    def cols(ref, t):
        return ref.at[:, pl.ds(pl.multiple_of(t * width, width), width)]

    def rows(ref, t):
        return ref.at[pl.ds(pl.multiple_of(t * Q_ROWS, Q_ROWS), Q_ROWS)]

    def ends(t):
        if spread:
            return cols(in_ref, t), rows(out_ref, s)
        return rows(in_ref, t), cols(out_ref, s)

    def copy(j):
        t = lax.rem(s + j, GROUP)
        src, dst = ends(t)
        return remote(src, dst, send.at[j], recv.at[j], start + t)

    for j in (2, 1, 3):
        copy(j).start()
    src, dst = ends(s)
    keep = pltpu.make_async_copy(src, dst, keep_sem.at[0])
    keep.start()
    for j in range(1, GROUP):
        copy(j).wait()
    keep.wait()


def swap(x, spread):
    shape = (x.shape[0] * GROUP, x.shape[1] // GROUP) if spread else (
        x.shape[0] // GROUP, x.shape[1] * GROUP
    )
    dma = lambda n: pltpu.SemaphoreType.DMA((n,))
    return pl.pallas_call(
        functools.partial(swap_kernel, spread),
        in_specs=[pl.BlockSpec(memory_space=pltpu.VMEM)],
        out_specs=pl.BlockSpec(memory_space=pltpu.VMEM),
        out_shape=jax.ShapeDtypeStruct(shape, x.dtype),
        scratch_shapes=[dma(GROUP), dma(GROUP), dma(1)],
        compiler_params=pltpu.CompilerParams(
            collective_id=2 if spread else 3, has_side_effects=True
        ),
        name="swap_out" if spread else "swap_back",
    )(x)


def body(
    n_dev,
    tokens,
    segment_ids,
    pad_mask,
    w_qkv,
    bias_query,
    bias_value,
    w_out,
    bias_out,
    gain_one,
    shift_one,
    w_up,
    bias_up,
    w_down,
    bias_down,
    gain_two,
    shift_two,
    cotangent,
):
    row_count = tokens.shape[0]
    rows_w = w_qkv.shape[0]
    own = GROUP * row_count
    window = own + 2 * LEN_MAX
    me = lax.axis_index("fsdp")
    place = me % GROUP
    group_id = me // GROUP
    n_group = n_dev // GROUP
    up = [(i, i + GROUP) for i in range(n_dev - GROUP)]
    down = [(i + GROUP, i) for i in range(n_dev - GROUP)]

    wq = w_qkv[:, :D].reshape(rows_w, GROUP, Q_ROWS)
    wk = w_qkv[:, D : 2 * D].reshape(rows_w, GROUP, OWN_HEADS, 1, HEAD_DIM)
    wv = w_qkv[:, 2 * D :].reshape(rows_w, GROUP, OWN_HEADS, 1, HEAD_DIM)
    wkv = jnp.concatenate([wk, wv], axis=3).reshape(rows_w, GROUP, KV_ROWS)
    gap = KV_AT - Q_ROWS
    lane = jnp.arange(gap)[None, :]
    small_cols = jnp.pad(bias_up.reshape(rows_w, -1), ((0, 0), (6, gap - 10)))
    for j, v in enumerate([bias_out, gain_one, shift_one, bias_down, gain_two, shift_two]):
        small_cols = jnp.where(lane == j, v[:, None], small_cols)
    small_cols = jnp.broadcast_to(small_cols[:, None], (rows_w, GROUP, gap))
    w_cut = jnp.concatenate([wq, small_cols, wkv], axis=2).transpose(1, 0, 2)
    column = me * rows_w + jnp.arange(rows_w)
    feature = jnp.arange(D)
    spread = lambda bias: jnp.sum(
        jnp.where(feature[None] == column[:, None], bias.astype(f32)[:, None], 0.0), axis=0
    )
    bias_q = spread(bias_query).reshape(GROUP, Q_ROWS)
    bias_v = spread(bias_value).reshape(GROUP, OWN_HEADS, 1, HEAD_DIM)
    bias_kv = jnp.concatenate([jnp.zeros_like(bias_v), bias_v], axis=2).reshape(GROUP, KV_ROWS)
    bias_cut = jnp.concatenate([bias_q, jnp.zeros((GROUP, gap), f32), bias_kv], axis=1)
    fill = -rows_w % 8
    bias_cut = jnp.pad(bias_cut.astype(bf16)[:, None], ((0, 0), (fill, 7), (0, 0)))
    w_send = jnp.concatenate([w_cut, bias_cut], axis=1)
    ff = w_up.shape[1]
    out_down = jnp.concatenate([w_out, w_down], axis=0)
    out_down = lax.all_gather(out_down, "fsdp", axis=0)
    wo_full = out_down[:, :rows_w].reshape(D, D)
    wd_full = lax.optimization_barrier(out_down[:, rows_w:].reshape(ff, D))
    wu_full = lax.all_gather(w_up, "fsdp", axis=0, tiled=True)

    code = (segment_ids * 2 + pad_mask).reshape(8, row_count // 8)
    x_own, code_win, ktag, w_turn, qt, kv, kvt = share(n_dev, rows_w, tokens, code, w_send)
    x_own = x_own.reshape(own, D)
    code_win = code_win.reshape(window)
    code_own = code_win[LEN_MAX : LEN_MAX + own]
    small_all = w_turn[Q_ROWS : Q_ROWS + 10].astype(f32)
    bu_full = small_all[6:].T.reshape(-1)
    bo_full, g1_full, s1_full, bd_full, g2_full, s2_full = [small_all[j] for j in range(6)]
    seg_win = code_win >> 1
    seg_own = code_own >> 1
    qtag = (seg_own + 1).reshape(1, own)
    first_seg = seg_own[::BQ]
    last_seg = seg_own[BQ - 1 :: BQ]
    low = jnp.sum((seg_win[None, :] < first_seg[:, None]).astype(jnp.int32), axis=1)
    high = jnp.sum((seg_win[None, :] <= last_seg[:, None]).astype(jnp.int32), axis=1)
    spans = [jnp.stack([low // b, (high + b - 1) // b], axis=1) for b in (FK, BK)]

    ot, lse = attend(spans[0], qtag, ktag, qt, kv, kvt)
    ctx_t = swap(ot, True)

    tokens_f = tokens.astype(f32)
    branch = jnp.einsum("ir,io->ro", ctx_t, wo_full, preferred_element_type=f32) + bo_full
    first, norm_one_back = jax.vjp(norm_rows, tokens_f + branch, g1_full, s1_full)
    up_in = lax.optimization_barrier(first.astype(bf16))
    pre_act = jnp.dot(up_in, wu_full, preferred_element_type=f32) + bu_full
    gelu_val, gelu_back = jax.vjp(gelu_exact, pre_act)
    hidden = gelu_val.astype(bf16)
    ffn = jnp.dot(hidden, wd_full, preferred_element_type=f32) + bd_full
    result, norm_two_back = jax.vjp(norm_rows, first + ffn, g2_full, s2_full)
    layer_out = result.astype(bf16)
    d_second, d_gain_two, d_shift_two = norm_two_back(cotangent.astype(f32))
    d_ffn = d_second.astype(bf16)
    d_bias_down = jnp.sum(d_ffn.astype(f32), axis=0)
    d_w_down = jnp.einsum("rf,rd->fd", hidden, d_ffn, preferred_element_type=f32)
    d_hidden = jnp.einsum("rd,fd->rf", d_ffn, wd_full, preferred_element_type=f32)
    d_pre = gelu_back(d_hidden)[0].astype(bf16)
    d_bias_up = jnp.sum(d_pre.astype(f32), axis=0)
    d_w_up = jnp.einsum("rd,rf->df", up_in, d_pre, preferred_element_type=f32).astype(bf16)
    d_w_up = lax.optimization_barrier(d_w_up)
    d_first = d_second + jnp.einsum("rf,df->rd", d_pre, wu_full, preferred_element_type=f32)
    d_mid, d_gain_one, d_shift_one = norm_one_back(d_first)
    d_branch = d_mid.astype(bf16)
    d_bias_out = jnp.sum(d_branch.astype(f32), axis=0)
    d_w_out = jnp.einsum("ir,ro->io", ctx_t, d_branch, preferred_element_type=f32)
    dctx_t = jnp.einsum("ro,io->ir", d_branch, wo_full, preferred_element_type=f32).astype(bf16)
    n_up = ff // D
    big_grad = jnp.concatenate(
        [
            d_w_down.astype(bf16).reshape(n_dev, -1, D),
            d_w_out.astype(bf16).reshape(n_dev, rows_w, D),
        ]
        + [d_w_up[:, D * j : D * (j + 1)].reshape(n_dev, rows_w, D) for j in range(n_up)],
        axis=1,
    )
    big_owned = lax.psum_scatter(big_grad, "fsdp", scatter_dimension=0).astype(f32)
    rows_d = w_down.shape[0]
    g_down, g_out = big_owned[:rows_d], big_owned[rows_d : rows_d + rows_w]
    g_up = jnp.concatenate(
        [big_owned[rows_d + rows_w * (j + 1) : rows_d + rows_w * (j + 2)] for j in range(n_up)], axis=1
    )

    d_out = swap(dctx_t, False)
    edge, inside = LEN_MAX // BK, own // BK
    far_parts = ((0, edge), (edge + inside, 2 * edge + inside))
    own_parts = ((edge, edge + inside),)
    dq_far, dkv_left, dkv_right = attend_grad(
        far_parts, False, spans[1], qtag, ktag, qt, d_out, ot, lse, kv, kvt
    )
    from_right = lax.ppermute(dkv_left, "fsdp", down)
    from_left = lax.ppermute(dkv_right, "fsdp", up)
    dq_t, dkv_own = attend_grad(
        own_parts, True, spans[1], qtag, ktag, qt, d_out, ot, lse, kv, kvt, dq_far
    )
    dkv = jnp.concatenate(
        [
            dkv_own[:, :LEN_MAX] + from_left.astype(f32),
            dkv_own[:, LEN_MAX : own - LEN_MAX],
            dkv_own[:, own - LEN_MAX :] + from_right.astype(f32),
        ],
        axis=1,
    ).astype(bf16)
    vecs = jnp.stack([d_bias_out, d_gain_one, d_shift_one, d_bias_down, d_gain_two, d_shift_two])
    vec_send = jnp.concatenate(
        [
            vecs.reshape(6, n_dev, rows_w).transpose(1, 0, 2).reshape(n_dev, 6 * rows_w),
            d_bias_up.reshape(n_dev, 4 * rows_w),
        ],
        axis=1,
    )
    vec_send = jnp.pad(vec_send, ((0, 0), (0, 1024 - vec_send.shape[1]))).reshape(n_dev, 8, 128)
    own_x, near, far, got, vec = settle(n_dev, rows_w, dq_t, dkv, x_own, w_turn, vec_send)
    grad_tokens = d_mid + ((own_x + near.astype(f32)) + far.astype(f32))
    grad_w_qkv = got[:rows_w]
    bias_rows = got[-8].reshape(3, D)
    bias_own = lax.dynamic_slice(bias_rows, (0, me * rows_w), (3, rows_w))
    vec = vec.reshape(-1)[: 10 * rows_w]
    own_vec = [bias_own[0], bias_own[2]] + [vec[j * rows_w : (j + 1) * rows_w] for j in range(6)]
    return (
        layer_out,
        grad_tokens,
        grad_w_qkv,
        own_vec[0],
        own_vec[1],
        g_out,
        own_vec[2],
        own_vec[3],
        own_vec[4],
        g_up,
        vec[6 * rows_w :],
        g_down,
        own_vec[5],
        own_vec[6],
        own_vec[7],
    )


def solution(mesh):
    rows, flat = P("fsdp", None), P("fsdp")
    return jax.shard_map(
        functools.partial(body, mesh.shape["fsdp"]),
        mesh=mesh,
        in_specs=(
            rows, flat, flat, rows, flat, flat, rows, flat, flat, flat, rows, flat, rows, flat,
            flat, flat, rows,
        ),
        out_specs=(
            rows, rows, rows, flat, flat, rows, flat, flat, flat, rows, flat, rows, flat, flat,
            flat,
        ),
        check_vma=False,
    )
```

```python
import functools

import jax
import jax.numpy as jnp
from jax import lax
from jax.experimental import pallas as pl
from jax.experimental.pallas import tpu as pltpu
from jax.sharding import PartitionSpec as P

D = 768
HEADS = 12
HEAD_DIM = 64
LEN_MAX = 2048
GROUP = 4
OWN_HEADS = HEADS // GROUP
Q_ROWS = OWN_HEADS * HEAD_DIM
KV_ROWS = 2 * Q_ROWS
MIX_ROWS = Q_ROWS + KV_ROWS
BQ = 512
FK = 512
BK = 256
NEG = -1e30

bf16 = jnp.bfloat16
f32 = jnp.float32
eps_norm = 1e-12
score_scale = 0.125

NN = (((1,), (0,)), ((), ()))
NT = (((1,), (1,)), ((), ()))


def mm(a, b, dims=NN):
    return lax.dot_general(a, b, dims, preferred_element_type=f32)


def norm_rows(hidden, gain_row, shift_row):
    centre = hidden - jnp.mean(hidden, axis=-1, keepdims=True)
    spread = jnp.mean(centre * centre, axis=-1, keepdims=True)
    return centre * lax.rsqrt(spread + eps_norm) * gain_row + shift_row


def gelu_exact(pre_act):
    return 0.5 * pre_act * (1.0 + jax.scipy.special.erf(pre_act * 0.7071067811865476))


def head_rows(block, h, upper):
    zero = jnp.zeros_like(block[:HEAD_DIM])
    rows = block[h * HEAD_DIM : (h + 1) * HEAD_DIM]
    return jnp.concatenate([zero, rows] if upper else [rows, zero], axis=0)


def attend_kernel(
    span, qtag_ref, ktag_ref, qt_ref, kv_ref, kvt_ref, ot_ref, lse_ref, m_sc, l_sc, acc_sc
):
    i = pl.program_id(0)
    m_sc[...] = jnp.full_like(m_sc, NEG)
    l_sc[...] = jnp.zeros_like(l_sc)
    acc_sc[...] = jnp.zeros_like(acc_sc)
    qtag = qtag_ref[...]
    qt = qt_ref[...]
    q_pad = [head_rows(qt, h, False) for h in range(OWN_HEADS)]

    def step(kb, carry):
        rows = pl.ds(pl.multiple_of(kb * FK, FK), FK)
        seen = ktag_ref[rows, :] == qtag
        hs = range(OWN_HEADS)
        s = [mm(kv_ref[rows, 128 * h : 128 * (h + 1)], q_pad[h]) for h in hs]
        s = [jnp.where(seen, v, NEG) for v in s]
        m_old = [m_sc[h : h + 1, :] for h in hs]
        l_old = [l_sc[h : h + 1, :] for h in hs]
        m_new = [jnp.maximum(m_old[h], jnp.max(s[h], axis=0, keepdims=True)) for h in hs]
        p = [jnp.exp(s[h] - m_new[h]).astype(bf16) for h in hs]
        fade = [jnp.exp(m_old[h] - m_new[h]) for h in hs]
        one = jnp.ones((16, FK), bf16)
        v_one = [
            jnp.concatenate([kvt_ref[128 * h + HEAD_DIM : 128 * (h + 1), rows], one], axis=0)
            for h in hs
        ]
        out = [mm(v_one[h], p[h]) for h in hs]
        for h in hs:
            own = slice(HEAD_DIM * h, HEAD_DIM * (h + 1))
            acc_sc[own, :] = acc_sc[own, :] * fade[h] + out[h][:HEAD_DIM]
            l_sc[h : h + 1, :] = fade[h] * l_old[h] + out[h][HEAD_DIM : HEAD_DIM + 1]
            m_sc[h : h + 1, :] = m_new[h]
        return carry

    lax.fori_loop(span[i, 0], span[i, 1], step, 0)
    for h in range(OWN_HEADS):
        own = slice(HEAD_DIM * h, HEAD_DIM * (h + 1))
        total = l_sc[h : h + 1, :]
        ot_ref[own, :] = (acc_sc[own, :] / total).astype(bf16)
        lse_ref[h : h + 1, :] = m_sc[h : h + 1, :] + jnp.log(total)
    lse_ref[OWN_HEADS:, :] = jnp.zeros_like(lse_ref[OWN_HEADS:, :])


def attend(span, qtag, ktag, qt, kv, kvt):
    own = qt.shape[1]
    window = kv.shape[0]
    whole = lambda shape: pl.BlockSpec(shape, lambda i, s: (0, 0), pipeline_mode=pl.Buffered(1))
    cols = lambda rows: pl.BlockSpec((rows, BQ), lambda i, s: (0, i))
    return pl.pallas_call(
        attend_kernel,
        grid_spec=pltpu.PrefetchScalarGridSpec(
            num_scalar_prefetch=1,
            grid=(own // BQ,),
            in_specs=[
                cols(1),
                whole((window, 1)),
                cols(Q_ROWS),
                whole((window, KV_ROWS)),
                whole((KV_ROWS, window)),
            ],
            out_specs=[cols(Q_ROWS), cols(8)],
            scratch_shapes=[
                pltpu.VMEM((8, BQ), f32),
                pltpu.VMEM((8, BQ), f32),
                pltpu.VMEM((Q_ROWS, BQ), f32),
            ],
        ),
        out_shape=[
            jax.ShapeDtypeStruct((Q_ROWS, own), bf16),
            jax.ShapeDtypeStruct((8, own), f32),
        ],
        compiler_params=pltpu.CompilerParams(vmem_limit_bytes=60 << 20),
        cost_estimate=pl.CostEstimate(
            flops=4 * own * 2048 * Q_ROWS, bytes_accessed=20 << 20, transcendentals=own * 6144
        ),
        name="attend",
    )(span, qtag, ktag, qt, kv, kvt)


def grad_kernel(
    parts, final, span, qtag_ref, ktag_ref, qt_ref, dot_ref, ot_ref, lse_ref, kv_ref, kvt_ref, *rest
):
    if final:
        dq_in, dq_ref, *rest = rest
    else:
        dq_in, (dq_ref, *rest) = None, rest
    outs, (dq_sc, dkv_sc) = rest[: len(parts)], rest[len(parts) :]
    i = pl.program_id(0)

    @pl.when(i == 0)
    def _():
        dkv_sc[...] = jnp.zeros_like(dkv_sc)

    if final:
        dq_sc[...] = dq_in[...]
    else:
        dq_sc[...] = jnp.zeros_like(dq_sc)
    qtag = qtag_ref[...]
    qt, d_out, out = qt_ref[...], dot_ref[...], ot_ref[...]
    q_pad = [head_rows(qt, h, False) for h in range(OWN_HEADS)]
    d_pad = [head_rows(d_out, h, True) for h in range(OWN_HEADS)]
    product = d_out.astype(f32) * out.astype(f32)
    inner = [
        jnp.sum(product[HEAD_DIM * h : HEAD_DIM * (h + 1)], axis=0, keepdims=True)
        for h in range(OWN_HEADS)
    ]
    log_row = [lse_ref[h : h + 1, :] for h in range(OWN_HEADS)]

    def step(shift, kb, carry):
        rows = pl.ds(pl.multiple_of(kb * BK, BK), BK)
        place = pl.ds(pl.multiple_of((kb - shift) * BK, BK), BK)
        seen = ktag_ref[rows, :] == qtag
        hs = range(OWN_HEADS)
        kv = [kv_ref[rows, 128 * h : 128 * (h + 1)] for h in hs]
        s = [mm(kv[h], q_pad[h]) for h in hs]
        d_p = [mm(kv[h], d_pad[h]) for h in hs]
        p = [jnp.where(seen, jnp.exp(s[h] - log_row[h]), 0.0) for h in hs]
        d_s = [(p[h] * (d_p[h] - inner[h])).astype(bf16) for h in hs]
        p = [v.astype(bf16) for v in p]
        g_kv = [mm(q_pad[h], d_s[h], NT) + mm(d_pad[h], p[h], NT) for h in hs]
        g_q = [mm(kvt_ref[128 * h : 128 * h + HEAD_DIM, rows], d_s[h]) for h in hs]
        for h in hs:
            dkv_sc[128 * h : 128 * (h + 1), place] += g_kv[h]
            own = slice(HEAD_DIM * h, HEAD_DIM * (h + 1))
            dq_sc[own, :] += g_q[h]
        return carry

    (first, last), (first_b, last_b) = parts[0], parts[-1]
    low = jnp.maximum(span[i, 0], first)
    count = jnp.maximum(jnp.minimum(span[i, 1], last) - low, 0)
    if len(parts) == 1:
        lax.fori_loop(0, count, lambda n, c: step(first, low + n, c), 0)
    else:
        low_b = jnp.maximum(span[i, 0], first_b)
        count_b = jnp.maximum(jnp.minimum(span[i, 1], last_b) - low_b, 0)

        def either(n, c):
            right = n >= count
            kb = jnp.where(right, low_b + n - count, low + n)
            return step(jnp.where(right, first_b - (last - first), first), kb, c)

        lax.fori_loop(0, count + count_b, either, 0)
    if final:
        dq_ref[...] = (dq_sc[...] * score_scale).astype(bf16)
    else:
        dq_ref[...] = dq_sc[...]

    @pl.when(i == pl.num_programs(0) - 1)
    def _():
        base = 0
        for (first, last), ref in zip(parts, outs):
            width = (last - first) * BK
            ref[...] = dkv_sc[:, base : base + width].astype(ref.dtype)
            base += width


def attend_grad(parts, final, span, qtag, ktag, qt, d_out, out, lse, kv, kvt, dq_in=None):
    own = qt.shape[1]
    window = kv.shape[0]
    whole = lambda shape: pl.BlockSpec(shape, lambda i, s: (0, 0), pipeline_mode=pl.Buffered(1))
    cols = lambda rows: pl.BlockSpec((rows, BQ), lambda i, s: (0, i))
    widths = [(last - first) * BK for first, last in parts]
    dtype = f32 if final else bf16
    args = [span, qtag, ktag, qt, d_out, out, lse, kv, kvt] + ([dq_in] if final else [])
    return pl.pallas_call(
        functools.partial(grad_kernel, parts, final),
        grid_spec=pltpu.PrefetchScalarGridSpec(
            num_scalar_prefetch=1,
            grid=(own // BQ,),
            in_specs=[
                cols(1),
                whole((window, 1)),
                cols(Q_ROWS),
                cols(Q_ROWS),
                cols(Q_ROWS),
                cols(8),
                whole((window, KV_ROWS)),
                whole((KV_ROWS, window)),
            ]
            + ([cols(Q_ROWS)] if final else []),
            out_specs=[cols(Q_ROWS)] + [whole((KV_ROWS, w)) for w in widths],
            scratch_shapes=[
                pltpu.VMEM((Q_ROWS, BQ), f32),
                pltpu.VMEM((KV_ROWS, sum(widths)), f32),
            ],
        ),
        out_shape=[jax.ShapeDtypeStruct((Q_ROWS, own), bf16 if final else f32)]
        + [jax.ShapeDtypeStruct((KV_ROWS, w), dtype) for w in widths],
        compiler_params=pltpu.CompilerParams(vmem_limit_bytes=60 << 20),
        cost_estimate=pl.CostEstimate(
            flops=(10 if final else 2) * own * 1536 * Q_ROWS,
            bytes_accessed=20 << 20,
            transcendentals=own * 4096,
        ),
        name="grad_own" if final else "grad_far",
    )(*args)


MESH = pl.DeviceIdType.MESH
CHUNKS = 8
W_LANES = 640
KV_AT = 256


def remote(src, dst, send, recv, target):
    return pltpu.make_async_remote_copy(
        src_ref=src,
        dst_ref=dst,
        send_sem=send,
        recv_sem=recv,
        device_id=(target,),
        device_id_type=MESH,
    )


def share_kernel(
    n_dev, rows_w, tok_ref, code_ref, w_ref, x_own, code_out, ktag_out, w_turn, qt_out, kv_out, kvt_out,
    c_out, x_out, w_out, w_wide, w_full, qt_sc, kv_sc, kvt_sc,
    w_send, w_recv, c_send, c_recv, part_send, part_recv, mate_send, mate_recv,
    up_send, up_recv, down_send, down_recv, cross_send, cross_recv,
    fwd_send, fwd_recv, keep_sem, x_sem, q_sem, kv_sem, kvt_sem,
):
    n_group = n_dev // GROUP
    me = lax.axis_index("fsdp")
    g = me // GROUP
    s = me % GROUP
    k = s % 2
    hi = s // 2
    partner = me + 1 - 2 * k
    mate = me + 2 - 4 * hi
    mate_block = 4 + k - 2 * hi
    has_up = g < n_group - 1
    has_down = g > 0
    rows = tok_ref.shape[0] // CHUNKS
    half = CHUNKS // 2

    barrier = pltpu.get_barrier_semaphore()

    def greet(r, carry):
        pl.semaphore_signal(
            barrier, inc=1, device_id=(lax.rem(me + r, n_dev),), device_id_type=MESH
        )
        return carry

    lax.fori_loop(1, n_dev, greet, 0)
    pl.semaphore_wait(barrier, n_dev - 1)

    def chunk(ref, c):
        return ref.at[pl.ds(pl.multiple_of(c * rows, rows), rows)]

    def spot(b, c):
        return x_out.at[b, pl.ds(pl.multiple_of(c * rows, rows), rows)]

    def to_partner(c):
        return remote(chunk(tok_ref, c), spot(2 + s, c), part_send.at[c], part_recv.at[c], partner)

    def to_mate(c):
        return remote(chunk(tok_ref, c), spot(2 + s, c), mate_send.at[c], mate_recv.at[c], mate)

    def up_own(c):
        return remote(chunk(tok_ref, c), spot(k, c), up_send.at[c], up_recv.at[c], me + GROUP)

    def up_mate(c):
        return remote(spot(mate_block, c), spot(k, c), up_send.at[c], up_recv.at[c], me + GROUP)

    def down_own(c):
        return remote(
            chunk(tok_ref, c), spot(6 + k, c), down_send.at[c], down_recv.at[c], me - GROUP
        )

    def down_mate(c):
        return remote(
            spot(mate_block, c + half), spot(6 + k, c + half), down_send.at[c], down_recv.at[c],
            me - GROUP,
        )

    def cross(c):
        at = c + half * hi
        return remote(spot(6 + k, at), spot(6 + k, at), cross_send.at[c], cross_recv.at[c], mate)

    def forward(b, c, slot):
        return remote(spot(b, c), spot(b, c), fwd_send.at[slot], fwd_recv.at[slot], partner)

    keep_x = pltpu.make_async_copy(tok_ref, x_out.at[2 + s], keep_sem.at[0])
    keep_c = pltpu.make_async_copy(code_ref, c_out.at[2 + s], keep_sem.at[1])
    keep_w = pltpu.make_async_copy(w_ref.at[s], w_out.at[me], keep_sem.at[2])
    keep_x.start()
    keep_c.start()
    keep_w.start()

    def w_copy(r):
        target = lax.rem(me + r, n_dev)
        return remote(
            w_ref.at[lax.rem(target, GROUP)], w_out.at[me], w_send.at[r], w_recv.at[r], target
        )

    def w_start(r, carry):
        w_copy(r).start()
        return carry

    def c_group(j):
        target = GROUP * g + lax.rem(s + j, GROUP)
        return remote(code_ref, c_out.at[2 + s], c_send.at[j], c_recv.at[2 + s], target)

    def c_far(j):
        step = GROUP * (2 * hi - 1)
        b = 6 + s - 8 * hi
        target = GROUP * g + step + j
        return remote(code_ref, c_out.at[b], c_send.at[GROUP + j], c_recv.at[b], target)

    sends_far = jnp.where(hi == 1, g < n_group - 1, g > 0)
    for j in range(1, GROUP):
        c_group(j).start()

    @pl.when(sends_far)
    def _():
        for j in range(GROUP):
            c_far(j).start()

    order = list(range(half, CHUNKS)) + list(range(half))

    @pl.when((hi == 0) & has_down)
    def _():
        for c in range(half):
            down_own(c).start()

    for n, c in enumerate(order):
        to_mate(c).start()
        to_partner(c).start()
        if n < half:

            @pl.when((hi == 1) & has_up)
            def _():
                up_own(c).start()

        if n == half - 1:
            lax.fori_loop(1, n_dev, w_start, 0)

    for n, c in enumerate(order):
        to_mate(c).wait_recv()
        forward(mate_block, c, c).start()

        @pl.when((hi == 0) & has_up)
        def _():
            up_mate(c).start()

        if n < half:

            @pl.when((hi == 1) & has_down)
            def _():
                down_mate(c - half).start()

        else:

            @pl.when((hi == 1) & has_up)
            def _():
                up_own(c).start()

    @pl.when(has_up)
    def _():
        for c in range(half):
            down_own(c).wait_recv()
            cross(c).start()
            forward(6 + k, c + half * hi, 2 * CHUNKS + c).start()

    def w_wait(r, carry):
        w_copy(r).wait_recv()
        return carry

    lax.fori_loop(1, n_dev, w_wait, 0)
    keep_w.wait()
    keep_x.wait()
    bias_row = jnp.zeros((8, W_LANES), f32)
    bias_at = w_ref.shape[1] - 8
    for j in range(n_dev):
        w_wide[rows_w * j : rows_w * (j + 1), :] = w_out[j, :rows_w, :].astype(f32)
        bias_row = bias_row + w_out[j, bias_at:, :].astype(f32)
    bias_row = jnp.sum(bias_row, axis=0, keepdims=True)
    bias_col = jnp.broadcast_to(bias_row, (128, W_LANES)).T[:, :1]
    w_full[...] = w_wide[...].astype(bf16)
    w_turn[...] = w_wide[...].T.astype(bf16)
    piece = 512
    pieces = tok_ref.shape[0] // piece

    def project(b, inside):
        def one(j, carry):
            x = x_out[b, pl.ds(pl.multiple_of(j * piece, piece), piece), :]
            at = pl.ds(pl.multiple_of((b * pieces + j) * piece, piece), piece)
            kv = mm(x, w_full[:, KV_AT:]) + bias_row[:, KV_AT:]
            kv_sc[at, :] = kv.astype(bf16)
            kvt_sc[:, at] = (mm(w_turn[KV_AT:, :], x, NT) + bias_col[KV_AT:]).astype(bf16)
            if inside:
                to = pl.ds(pl.multiple_of(((b - 2) * pieces + j) * piece, piece), piece)
                q = (mm(w_turn[:Q_ROWS, :], x, NT) + bias_col[:Q_ROWS]).astype(bf16)
                qt_sc[:, to] = q * jnp.asarray(score_scale, bf16)
            return carry

        lax.fori_loop(0, pieces, one, 0)

    def outs(b, inside):
        whole = tok_ref.shape[0]
        at = pl.ds(pl.multiple_of(b * whole, whole), whole)
        copies = [
            pltpu.make_async_copy(kv_sc.at[at], kv_out.at[at], kv_sem.at[b]),
            pltpu.make_async_copy(kvt_sc.at[:, at], kvt_out.at[:, at], kvt_sem.at[b]),
        ]
        if inside:
            to = pl.ds(pl.multiple_of((b - 2) * whole, whole), whole)
            copies.append(pltpu.make_async_copy(qt_sc.at[:, to], qt_out.at[:, to], q_sem.at[b - 2]))
            copies.append(pltpu.make_async_copy(x_out.at[b], x_own.at[b - 2], x_sem.at[b - 2]))
        return copies

    def put(b, inside):
        for copy in outs(b, inside):
            copy.start()

    keep_c.wait()
    for j in range(1, GROUP):
        remote(
            code_ref, c_out.at[0], c_send.at[j], c_recv.at[2 + lax.rem(s + j, GROUP)], partner
        ).wait_recv()

    @pl.when(has_down)
    def _():
        for b in range(2):
            remote(code_ref, c_out.at[b], c_send.at[0], c_recv.at[b], partner).wait_recv()

    @pl.when(has_up)
    def _():
        for b in range(6, 8):
            remote(code_ref, c_out.at[b], c_send.at[0], c_recv.at[b], partner).wait_recv()

    for b in range(8):
        code = c_out[b]
        if b < 2:
            code = jnp.where(has_down, code, -2)
        if b >= 6:
            code = jnp.where(has_up, code, 2 * n_dev * tok_ref.shape[0])
        code_out[b] = code
        tag = jnp.where((code & 1) == 1, (code >> 1) + 1, 0)
        lanes = tag.shape[1]
        for r in range(8):
            turned = jnp.broadcast_to(tag[r : r + 1, :], (lanes, lanes)).T
            at = (8 * b + r) * lanes
            ktag_out[at : at + lanes, :] = turned[:, :1]

    own_block = 2 + s
    near_block = own_block + 1 - 2 * k
    across_block = mate_block + 1 - 2 * k
    project(own_block, True)

    project(mate_block, True)
    put(own_block, True)

    @pl.when(has_down)
    def _():
        for c in order:
            up_own(c).wait_recv()
            forward(k, c, CHUNKS + c).start()

    for c in range(CHUNKS):
        to_partner(c).wait_recv()
    project(near_block, True)
    put(mate_block, True)

    @pl.when(has_up)
    def _():
        for c in range(half):
            cross(c).wait_recv()
            forward(6 + k, c + half * (1 - hi), 2 * CHUNKS + half + c).start()

    for c in range(CHUNKS):
        forward(mate_block, c, c).wait_recv()
    project(across_block, True)
    put(near_block, True)

    @pl.when(has_down)
    def _():
        project(k, False)
        for c in range(CHUNKS):
            forward(k, c, CHUNKS + c).wait_recv()
        project(1 - k, False)
        put(k, False)

    put(across_block, True)

    @pl.when(has_up)
    def _():
        project(6 + k, False)
        for c in range(half):
            forward(6 + k, c, 2 * CHUNKS + c).wait_recv()
            forward(6 + k, c, 2 * CHUNKS + half + c).wait_recv()
        project(7 - k, False)
        put(6 + k, False)

    for c in range(CHUNKS):
        to_partner(c).wait_send()
        to_mate(c).wait_send()
        forward(mate_block, c, c).wait_send()

    @pl.when(has_down)
    def _():
        put(1 - k, False)
        for c in range(CHUNKS):
            forward(k, c, CHUNKS + c).wait_send()
        for c in range(half):
            down_own(c).wait_send()

    @pl.when(has_up)
    def _():
        for c in range(half):
            cross(c).wait_send()
            forward(6 + k, c, 2 * CHUNKS + c).wait_send()
            forward(6 + k, c, 2 * CHUNKS + half + c).wait_send()
        for c in range(CHUNKS):
            up_own(c).wait_send()
        put(7 - k, False)

    for j in range(1, GROUP):
        c_group(j).wait_send()

    @pl.when(sends_far)
    def _():
        for j in range(GROUP):
            c_far(j).wait_send()

    def w_sent(r, carry):
        w_copy(r).wait_send()
        return carry

    lax.fori_loop(1, n_dev, w_sent, 0)
    for b in range(2, 6):
        for copy in outs(b, True):
            copy.wait()

    @pl.when(has_down)
    def _():
        for b in range(2):
            for copy in outs(b, False):
                copy.wait()

    @pl.when(has_up)
    def _():
        for b in range(6, 8):
            for copy in outs(b, False):
                copy.wait()


def share(n_dev, rows_w, tokens, code, w_send):
    vmem = pl.BlockSpec(memory_space=pltpu.VMEM)
    anywhere = pl.BlockSpec(memory_space=pl.ANY)
    dma = lambda n: pltpu.SemaphoreType.DMA((n,))
    half = CHUNKS // 2
    rows, width = tokens.shape
    own, window = GROUP * rows, 8 * rows
    return pl.pallas_call(
        functools.partial(share_kernel, n_dev, rows_w),
        in_specs=[vmem] * 3,
        out_specs=[anywhere, vmem, vmem, vmem, anywhere, anywhere, anywhere],
        out_shape=[
            jax.ShapeDtypeStruct((GROUP, rows, width), bf16),
            jax.ShapeDtypeStruct((8,) + code.shape, code.dtype),
            jax.ShapeDtypeStruct((window, 1), code.dtype),
            jax.ShapeDtypeStruct((W_LANES, width), bf16),
            jax.ShapeDtypeStruct((Q_ROWS, own), bf16),
            jax.ShapeDtypeStruct((window, KV_ROWS), bf16),
            jax.ShapeDtypeStruct((KV_ROWS, window), bf16),
        ],
        scratch_shapes=[
            pltpu.VMEM((8,) + code.shape, code.dtype),
            pltpu.VMEM((8, rows, width), bf16),
            pltpu.VMEM((n_dev,) + w_send.shape[1:], bf16),
            pltpu.VMEM((width, W_LANES), f32),
            pltpu.VMEM((width, W_LANES), bf16),
            pltpu.VMEM((Q_ROWS, own), bf16),
            pltpu.VMEM((window, KV_ROWS), bf16),
            pltpu.VMEM((KV_ROWS, window), bf16),
            dma(n_dev), dma(n_dev), dma(2 * GROUP), dma(8),
            dma(CHUNKS), dma(CHUNKS), dma(CHUNKS), dma(CHUNKS),
            dma(CHUNKS), dma(CHUNKS), dma(half), dma(half), dma(half), dma(half),
            dma(3 * CHUNKS), dma(3 * CHUNKS), dma(3), dma(GROUP), dma(GROUP), dma(8), dma(8),
        ],
        compiler_params=pltpu.CompilerParams(
            collective_id=0, has_side_effects=True, vmem_limit_bytes=60 << 20
        ),
        name="share",
    )(tokens, code, w_send)


PARTS = 4
TN = (((0,), (0,)), ((), ()))


def settle_kernel(
    n_dev, rows_w, q_ref, kv_ref, x_ref, w_ref, vec_ref, own_out, near_out, far_out, grad_out, vec_sum,
    w_out, vec_out, wide, slabs, across, near, relay, total,
    w_send, w_recv, vec_send, vec_recv, near_send, near_recv, relay_send, relay_recv,
    far_send, far_recv, keep_sem,
):
    me = lax.axis_index("fsdp")
    s = me % GROUP
    k = s % 2
    hi = s // 2
    partner = me + 1 - 2 * k
    mate = me + 2 - 4 * hi
    s_partner = s + 1 - 2 * k
    s_mate = s + 2 - 4 * hi
    s_across = 3 - s
    block = own_out.shape[0]
    rows = block // PARTS

    barrier = pltpu.get_barrier_semaphore()

    def greet(r, carry):
        pl.semaphore_signal(
            barrier, inc=1, device_id=(lax.rem(me + r, n_dev),), device_id_type=MESH
        )
        return carry

    lax.fori_loop(1, n_dev, greet, 0)
    pl.semaphore_wait(barrier, n_dev - 1)

    def part(c):
        return pl.ds(pl.multiple_of(c * rows, rows), rows)

    def to_relay(c):
        return remote(
            across.at[part(c)], relay.at[part(c)], relay_send.at[c], relay_recv.at[c], partner
        )

    def to_near(c):
        return remote(
            near.at[part(c)], near_out.at[part(c)], near_send.at[c], near_recv.at[c], partner
        )

    def to_far(c):
        return remote(total.at[part(c)], far_out.at[part(c)], far_send.at[c], far_recv.at[c], mate)

    def w_copy(r):
        target = lax.rem(me + r, n_dev)
        return remote(slabs.at[target], w_out.at[me], w_send.at[r], w_recv.at[r], target)

    def vec_copy(r):
        target = lax.rem(me + r, n_dev)
        return remote(vec_ref.at[target], vec_out.at[me], vec_send.at[r], vec_recv.at[r], target)

    def vec_start(r, carry):
        vec_copy(r).start()
        return carry

    lax.fori_loop(1, n_dev, vec_start, 0)
    keep_vec = pltpu.make_async_copy(vec_ref.at[me], vec_out.at[me], keep_sem.at[1])
    keep_vec.start()

    def back(t, c):
        at = pl.ds(pl.multiple_of(t * block + c * rows, rows), rows)
        return mm(q_ref[:, at], w_ref[:Q_ROWS, :], TN) + mm(kv_ref[:, at], w_ref[KV_AT:, :], TN)

    def add_rows(j, carry):
        at = pl.ds(pl.multiple_of(j * block, block), block)
        wide[:Q_ROWS, :] += mm(q_ref[:, at], x_ref[at, :])
        wide[Q_ROWS:MIX_ROWS, :] += mm(kv_ref[:, at], x_ref[at, :])

        @pl.when(j == 0)
        def _():
            to_far(PARTS - 1).start()

        return carry

    def w_start(r, carry):
        w_copy(r).start()
        return carry

    def make_across(c, carry):
        across[part(c), :] = back(s_across, c).astype(bf16)

        @pl.when(c > 0)
        def _():
            to_relay(c - 1).start()

        return carry

    def make_far(c, carry):
        mine = back(s_mate, c)

        @pl.when(c == 0)
        def _():
            to_relay(PARTS - 1).start()

        to_relay(c).wait_recv()
        total[part(c), :] = (mine + relay[part(c), :].astype(f32)).astype(bf16)

        @pl.when(c > 0)
        def _():
            to_far(c - 1).start()

        return carry

    def make_near(c, carry):
        near[part(c), :] = back(s_partner, c).astype(bf16)

        @pl.when(c == 0)
        def _():
            lax.fori_loop(1, n_dev, w_start, 0)

        @pl.when(c > 0)
        def _():
            to_near(c - 1).start()

        return carry

    def make_own(c, carry):
        own_out[part(c), :] = back(s, c)

        @pl.when(c == 0)
        def _():
            to_near(PARTS - 1).start()

        return carry

    lax.fori_loop(0, PARTS, make_across, 0)
    wide[...] = jnp.zeros_like(wide)
    lax.fori_loop(0, PARTS, make_far, 0)
    lax.fori_loop(0, GROUP, add_rows, 0)
    turned = wide[...].T
    one = jnp.ones((8, GROUP * block), bf16)
    bias_q = mm(one, q_ref[...], NT).astype(bf16)
    bias_kv = mm(one, kv_ref[...], NT).astype(bf16)
    bias_at = slabs.shape[1] - 8
    for j in range(n_dev):
        slabs[j, :rows_w, :] = turned[rows_w * j : rows_w * (j + 1), :].astype(bf16)
        slabs[j, bias_at:, :Q_ROWS] = bias_q
        slabs[j, bias_at:, Q_ROWS:MIX_ROWS] = bias_kv
    lax.fori_loop(0, PARTS, make_near, 0)
    keep_w = pltpu.make_async_copy(slabs.at[me], w_out.at[me], keep_sem.at[0])
    keep_w.start()
    lax.fori_loop(0, PARTS, make_own, 0)
    for c in range(PARTS):
        to_relay(c).wait_send()
        to_near(c).wait()
        to_far(c).wait()

    def finish(r, carry):
        w_copy(r).wait()
        vec_copy(r).wait()
        return carry

    lax.fori_loop(1, n_dev, finish, 0)
    keep_w.wait()
    keep_vec.wait()
    vec_sum[...] = jnp.sum(vec_out[...], axis=0)
    for t in range(GROUP):
        got = w_out[t].astype(f32)
        for j in range(1, n_dev // GROUP):
            got = got + w_out[GROUP * j + t].astype(f32)
        grad_out[:, Q_ROWS * t : Q_ROWS * (t + 1)] = got[:, :Q_ROWS]
        for h in range(OWN_HEADS):
            for part_at in range(2):
                at = Q_ROWS + 128 * h + HEAD_DIM * part_at
                to = D * (1 + part_at) + Q_ROWS * t + HEAD_DIM * h
                grad_out[:, to : to + HEAD_DIM] = got[:, at : at + HEAD_DIM]


def settle(n_dev, rows_w, d_q, d_kv, x, w, vec):
    vmem = pl.BlockSpec(memory_space=pltpu.VMEM)
    anywhere = pl.BlockSpec(memory_space=pl.ANY)
    dma = lambda n: pltpu.SemaphoreType.DMA((n,))
    block = (x.shape[0] // GROUP, x.shape[1])
    slabs = (n_dev, rows_w + -rows_w % 8 + 8, W_LANES)
    return pl.pallas_call(
        functools.partial(settle_kernel, n_dev, rows_w),
        in_specs=[vmem] * 5,
        out_specs=[vmem, anywhere, anywhere, vmem, vmem],
        out_shape=[
            jax.ShapeDtypeStruct(block, f32),
            jax.ShapeDtypeStruct(block, bf16),
            jax.ShapeDtypeStruct(block, bf16),
            jax.ShapeDtypeStruct((slabs[1], 3 * D), f32),
            jax.ShapeDtypeStruct(vec.shape[1:], vec.dtype),
        ],
        scratch_shapes=[
            pltpu.VMEM(slabs, bf16),
            pltpu.VMEM(vec.shape, vec.dtype),
            pltpu.VMEM((W_LANES, x.shape[1]), f32),
            pltpu.VMEM(slabs, bf16),
            pltpu.VMEM(block, bf16), pltpu.VMEM(block, bf16),
            pltpu.VMEM(block, bf16), pltpu.VMEM(block, bf16),
            dma(n_dev), dma(n_dev), dma(n_dev), dma(n_dev),
            dma(PARTS), dma(PARTS), dma(PARTS), dma(PARTS), dma(PARTS), dma(PARTS), dma(2),
        ],
        compiler_params=pltpu.CompilerParams(
            collective_id=1, has_side_effects=True, vmem_limit_bytes=60 << 20
        ),
        name="settle",
    )(d_q, d_kv, x, w, vec)


def swap_kernel(spread, in_ref, out_ref, send, recv, keep_sem):
    me = lax.axis_index("fsdp")
    s = me % GROUP
    start = me - s
    width = (in_ref if spread else out_ref).shape[1] // GROUP

    barrier = pltpu.get_barrier_semaphore()
    for j in range(1, GROUP):
        target = start + lax.rem(s + j, GROUP)
        pl.semaphore_signal(barrier, inc=1, device_id=(target,), device_id_type=MESH)
    pl.semaphore_wait(barrier, GROUP - 1)

    def cols(ref, t):
        return ref.at[:, pl.ds(pl.multiple_of(t * width, width), width)]

    def rows(ref, t):
        return ref.at[pl.ds(pl.multiple_of(t * Q_ROWS, Q_ROWS), Q_ROWS)]

    def ends(t):
        if spread:
            return cols(in_ref, t), rows(out_ref, s)
        return rows(in_ref, t), cols(out_ref, s)

    def copy(j):
        t = lax.rem(s + j, GROUP)
        src, dst = ends(t)
        return remote(src, dst, send.at[j], recv.at[j], start + t)

    for j in (2, 1, 3):
        copy(j).start()
    src, dst = ends(s)
    keep = pltpu.make_async_copy(src, dst, keep_sem.at[0])
    keep.start()
    for j in range(1, GROUP):
        copy(j).wait()
    keep.wait()


def swap(x, spread):
    shape = (x.shape[0] * GROUP, x.shape[1] // GROUP) if spread else (
        x.shape[0] // GROUP, x.shape[1] * GROUP
    )
    dma = lambda n: pltpu.SemaphoreType.DMA((n,))
    return pl.pallas_call(
        functools.partial(swap_kernel, spread),
        in_specs=[pl.BlockSpec(memory_space=pltpu.VMEM)],
        out_specs=pl.BlockSpec(memory_space=pltpu.VMEM),
        out_shape=jax.ShapeDtypeStruct(shape, x.dtype),
        scratch_shapes=[dma(GROUP), dma(GROUP), dma(1)],
        compiler_params=pltpu.CompilerParams(
            collective_id=2 if spread else 3, has_side_effects=True
        ),
        name="swap_out" if spread else "swap_back",
    )(x)


def body(
    n_dev,
    tokens,
    segment_ids,
    pad_mask,
    w_qkv,
    bias_query,
    bias_value,
    w_out,
    bias_out,
    gain_one,
    shift_one,
    w_up,
    bias_up,
    w_down,
    bias_down,
    gain_two,
    shift_two,
    cotangent,
):
    row_count = tokens.shape[0]
    rows_w = w_qkv.shape[0]
    own = GROUP * row_count
    window = own + 2 * LEN_MAX
    me = lax.axis_index("fsdp")
    place = me % GROUP
    group_id = me // GROUP
    n_group = n_dev // GROUP
    up = [(i, i + GROUP) for i in range(n_dev - GROUP)]
    down = [(i + GROUP, i) for i in range(n_dev - GROUP)]

    wq = w_qkv[:, :D].reshape(rows_w, GROUP, Q_ROWS)
    wk = w_qkv[:, D : 2 * D].reshape(rows_w, GROUP, OWN_HEADS, 1, HEAD_DIM)
    wv = w_qkv[:, 2 * D :].reshape(rows_w, GROUP, OWN_HEADS, 1, HEAD_DIM)
    wkv = jnp.concatenate([wk, wv], axis=3).reshape(rows_w, GROUP, KV_ROWS)
    gap = KV_AT - Q_ROWS
    lane = jnp.arange(gap)[None, :]
    small_cols = jnp.pad(bias_up.reshape(rows_w, -1), ((0, 0), (6, gap - 10)))
    for j, v in enumerate([bias_out, gain_one, shift_one, bias_down, gain_two, shift_two]):
        small_cols = jnp.where(lane == j, v[:, None], small_cols)
    small_cols = jnp.broadcast_to(small_cols[:, None], (rows_w, GROUP, gap))
    w_cut = jnp.concatenate([wq, small_cols, wkv], axis=2).transpose(1, 0, 2)
    column = me * rows_w + jnp.arange(rows_w)
    feature = jnp.arange(D)
    spread = lambda bias: jnp.sum(
        jnp.where(feature[None] == column[:, None], bias.astype(f32)[:, None], 0.0), axis=0
    )
    bias_q = spread(bias_query).reshape(GROUP, Q_ROWS)
    bias_v = spread(bias_value).reshape(GROUP, OWN_HEADS, 1, HEAD_DIM)
    bias_kv = jnp.concatenate([jnp.zeros_like(bias_v), bias_v], axis=2).reshape(GROUP, KV_ROWS)
    bias_cut = jnp.concatenate([bias_q, jnp.zeros((GROUP, gap), f32), bias_kv], axis=1)
    fill = -rows_w % 8
    bias_cut = jnp.pad(bias_cut.astype(bf16)[:, None], ((0, 0), (fill, 7), (0, 0)))
    w_send = jnp.concatenate([w_cut, bias_cut], axis=1)
    ff = w_up.shape[1]
    out_down = jnp.concatenate([w_out, w_down], axis=0)
    out_down = lax.all_gather(out_down, "fsdp", axis=0)
    wo_full = out_down[:, :rows_w].reshape(D, D)
    wd_full = lax.optimization_barrier(out_down[:, rows_w:].reshape(ff, D))
    wu_full = lax.all_gather(w_up, "fsdp", axis=0, tiled=True)

    code = (segment_ids * 2 + pad_mask).reshape(8, row_count // 8)
    x_own, code_win, ktag, w_turn, qt, kv, kvt = share(n_dev, rows_w, tokens, code, w_send)
    x_own = x_own.reshape(own, D)
    code_win = code_win.reshape(window)
    code_own = code_win[LEN_MAX : LEN_MAX + own]
    small_all = w_turn[Q_ROWS : Q_ROWS + 10].astype(f32)
    bu_full = small_all[6:].T.reshape(-1)
    bo_full, g1_full, s1_full, bd_full, g2_full, s2_full = [small_all[j] for j in range(6)]
    seg_win = code_win >> 1
    seg_own = code_own >> 1
    qtag = (seg_own + 1).reshape(1, own)
    first_seg = seg_own[::BQ]
    last_seg = seg_own[BQ - 1 :: BQ]
    low = jnp.sum((seg_win[None, :] < first_seg[:, None]).astype(jnp.int32), axis=1)
    high = jnp.sum((seg_win[None, :] <= last_seg[:, None]).astype(jnp.int32), axis=1)
    spans = [jnp.stack([low // b, (high + b - 1) // b], axis=1) for b in (FK, BK)]

    ot, lse = attend(spans[0], qtag, ktag, qt, kv, kvt)
    ctx_t = swap(ot, True)

    tokens_f = tokens.astype(f32)
    branch = jnp.einsum("ir,io->ro", ctx_t, wo_full, preferred_element_type=f32) + bo_full
    first, norm_one_back = jax.vjp(norm_rows, tokens_f + branch, g1_full, s1_full)
    up_in = lax.optimization_barrier(first.astype(bf16))
    pre_act = jnp.dot(up_in, wu_full, preferred_element_type=f32) + bu_full
    hidden = gelu_exact(pre_act).astype(bf16)
    pre_kept = lax.optimization_barrier(pre_act.astype(bf16)).astype(f32)
    gelu_back = jax.vjp(gelu_exact, pre_kept)[1]
    ffn = jnp.dot(hidden, wd_full, preferred_element_type=f32) + bd_full
    result, norm_two_back = jax.vjp(norm_rows, first + ffn, g2_full, s2_full)
    layer_out = result.astype(bf16)
    d_second, d_gain_two, d_shift_two = norm_two_back(cotangent.astype(f32))
    d_ffn = d_second.astype(bf16)
    d_bias_down = jnp.sum(d_ffn.astype(f32), axis=0)
    d_w_down = jnp.einsum("rf,rd->fd", hidden, d_ffn, preferred_element_type=f32)
    d_hidden = jnp.einsum("rd,fd->rf", d_ffn, wd_full, preferred_element_type=f32)
    d_pre = gelu_back(d_hidden)[0].astype(bf16)
    d_bias_up = jnp.sum(d_pre.astype(f32), axis=0)
    d_w_up = jnp.einsum("rd,rf->df", up_in, d_pre, preferred_element_type=f32).astype(bf16)
    d_w_up = lax.optimization_barrier(d_w_up)
    d_first = d_second + jnp.einsum("rf,df->rd", d_pre, wu_full, preferred_element_type=f32)
    d_mid, d_gain_one, d_shift_one = norm_one_back(d_first)
    d_branch = d_mid.astype(bf16)
    d_bias_out = jnp.sum(d_branch.astype(f32), axis=0)
    d_w_out = jnp.einsum("ir,ro->io", ctx_t, d_branch, preferred_element_type=f32)
    dctx_t = jnp.einsum("ro,io->ir", d_branch, wo_full, preferred_element_type=f32).astype(bf16)
    n_up = ff // D
    big_grad = jnp.concatenate(
        [
            d_w_down.astype(bf16).reshape(n_dev, -1, D),
            d_w_out.astype(bf16).reshape(n_dev, rows_w, D),
        ]
        + [d_w_up[:, D * j : D * (j + 1)].reshape(n_dev, rows_w, D) for j in range(n_up)],
        axis=1,
    )
    big_owned = lax.psum_scatter(big_grad, "fsdp", scatter_dimension=0).astype(f32)
    rows_d = w_down.shape[0]
    g_down, g_out = big_owned[:rows_d], big_owned[rows_d : rows_d + rows_w]
    g_up = jnp.concatenate(
        [big_owned[rows_d + rows_w * (j + 1) : rows_d + rows_w * (j + 2)] for j in range(n_up)], axis=1
    )

    d_out = swap(dctx_t, False)
    edge, inside = LEN_MAX // BK, own // BK
    far_parts = ((0, edge), (edge + inside, 2 * edge + inside))
    own_parts = ((edge, edge + inside),)
    dq_far, dkv_left, dkv_right = attend_grad(
        far_parts, False, spans[1], qtag, ktag, qt, d_out, ot, lse, kv, kvt
    )
    from_right = lax.ppermute(dkv_left, "fsdp", down)
    from_left = lax.ppermute(dkv_right, "fsdp", up)
    dq_t, dkv_own = attend_grad(
        own_parts, True, spans[1], qtag, ktag, qt, d_out, ot, lse, kv, kvt, dq_far
    )
    dkv = jnp.concatenate(
        [
            dkv_own[:, :LEN_MAX] + from_left.astype(f32),
            dkv_own[:, LEN_MAX : own - LEN_MAX],
            dkv_own[:, own - LEN_MAX :] + from_right.astype(f32),
        ],
        axis=1,
    ).astype(bf16)
    vecs = jnp.stack([d_bias_out, d_gain_one, d_shift_one, d_bias_down, d_gain_two, d_shift_two])
    vec_send = jnp.concatenate(
        [
            vecs.reshape(6, n_dev, rows_w).transpose(1, 0, 2).reshape(n_dev, 6 * rows_w),
            d_bias_up.reshape(n_dev, 4 * rows_w),
        ],
        axis=1,
    )
    vec_send = jnp.pad(vec_send, ((0, 0), (0, 1024 - vec_send.shape[1]))).reshape(n_dev, 8, 128)
    own_x, near, far, got, vec = settle(n_dev, rows_w, dq_t, dkv, x_own, w_turn, vec_send)
    grad_tokens = d_mid + ((own_x + near.astype(f32)) + far.astype(f32))
    grad_w_qkv = got[:rows_w]
    bias_rows = got[-8].reshape(3, D)
    bias_own = lax.dynamic_slice(bias_rows, (0, me * rows_w), (3, rows_w))
    vec = vec.reshape(-1)[: 10 * rows_w]
    own_vec = [bias_own[0], bias_own[2]] + [vec[j * rows_w : (j + 1) * rows_w] for j in range(6)]
    return (
        layer_out,
        grad_tokens,
        grad_w_qkv,
        own_vec[0],
        own_vec[1],
        g_out,
        own_vec[2],
        own_vec[3],
        own_vec[4],
        g_up,
        vec[6 * rows_w :],
        g_down,
        own_vec[5],
        own_vec[6],
        own_vec[7],
    )


def solution(mesh):
    rows, flat = P("fsdp", None), P("fsdp")
    return jax.shard_map(
        functools.partial(body, mesh.shape["fsdp"]),
        mesh=mesh,
        in_specs=(
            rows, flat, flat, rows, flat, flat, rows, flat, flat, flat, rows, flat, rows, flat,
            flat, flat, rows,
        ),
        out_specs=(
            rows, rows, rows, flat, flat, rows, flat, flat, flat, rows, flat, rows, flat, flat,
            flat,
        ),
        check_vma=False,
    )
```
